32 devices in a mesh: dp: 2 (over x), tp: 4 (over z), pp: 4 (over y, core).
Axes of the slice: x: 2, y: 2, z: 4, core: 2. Of those that a mesh axis runs over, the one named last changes fastest.
Arguments:
- x_in: bfloat16 [4, 2, 1024, 512], P('dp'), parts along dimension 0
- g_out: float32 [4, 2, 1024, 512], P('dp'), parts along dimension 0
- ln1_gain: float32 [4, 512], P('pp')
- ln1_bias: float32 [4, 512], P('pp')
- w_qkv: bfloat16 [4, 512, 8, 3, 64], P('pp', None, 'tp')
- b_qkv: bfloat16 [4, 8, 3, 64], P('pp', 'tp')
- w_out: bfloat16 [4, 8, 64, 512], P('pp', 'tp')
- b_out: bfloat16 [4, 512], P('pp')
- ln2_gain: float32 [4, 512], P('pp')
- ln2_bias: float32 [4, 512], P('pp')
- w_up: bfloat16 [4, 512, 2048], P('pp', None, 'tp')
- b_up: bfloat16 [4, 2048], P('pp', 'tp')
- w_down: bfloat16 [4, 2048, 512], P('pp', 'tp')
- b_down: bfloat16 [4, 512], P('pp')
Outputs:
- output 1: bfloat16 [4, 2, 1024, 512], P('dp'), parts along dimension 0
- output 2: float32 [8, 512], P(('dp', 'pp')), parts along dimension 0
- output 3: float32 [8, 512], P(('dp', 'pp')), parts along dimension 0
- output 4: float32 [8, 512, 8, 3, 64], P(('dp', 'pp'), None, 'tp'), parts along dimension 0
- output 5: float32 [8, 8, 3, 64], P(('dp', 'pp'), 'tp'), parts along dimension 0
- output 6: float32 [8, 8, 64, 512], P(('dp', 'pp'), 'tp'), parts along dimension 0
- output 7: float32 [8, 512], P(('dp', 'pp')), parts along dimension 0
- output 8: float32 [8, 512], P(('dp', 'pp')), parts along dimension 0
- output 9: float32 [8, 512], P(('dp', 'pp')), parts along dimension 0
- output 10: float32 [8, 512, 2048], P(('dp', 'pp'), None, 'tp'), parts along dimension 0
- output 11: float32 [8, 2048], P(('dp', 'pp'), 'tp'), parts along dimension 0
- output 12: float32 [8, 2048, 512], P(('dp', 'pp'), 'tp'), parts along dimension 0
- output 13: float32 [8, 512], P(('dp', 'pp')), parts along dimension 0
There are 2 independent parts. The reference program is written for one: setup_inputs(seed, part) draws one part's arguments, and reference() takes and returns one part's arrays. A program takes and returns all parts, laid end to end along the dimension named above; an argument that names none is the same for every part.
All inputs are finite; a program needn't handle non-finite values.
Results may differ from the reference program's by a relative error of at most 0.0183014.
Values are sent between devices in bfloat16 or wider.
A program may use at most 1 GiB of HBM per device.

```python
import jax
import jax.numpy as jnp
from jax import lax

NUM_MICRO = 2
MICRO_ROWS = 2
SEQ_LEN = 1024
MODEL_DIM = 512
NUM_HEADS = 8
HEAD_DIM = 64
FFN_DIM = 2048
NUM_STAGES = 4
ROT_DIM = HEAD_DIM // 4


def norm_core(hidden, gain, shift):
    center = hidden - jnp.mean(hidden, axis=-1, keepdims=True)
    var_term = jnp.mean(center * center, axis=-1, keepdims=True)
    return center * lax.rsqrt(var_term + 1e-5) * gain + shift


def rotary_tables():
    half_rot = ROT_DIM // 2
    inv_freq = 10000.0 ** (-(jnp.arange(half_rot, dtype=jnp.float32) * 2.0) / ROT_DIM)
    angles = jnp.arange(SEQ_LEN, dtype=jnp.float32)[:, None] * inv_freq[None, :]
    angles = jnp.concatenate([angles, angles], axis=-1)
    return jnp.cos(angles)[None, :, None, :], jnp.sin(angles)[None, :, None, :]


def apply_rotary(values, cos_tab, sin_tab):
    half_rot = ROT_DIM // 2
    rot_part = values[..., :ROT_DIM]
    turned = jnp.concatenate([-rot_part[..., half_rot:], rot_part[..., :half_rot]], axis=-1)
    return jnp.concatenate([rot_part * cos_tab + turned * sin_tab, values[..., ROT_DIM:]], axis=-1)


def attention(qkv_proj, cos_tab, sin_tab):
    query = apply_rotary(qkv_proj[:, :, :, 0].astype(jnp.float32), cos_tab, sin_tab).astype(jnp.bfloat16)
    key_rot = apply_rotary(qkv_proj[:, :, :, 1].astype(jnp.float32), cos_tab, sin_tab).astype(jnp.bfloat16)
    value_part = qkv_proj[:, :, :, 2]
    scores = jnp.einsum('bqhe,bkhe->bhqk', query.astype(jnp.float32), key_rot.astype(jnp.float32)) * (HEAD_DIM ** -0.5)
    positions = jnp.arange(SEQ_LEN)
    causal = positions[:, None] >= positions[None, :]
    scores = jnp.where(causal, scores, -1e30)
    probs = jax.nn.softmax(scores, axis=-1).astype(jnp.bfloat16)
    context = jnp.einsum('bhqk,bkhe->bqhe', probs.astype(jnp.float32), value_part.astype(jnp.float32))
    return context.astype(jnp.bfloat16)


def layer_forward(hidden, layer_wts, cos_tab, sin_tab):
    ln1_gain, ln1_bias, w_qkv, b_qkv, w_out, b_out, ln2_gain, ln2_bias, w_up, b_up, w_down, b_down = layer_wts
    tokens = MICRO_ROWS * SEQ_LEN
    hidden_f = hidden.reshape(tokens, MODEL_DIM).astype(jnp.float32)
    normed_a = norm_core(hidden_f, ln1_gain, ln1_bias).astype(jnp.bfloat16)
    normed_m = norm_core(hidden_f, ln2_gain, ln2_bias).astype(jnp.bfloat16)
    qkv_proj = jnp.dot(normed_a, w_qkv.reshape(MODEL_DIM, 3 * MODEL_DIM), preferred_element_type=jnp.float32)
    qkv_proj = (qkv_proj + b_qkv.reshape(3 * MODEL_DIM).astype(jnp.float32)).astype(jnp.bfloat16)
    qkv_proj = qkv_proj.reshape(MICRO_ROWS, SEQ_LEN, NUM_HEADS, 3, HEAD_DIM)
    context = attention(qkv_proj, cos_tab, sin_tab).reshape(tokens, MODEL_DIM)
    attn_sum = jnp.dot(context, w_out.reshape(MODEL_DIM, MODEL_DIM), preferred_element_type=jnp.float32)
    pre_act = jnp.dot(normed_m, w_up, preferred_element_type=jnp.float32) + b_up.astype(jnp.float32)
    hidden_mlp = jax.nn.gelu(pre_act, approximate=False).astype(jnp.bfloat16)
    mlp_sum = jnp.dot(hidden_mlp, w_down, preferred_element_type=jnp.float32)
    total = hidden_f + attn_sum + b_out.astype(jnp.float32) + mlp_sum + b_down.astype(jnp.float32)
    return total.astype(jnp.bfloat16).reshape(MICRO_ROWS, SEQ_LEN, MODEL_DIM)


def setup_inputs(seed: int = 0, part: int = 0) -> dict:
    weight_keys = jax.random.split(jax.random.key(seed), 12)
    data_keys = jax.random.split(jax.random.fold_in(jax.random.key(seed + 1), part), 2)
    act_shape = (NUM_MICRO, MICRO_ROWS, SEQ_LEN, MODEL_DIM)
    tokens = NUM_MICRO * MICRO_ROWS * SEQ_LEN
    vec_shape = (NUM_STAGES, MODEL_DIM)
    x_in = jax.random.normal(data_keys[0], act_shape, jnp.float32).astype(jnp.bfloat16)
    g_out = jax.random.normal(data_keys[1], act_shape, jnp.float32) * (tokens ** -0.5)
    return {
        'x_in': x_in,
        'g_out': g_out,
        'ln1_gain': 1.0 + 0.3 * jax.random.normal(weight_keys[0], vec_shape, jnp.float32),
        'ln1_bias': 0.3 * jax.random.normal(weight_keys[1], vec_shape, jnp.float32),
        'w_qkv': (jax.random.normal(weight_keys[2], (NUM_STAGES, MODEL_DIM, NUM_HEADS, 3, HEAD_DIM), jnp.float32) * MODEL_DIM ** -0.5).astype(jnp.bfloat16),
        'b_qkv': (0.5 * jax.random.normal(weight_keys[3], (NUM_STAGES, NUM_HEADS, 3, HEAD_DIM), jnp.float32)).astype(jnp.bfloat16),
        'w_out': (jax.random.normal(weight_keys[4], (NUM_STAGES, NUM_HEADS, HEAD_DIM, MODEL_DIM), jnp.float32) * MODEL_DIM ** -0.5).astype(jnp.bfloat16),
        'b_out': (0.5 * jax.random.normal(weight_keys[5], vec_shape, jnp.float32)).astype(jnp.bfloat16),
        'ln2_gain': 1.0 + 0.3 * jax.random.normal(weight_keys[6], vec_shape, jnp.float32),
        'ln2_bias': 0.3 * jax.random.normal(weight_keys[7], vec_shape, jnp.float32),
        'w_up': (jax.random.normal(weight_keys[8], (NUM_STAGES, MODEL_DIM, FFN_DIM), jnp.float32) * MODEL_DIM ** -0.5).astype(jnp.bfloat16),
        'b_up': (0.5 * jax.random.normal(weight_keys[9], (NUM_STAGES, FFN_DIM), jnp.float32)).astype(jnp.bfloat16),
        'w_down': (jax.random.normal(weight_keys[10], (NUM_STAGES, FFN_DIM, MODEL_DIM), jnp.float32) * FFN_DIM ** -0.5).astype(jnp.bfloat16),
        'b_down': (0.5 * jax.random.normal(weight_keys[11], vec_shape, jnp.float32)).astype(jnp.bfloat16),
    }


def reference(x_in, g_out, ln1_gain, ln1_bias, w_qkv, b_qkv, w_out, b_out, ln2_gain, ln2_bias, w_up, b_up, w_down, b_down):
    params = (ln1_gain, ln1_bias, w_qkv, b_qkv, w_out, b_out, ln2_gain, ln2_bias, w_up, b_up, w_down, b_down)
    cos_tab, sin_tab = rotary_tables()

    def layer_step(hidden, layer_wts):
        return layer_forward(hidden, layer_wts, cos_tab, sin_tab), None

    def stack_forward(layer_stack, hidden):
        final, unused = lax.scan(jax.checkpoint(layer_step), hidden, layer_stack)
        return final

    def micro_step(grad_acc, micro_pair):
        x_micro, g_micro = micro_pair
        y_micro, pullback = jax.vjp(lambda layer_stack: stack_forward(layer_stack, x_micro), params)
        (grads,) = pullback(g_micro.astype(jnp.bfloat16))
        grad_acc = jax.tree.map(lambda running, update: running + update.astype(jnp.float32), grad_acc, grads)
        return grad_acc, y_micro

    zeros = jax.tree.map(lambda weight: jnp.zeros(weight.shape, jnp.float32), params)
    grad_sum, y_all = lax.scan(micro_step, zeros, (x_in, g_out))
    return (y_all, grad_sum[0], grad_sum[1], grad_sum[2], grad_sum[3], grad_sum[4], grad_sum[5], grad_sum[6], grad_sum[7], grad_sum[8], grad_sum[9], grad_sum[10], grad_sum[11])
```

```python
import functools
import math

import jax
import jax.numpy as jnp
import numpy as np
from jax import lax
from jax.experimental import pallas as pl
from jax.experimental.pallas import tpu as pltpu
from jax.sharding import PartitionSpec as P

ROPE_BASE = 10000.0
LN_EPS = 1e-5
STAGE_SPECS = (P('pp', None), P('pp', None), P('pp', None, 'tp', None, None), P('pp', 'tp', None, None), P('pp', 'tp', None, None), P('pp', None), P('pp', None), P('pp', None), P('pp', None, 'tp'), P('pp', 'tp'), P('pp', 'tp', None), P('pp', None))
GRAD_SPECS = (P(('dp', 'pp'), None), P(('dp', 'pp'), None), P(('dp', 'pp'), None, 'tp', None, None), P(('dp', 'pp'), 'tp', None, None), P(('dp', 'pp'), 'tp', None, None), P(('dp', 'pp'), None), P(('dp', 'pp'), None), P(('dp', 'pp'), None), P(('dp', 'pp'), None, 'tp'), P(('dp', 'pp'), 'tp'), P(('dp', 'pp'), 'tp', None), P(('dp', 'pp'), None))

F32 = jnp.float32
BF16 = jnp.bfloat16
NL = 4
NT = 4
NC = 4
SUB = 2
LOG2E = 1.4426950408889634
RSQRT2 = 0.7071067811865476
INV_SQRT_2PI = 0.3989422804014327


def nn(a, b):
    return lax.dot_general(a, b, (((1,), (0,)), ((), ())), preferred_element_type=F32)


def nt(a, b):
    return lax.dot_general(a, b, (((1,), (1,)), ((), ())), preferred_element_type=F32)


def tn(a, b):
    return lax.dot_general(a, b, (((0,), (0,)), ((), ())), preferred_element_type=F32)


def rotary_base(chunk, n_chunks, head_dim, n_heads):
    rot_dim = head_dim // 4
    half = rot_dim // 2
    inv_freq = np.zeros((head_dim,), np.float64)
    inv_freq[:rot_dim] = np.tile(ROPE_BASE ** (-(np.arange(half) * 2.0) / rot_dim), 2)
    inv_freq = np.tile(inv_freq, n_heads)
    pos = np.concatenate([np.arange(chunk), np.arange(8) * (np.arange(8) < n_chunks) * chunk]).astype(np.float64)
    ang = pos[:, None] * inv_freq[None, :]
    return np.stack([np.cos(ang), np.sin(ang)]).astype(np.float32)


def body(dims, x, g, wqkv, wo, wup, wdn, vec, tab,
         y, oqkv, oo, oup, odn, ovec,
         WQ, WO, WU, WD, VEC, H, Q, K, V, KT, VT, CTX, P0, P1, P2, P3, HID, GP, RA, RB, PS, PF,
         GQ, GO, GU, GD, R2Q, R2O, R2U, R2D, DK, DV, TAB, COS, SIN, GV, ZR, GZ, PR,
         AS, MS, PRE, DPB, DS, ST,
         wl, ws, wr, wf, xs, gs, sab, sc, ra_s, rb_s, rc_s, ys, yr, g1s, g1r, g2s, g2r, g3s, g3r, v1s, v1r, v2s, v2r, osem):
    S, D, E, C, F = dims
    E2 = 2 * E
    SR = C // SUB
    z = lax.axis_index('tp')
    s = lax.axis_index('pp')
    ys_ = s // 2
    c = s % 2
    sib = s + 1 - 2 * c
    oy = 2 * (1 - ys_)
    is_end = z * (NT - 1 - z) == 0
    inner = z * (NT - 1 - z) > 0
    hub = 1 + z // 3
    leaf = jnp.where(z == 1, 0, 3)
    peer = 3 - z
    PX = (P0, P1, P2, P3)
    W_IN = (wqkv, wo, wup, wdn)
    W_BUF = (WQ, WO, WU, WD)
    W_HALF = (D // 2, E, D // 2, F // 2)
    G_BUF = (GQ, GO, GU, GD)
    G_OUT = (oqkv, oo, oup, odn)
    G_HALF = W_HALF
    G_COLS = (3 * E2, D, F, D)
    R1_OFF = (0, D // 2, D // 2 + E, D + E)
    R2 = (R2Q, R2O, R2U, R2D)

    def rcopy(src, dst, ss, rs, **dev):
        return pltpu.make_async_remote_copy(src_ref=src, dst_ref=dst, send_sem=ss, recv_sem=rs, device_id=dev, device_id_type=pl.DeviceIdType.MESH)

    def lcopy(src, dst, sem):
        return pltpu.make_async_copy(src, dst, sem)

    def rows(start, n):
        return pl.ds(pl.multiple_of(start, n), n)

    xcopy = lcopy(x.at[ys_, c], H.at[0], xs.at[0])
    xcopy.start()
    gcopy = lcopy(g.at[ys_, c], GP.at[NL], gs.at[0])
    gcopy.start()
    tcopy = lcopy(tab, TAB, xs.at[1])
    tcopy.start()
    for a in range(4):
        lcopy(W_IN[a], W_BUF[a].at[s], wl.at[a]).start()
    lcopy(vec, VEC.at[s], wl.at[4]).start()

    bar = pltpu.get_barrier_semaphore()
    for o in range(1, NT):
        pl.semaphore_signal(bar, inc=1, device_id={'tp': (z + o) % NT}, device_id_type=pl.DeviceIdType.MESH)
    for o in range(1, NL):
        pl.semaphore_signal(bar, inc=1, device_id={'pp': (s + o) % NL}, device_id_type=pl.DeviceIdType.MESH)
    pl.semaphore_wait(bar, NT - 1 + NL - 1)

    def w_half(a, k):
        return rows(k * W_HALF[a], W_HALF[a])

    def sib_copies():
        out = []
        for a in range(4):
            for k in range(2):
                out.append(rcopy(W_IN[a].at[w_half(a, k)], W_BUF[a].at[s, w_half(a, k)], ws.at[2 * a + k], wr.at[s, 2 * a + k], pp=sib))
        out.append(rcopy(vec, VEC.at[s], ws.at[16], wr.at[s, 8], pp=sib))
        return out

    def y_copies():
        out = [rcopy(vec, VEC.at[s], ws.at[17 + k], wr.at[s, 8], pp=oy + k) for k in range(2)]
        for a in range(4):
            for k in range(2):
                out.append(rcopy(W_IN[a].at[w_half(a, k)], W_BUF[a].at[s, w_half(a, k)], ws.at[8 + 2 * a + k], wr.at[s, 2 * a + k], pp=oy + k))
        return out

    def start_all(copies):
        for cp in copies:
            cp.start()

    @pl.when(s != 1)
    def _():
        start_all(y_copies())
    start_all(sib_copies())

    def arrived(l, a, k):
        rcopy(W_BUF[a].at[l, w_half(a, k)], W_BUF[a].at[l, w_half(a, k)], ws.at[2 * a], wr.at[l, 2 * a + k], pp=sib).wait_recv()

    def fwd_copy(l, a):
        part = W_BUF[a].at[l, w_half(a, c)]
        return rcopy(part, part, wf.at[l % 2, a], wr.at[l, 2 * a + c], pp=sib)

    def fetch(l):
        @pl.when(l == s)
        def _():
            for a in range(4):
                lcopy(W_IN[a], W_BUF[a].at[s], wl.at[a]).wait()
            lcopy(vec, VEC.at[s], wl.at[4]).wait()

        @pl.when(l != s)
        def _():
            @pl.when(l // 2 == ys_)
            def _():
                for a in range(4):
                    for k in range(2):
                        arrived(l, a, k)

            @pl.when(l // 2 != ys_)
            def _():
                for a in range(4):
                    arrived(l, a, c)
                    fwd_copy(l, a).start()
                for a in range(4):
                    arrived(l, a, 1 - c)
            rcopy(VEC.at[l], VEC.at[l], ws.at[16], wr.at[l, 8], pp=sib).wait_recv()

    tcopy.wait()
    for i in range(NC):
        cb, sb = TAB[0, 0:C, :], TAB[1, 0:C, :]
        cr, sr = TAB[0, C + i:C + i + 1, :], TAB[1, C + i:C + i + 1, :]
        COS[i * C:(i + 1) * C, :] = cb * cr - sb * sr
        SIN[i * C:(i + 1) * C, :] = sb * cr + cb * sr

    lane = lax.broadcasted_iota(jnp.int32, (C, E2), 1)
    head_lane = lane // E
    in_head = lane % E
    rot_half = E // 8
    low = in_head < rot_half
    sub_head = lax.broadcasted_iota(jnp.int32, (E2, C), 0) // E
    lower = lax.broadcasted_iota(jnp.int32, (C, C), 0) <= lax.broadcasted_iota(jnp.int32, (C, C), 1)
    c1 = E ** -0.5 * LOG2E

    def tabs(i):
        cs, sn = COS[i * C:(i + 1) * C, :], SIN[i * C:(i + 1) * C, :]
        return cs, jnp.where(low, -sn, 0.0), jnp.where(low, 0.0, sn)

    def rotate(v, t):
        cs, sa, sb = t
        return v * cs + pltpu.roll(v, E2 - rot_half, 1) * sa + pltpu.roll(v, rot_half, 1) * sb

    def unrotate(v, t):
        cs, sa, sb = t
        return v * cs + pltpu.roll(v * sa, rot_half, 1) + pltpu.roll(v * sb, E2 - rot_half, 1)

    def end_copy(p, t):
        return rcopy(PS.at[t * SR:(t + 1) * SR], RA.at[p % 2, t * SR:(t + 1) * SR], sab.at[t], ra_s.at[p % 2, t], tp=hub)

    def peer_copy(p, t):
        return rcopy(PS.at[t * SR:(t + 1) * SR], RB.at[p % 2, t * SR:(t + 1) * SR], sab.at[t], rb_s.at[p % 2, t], tp=peer)

    def back_copy(p, di, t):
        return rcopy(H.at[di, t * SR:(t + 1) * SR], H.at[di, t * SR:(t + 1) * SR], sc.at[t], rc_s.at[p % 2, t], tp=leaf)

    def pf_row(i, back):
        return (NC if back and i == NC - 1 else i) * C

    def ar_send(p, i, back=False):
        @pl.when(is_end)
        def _():
            for t in range(i * SUB, (i + 1) * SUB):
                @pl.when(p > 0)
                def _():
                    end_copy(p, t).wait_send()
                f0 = pf_row(i, back) + (t - i * SUB) * SR
                PS[t * SR:(t + 1) * SR, :] = PF[f0:f0 + SR, :].astype(BF16)
                end_copy(p, t).start()

    def ar_mid(p, i, back=False):
        @pl.when(inner)
        def _():
            for t in range(i * SUB, (i + 1) * SUB):
                end_copy(p, t).wait_recv()
                @pl.when(p > 0)
                def _():
                    peer_copy(p, t).wait_send()
                r = slice(t * SR, (t + 1) * SR)
                f0 = pf_row(i, back) + (t - i * SUB) * SR
                PS[r, :] = (PF[f0:f0 + SR, :] + RA[p % 2, r, :].astype(F32)).astype(BF16)
                peer_copy(p, t).start()

    def ar_last(p, ri, di, i):
        @pl.when(inner)
        def _():
            keep = jnp.where(p < NL, 1.0, 0.0)
            lv = jnp.minimum(p, NL - 1)
            bias = (VEC[lv, 4:5, :] + VEC[lv, 5:6, :]) * keep
            for t in range(i * SUB, (i + 1) * SUB):
                peer_copy(p, t).wait_recv()
                @pl.when(p > 0)
                def _():
                    back_copy(p, di, t).wait_send()
                r = slice(t * SR, (t + 1) * SR)
                both = PS[r, :].astype(F32) + RB[p % 2, r, :].astype(F32)
                H[di, r, :] = (H[ri, r, :].astype(F32) + both + bias).astype(BF16)
                back_copy(p, di, t).start()

    def ar_wait(p, di, i):
        @pl.when(is_end)
        def _():
            for t in range(i * SUB, (i + 1) * SUB):
                back_copy(p, di, t).wait_recv()

    def stats(hf):
        cen = hf - jnp.mean(hf, axis=-1, keepdims=True)
        rstd = lax.rsqrt(jnp.mean(cen * cen, axis=-1, keepdims=True) + LN_EPS)
        return cen * rstd, rstd

    LB = 64

    def norms(l, i):
        g1, b1, g2, b2 = (VEC[l, k:k + 1, :] for k in range(4))

        def step(b, carry):
            hf = H[l, rows(i * C + b * LB, LB), :].astype(F32)
            xhat, unused = stats(hf)
            AS[rows(b * LB, LB), :] = (xhat * g1 + b1).astype(BF16)
            MS[rows(b * LB, LB), :] = (xhat * g2 + b2).astype(BF16)
            return carry
        lax.fori_loop(0, C // LB, step, 0)

    def forward(l, i):
        r0, r1 = i * C, (i + 1) * C
        norms(l, i)
        qkv = nn(AS[...], WQ[l]) + VEC[l, 7:8, 0:3 * E2]
        qkv = qkv.astype(BF16).astype(F32)
        t = tabs(i)
        q = rotate(qkv[:, 0:E2], t).astype(BF16)
        kf = rotate(qkv[:, E2:2 * E2], t)
        vf = qkv[:, 2 * E2:3 * E2]
        Q[l, r0:r1, :] = q
        K[l, r0:r1, :] = kf.astype(BF16)
        V[l, r0:r1, :] = vf.astype(BF16)
        KT[l, :, r0:r1] = jnp.transpose(kf).astype(BF16)
        VT[:, r0:r1] = jnp.transpose(vf).astype(BF16)
        RBK = C // 2
        outs = []
        for h in range(2):
            qm = jnp.where(head_lane == h, Q[l, r0:r1, :].astype(F32), 0.0).astype(BF16)
            ST[0:r1, :] = nt(K[l, 0:r1, :], qm)
            ST[r0:r1, :] = jnp.where(lower, ST[r0:r1, :], -1e30)

            def top(b, m):
                return jnp.maximum(m, jnp.max(ST[rows(b * RBK, RBK), :].reshape(RBK // 8, 8, C), axis=0))
            m = jnp.max(lax.fori_loop(0, r1 // RBK, top, jnp.full((8, C), -3e38, F32)), axis=0, keepdims=True)
            mc = m * c1

            def expo(b, tot):
                e = jnp.exp2(ST[rows(b * RBK, RBK), :] * c1 - mc)
                ST[rows(b * RBK, RBK), :] = e
                return tot + jnp.sum(e.reshape(RBK // 8, 8, C), axis=0)
            tot = jnp.sum(lax.fori_loop(0, r1 // RBK, expo, jnp.zeros((8, C), F32)), axis=0, keepdims=True)
            inv = 1.0 / tot

            def put(b, carry):
                PX[i][l, h, rows(b * RBK, RBK), :] = (ST[rows(b * RBK, RBK), :] * inv).astype(BF16)
                return carry
            lax.fori_loop(0, r1 // RBK, put, 0)
            outs.append(nn(VT[:, 0:r1], PX[i][l, h]))
        ctx = jnp.transpose(jnp.where(sub_head == 0, outs[0], outs[1])).astype(BF16)
        CTX[l, r0:r1, :] = ctx
        PF[r0:r1, :] = nn(ctx, WO[l])
        PRE[...] = nn(MS[...], WU[l])
        bup = VEC[l, 6:7, :]
        GB = 32

        def act(b, carry):
            u = PRE[rows(b * GB, GB), :] + bup
            cdf = 0.5 * (1.0 + lax.erf(u * RSQRT2))
            pdf = jnp.exp2(u * u * (-0.5 * LOG2E)) * INV_SQRT_2PI
            HID[l, rows(r0 + b * GB, GB), :] = (u * cdf).astype(BF16)
            GP[l, rows(r0 + b * GB, GB), :] = cdf + u * pdf
            return carry
        lax.fori_loop(0, C // GB, act, 0)
        PF[r0:r1, :] += nn(HID[l, r0:r1, :], WD[l])

    def backward(l, dl, i, last):
        r0, r1 = i * C, (i + 1) * C
        par = l % 2
        first = i == NC - 1

        def acc(ref, val):
            if first:
                ref[par] = val
            else:
                ref[par] += val

        def acc_row(k, val, w=D):
            GV[l, k:k + 1, 0:w] += val

        norms(l, i)
        dy = H[dl, r0:r1, :]
        acc_row(4, jnp.sum(dy.astype(F32), axis=0, keepdims=True))
        PRE[...] = nt(dy, WD[l])
        GB = 32

        def act(b, tot):
            d = PRE[rows(b * GB, GB), :] * GP[l, rows(r0 + b * GB, GB), :]
            DPB[rows(b * GB, GB), :] = d.astype(BF16)
            return tot + jnp.sum(d.reshape(GB // 8, 8, F), axis=0)
        dbu = lax.fori_loop(0, C // GB, act, jnp.zeros((8, F), F32))
        acc_row(5, jnp.sum(dbu, axis=0, keepdims=True))
        acc(GD, tn(HID[l, r0:r1, :], dy))
        acc(GU, tn(MS[...], DPB[...]))
        f0 = pf_row(i, True)
        PF[f0:f0 + C, :] = nt(DPB[...], WU[l])
        dctx = nt(dy, WO[l]).astype(BF16)
        ctx = CTX[l, r0:r1, :]
        acc(GO, tn(ctx, dy))
        prod = dctx.astype(F32) * ctx.astype(F32)
        q = Q[l, r0:r1, :].astype(F32)
        dcf = dctx.astype(F32)
        RBK = C // 2
        dqt = []
        for h in range(2):
            sel = head_lane == h
            qm = jnp.where(sel, q, 0.0).astype(BF16)
            dcm = jnp.where(sel, dcf, 0.0).astype(BF16)
            dsum = jnp.transpose(jnp.where(sel, prod, 0.0))
            drow = jnp.sum(dsum, axis=0, keepdims=True)
            ST[0:r1, :] = nt(V[l, 0:r1, :], dcm)

            def sub(b, carry):
                pr = PX[i][l, h, rows(b * RBK, RBK), :].astype(F32)
                DS[rows(b * RBK, RBK), :] = (pr * (ST[rows(b * RBK, RBK), :] - drow)).astype(BF16)
                return carry
            lax.fori_loop(0, r1 // RBK, sub, 0)
            dk = nn(DS[0:r1, :], qm)
            dv = nn(PX[i][l, h], dcm)
            if first and h == 0:
                DK[0:r1, :] = dk
                DV[0:r1, :] = dv
            else:
                DK[0:r1, :] += dk
                DV[0:r1, :] += dv
            dqt.append(nn(KT[l, :, 0:r1], DS[0:r1, :]))
        scale = E ** -0.5
        t = tabs(i)
        dq = unrotate(jnp.transpose(jnp.where(sub_head == 0, dqt[0], dqt[1])) * scale, t)
        dk = unrotate(DK[r0:r1, :] * scale, t)
        dv = DV[r0:r1, :]
        dqkv = jnp.concatenate([dq, dk, dv], axis=1)
        acc_row(6, jnp.sum(dqkv, axis=0, keepdims=True), 3 * E2)
        dqkv = dqkv.astype(BF16)
        acc(GQ, tn(AS[...], dqkv))
        PRE[...] = nt(dqkv, WQ[l])
        g1, g2 = VEC[l, 0:1, :], VEC[l, 2:3, :]

        def lnb(b, tots):
            hf = H[l, rows(r0 + b * LB, LB), :].astype(F32)
            xhat, rstd = stats(hf)
            da = PRE[rows(b * LB, LB), :]
            dm = PF[rows(f0 + b * LB, LB), :]
            dx = da * g1 + dm * g2
            m1 = jnp.mean(dx, axis=-1, keepdims=True)
            m2 = jnp.mean(dx * xhat, axis=-1, keepdims=True)
            if not last:
                PF[rows(f0 + b * LB, LB), :] = rstd * (dx - m1 - xhat * m2)
            terms = (da * xhat, da, dm * xhat, dm)
            return tuple(a + jnp.sum(v.reshape(LB // 8, 8, D), axis=0) for a, v in zip(tots, terms))
        tots = lax.fori_loop(0, C // LB, lnb, tuple(jnp.zeros((8, D), F32) for _ in range(4)))
        for k in range(4):
            acc_row(k, jnp.sum(tots[k], axis=0, keepdims=True))

    def g_half(a, k):
        return rows(k * G_HALF[a], G_HALF[a])

    def r1_view(l, a):
        return GP.at[l + 1, R1_OFF[a]:R1_OFF[a] + G_HALF[a], 0:G_COLS[a]]

    def g1_copy(l, a):
        return rcopy(G_BUF[a].at[l % 2, g_half(a, 1 - c)], r1_view(l, a), g1s.at[a], g1r.at[l % 2, a], pp=sib)

    def g2_copy(l, a):
        return rcopy(HID.at[l, R1_OFF[a]:R1_OFF[a] + G_HALF[a], 0:G_COLS[a]], R2[a].at[l % 2], g2s.at[a], g2r.at[l % 2, a], pp=2 * (l // 2) + c)

    def g3_local(l, a):
        return lcopy(G_BUF[a].at[l % 2, g_half(a, c)], G_OUT[a].at[g_half(a, c)], g3s.at[a])

    def g3_remote(l, a):
        return rcopy(G_BUF[a].at[l % 2, g_half(a, c)], G_OUT[a].at[g_half(a, c)], g3s.at[a], g3r.at[a], pp=sib)

    def v1_copies(l):
        return [rcopy(GV.at[l], ZR.at[l, z], v1s.at[l, o - 1], v1r.at[l, z], tp=(z + o) % NT) for o in range(1, NT)]

    def grads_out(l):
        for a in range(4):
            g1_copy(l, a).start()
        for cp in v1_copies(l):
            cp.start()

    def grads_mid(l):
        for a in range(4):
            g1_copy(l, a).wait_recv()
            n = G_HALF[a]
            nb = n // 32

            def add(b, carry):
                rr = rows(c * n + b * 32, 32)
                tot = G_BUF[a][l % 2, rr, :] + GP[l + 1, rows(R1_OFF[a] + b * 32, 32), 0:G_COLS[a]]
                G_BUF[a][l % 2, rr, :] = tot
                HID[l, rows(R1_OFF[a] + b * 32, 32), 0:G_COLS[a]] = tot.astype(BF16)
                return carry
            lax.fori_loop(0, nb, add, 0)

            @pl.when(l // 2 != ys_)
            def _():
                g2_copy(l, a).start()

    def grads_last(l):
        @pl.when(l // 2 == ys_)
        def _():
            for a in range(4):
                g2_copy(l, a).wait_recv()
                n = G_HALF[a]

                def add(b, carry):
                    rr = rows(c * n + b * 32, 32)
                    G_BUF[a][l % 2, rr, :] += R2[a][l % 2, rows(b * 32, 32), :].astype(F32)
                    return carry
                lax.fori_loop(0, n // 32, add, 0)

                @pl.when(l == s)
                def _():
                    g3_local(l, a).start()

                @pl.when(l != s)
                def _():
                    g3_remote(l, a).start()

    def grads_done(l):
        for a in range(4):
            g1_copy(l, a).wait_send()

            @pl.when(l // 2 != ys_)
            def _():
                g2_copy(l, a).wait_send()

            @pl.when(l == s)
            def _():
                g3_local(l, a).wait()

            @pl.when((l // 2 == ys_) & (l != s))
            def _():
                g3_remote(l, a).wait_send()

    def v2_copy(l):
        return rcopy(GZ.at[l], PR.at[s], v2s.at[l], v2r.at[s], pp=l)

    def vec_mid(l):
        ZR[l, z] = GV[l]
        for o in range(1, NT):
            q = (z + o) % NT
            rcopy(GV.at[l], ZR.at[l, q], v1s.at[l, o - 1], v1r.at[l, q], tp=q).wait_recv()
        tot = ZR[l, 0] + ZR[l, 1] + ZR[l, 2] + ZR[l, 3]
        row = lax.broadcasted_iota(jnp.int32, (8, D), 0)
        GZ[l] = jnp.where(row < 4, tot, GV[l])

        @pl.when(l == s)
        def _():
            PR[s] = GZ[l]

        @pl.when(l != s)
        def _():
            v2_copy(l).start()

    GV[...] = jnp.zeros_like(GV)
    fetch(0)
    xcopy.wait()

    def fwd_layer(l, carry):
        for i in range(NC):
            @pl.when(l > 0)
            def _():
                ar_wait(l - 1, l, i)
            forward(l, i)
            ar_send(l, i)
            if i == 0:
                @pl.when(l > 0)
                def _():
                    ar_last(l - 1, l - 1, l, 2)
                    ar_mid(l - 1, 3)
            elif i == 1:
                @pl.when(l > 0)
                def _():
                    ar_last(l - 1, l - 1, l, 3)
                ar_mid(l, 0)

                @pl.when(l == 0)
                def _():
                    gcopy.wait()
                    H[NL + 1] = GP[NL].astype(BF16)
            else:
                ar_last(l, l, l + 1, i - 2)
                ar_mid(l, i - 1)

            if i == 2:
                @pl.when((l == 0) & (s == 1))
                def _():
                    start_all(y_copies())

        @pl.when(l < NL - 1)
        def _():
            fetch(l + 1)
        return carry
    lax.fori_loop(0, NL, fwd_layer, 0)

    def y_copies_out():
        return [rcopy(H.at[NL], y.at[ys_, c], ys.at[o], yr.at[s], pp=(s + o) % NL) for o in range(1, NL)]

    y_local = lcopy(H.at[NL], y.at[ys_, c], ys.at[0])

    def ri(l):
        return jnp.where(l == NL - 1, NL + 1, l + 1)

    def bwd_layer(lb, carry):
        l = NL - 1 - lb
        p = NL + lb
        for n in range(NC):
            i = NC - 1 - n

            @pl.when(lb > 0)
            def _():
                ar_wait(p - 1, l + 1, i)
            backward(l, ri(l), i, False)

            @pl.when(l > 0)
            def _():
                ar_send(p, i, True)
            if n == 0:
                @pl.when(lb == 0)
                def _():
                    ar_last(NL - 1, NL - 1, NL, 2)
                    ar_mid(NL - 1, 3)

                @pl.when(lb > 0)
                def _():
                    ar_last(p - 1, ri(l + 1), l + 1, 1)
                    ar_mid(p - 1, 0, True)
                    grads_mid(l + 1)
            elif n == 1:
                @pl.when(lb == 0)
                def _():
                    ar_last(NL - 1, NL - 1, NL, 3)

                @pl.when(lb > 0)
                def _():
                    ar_last(p - 1, ri(l + 1), l + 1, 0)
                    vec_mid(l + 1)

                @pl.when(l > 0)
                def _():
                    ar_mid(p, NC - 1, True)
            else:
                @pl.when(l > 0)
                def _():
                    ar_last(p, ri(l), l, NC - 1 - (n - 2))
                    ar_mid(p, NC - 1 - (n - 1), True)
                if n == 2:
                    @pl.when(lb == 0)
                    def _():
                        for j in range(NC):
                            ar_wait(NL - 1, NL, j)
                        y_local.start()
                        start_all(y_copies_out())

                    @pl.when(lb > 0)
                    def _():
                        grads_last(l + 1)

        @pl.when(lb > 0)
        def _():
            grads_done(l + 1)
        grads_out(l)
        return carry
    lax.fori_loop(0, NL, bwd_layer, 0)

    grads_mid(0)
    vec_mid(0)
    grads_last(0)
    grads_done(0)

    for o in range(1, NL):
        q = (s + o) % NL
        rcopy(GZ.at[0], PR.at[q], v2s.at[0], v2r.at[q], pp=q).wait_recv()
    PRE[0:8, 0:D] = PR[0] + PR[1] + PR[2] + PR[3]
    vout = lcopy(PRE.at[0:8, 0:D], ovec, osem.at[0])
    vout.start()
    for l in range(NL):
        for cp in v1_copies(l):
            cp.wait_send()
    for l in range(NL):
        @pl.when(l != s)
        def _():
            v2_copy(l).wait_send()
    for a in range(4):
        rcopy(G_OUT[a].at[g_half(a, 1 - c)], G_OUT[a].at[g_half(a, 1 - c)], g3s.at[a], g3r.at[a], pp=sib).wait_recv()
    y_local.wait()
    for o, cp in enumerate(y_copies_out()):
        cp.wait_send()
        q = (s + o + 1) % NL
        rcopy(H.at[NL], y.at[q // 2, q % 2], ys.at[o + 1], yr.at[q], pp=q).wait_recv()
    for cp in sib_copies():
        cp.wait_send()
    for cp in y_copies():
        cp.wait_send()
    for k in range(2):
        for a in range(4):
            fwd_copy(oy + k, a).wait_send()

    @pl.when(is_end)
    def _():
        for t in range(NC * SUB):
            end_copy(0, t).wait_send()

    @pl.when(inner)
    def _():
        for t in range(NC * SUB):
            peer_copy(0, t).wait_send()
            back_copy(0, 1, t).wait_send()
    vout.wait()


def group_step(dims, x, g, wqkv, wo, wup, wdn, vec, tab):
    S, D, E, C, F = dims
    E2 = 2 * E
    hbm = pl.BlockSpec(memory_space=pl.ANY)
    out_shape = [
        jax.ShapeDtypeStruct(x.shape, BF16),
        jax.ShapeDtypeStruct((D, 3 * E2), F32),
        jax.ShapeDtypeStruct((E2, D), F32),
        jax.ShapeDtypeStruct((D, F), F32),
        jax.ShapeDtypeStruct((F, D), F32),
        jax.ShapeDtypeStruct((8, D), F32),
    ]

    def vm(*shape, dtype=BF16):
        return pltpu.VMEM(shape, dtype)
    dma = pltpu.SemaphoreType.DMA
    scratch = [
        vm(NL, D, 3 * E2), vm(NL, E2, D), vm(NL, D, F), vm(NL, F, D), vm(NL, 8, D, dtype=F32),
        vm(NL + 2, S, D),
        vm(NL, S, E2), vm(NL, S, E2), vm(NL, S, E2), vm(NL, E2, S), vm(E2, S), vm(NL, S, E2),
        *[vm(NL, 2, (i + 1) * C, C) for i in range(NC)],
        vm(NL, S, F), vm(NL + 1, S, F, dtype=F32),
        vm(2, S, D), vm(2, S, D), vm(S, D), vm(S + C, D, dtype=F32),
        vm(2, D, 3 * E2, dtype=F32), vm(2, E2, D, dtype=F32), vm(2, D, F, dtype=F32), vm(2, F, D, dtype=F32),
        vm(2, D // 2, 3 * E2), vm(2, E, D), vm(2, D // 2, F), vm(2, F // 2, D),
        vm(S, E2, dtype=F32), vm(S, E2, dtype=F32),
        vm(2, C + 8, E2, dtype=F32), vm(S, E2, dtype=F32), vm(S, E2, dtype=F32),
        vm(NL, 8, D, dtype=F32), vm(NL, NT, 8, D, dtype=F32), vm(NL, 8, D, dtype=F32), vm(NL, 8, D, dtype=F32),
        vm(C, D), vm(C, D), vm(C, max(D, F), dtype=F32), vm(C, F), vm(S, C), vm(S, C, dtype=F32),
        dma((5,)), dma((19,)), dma((NL, 9)), dma((2, 4)), dma((2,)), dma((1,)),
        dma((NC * SUB,)), dma((NC * SUB,)), dma((2, NC * SUB)), dma((2, NC * SUB)), dma((2, NC * SUB)),
        dma((NL,)), dma((NL,)), dma((4,)), dma((2, 4)), dma((4,)), dma((2, 4)), dma((4,)), dma((4,)),
        dma((NL, NT - 1)), dma((NL, NT)), dma((NL,)), dma((NL,)), dma((1,)),
    ]
    return pl.pallas_call(
        functools.partial(body, dims),
        out_shape=out_shape,
        in_specs=[hbm] * 8,
        out_specs=[hbm] * 6,
        scratch_shapes=scratch,
        compiler_params=pltpu.CompilerParams(collective_id=0, has_side_effects=True, vmem_limit_bytes=67043328),
        name='neox_group',
    )(x, g, wqkv, wo, wup, wdn, vec, tab)


def solution(mesh):
    def device_fn(x_in, g_out, ln1_gain, ln1_bias, w_qkv, b_qkv, w_out, b_out, ln2_gain, ln2_bias, w_up, b_up, w_down, b_down):
        n_micro, n_rows, S, D = x_in.shape
        heads, E = w_qkv.shape[2], w_qkv.shape[4]
        F = w_up.shape[2]
        C = S // NC
        qcols = heads * 3 * E
        wqkv = jnp.transpose(w_qkv[0], (0, 2, 1, 3)).reshape(D, qcols)
        bqkv = jnp.transpose(b_qkv[0], (1, 0, 2)).reshape(1, qcols).astype(F32)
        bqkv = jnp.pad(bqkv, ((0, 0), (0, D - qcols)))
        vec = jnp.concatenate([ln1_gain, ln1_bias, ln2_gain, ln2_bias, b_out.astype(F32), b_down.astype(F32), b_up.astype(F32), bqkv], axis=0)
        tab = jnp.asarray(rotary_base(C, NC, E, heads))
        y, gqkv, go, gup, gdn, gvec = group_step((S, D, E, C, F), x_in, g_out, wqkv, w_out[0].reshape(heads * E, D), w_up[0], w_down[0], vec, tab)
        gq = jnp.transpose(gqkv.reshape(D, 3, heads, E), (0, 2, 1, 3))[None]
        gbq = jnp.transpose(gvec[6, :qcols].reshape(3, heads, E), (1, 0, 2))[None]
        bias_out = gvec[4:5]
        return (y, gvec[0:1], gvec[1:2], gq, gbq, go.reshape(1, heads, E, D), bias_out, gvec[2:3], gvec[3:4], gup[None], gvec[5:6], gdn[None], bias_out)

    return jax.shard_map(device_fn, mesh=mesh, in_specs=(P('dp'), P('dp')) + STAGE_SPECS, out_specs=(P('dp'),) + GRAD_SPECS, check_vma=False)
```

```python
import functools
import math

import jax
import jax.numpy as jnp
import numpy as np
from jax import lax
from jax.experimental import pallas as pl
from jax.experimental.pallas import tpu as pltpu
from jax.sharding import PartitionSpec as P

ROPE_BASE = 10000.0
LN_EPS = 1e-5
STAGE_SPECS = (P('pp'), P('pp'), P('pp', None, 'tp'), P('pp', 'tp'), P('pp', 'tp'), P('pp'), P('pp'), P('pp'), P('pp', None, 'tp'), P('pp', 'tp'), P('pp', 'tp'), P('pp'))
OWN = ('dp', 'pp')
GRAD_SPECS = (P(OWN), P(OWN), P(OWN, None, 'tp'), P(OWN, 'tp'), P(OWN, 'tp'), P(OWN), P(OWN), P(OWN), P(OWN, None, 'tp'), P(OWN, 'tp'), P(OWN, 'tp'), P(OWN))


F32 = jnp.float32
BF16 = jnp.bfloat16
NL = 4
NT = 4
NC = 4
NA = 4
SUB = 2
FWD_AT = {0: (('mid', 1, 0), ('last', 2, 0)), 2: (('mid', 1, 1), ('last', 2, 1))}
BWD_AT = {0: (('last', 2, 0),), 1: (('mid', 1, 0),), 3: (('last', 2, 1),), 4: (('mid', 1, 1),)}
LOG2E = 1.4426950408889634
RSQRT2 = 0.7071067811865476
INV_SQRT_2PI = 0.3989422804014327


def nn(a, b):
    return lax.dot_general(a, b, (((1,), (0,)), ((), ())), preferred_element_type=F32)


def nt(a, b):
    return lax.dot_general(a, b, (((1,), (1,)), ((), ())), preferred_element_type=F32)


def tn(a, b):
    return lax.dot_general(a, b, (((0,), (0,)), ((), ())), preferred_element_type=F32)


def rotary_base(chunk, n_chunks, head_dim, n_heads):
    rot_dim = head_dim // 4
    half = rot_dim // 2
    inv_freq = np.zeros((head_dim,), np.float64)
    inv_freq[:rot_dim] = np.tile(ROPE_BASE ** (-(np.arange(half) * 2.0) / rot_dim), 2)
    inv_freq = np.tile(inv_freq, n_heads)
    pos = np.concatenate([np.arange(chunk), np.arange(8) * (np.arange(8) < n_chunks) * chunk]).astype(np.float64)
    ang = pos[:, None] * inv_freq[None, :]
    return np.stack([np.cos(ang), np.sin(ang)]).astype(np.float32)


def body(dims, x, g, wqkv, wo, wup, wdn, vec, tab,
         y, oqkv, oo, oup, odn, ovec,
         WQ, WO, WU, WD, VEC, H, Q, K, V, KT, VT, CTX, P0, P1, P2, P3, HID, GP, RA, RB, PS, PF,
         GQ, GO, GU, GD, R2Q, R2O, R2U, R2D, DK, DV, TAB, COS, SIN, GV, ZR, GZ, PR,
         AS, MS, PRE, DPB, DS, ST,
         wl, ws, wr, wf, xs, gs, sab, sc, ra_s, rb_s, rc_s, ys, yr, g1s, g1r, g2s, g2r, g3s, g3r, v1s, v1r, v2s, v2r, osem):
    S, D, E, C, F = dims
    E2 = 2 * E
    SR = C // SUB
    z = lax.axis_index('tp')
    s = lax.axis_index('pp')
    ys_ = s // 2
    c = s % 2
    sib = s + 1 - 2 * c
    oy = 2 * (1 - ys_)
    is_end = z * (NT - 1 - z) == 0
    inner = z * (NT - 1 - z) > 0
    hub = 1 + z // 3
    leaf = jnp.where(z == 1, 0, 3)
    peer = 3 - z
    PX = (P0, P1, P2, P3)
    W_IN = (wqkv, wo, wup, wdn)
    W_BUF = (WQ, WO, WU, WD)
    W_HALF = (D // 2, E, D // 2, F // 2)
    G_BUF = (GQ, GO, GU, GD)
    G_OUT = (oqkv, oo, oup, odn)
    G_HALF = W_HALF
    G_COLS = (3 * E2, D, F, D)
    R1_OFF = (0, D // 2, D // 2 + E, D + E)
    R2 = (R2Q, R2O, R2U, R2D)

    def rcopy(src, dst, ss, rs, **dev):
        return pltpu.make_async_remote_copy(src_ref=src, dst_ref=dst, send_sem=ss, recv_sem=rs, device_id=dev, device_id_type=pl.DeviceIdType.MESH)

    def lcopy(src, dst, sem):
        return pltpu.make_async_copy(src, dst, sem)

    def rows(start, n):
        return pl.ds(pl.multiple_of(start, n), n)

    xcopy = lcopy(x.at[ys_, c], H.at[0], xs.at[0])
    xcopy.start()
    gcopy = lcopy(g.at[ys_, c], GP.at[NL], gs.at[0])
    gcopy.start()
    tcopy = lcopy(tab, TAB, xs.at[1])
    tcopy.start()
    for a in range(NA):
        lcopy(W_IN[a], W_BUF[a].at[s], wl.at[a]).start()
    lcopy(vec, VEC.at[s], wl.at[4]).start()

    bar = pltpu.get_barrier_semaphore()
    for o in range(1, NT):
        pl.semaphore_signal(bar, inc=1, device_id={'tp': (z + o) % NT}, device_id_type=pl.DeviceIdType.MESH)
    for o in range(1, NL):
        pl.semaphore_signal(bar, inc=1, device_id={'pp': (s + o) % NL}, device_id_type=pl.DeviceIdType.MESH)
    pl.semaphore_wait(bar, NT - 1 + NL - 1)

    def w_half(a, k):
        return rows(k * W_HALF[a], W_HALF[a])

    def sib_copies():
        out = []
        for a in range(NA):
            for k in range(2):
                out.append(rcopy(W_IN[a].at[w_half(a, k)], W_BUF[a].at[s, w_half(a, k)], ws.at[2 * a + k], wr.at[s, 2 * a + k], pp=sib))
        out.append(rcopy(vec, VEC.at[s], ws.at[16], wr.at[s, 8], pp=sib))
        return out

    def y_copies():
        out = [rcopy(vec, VEC.at[s], ws.at[17 + k], wr.at[s, 8], pp=oy + k) for k in range(2)]
        for a in range(NA):
            for k in range(2):
                out.append(rcopy(W_IN[a].at[w_half(a, k)], W_BUF[a].at[s, w_half(a, k)], ws.at[8 + 2 * a + k], wr.at[s, 2 * a + k], pp=oy + k))
        return out

    def start_all(copies):
        for cp in copies:
            cp.start()

    @pl.when(s != 1)
    def _():
        start_all(y_copies())
    start_all(sib_copies())

    def arrived(l, a, k):
        rcopy(W_BUF[a].at[l, w_half(a, k)], W_BUF[a].at[l, w_half(a, k)], ws.at[2 * a], wr.at[l, 2 * a + k], pp=sib).wait_recv()

    def fwd_copy(l, a):
        part = W_BUF[a].at[l, w_half(a, c)]
        return rcopy(part, part, wf.at[l % 2, a], wr.at[l, 2 * a + c], pp=sib)

    def fetch(l):
        @pl.when(l == s)
        def _():
            for a in range(NA):
                lcopy(W_IN[a], W_BUF[a].at[s], wl.at[a]).wait()
            lcopy(vec, VEC.at[s], wl.at[4]).wait()

        @pl.when(l != s)
        def _():
            @pl.when(l // 2 == ys_)
            def _():
                for a in range(NA):
                    for k in range(2):
                        arrived(l, a, k)

            @pl.when(l // 2 != ys_)
            def _():
                for a in range(NA):
                    arrived(l, a, c)
                    fwd_copy(l, a).start()
                for a in range(NA):
                    arrived(l, a, 1 - c)
            rcopy(VEC.at[l], VEC.at[l], ws.at[16], wr.at[l, 8], pp=sib).wait_recv()

    tcopy.wait()
    for i in range(NC):
        cb, sb = TAB[0, :C, :], TAB[1, :C, :]
        cr, sr = TAB[0, C + i:C + i + 1, :], TAB[1, C + i:C + i + 1, :]
        COS[i * C:(i + 1) * C, :] = cb * cr - sb * sr
        SIN[i * C:(i + 1) * C, :] = sb * cr + cb * sr

    lane = lax.broadcasted_iota(jnp.int32, (C, E2), 1)
    head_lane = lane // E
    in_head = lane % E
    rot_half = E // 8
    low = in_head < rot_half
    sub_head = lax.broadcasted_iota(jnp.int32, (E2, C), 0) // E
    lower = lax.broadcasted_iota(jnp.int32, (C, C), 0) <= lax.broadcasted_iota(jnp.int32, (C, C), 1)
    c1 = E ** -0.5 * LOG2E

    def tabs(i):
        cs, sn = COS[i * C:(i + 1) * C, :], SIN[i * C:(i + 1) * C, :]
        return cs, jnp.where(low, -sn, 0.0), jnp.where(low, 0.0, sn)

    def rotate(v, t):
        cs, sa, sb = t
        return v * cs + pltpu.roll(v, E2 - rot_half, 1) * sa + pltpu.roll(v, rot_half, 1) * sb

    def unrotate(v, t):
        cs, sa, sb = t
        return v * cs + pltpu.roll(v * sa, rot_half, 1) + pltpu.roll(v * sb, E2 - rot_half, 1)

    def end_copy(p, t):
        return rcopy(PS.at[t * SR:(t + 1) * SR], RA.at[p % 2, t * SR:(t + 1) * SR], sab.at[t], ra_s.at[p % 2, t], tp=hub)

    def peer_copy(p, t):
        return rcopy(PS.at[t * SR:(t + 1) * SR], RB.at[p % 2, t * SR:(t + 1) * SR], sab.at[t], rb_s.at[p % 2, t], tp=peer)

    def back_copy(p, di, t):
        return rcopy(H.at[di, t * SR:(t + 1) * SR], H.at[di, t * SR:(t + 1) * SR], sc.at[t], rc_s.at[p % 2, t], tp=leaf)

    def pf_row(i, back):
        return (NC if back and i == NC - 1 else i) * C

    def ar_send(p, i, back=False):
        @pl.when(is_end)
        def _():
            for t in range(i * SUB, (i + 1) * SUB):
                @pl.when(p > 0)
                def _():
                    end_copy(p, t).wait_send()
                f0 = pf_row(i, back) + (t - i * SUB) * SR
                PS[t * SR:(t + 1) * SR, :] = PF[f0:f0 + SR, :].astype(BF16)
                end_copy(p, t).start()

    def ar_mid(p, i, u, back=False):
        t = i * SUB + u
        r = slice(t * SR, (t + 1) * SR)
        f0 = pf_row(i, back) + u * SR

        @pl.when(inner)
        def _():
            end_copy(p, t).wait_recv()
            @pl.when(p > 0)
            def _():
                peer_copy(p, t).wait_send()
            PS[r, :] = (PF[f0:f0 + SR, :] + RA[p % 2, r, :].astype(F32)).astype(BF16)
            peer_copy(p, t).start()

    def ar_last(p, ri, di, i, u):
        t = i * SUB + u
        r = slice(t * SR, (t + 1) * SR)

        @pl.when(inner)
        def _():
            lv = jnp.minimum(p, NL - 1)
            bias = (VEC[lv, 4:5, :] + VEC[lv, 5:6, :]) * jnp.where(p < NL, 1.0, 0.0)
            peer_copy(p, t).wait_recv()
            @pl.when(p > 0)
            def _():
                back_copy(p, di, t).wait_send()
            both = PS[r, :].astype(F32) + RB[p % 2, r, :].astype(F32)
            H[di, r, :] = (H[ri, r, :].astype(F32) + both + bias).astype(BF16)
            back_copy(p, di, t).start()

    def ar_wait(p, di, i):
        @pl.when(is_end)
        def _():
            for t in range(i * SUB, (i + 1) * SUB):
                back_copy(p, di, t).wait_recv()

    def stats(hf):
        cen = hf - jnp.mean(hf, axis=-1, keepdims=True)
        rstd = lax.rsqrt(jnp.mean(cen * cen, axis=-1, keepdims=True) + LN_EPS)
        return cen * rstd, rstd

    LB = 64
    GR = 32

    def norms(l, i):
        g1, b1, g2, b2 = (VEC[l, k:k + 1, :] for k in range(NA))

        def step(b, carry):
            hf = H[l, rows(i * C + b * LB, LB), :].astype(F32)
            xhat, unused = stats(hf)
            AS[rows(b * LB, LB), :] = (xhat * g1 + b1).astype(BF16)
            MS[rows(b * LB, LB), :] = (xhat * g2 + b2).astype(BF16)
            return carry
        lax.fori_loop(0, C // LB, step, 0)

    def forward(l, i):
        r0, r1 = i * C, (i + 1) * C
        norms(l, i)
        qkv = nn(AS[...], WQ[l]) + VEC[l, 7:8, :3 * E2]
        qkv = qkv.astype(BF16).astype(F32)
        t = tabs(i)
        q = rotate(qkv[:, :E2], t).astype(BF16)
        kf = rotate(qkv[:, E2:2 * E2], t)
        vf = qkv[:, 2 * E2:3 * E2]
        Q[l, r0:r1, :] = q
        K[l, r0:r1, :] = kf.astype(BF16)
        V[l, r0:r1, :] = vf.astype(BF16)
        KT[l, :, r0:r1] = jnp.transpose(kf).astype(BF16)
        VT[:, r0:r1] = jnp.transpose(vf).astype(BF16)
        yield
        RBK = C // 2
        outs = []
        for h in range(2):
            qm = jnp.where(head_lane == h, Q[l, r0:r1, :].astype(F32), 0.0).astype(BF16)
            ST[:r1, :] = nt(K[l, :r1, :], qm)
            ST[r0:r1, :] = jnp.where(lower, ST[r0:r1, :], -1e30)

            def top(b, m):
                return jnp.maximum(m, jnp.max(ST[rows(b * RBK, RBK), :].reshape(RBK // 8, 8, C), axis=0))
            m = jnp.max(lax.fori_loop(0, r1 // RBK, top, jnp.full((8, C), -3e38, F32)), axis=0, keepdims=True)
            mc = m * c1

            def expo(b, tot):
                e = jnp.exp2(ST[rows(b * RBK, RBK), :] * c1 - mc)
                ST[rows(b * RBK, RBK), :] = e
                return tot + jnp.sum(e.reshape(RBK // 8, 8, C), axis=0)
            tot = jnp.sum(lax.fori_loop(0, r1 // RBK, expo, jnp.zeros((8, C), F32)), axis=0, keepdims=True)
            inv = 1.0 / tot

            def put(b, carry):
                PX[i][l, h, rows(b * RBK, RBK), :] = (ST[rows(b * RBK, RBK), :] * inv).astype(BF16)
                return carry
            lax.fori_loop(0, r1 // RBK, put, 0)
            outs.append(nn(VT[:, :r1], PX[i][l, h]))
            if h == 0:
                yield
        ctx = jnp.transpose(jnp.where(sub_head == 0, outs[0], outs[1])).astype(BF16)
        CTX[l, r0:r1, :] = ctx
        yield
        PF[r0:r1, :] = nn(ctx, WO[l])
        PRE[...] = nn(MS[...], WU[l])
        bup = VEC[l, 6:7, :]
        GB = 32

        def act(b, carry):
            u = PRE[rows(b * GB, GB), :] + bup
            cdf = 0.5 * (1.0 + lax.erf(u * RSQRT2))
            pdf = jnp.exp2(u * u * (-0.5 * LOG2E)) * INV_SQRT_2PI
            HID[l, rows(r0 + b * GB, GB), :] = (u * cdf).astype(BF16)
            GP[l, rows(r0 + b * GB, GB), :] = cdf + u * pdf
            return carry
        lax.fori_loop(0, C // GB, act, 0)
        PF[r0:r1, :] += nn(HID[l, r0:r1, :], WD[l])
        yield

    def backward(l, dl, i, last):
        r0, r1 = i * C, (i + 1) * C
        par = l % 2
        first = i == NC - 1

        def acc(ref, val):
            if first:
                ref[par] = val
            else:
                ref[par] += val

        def acc_row(k, val, w=D):
            GV[l, k:k + 1, :w] += val

        norms(l, i)
        dy = H[dl, r0:r1, :]
        acc_row(4, jnp.sum(dy.astype(F32), axis=0, keepdims=True))
        PRE[...] = nt(dy, WD[l])
        GB = 32

        def act(b, tot):
            d = PRE[rows(b * GB, GB), :] * GP[l, rows(r0 + b * GB, GB), :]
            DPB[rows(b * GB, GB), :] = d.astype(BF16)
            return tot + jnp.sum(d.reshape(GB // 8, 8, F), axis=0)
        dbu = lax.fori_loop(0, C // GB, act, jnp.zeros((8, F), F32))
        acc_row(5, jnp.sum(dbu, axis=0, keepdims=True))
        acc(GD, tn(HID[l, r0:r1, :], dy))
        yield
        acc(GU, tn(MS[...], DPB[...]))
        f0 = pf_row(i, True)
        PF[f0:f0 + C, :] = nt(DPB[...], WU[l])
        yield
        dctx = nt(dy, WO[l]).astype(BF16)
        ctx = CTX[l, r0:r1, :]
        acc(GO, tn(ctx, dy))
        prod = dctx.astype(F32) * ctx.astype(F32)
        q = Q[l, r0:r1, :].astype(F32)
        dcf = dctx.astype(F32)
        RBK = C // 2
        dqt = []
        for h in range(2):
            sel = head_lane == h
            qm = jnp.where(sel, q, 0.0).astype(BF16)
            dcm = jnp.where(sel, dcf, 0.0).astype(BF16)
            dsum = jnp.transpose(jnp.where(sel, prod, 0.0))
            drow = jnp.sum(dsum, axis=0, keepdims=True)
            ST[:r1, :] = nt(V[l, :r1, :], dcm)

            def sub(b, carry):
                pr = PX[i][l, h, rows(b * RBK, RBK), :].astype(F32)
                DS[rows(b * RBK, RBK), :] = (pr * (ST[rows(b * RBK, RBK), :] - drow)).astype(BF16)
                return carry
            lax.fori_loop(0, r1 // RBK, sub, 0)
            dk = nn(DS[:r1, :], qm)
            dv = nn(PX[i][l, h], dcm)
            if first and h == 0:
                DK[:r1, :] = dk
                DV[:r1, :] = dv
            else:
                DK[:r1, :] += dk
                DV[:r1, :] += dv
            dqt.append(nn(KT[l, :, :r1], DS[:r1, :]))
            yield
        scale = E ** -0.5
        t = tabs(i)
        dq = unrotate(jnp.transpose(jnp.where(sub_head == 0, dqt[0], dqt[1])) * scale, t)
        dk = unrotate(DK[r0:r1, :] * scale, t)
        dv = DV[r0:r1, :]
        dqkv = jnp.concatenate([dq, dk, dv], axis=1)
        acc_row(6, jnp.sum(dqkv, axis=0, keepdims=True), 3 * E2)
        dqkv = dqkv.astype(BF16)
        acc(GQ, tn(AS[...], dqkv))
        PRE[...] = nt(dqkv, WQ[l])
        yield
        g1, g2 = VEC[l, 0:1, :], VEC[l, 2:3, :]

        def lnb(b, tots):
            hf = H[l, rows(r0 + b * LB, LB), :].astype(F32)
            xhat, rstd = stats(hf)
            da = PRE[rows(b * LB, LB), :]
            dm = PF[rows(f0 + b * LB, LB), :]
            dx = da * g1 + dm * g2
            m1 = jnp.mean(dx, axis=-1, keepdims=True)
            m2 = jnp.mean(dx * xhat, axis=-1, keepdims=True)
            if not last:
                PF[rows(f0 + b * LB, LB), :] = rstd * (dx - m1 - xhat * m2)
            terms = (da * xhat, da, dm * xhat, dm)
            return tuple(a + jnp.sum(v.reshape(LB // 8, 8, D), axis=0) for a, v in zip(tots, terms))
        tots = lax.fori_loop(0, C // LB, lnb, tuple(jnp.zeros((8, D), F32) for _ in range(NA)))
        for k in range(NA):
            acc_row(k, jnp.sum(tots[k], axis=0, keepdims=True))
        yield

    def g_half(a, k):
        return rows(k * G_HALF[a], G_HALF[a])

    def r1_view(l, a):
        return GP.at[l + 1, R1_OFF[a]:R1_OFF[a] + G_HALF[a], :G_COLS[a]]

    def g1_copy(l, a):
        return rcopy(G_BUF[a].at[l % 2, g_half(a, 1 - c)], r1_view(l, a), g1s.at[a], g1r.at[l % 2, a], pp=sib)

    def g2_copy(l, a):
        return rcopy(HID.at[l, R1_OFF[a]:R1_OFF[a] + G_HALF[a], :G_COLS[a]], R2[a].at[l % 2], g2s.at[l % 2, a], g2r.at[l % 2, a], pp=2 * (l // 2) + c)

    def g3_local(l, a):
        return lcopy(r1_view(l, a), G_OUT[a].at[g_half(a, c)], g3s.at[l % 2, a])

    def g3_remote(l, a):
        return rcopy(r1_view(l, a), G_OUT[a].at[g_half(a, c)], g3s.at[l % 2, a], g3r.at[a], pp=sib)

    def v1_copies(l):
        return [rcopy(GV.at[l], ZR.at[l, z], v1s.at[l, o - 1], v1r.at[l, z], tp=(z + o) % NT) for o in range(1, NT)]

    def grads_out(l):
        for a in range(NA):
            g1_copy(l, a).start()
        for cp in v1_copies(l):
            cp.start()

    def grads_mid(l):
        for a in range(NA):
            g1_copy(l, a).wait_recv()
            n = G_HALF[a]

            def add(b, carry):
                rr = rows(R1_OFF[a] + b * GR, GR)
                tot = G_BUF[a][l % 2, rows(c * n + b * GR, GR), :] + GP[l + 1, rr, :G_COLS[a]]
                GP[l + 1, rr, :G_COLS[a]] = tot
                HID[l, rr, :G_COLS[a]] = tot.astype(BF16)
                return carry
            lax.fori_loop(0, n // GR, add, 0)

            @pl.when(l // 2 != ys_)
            def _():
                g2_copy(l, a).start()

    def grads_last(l):
        @pl.when(l // 2 == ys_)
        def _():
            for a in range(NA):
                g2_copy(l, a).wait_recv()

                def add(b, carry):
                    rr = rows(R1_OFF[a] + b * GR, GR)
                    GP[l + 1, rr, :G_COLS[a]] += R2[a][l % 2, rows(b * GR, GR), :].astype(F32)
                    return carry
                lax.fori_loop(0, G_HALF[a] // GR, add, 0)

                @pl.when(l == s)
                def _():
                    g3_local(l, a).start()

                @pl.when(l != s)
                def _():
                    g3_remote(l, a).start()

    def grads_sent(l):
        for a in range(NA):
            @pl.when(l // 2 != ys_)
            def _():
                g2_copy(l, a).wait_send()

            @pl.when(l == s)
            def _():
                g3_local(l, a).wait()

            @pl.when((l // 2 == ys_) & (l != s))
            def _():
                g3_remote(l, a).wait_send()

    def v2_copy(l):
        return rcopy(GZ.at[l], PR.at[s], v2s.at[l], v2r.at[s], pp=l)

    def vec_mid(l):
        ZR[l, z] = GV[l]
        for o in range(1, NT):
            q = (z + o) % NT
            rcopy(GV.at[l], ZR.at[l, q], v1s.at[l, o - 1], v1r.at[l, q], tp=q).wait_recv()
        tot = ZR[l, 0] + ZR[l, 1] + ZR[l, 2] + ZR[l, 3]
        row = lax.broadcasted_iota(jnp.int32, (8, D), 0)
        GZ[l] = jnp.where(row < 4, tot, GV[l])

        @pl.when(l == s)
        def _():
            PR[s] = GZ[l]

        @pl.when(l != s)
        def _():
            v2_copy(l).start()

    GV[...] = jnp.zeros_like(GV)
    fetch(0)
    xcopy.wait()

    def run(phases, at, handle):
        for k, unused in enumerate(phases):
            for op, lag, u in at.get(k, ()):
                handle(op, lag, u)

    def fwd_layer(l, carry):
        for i in range(NC):
            @pl.when(l > 0)
            def _():
                ar_wait(l - 1, l, i)

            def handle(op, lag, u):
                m = i - lag

                def go(p, j):
                    if op == 'mid':
                        ar_mid(p, j, u)
                    else:
                        ar_last(p, p, p + 1, j, u)
                if m >= 0:
                    go(l, m)
                else:
                    @pl.when(l > 0)
                    def _():
                        go(l - 1, m + NC)
            run(forward(l, i), FWD_AT, handle)
            ar_send(l, i)
            if i == 1:
                @pl.when(l == 0)
                def _():
                    gcopy.wait()
                    H[NL + 1] = GP[NL].astype(BF16)
            if i == 2:
                @pl.when((l == 0) & (s == 1))
                def _():
                    start_all(y_copies())

        @pl.when(l < NL - 1)
        def _():
            fetch(l + 1)
        return carry
    lax.fori_loop(0, NL, fwd_layer, 0)

    y_local = lcopy(H.at[NL], y.at[ys_, c], ys.at[0])
    y_sib = rcopy(H.at[NL], y.at[ys_, c], ys.at[1], yr.at[s], pp=sib)
    y_far = rcopy(H.at[NL], y.at[ys_, c], ys.at[2], yr.at[s], pp=oy + c)
    y_fwd = rcopy(y.at[1 - ys_, c], y.at[1 - ys_, c], ys.at[3], yr.at[oy + c], pp=sib)

    def y_arrived(q):
        rcopy(H.at[NL], y.at[q // 2, q % 2], ys.at[1], yr.at[q], pp=sib).wait_recv()

    def ri(l):
        return jnp.where(l == NL - 1, NL + 1, l + 1)

    def bwd_layer(lb, carry):
        l = NL - 1 - lb
        p = NL + lb
        for n in range(NC):
            i = NC - 1 - n

            @pl.when(lb > 0)
            def _():
                ar_wait(p - 1, l + 1, i)

            def handle(op, lag, u):
                m = n - lag

                def go(q, lq, j):
                    if op == 'mid':
                        ar_mid(q, j, u, True)
                    else:
                        ar_last(q, ri(lq), lq, j, u)
                if m >= 0:
                    @pl.when(l > 0)
                    def _():
                        go(p, l, NC - 1 - m)
                else:
                    @pl.when(lb > 0)
                    def _():
                        go(p - 1, l + 1, -1 - m)

                    @pl.when(lb == 0)
                    def _():
                        if op == 'mid':
                            ar_mid(NL - 1, m + NC, u)
                        else:
                            ar_last(NL - 1, NL - 1, NL, m + NC, u)
            run(backward(l, ri(l), i, False), BWD_AT, handle)

            @pl.when(l > 0)
            def _():
                ar_send(p, i, True)
            if n == 0:
                @pl.when(lb > 0)
                def _():
                    grads_mid(l + 1)

                @pl.when(lb == 2)
                def _():
                    y_arrived(oy + c)
                    y_fwd.start()
            if n == 1:
                @pl.when(lb > 0)
                def _():
                    vec_mid(l + 1)
            if n == 2:
                @pl.when(lb == 0)
                def _():
                    for j in range(NC):
                        ar_wait(NL - 1, NL, j)
                    start_all((y_local, y_sib, y_far))

                @pl.when(lb > 1)
                def _():
                    grads_last(l + 2)

        @pl.when(lb > 0)
        def _():
            for a in range(NA):
                g1_copy(l + 1, a).wait_send()
        grads_out(l)
        return carry
    lax.fori_loop(0, NL, bwd_layer, 0)

    grads_mid(0)
    grads_last(1)
    vec_mid(0)
    grads_last(0)

    for o in range(1, NL):
        q = (s + o) % NL
        rcopy(GZ.at[0], PR.at[q], v2s.at[0], v2r.at[q], pp=q).wait_recv()
    PRE[0:8, 0:D] = PR[0] + PR[1] + PR[2] + PR[3]
    vout = lcopy(PRE.at[0:8, 0:D], ovec, osem.at[0])
    vout.start()
    for l in range(NL):
        for cp in v1_copies(l):
            cp.wait_send()
    for l in range(NL):
        @pl.when(l != s)
        def _():
            v2_copy(l).wait_send()
    for a in range(NA):
        rcopy(G_OUT[a].at[g_half(a, 1 - c)], G_OUT[a].at[g_half(a, 1 - c)], g3s.at[a], g3r.at[a], pp=sib).wait_recv()
    y_local.wait()
    for cp in (y_sib, y_far, y_fwd):
        cp.wait_send()
    y_arrived(sib)
    y_arrived(oy + 1 - c)
    for a in range(NA):
        g1_copy(0, a).wait_send()
    for l in range(NL):
        grads_sent(l)
    for cp in sib_copies():
        cp.wait_send()
    for cp in y_copies():
        cp.wait_send()
    for k in range(2):
        for a in range(NA):
            fwd_copy(oy + k, a).wait_send()

    @pl.when(is_end)
    def _():
        for t in range(NC * SUB):
            end_copy(0, t).wait_send()

    @pl.when(inner)
    def _():
        for t in range(NC * SUB):
            peer_copy(0, t).wait_send()
            back_copy(0, 1, t).wait_send()
    vout.wait()


def group_step(dims, x, g, wqkv, wo, wup, wdn, vec, tab):
    S, D, E, C, F = dims
    E2 = 2 * E
    hbm = pl.BlockSpec(memory_space=pl.ANY)
    out_shape = [
        jax.ShapeDtypeStruct(x.shape, BF16),
        jax.ShapeDtypeStruct((D, 3 * E2), F32),
        jax.ShapeDtypeStruct((E2, D), F32),
        jax.ShapeDtypeStruct((D, F), F32),
        jax.ShapeDtypeStruct((F, D), F32),
        jax.ShapeDtypeStruct((8, D), F32),
    ]

    def vm(*shape, dtype=BF16):
        return pltpu.VMEM(shape, dtype)
    dma = pltpu.SemaphoreType.DMA
    scratch = [
        vm(NL, D, 3 * E2), vm(NL, E2, D), vm(NL, D, F), vm(NL, F, D), vm(NL, 8, D, dtype=F32),
        vm(NL + 2, S, D),
        vm(NL, S, E2), vm(NL, S, E2), vm(NL, S, E2), vm(NL, E2, S), vm(E2, S), vm(NL, S, E2),
        *[vm(NL, 2, (i + 1) * C, C) for i in range(NC)],
        vm(NL, S, F), vm(NL + 1, S, F, dtype=F32),
        vm(2, S, D), vm(2, S, D), vm(S, D), vm(S + C, D, dtype=F32),
        vm(2, D, 3 * E2, dtype=F32), vm(2, E2, D, dtype=F32), vm(2, D, F, dtype=F32), vm(2, F, D, dtype=F32),
        vm(2, D // 2, 3 * E2), vm(2, E, D), vm(2, D // 2, F), vm(2, F // 2, D),
        vm(S, E2, dtype=F32), vm(S, E2, dtype=F32),
        vm(2, C + 8, E2, dtype=F32), vm(S, E2, dtype=F32), vm(S, E2, dtype=F32),
        vm(NL, 8, D, dtype=F32), vm(NL, NT, 8, D, dtype=F32), vm(NL, 8, D, dtype=F32), vm(NL, 8, D, dtype=F32),
        vm(C, D), vm(C, D), vm(C, max(D, F), dtype=F32), vm(C, F), vm(S, C), vm(S, C, dtype=F32),
        dma((5,)), dma((19,)), dma((NL, 9)), dma((2, 4)), dma((2,)), dma((1,)),
        dma((NC * SUB,)), dma((NC * SUB,)), dma((2, NC * SUB)), dma((2, NC * SUB)), dma((2, NC * SUB)),
        dma((NL,)), dma((NL,)), dma((4,)), dma((2, 4)), dma((2, 4)), dma((2, 4)), dma((2, 4)), dma((4,)),
        dma((NL, NT - 1)), dma((NL, NT)), dma((NL,)), dma((NL,)), dma((1,)),
    ]
    return pl.pallas_call(
        functools.partial(body, dims),
        out_shape=out_shape,
        in_specs=[hbm] * 8,
        out_specs=[hbm] * 6,
        scratch_shapes=scratch,
        compiler_params=pltpu.CompilerParams(collective_id=0, has_side_effects=True, vmem_limit_bytes=67043328),
        name='neox_group',
    )(x, g, wqkv, wo, wup, wdn, vec, tab)


def solution(mesh):
    def device_fn(x_in, g_out, ln1_gain, ln1_bias, w_qkv, b_qkv, w_out, b_out, ln2_gain, ln2_bias, w_up, b_up, w_down, b_down):
        n_micro, n_rows, S, D = x_in.shape
        heads, E = w_qkv.shape[2], w_qkv.shape[4]
        F = w_up.shape[2]
        C = S // NC
        qcols = heads * 3 * E
        wqkv = jnp.transpose(w_qkv[0], (0, 2, 1, 3)).reshape(D, qcols)
        bqkv = jnp.transpose(b_qkv[0], (1, 0, 2)).reshape(1, qcols).astype(F32)
        bqkv = jnp.pad(bqkv, ((0, 0), (0, D - qcols)))
        vec = jnp.concatenate([ln1_gain, ln1_bias, ln2_gain, ln2_bias, b_out.astype(F32), b_down.astype(F32), b_up.astype(F32), bqkv], axis=0)
        tab = jnp.asarray(rotary_base(C, NC, E, heads))
        y, gqkv, go, gup, gdn, gvec = group_step((S, D, E, C, F), x_in, g_out, wqkv, w_out[0].reshape(heads * E, D), w_up[0], w_down[0], vec, tab)
        gq = jnp.transpose(gqkv.reshape(D, 3, heads, E), (0, 2, 1, 3))[None]
        gbq = jnp.transpose(gvec[6, :qcols].reshape(3, heads, E), (1, 0, 2))[None]
        bias_out = gvec[4:5]
        return (y, gvec[0:1], gvec[1:2], gq, gbq, go.reshape(1, heads, E, D), bias_out, gvec[2:3], gvec[3:4], gup[None], gvec[5:6], gdn[None], bias_out)

    return jax.shard_map(device_fn, mesh=mesh, in_specs=(P('dp'), P('dp')) + STAGE_SPECS, out_specs=(P('dp'),) + GRAD_SPECS, check_vma=False)
```

```python
import functools
import math

import jax
import jax.numpy as jnp
import numpy as np
from jax import lax
from jax.experimental import pallas as pl
from jax.experimental.pallas import tpu as pltpu
from jax.sharding import PartitionSpec as P

ROPE_BASE = 10000.0
LN_EPS = 1e-5
STAGE_SPECS = (P('pp'), P('pp'), P('pp', None, 'tp'), P('pp', 'tp'), P('pp', 'tp'), P('pp'), P('pp'), P('pp'), P('pp', None, 'tp'), P('pp', 'tp'), P('pp', 'tp'), P('pp'))
OWN = ('dp', 'pp')
GRAD_SPECS = (P(OWN), P(OWN), P(OWN, None, 'tp'), P(OWN, 'tp'), P(OWN, 'tp'), P(OWN), P(OWN), P(OWN), P(OWN, None, 'tp'), P(OWN, 'tp'), P(OWN, 'tp'), P(OWN))


F32 = jnp.float32
BF16 = jnp.bfloat16
NL = 4
NT = 4
NC = 4
NA = 4
SUB = 2
FWD_AT = {0: (('mid', 1, 0), ('last', 2, 0)), 2: (('mid', 1, 1), ('last', 2, 1))}
BWD_AT = {0: (('last', 2, 0),), 1: (('mid', 1, 0),), 3: (('last', 2, 1),), 4: (('mid', 1, 1),)}
LOG2E = 1.4426950408889634
RSQRT2 = 0.7071067811865476
INV_SQRT_2PI = 0.3989422804014327


def nn(a, b):
    return lax.dot_general(a, b, (((1,), (0,)), ((), ())), preferred_element_type=F32)


def nt(a, b):
    return lax.dot_general(a, b, (((1,), (1,)), ((), ())), preferred_element_type=F32)


def tn(a, b):
    return lax.dot_general(a, b, (((0,), (0,)), ((), ())), preferred_element_type=F32)


def col_sum(v):
    return jnp.sum(v, axis=0, keepdims=True)


def row_mean(v):
    return jnp.mean(v, axis=-1, keepdims=True)


def fold(v):
    return jnp.sum(v.reshape(v.shape[0] // 8, 8, v.shape[1]), axis=0)


def rotary_base(chunk, n_chunks, head_dim, n_heads):
    rot_dim = head_dim // 4
    half = rot_dim // 2
    inv_freq = np.zeros((head_dim,), np.float64)
    inv_freq[:rot_dim] = np.tile(ROPE_BASE ** (-(np.arange(half) * 2.0) / rot_dim), 2)
    inv_freq = np.tile(inv_freq, n_heads)
    pos = np.concatenate([np.arange(chunk), np.arange(8) * (np.arange(8) < n_chunks) * chunk]).astype(np.float64)
    ang = pos[:, None] * inv_freq[None, :]
    return np.stack([np.cos(ang), np.sin(ang)]).astype(np.float32)


def body(dims, x, g, wqkv, wo, wup, wdn, n0, n1, n2, n3, n4, n5, n6, bq, tab,
         y, oqkv, oo, oup, odn, ovec,
         WQ, WO, WU, WD, VEC, H, Q, K, V, KT, VT, CTX, P0, P1, P2, P3, HID, GP, RA, RB, PS, PF,
         GQ, GO, GU, GD, R2Q, R2O, R2U, R2D, DK, DV, TAB, COS, SIN, GV, ZR, GZ, PR,
         AS, MS, PRE, DPB, DS, ST, N0, N1, N2, N3, N4, N5, N6, BQ,
         wl, ws, wr, wf, xs, gs, sab, sc, ra_s, rb_s, rc_s, ys, yr, g1s, g1r, g2s, g2r, g3s, g3r, v1s, v1r, v2s, v2r, osem, ns):
    S, D, E, C, F = dims
    E2 = 2 * E
    SR = C // SUB
    z = lax.axis_index('tp')
    s = lax.axis_index('pp')
    ys_ = s // 2
    c = s % 2
    sib = s + 1 - 2 * c
    oy = 2 * (1 - ys_)
    is_end = z * (NT - 1 - z) == 0
    inner = z * (NT - 1 - z) > 0
    hub = 1 + z // 3
    leaf = jnp.where(z == 1, 0, 3)
    peer = 3 - z
    PX = (P0, P1, P2, P3)
    W_IN = (wqkv, wo, wup, wdn)
    W_BUF = (WQ, WO, WU, WD)
    W_HALF = (3 * E, E, D // 2, F // 2)
    G_BUF = (GQ, GO, GU, GD)
    G_OUT = (oqkv, oo, oup, odn)
    G_HALF = W_HALF
    G_COLS = (D, D, F, D)
    R1_OFF = (0, 3 * E, 4 * E, 4 * E + D // 2)
    R2 = (R2Q, R2O, R2U, R2D)

    def rcopy(src, dst, ss, rs, **dev):
        return pltpu.make_async_remote_copy(src_ref=src, dst_ref=dst, send_sem=ss, recv_sem=rs, device_id=dev, device_id_type=pl.DeviceIdType.MESH)

    def lcopy(src, dst, sem):
        return pltpu.make_async_copy(src, dst, sem)

    def rows(start, n):
        return pl.ds(pl.multiple_of(start, n), n)

    xcopy = lcopy(x.at[ys_, c], H.at[0], xs.at[0])
    xcopy.start()
    gcopy = lcopy(g.at[ys_, c], GP.at[NL], gs.at[0])
    gcopy.start()
    tcopy = lcopy(tab, TAB, xs.at[1])
    tcopy.start()
    for a in range(NA):
        lcopy(W_IN[a], W_BUF[a].at[s], wl.at[a]).start()
    small = [lcopy(a, b, ns.at[k]) for k, (a, b) in enumerate(((n0, N0), (n1, N1), (n2, N2), (n3, N3), (n4, N4), (n5, N5), (n6, N6), (bq, BQ)))]
    for cp in small:
        cp.start()

    bar = pltpu.get_barrier_semaphore()
    for o in range(1, NT):
        pl.semaphore_signal(bar, inc=1, device_id={'tp': (z + o) % NT}, device_id_type=pl.DeviceIdType.MESH)
    for o in range(1, NL):
        pl.semaphore_signal(bar, inc=1, device_id={'pp': (s + o) % NL}, device_id_type=pl.DeviceIdType.MESH)
    pl.semaphore_wait(bar, NT - 1 + NL - 1)

    def w_half(a, k):
        return rows(k * W_HALF[a], W_HALF[a])

    def sib_copies():
        out = []
        for a in range(NA):
            for k in range(2):
                out.append(rcopy(W_IN[a].at[w_half(a, k)], W_BUF[a].at[s, w_half(a, k)], ws.at[2 * a + k], wr.at[s, 2 * a + k], pp=sib))
        out.append(rcopy(VEC.at[s], VEC.at[s], ws.at[16], wr.at[s, 8], pp=sib))
        return out

    def y_copies():
        out = []
        for a in range(NA):
            for k in range(2):
                out.append(rcopy(W_IN[a].at[w_half(a, k)], W_BUF[a].at[s, w_half(a, k)], ws.at[8 + 2 * a + k], wr.at[s, 2 * a + k], pp=oy + k))
        out += [rcopy(VEC.at[s], VEC.at[s], ws.at[17 + k], wr.at[s, 8], pp=oy + k) for k in range(2)]
        return out

    def start_all(copies):
        for cp in copies:
            cp.start()

    for cp in small:
        cp.wait()
    for k, ref in enumerate((N0, N1, N2, N3, N4, N5, N6)):
        VEC[s, k:k + 1, :] = ref[...].astype(F32)
    VEC[s, 7:8, :3 * E2] = jnp.concatenate([BQ[k, h:h + 1, :].astype(F32) for k in range(3) for h in range(2)], axis=1)

    @pl.when(s != 1)
    def _():
        start_all(y_copies())
    start_all(sib_copies())

    def arrived(l, a, k):
        rcopy(W_BUF[a].at[l, w_half(a, k)], W_BUF[a].at[l, w_half(a, k)], ws.at[2 * a], wr.at[l, 2 * a + k], pp=sib).wait_recv()

    def fwd_copy(l, a):
        part = W_BUF[a].at[l, w_half(a, c)]
        return rcopy(part, part, wf.at[l % 2, a], wr.at[l, 2 * a + c], pp=sib)

    def fetch(l):
        @pl.when(l == s)
        def _():
            for a in range(NA):
                lcopy(W_IN[a], W_BUF[a].at[s], wl.at[a]).wait()

        @pl.when(l != s)
        def _():
            @pl.when(l // 2 == ys_)
            def _():
                for a in range(NA):
                    for k in range(2):
                        arrived(l, a, k)

            @pl.when(l // 2 != ys_)
            def _():
                for a in range(NA):
                    arrived(l, a, c)
                    fwd_copy(l, a).start()
                for a in range(NA):
                    arrived(l, a, 1 - c)
            rcopy(VEC.at[l], VEC.at[l], ws.at[16], wr.at[l, 8], pp=sib).wait_recv()

    tcopy.wait()
    for i in range(NC):
        cb, sb = TAB[0, :C, :], TAB[1, :C, :]
        cr, sr = TAB[0, C + i:C + i + 1, :], TAB[1, C + i:C + i + 1, :]
        COS[i * C:(i + 1) * C, :] = cb * cr - sb * sr
        SIN[i * C:(i + 1) * C, :] = sb * cr + cb * sr

    lane = lax.broadcasted_iota(jnp.int32, (C, E2), 1)
    head_lane = lane // E
    in_head = lane % E
    rot_half = E // 8
    low = in_head < rot_half
    sub_head = lax.broadcasted_iota(jnp.int32, (E2, C), 0) // E
    lower = lax.broadcasted_iota(jnp.int32, (C, C), 0) <= lax.broadcasted_iota(jnp.int32, (C, C), 1)
    c1 = E ** -0.5 * LOG2E

    def tabs(i):
        cs, sn = COS[i * C:(i + 1) * C, :], SIN[i * C:(i + 1) * C, :]
        return cs, jnp.where(low, -sn, 0.0), jnp.where(low, 0.0, sn)

    def rotate(v, t):
        cs, sa, sb = t
        return v * cs + pltpu.roll(v, E2 - rot_half, 1) * sa + pltpu.roll(v, rot_half, 1) * sb

    def unrotate(v, t):
        cs, sa, sb = t
        return v * cs + pltpu.roll(v * sa, rot_half, 1) + pltpu.roll(v * sb, E2 - rot_half, 1)

    def end_copy(p, t):
        return rcopy(PS.at[t * SR:(t + 1) * SR], RA.at[p % 2, t * SR:(t + 1) * SR], sab.at[t], ra_s.at[p % 2, t], tp=hub)

    def peer_copy(p, t):
        return rcopy(PS.at[t * SR:(t + 1) * SR], RB.at[p % 2, t * SR:(t + 1) * SR], sab.at[t], rb_s.at[p % 2, t], tp=peer)

    def back_copy(p, di, t):
        return rcopy(H.at[di, t * SR:(t + 1) * SR], H.at[di, t * SR:(t + 1) * SR], sc.at[t], rc_s.at[p % 2, t], tp=leaf)

    def pf_row(i, back):
        return (NC if back and i == NC - 1 else i) * C

    def ar_send(p, i, back=False):
        @pl.when(is_end)
        def _():
            for t in range(i * SUB, (i + 1) * SUB):
                @pl.when(p > 0)
                def _():
                    end_copy(p, t).wait_send()
                f0 = pf_row(i, back) + (t - i * SUB) * SR
                PS[t * SR:(t + 1) * SR, :] = PF[f0:f0 + SR, :].astype(BF16)
                end_copy(p, t).start()

    def ar_mid(p, i, u, back=False):
        t = i * SUB + u
        r = slice(t * SR, (t + 1) * SR)
        f0 = pf_row(i, back) + u * SR

        @pl.when(inner)
        def _():
            end_copy(p, t).wait_recv()
            @pl.when(p > 0)
            def _():
                peer_copy(p, t).wait_send()
            PS[r, :] = (PF[f0:f0 + SR, :] + RA[p % 2, r, :].astype(F32)).astype(BF16)
            peer_copy(p, t).start()

    def ar_last(p, ri, di, i, u):
        t = i * SUB + u
        r = slice(t * SR, (t + 1) * SR)

        @pl.when(inner)
        def _():
            lv = jnp.minimum(p, NL - 1)
            bias = (VEC[lv, 4:5, :] + VEC[lv, 5:6, :]) * jnp.where(p < NL, 1.0, 0.0)
            peer_copy(p, t).wait_recv()
            @pl.when(p > 0)
            def _():
                back_copy(p, di, t).wait_send()
            both = PS[r, :].astype(F32) + RB[p % 2, r, :].astype(F32)
            H[di, r, :] = (H[ri, r, :].astype(F32) + both + bias).astype(BF16)
            back_copy(p, di, t).start()

    def ar_wait(p, di, i):
        @pl.when(is_end)
        def _():
            for t in range(i * SUB, (i + 1) * SUB):
                back_copy(p, di, t).wait_recv()

    def stats(hf):
        cen = hf - row_mean(hf)
        rstd = lax.rsqrt(row_mean(cen * cen) + LN_EPS)
        return cen * rstd, rstd

    LB = 64
    GR = 32

    def norms(l, i):
        g1, b1, g2, b2 = (VEC[l, k:k + 1, :] for k in range(NA))

        def step(b, carry):
            hf = H[l, rows(i * C + b * LB, LB), :].astype(F32)
            xhat, unused = stats(hf)
            AS[rows(b * LB, LB), :] = (xhat * g1 + b1).astype(BF16)
            MS[rows(b * LB, LB), :] = (xhat * g2 + b2).astype(BF16)
            return carry
        lax.fori_loop(0, C // LB, step, 0)

    def by_kind():
        return [(h * 3 + k) * E for k in range(3) for h in range(2)]

    def wq(l):
        return jnp.concatenate([WQ[l, r:r + E, :] for r in by_kind()], axis=0)

    def forward(l, i):
        r0, r1 = i * C, (i + 1) * C
        norms(l, i)
        qkv = nt(AS[...], wq(l)) + VEC[l, 7:8, :3 * E2]
        qkv = qkv.astype(BF16).astype(F32)
        t = tabs(i)
        q = rotate(qkv[:, :E2], t).astype(BF16)
        kf = rotate(qkv[:, E2:2 * E2], t)
        vf = qkv[:, 2 * E2:3 * E2]
        Q[l, r0:r1, :] = q
        K[l, r0:r1, :] = kf.astype(BF16)
        V[l, r0:r1, :] = vf.astype(BF16)
        KT[l, :, r0:r1] = jnp.transpose(kf).astype(BF16)
        VT[:, r0:r1] = jnp.transpose(vf).astype(BF16)
        yield
        RBK = C // 2
        outs = []
        for h in range(2):
            qm = jnp.where(head_lane == h, Q[l, r0:r1, :].astype(F32), 0.0).astype(BF16)
            ST[:r1, :] = nt(K[l, :r1, :], qm)
            ST[r0:r1, :] = jnp.where(lower, ST[r0:r1, :], -1e30)

            def top(b, m):
                return jnp.maximum(m, jnp.max(ST[rows(b * RBK, RBK), :].reshape(RBK // 8, 8, C), axis=0))
            m = jnp.max(lax.fori_loop(0, r1 // RBK, top, jnp.full((8, C), -3e38, F32)), axis=0, keepdims=True)
            mc = m * c1

            def expo(b, tot):
                e = jnp.exp2(ST[rows(b * RBK, RBK), :] * c1 - mc)
                ST[rows(b * RBK, RBK), :] = e
                return tot + fold(e)
            tot = col_sum(lax.fori_loop(0, r1 // RBK, expo, jnp.zeros((8, C), F32)))
            inv = 1.0 / tot

            def put(b, carry):
                PX[i][l, h, rows(b * RBK, RBK), :] = (ST[rows(b * RBK, RBK), :] * inv).astype(BF16)
                return carry
            lax.fori_loop(0, r1 // RBK, put, 0)
            outs.append(nn(VT[:, :r1], PX[i][l, h]))
            if h == 0:
                yield
        ctx = jnp.transpose(jnp.where(sub_head == 0, outs[0], outs[1])).astype(BF16)
        CTX[l, r0:r1, :] = ctx
        yield
        PF[r0:r1, :] = nn(ctx, WO[l])
        PRE[...] = nn(MS[...], WU[l])
        bup = VEC[l, 6:7, :]
        GB = 32

        def act(b, carry):
            u = PRE[rows(b * GB, GB), :] + bup
            cdf = 0.5 * (1.0 + lax.erf(u * RSQRT2))
            pdf = jnp.exp2(u * u * (-0.5 * LOG2E)) * INV_SQRT_2PI
            HID[l, rows(r0 + b * GB, GB), :] = (u * cdf).astype(BF16)
            GP[l, rows(r0 + b * GB, GB), :] = cdf + u * pdf
            return carry
        lax.fori_loop(0, C // GB, act, 0)
        PF[r0:r1, :] += nn(HID[l, r0:r1, :], WD[l])
        yield

    def backward(l, dl, i, last):
        r0, r1 = i * C, (i + 1) * C
        par = l % 2
        first = i == NC - 1

        def acc(ref, val):
            if first:
                ref[par] = val
            else:
                ref[par] += val

        def acc_row(k, val, w=D):
            GV[l, k:k + 1, :w] += val

        norms(l, i)
        dy = H[dl, r0:r1, :]
        acc_row(4, col_sum(dy.astype(F32)))
        PRE[...] = nt(dy, WD[l])
        GB = 32

        def act(b, tot):
            d = PRE[rows(b * GB, GB), :] * GP[l, rows(r0 + b * GB, GB), :]
            DPB[rows(b * GB, GB), :] = d.astype(BF16)
            return tot + fold(d)
        dbu = lax.fori_loop(0, C // GB, act, jnp.zeros((8, F), F32))
        acc_row(5, col_sum(dbu))
        acc(GD, tn(HID[l, r0:r1, :], dy))
        yield
        acc(GU, tn(MS[...], DPB[...]))
        f0 = pf_row(i, True)
        PF[f0:f0 + C, :] = nt(DPB[...], WU[l])
        yield
        dctx = nt(dy, WO[l]).astype(BF16)
        ctx = CTX[l, r0:r1, :]
        acc(GO, tn(ctx, dy))
        prod = dctx.astype(F32) * ctx.astype(F32)
        q = Q[l, r0:r1, :].astype(F32)
        dcf = dctx.astype(F32)
        RBK = C // 2
        dqt = []
        for h in range(2):
            sel = head_lane == h
            qm = jnp.where(sel, q, 0.0).astype(BF16)
            dcm = jnp.where(sel, dcf, 0.0).astype(BF16)
            dsum = jnp.transpose(jnp.where(sel, prod, 0.0))
            drow = col_sum(dsum)
            ST[:r1, :] = nt(V[l, :r1, :], dcm)

            def sub(b, carry):
                pr = PX[i][l, h, rows(b * RBK, RBK), :].astype(F32)
                DS[rows(b * RBK, RBK), :] = (pr * (ST[rows(b * RBK, RBK), :] - drow)).astype(BF16)
                return carry
            lax.fori_loop(0, r1 // RBK, sub, 0)
            dk = nn(DS[:r1, :], qm)
            dv = nn(PX[i][l, h], dcm)
            if first and h == 0:
                DK[:r1, :] = dk
                DV[:r1, :] = dv
            else:
                DK[:r1, :] += dk
                DV[:r1, :] += dv
            dqt.append(nn(KT[l, :, :r1], DS[:r1, :]))
            yield
        scale = E ** -0.5
        t = tabs(i)
        dq = unrotate(jnp.transpose(jnp.where(sub_head == 0, dqt[0], dqt[1])) * scale, t)
        dk = unrotate(DK[r0:r1, :] * scale, t)
        dv = DV[r0:r1, :]
        dqkv = jnp.concatenate([dq, dk, dv], axis=1)
        acc_row(6, col_sum(dqkv), 3 * E2)
        dqkv = dqkv.astype(BF16)
        dwq = tn(dqkv, AS[...])
        for k, r in enumerate(by_kind()):
            if first:
                GQ[par, r:r + E, :] = dwq[k * E:(k + 1) * E]
            else:
                GQ[par, r:r + E, :] += dwq[k * E:(k + 1) * E]
        PRE[...] = nn(dqkv, wq(l))
        yield
        g1, g2 = VEC[l, 0:1, :], VEC[l, 2:3, :]

        def lnb(b, tots):
            hf = H[l, rows(r0 + b * LB, LB), :].astype(F32)
            xhat, rstd = stats(hf)
            da = PRE[rows(b * LB, LB), :]
            dm = PF[rows(f0 + b * LB, LB), :]
            dx = da * g1 + dm * g2
            m1 = row_mean(dx)
            m2 = row_mean(dx * xhat)
            if not last:
                PF[rows(f0 + b * LB, LB), :] = rstd * (dx - m1 - xhat * m2)
            terms = (da * xhat, da, dm * xhat, dm)
            return tuple(a + fold(v) for a, v in zip(tots, terms))
        tots = lax.fori_loop(0, C // LB, lnb, tuple(jnp.zeros((8, D), F32) for _ in range(NA)))
        for k in range(NA):
            acc_row(k, col_sum(tots[k]))
        yield

    def g_half(a, k):
        return rows(k * G_HALF[a], G_HALF[a])

    def r1_view(l, a):
        return GP.at[l + 1, R1_OFF[a]:R1_OFF[a] + G_HALF[a], :G_COLS[a]]

    def g1_copy(l, a):
        return rcopy(G_BUF[a].at[l % 2, g_half(a, 1 - c)], r1_view(l, a), g1s.at[a], g1r.at[l % 2, a], pp=sib)

    def g2_copy(l, a):
        return rcopy(HID.at[l, R1_OFF[a]:R1_OFF[a] + G_HALF[a], :G_COLS[a]], R2[a].at[l % 2], g2s.at[l % 2, a], g2r.at[l % 2, a], pp=2 * (l // 2) + c)

    def g3_local(l, a):
        return lcopy(r1_view(l, a), G_OUT[a].at[g_half(a, c)], g3s.at[l % 2, a])

    def g3_remote(l, a):
        return rcopy(r1_view(l, a), G_OUT[a].at[g_half(a, c)], g3s.at[l % 2, a], g3r.at[a], pp=sib)

    def v1_copies(l):
        return [rcopy(GV.at[l], ZR.at[l, z], v1s.at[l, o - 1], v1r.at[l, z], tp=(z + o) % NT) for o in range(1, NT)]

    def grads_out(l):
        for a in range(NA):
            g1_copy(l, a).start()
        for cp in v1_copies(l):
            cp.start()

    def grads_mid(l):
        for a in range(NA):
            g1_copy(l, a).wait_recv()
            n = G_HALF[a]

            def add(b, carry):
                rr = rows(R1_OFF[a] + b * GR, GR)
                tot = G_BUF[a][l % 2, rows(c * n + b * GR, GR), :] + GP[l + 1, rr, :G_COLS[a]]
                GP[l + 1, rr, :G_COLS[a]] = tot
                HID[l, rr, :G_COLS[a]] = tot.astype(BF16)
                return carry
            lax.fori_loop(0, n // GR, add, 0)

            @pl.when(l // 2 != ys_)
            def _():
                g2_copy(l, a).start()

    def grads_last(l):
        @pl.when(l // 2 == ys_)
        def _():
            for a in range(NA):
                g2_copy(l, a).wait_recv()

                def add(b, carry):
                    rr = rows(R1_OFF[a] + b * GR, GR)
                    GP[l + 1, rr, :G_COLS[a]] += R2[a][l % 2, rows(b * GR, GR), :].astype(F32)
                    return carry
                lax.fori_loop(0, G_HALF[a] // GR, add, 0)

                @pl.when(l == s)
                def _():
                    g3_local(l, a).start()

                @pl.when(l != s)
                def _():
                    g3_remote(l, a).start()

    def grads_sent(l):
        for a in range(NA):
            @pl.when(l // 2 != ys_)
            def _():
                g2_copy(l, a).wait_send()

            @pl.when(l == s)
            def _():
                g3_local(l, a).wait()

            @pl.when((l // 2 == ys_) & (l != s))
            def _():
                g3_remote(l, a).wait_send()

    def v2_copy(l):
        return rcopy(GZ.at[l], PR.at[s], v2s.at[l], v2r.at[s], pp=l)

    def vec_mid(l):
        ZR[l, z] = GV[l]
        for o in range(1, NT):
            q = (z + o) % NT
            rcopy(GV.at[l], ZR.at[l, q], v1s.at[l, o - 1], v1r.at[l, q], tp=q).wait_recv()
        tot = ZR[l, 0] + ZR[l, 1] + ZR[l, 2] + ZR[l, 3]
        row = lax.broadcasted_iota(jnp.int32, (8, D), 0)
        GZ[l] = jnp.where(row < 4, tot, GV[l])

        @pl.when(l == s)
        def _():
            PR[s] = GZ[l]

        @pl.when(l != s)
        def _():
            v2_copy(l).start()

    GV[...] = jnp.zeros_like(GV)
    fetch(0)
    xcopy.wait()

    def run(phases, at, handle):
        for k, unused in enumerate(phases):
            for op, lag, u in at.get(k, ()):
                handle(op, lag, u)

    def fwd_layer(l, carry):
        for i in range(NC):
            @pl.when(l > 0)
            def _():
                ar_wait(l - 1, l, i)

            def handle(op, lag, u):
                m = i - lag

                def go(p, j):
                    if op == 'mid':
                        ar_mid(p, j, u)
                    else:
                        ar_last(p, p, p + 1, j, u)
                if m >= 0:
                    go(l, m)
                else:
                    @pl.when(l > 0)
                    def _():
                        go(l - 1, m + NC)
            run(forward(l, i), FWD_AT, handle)
            ar_send(l, i)
            if i == 1:
                @pl.when(l == 0)
                def _():
                    gcopy.wait()
                    H[NL + 1] = GP[NL].astype(BF16)
            if i == 2:
                @pl.when((l == 0) & (s == 1))
                def _():
                    start_all(y_copies())

        @pl.when(l < NL - 1)
        def _():
            fetch(l + 1)
        return carry
    lax.fori_loop(0, NL, fwd_layer, 0)

    y_local = lcopy(H.at[NL], y.at[ys_, c], ys.at[0])
    y_sib = rcopy(H.at[NL], y.at[ys_, c], ys.at[1], yr.at[s], pp=sib)
    y_far = rcopy(H.at[NL], y.at[ys_, c], ys.at[2], yr.at[s], pp=oy + c)
    y_fwd = rcopy(y.at[1 - ys_, c], y.at[1 - ys_, c], ys.at[3], yr.at[oy + c], pp=sib)

    def y_arrived(q):
        rcopy(H.at[NL], y.at[q // 2, q % 2], ys.at[1], yr.at[q], pp=sib).wait_recv()

    def ri(l):
        return jnp.where(l == NL - 1, NL + 1, l + 1)

    def bwd_layer(lb, carry):
        l = NL - 1 - lb
        p = NL + lb
        for n in range(NC):
            i = NC - 1 - n

            @pl.when(lb > 0)
            def _():
                ar_wait(p - 1, l + 1, i)

            def handle(op, lag, u):
                m = n - lag

                def go(q, lq, j):
                    if op == 'mid':
                        ar_mid(q, j, u, True)
                    else:
                        ar_last(q, ri(lq), lq, j, u)
                if m >= 0:
                    @pl.when(l > 0)
                    def _():
                        go(p, l, NC - 1 - m)
                else:
                    @pl.when(lb > 0)
                    def _():
                        go(p - 1, l + 1, -1 - m)

                    @pl.when(lb == 0)
                    def _():
                        if op == 'mid':
                            ar_mid(NL - 1, m + NC, u)
                        else:
                            ar_last(NL - 1, NL - 1, NL, m + NC, u)
            run(backward(l, ri(l), i, False), BWD_AT, handle)

            @pl.when(l > 0)
            def _():
                ar_send(p, i, True)
            if n == 0:
                @pl.when(lb > 0)
                def _():
                    grads_mid(l + 1)

                @pl.when(lb == 2)
                def _():
                    y_arrived(oy + c)
                    y_fwd.start()
            if n == 1:
                @pl.when(lb > 0)
                def _():
                    vec_mid(l + 1)
            if n == 2:
                @pl.when(lb == 0)
                def _():
                    for j in range(NC):
                        ar_wait(NL - 1, NL, j)
                    start_all((y_local, y_sib, y_far))

                @pl.when(lb > 1)
                def _():
                    grads_last(l + 2)

        @pl.when(lb > 0)
        def _():
            for a in range(NA):
                g1_copy(l + 1, a).wait_send()
        grads_out(l)
        return carry
    lax.fori_loop(0, NL, bwd_layer, 0)

    grads_mid(0)
    grads_last(1)
    vec_mid(0)
    grads_last(0)

    for o in range(1, NL):
        q = (s + o) % NL
        rcopy(GZ.at[0], PR.at[q], v2s.at[0], v2r.at[q], pp=q).wait_recv()
    PRE[0:8, 0:D] = PR[0] + PR[1] + PR[2] + PR[3]
    vout = lcopy(PRE.at[0:8, 0:D], ovec, osem.at[0])
    vout.start()
    for l in range(NL):
        for cp in v1_copies(l):
            cp.wait_send()
    for l in range(NL):
        @pl.when(l != s)
        def _():
            v2_copy(l).wait_send()
    for a in range(NA):
        rcopy(G_OUT[a].at[g_half(a, 1 - c)], G_OUT[a].at[g_half(a, 1 - c)], g3s.at[a], g3r.at[a], pp=sib).wait_recv()
    y_local.wait()
    for cp in (y_sib, y_far, y_fwd):
        cp.wait_send()
    y_arrived(sib)
    y_arrived(oy + 1 - c)
    for a in range(NA):
        g1_copy(0, a).wait_send()
    for l in range(NL):
        grads_sent(l)
    for cp in sib_copies():
        cp.wait_send()
    for cp in y_copies():
        cp.wait_send()
    for k in range(2):
        for a in range(NA):
            fwd_copy(oy + k, a).wait_send()

    @pl.when(is_end)
    def _():
        for t in range(NC * SUB):
            end_copy(0, t).wait_send()

    @pl.when(inner)
    def _():
        for t in range(NC * SUB):
            peer_copy(0, t).wait_send()
            back_copy(0, 1, t).wait_send()
    vout.wait()


def finish(y, gq, go, gu, gd, gv, *rest):
    outs, small, bufs, got, put = rest[:5], rest[5:13], rest[13:18], rest[18], rest[19]
    loads = [pltpu.make_async_copy(a, b, got.at[k]) for k, (a, b) in enumerate(zip((y, gq, go, gu, gd), bufs))]
    stores = [pltpu.make_async_copy(b, a, put.at[k]) for k, (a, b) in enumerate(zip(outs, bufs))]
    order = loads[1:] + loads[:1]
    for cp in order:
        cp.start()
    for k, ref in enumerate(small[:7]):
        row = k if k < 5 else k - 1
        ref[...] = gv[row:row + 1, :]
    e = small[7].shape[2]
    for k in range(3):
        for h in range(2):
            small[7][k, h:h + 1, :] = gv[6:7, (2 * k + h) * e:(2 * k + h + 1) * e]
    for cp, out in zip(order, stores[1:] + stores[:1]):
        cp.wait()
        out.start()
    for cp in stores:
        cp.wait()


def finish_step(y, gq, go, gu, gd, gv, e):
    hbm, vmem = pl.BlockSpec(memory_space=pl.ANY), pl.BlockSpec(memory_space=pltpu.VMEM)
    big = [jax.ShapeDtypeStruct(a.shape, a.dtype) for a in (y, gq, go, gu, gd)]
    row = jax.ShapeDtypeStruct((1, gv.shape[1]), F32)
    return pl.pallas_call(
        finish,
        out_shape=big + [row] * 7 + [jax.ShapeDtypeStruct((3, 2, e), F32)],
        in_specs=[hbm] * 5 + [vmem],
        out_specs=[hbm] * 5 + [vmem] * 8,
        scratch_shapes=[pltpu.VMEM(a.shape, a.dtype) for a in big] + [pltpu.SemaphoreType.DMA((5,))] * 2,
        name='neox_out',
    )(y, gq, go, gu, gd, gv)


def group_step(dims, *args):
    x = args[0]
    S, D, E, C, F = dims
    E2 = 2 * E
    hbm = pl.BlockSpec(memory_space=pl.ANY)
    out_shape = [
        jax.ShapeDtypeStruct(x.shape, BF16),
        jax.ShapeDtypeStruct((3 * E2, D), F32),
        jax.ShapeDtypeStruct((E2, D), F32),
        jax.ShapeDtypeStruct((D, F), F32),
        jax.ShapeDtypeStruct((F, D), F32),
        jax.ShapeDtypeStruct((8, D), F32),
    ]

    def vm(*shape, dtype=BF16):
        return pltpu.VMEM(shape, dtype)
    dma = pltpu.SemaphoreType.DMA
    scratch = [
        vm(NL, 3 * E2, D), vm(NL, E2, D), vm(NL, D, F), vm(NL, F, D), vm(NL, 8, D, dtype=F32),
        vm(NL + 2, S, D),
        vm(NL, S, E2), vm(NL, S, E2), vm(NL, S, E2), vm(NL, E2, S), vm(E2, S), vm(NL, S, E2),
        *[vm(NL, 2, (i + 1) * C, C) for i in range(NC)],
        vm(NL, S, F), vm(NL + 1, S, F, dtype=F32),
        vm(2, S, D), vm(2, S, D), vm(S, D), vm(S + C, D, dtype=F32),
        vm(2, 3 * E2, D, dtype=F32), vm(2, E2, D, dtype=F32), vm(2, D, F, dtype=F32), vm(2, F, D, dtype=F32),
        vm(2, 3 * E, D), vm(2, E, D), vm(2, D // 2, F), vm(2, F // 2, D),
        vm(S, E2, dtype=F32), vm(S, E2, dtype=F32),
        vm(2, C + 8, E2, dtype=F32), vm(S, E2, dtype=F32), vm(S, E2, dtype=F32),
        vm(NL, 8, D, dtype=F32), vm(NL, NT, 8, D, dtype=F32), vm(NL, 8, D, dtype=F32), vm(NL, 8, D, dtype=F32),
        vm(C, D), vm(C, D), vm(C, max(D, F), dtype=F32), vm(C, F), vm(S, C), vm(S, C, dtype=F32),
        *[vm(1, D, dtype=F32)] * 4, vm(1, D), vm(1, D), vm(1, F), vm(3, 2, E),
        dma((5,)), dma((19,)), dma((NL, 9)), dma((2, NA)), dma((2,)), dma((1,)),
        dma((NC * SUB,)), dma((NC * SUB,)), dma((2, NC * SUB)), dma((2, NC * SUB)), dma((2, NC * SUB)),
        dma((NL,)), dma((NL,)), dma((NA,)), dma((2, NA)), dma((2, NA)), dma((2, NA)), dma((2, NA)), dma((NA,)),
        dma((NL, NT - 1)), dma((NL, NT)), dma((NL,)), dma((NL,)), dma((1,)), dma((8,)),
    ]
    return pl.pallas_call(
        functools.partial(body, dims),
        out_shape=out_shape,
        in_specs=[hbm] * len(args),
        out_specs=[hbm] * 6,
        scratch_shapes=scratch,
        compiler_params=pltpu.CompilerParams(collective_id=0, has_side_effects=True, vmem_limit_bytes=67043328),
        name='neox_group',
    )(*args)


def solution(mesh):
    def device_fn(x_in, g_out, ln1_gain, ln1_bias, w_qkv, b_qkv, w_out, b_out, ln2_gain, ln2_bias, w_up, b_up, w_down, b_down):
        n_micro, n_rows, S, D = x_in.shape
        heads, E = w_qkv.shape[2], w_qkv.shape[4]
        F = w_up.shape[2]
        C = S // NC
        wqkv = jnp.transpose(w_qkv[0], (1, 2, 3, 0)).reshape(heads * 3 * E, D)
        bqkv = jnp.transpose(b_qkv[0], (1, 0, 2))
        tab = jnp.asarray(rotary_base(C, NC, E, heads))
        part = group_step((S, D, E, C, F), x_in, g_out, wqkv, w_out[0].reshape(heads * E, D), w_up[0], w_down[0], ln1_gain, ln1_bias, ln2_gain, ln2_bias, b_out, b_down, b_up, bqkv, tab)
        y, gq, go, gup, gdn, n1g, n1b, n2g, n2b, gbo, gbd, gbu, gbq = finish_step(*part, E)
        gq = jnp.transpose(gq.reshape(heads, 3, E, D), (3, 0, 1, 2))[None]
        gbq = jnp.transpose(gbq, (1, 0, 2))[None]
        return (y, n1g, n1b, gq, gbq, go.reshape(1, heads, E, D), gbo, n2g, n2b, gup[None], gbu, gdn[None], gbd)

    return jax.shard_map(device_fn, mesh=mesh, in_specs=(P('dp'), P('dp')) + STAGE_SPECS, out_specs=(P('dp'),) + GRAD_SPECS, check_vma=False)
```

```python
import functools
import math

import jax
import jax.numpy as jnp
import numpy as np
from jax import lax
from jax.experimental import pallas as pl
from jax.experimental.pallas import tpu as pltpu
from jax.sharding import PartitionSpec as P

ROPE_BASE = 10000.0
LN_EPS = 1e-5
STAGE_SPECS = (P('pp'), P('pp'), P('pp', None, 'tp'), P('pp', 'tp'), P('pp', 'tp'), P('pp'), P('pp'), P('pp'), P('pp', None, 'tp'), P('pp', 'tp'), P('pp', 'tp'), P('pp'))
OWN = ('dp', 'pp')
GRAD_SPECS = (P(OWN), P(OWN), P(OWN, None, 'tp'), P(OWN, 'tp'), P(OWN, 'tp'), P(OWN), P(OWN), P(OWN), P(OWN, None, 'tp'), P(OWN, 'tp'), P(OWN, 'tp'), P(OWN))


F32 = jnp.float32
BF16 = jnp.bfloat16
NL = 4
NT = 4
NC = 4
NA = 4
SUB = 2
FWD_AT = {0: (('mid', 1, 0), ('last', 2, 0)), 2: (('mid', 1, 1), ('last', 2, 1))}
BWD_AT = {0: (('last', 2, 0),), 1: (('mid', 1, 0),), 3: (('last', 2, 1),), 4: (('mid', 1, 1),)}
LOG2E = 1.4426950408889634
RSQRT2 = 0.7071067811865476
INV_SQRT_2PI = 0.3989422804014327


def nn(a, b):
    return lax.dot_general(a, b, (((1,), (0,)), ((), ())), preferred_element_type=F32)


def nt(a, b):
    return lax.dot_general(a, b, (((1,), (1,)), ((), ())), preferred_element_type=F32)


def tn(a, b):
    return lax.dot_general(a, b, (((0,), (0,)), ((), ())), preferred_element_type=F32)


def col_sum(v):
    return jnp.sum(v, axis=0, keepdims=True)


def row_mean(v):
    return jnp.mean(v, axis=-1, keepdims=True)


def fold(v):
    return jnp.sum(v.reshape(v.shape[0] // 8, 8, v.shape[1]), axis=0)


def rotary_base(chunk, n_chunks, head_dim, n_heads):
    rot_dim = head_dim // 4
    half = rot_dim // 2
    inv_freq = np.zeros((head_dim,), np.float64)
    inv_freq[:rot_dim] = np.tile(ROPE_BASE ** (-(np.arange(half) * 2.0) / rot_dim), 2)
    inv_freq = np.tile(inv_freq, n_heads)
    pos = np.concatenate([np.arange(chunk), np.arange(8) * (np.arange(8) < n_chunks) * chunk]).astype(np.float64)
    ang = pos[:, None] * inv_freq[None, :]
    return np.stack([np.cos(ang), np.sin(ang)]).astype(np.float32)


def body(dims, x, g, wqkv, wo, wup, wdn, n0, n1, n2, n3, n4, n5, n6, bq, tab,
         y, oqkv, oo, oup, odn, ovec,
         WQ, WO, WU, WD, VEC, H, Q, K, V, KT, VT, CTX, P0, P1, P2, P3, HID, GP, RA, RB, PS, PF,
         GQ, GO, GU, GD, R2Q, R2O, R2U, R2D, DK, DV, TAB, COS, SIN, GV, ZR, GZ, PR,
         AS, MS, PRE, DPB, DS, ST, N0, N1, N2, N3, N4, N5, N6, BQ,
         wl, ws, wy, wr, wf, xs, gs, sab, sc, ra_s, rb_s, rc_s, ys, yr, g1s, g1r, g2s, g2r, g3s, g3r, v1s, v1r, v2s, v2r, osem, ns):
    S, D, E, C, F = dims
    E2 = 2 * E
    SR = C // SUB
    z = lax.axis_index('tp')
    xg = lax.axis_index('dp')
    s = lax.axis_index('pp')
    ys_ = s // 2
    c = s % 2
    sib = s + 1 - 2 * c
    oy = 2 * (1 - ys_)
    is_end = z * (NT - 1 - z) == 0
    inner = z * (NT - 1 - z) > 0
    hub = 1 + z // 3
    leaf = jnp.where(z == 1, 0, 3)
    peer = 3 - z
    PX = (P0, P1, P2, P3)
    W_IN = (wqkv, wo, wup, wdn)
    W_BUF = (WQ, WO, WU, WD)
    G_HALF = (3 * E, E, D // 2, F // 2)
    W_PART = tuple(n // 2 for n in G_HALF)
    ALL, FIRST, REST = tuple(range(NA)), (0,), (1, 2, 3)
    ATT, MLP = ALL[:2], ALL[2:]
    G_BUF = (GQ, GO, GU, GD)
    G_OUT = (oqkv, oo, oup, odn)
    G_COLS = (D, D, F, D)
    R1_OFF = (0, 3 * E, 4 * E, 4 * E + D // 2)
    R2 = (R2Q, R2O, R2U, R2D)

    def rcopy(src, dst, ss, rs, **dev):
        return pltpu.make_async_remote_copy(src_ref=src, dst_ref=dst, send_sem=ss, recv_sem=rs, device_id=dev, device_id_type=pl.DeviceIdType.MESH)

    def lcopy(src, dst, sem):
        return pltpu.make_async_copy(src, dst, sem)

    def rows(start, n):
        return pl.ds(pl.multiple_of(start, n), n)

    xcopy = lcopy(x.at[ys_, c], H.at[0], xs.at[0])
    xcopy.start()
    gcopy = lcopy(g.at[ys_, c], GP.at[NL], gs.at[0])
    gcopy.start()
    tcopy = lcopy(tab, TAB, xs.at[1])
    tcopy.start()
    for a in range(NA):
        lcopy(W_IN[a], W_BUF[a].at[s], wl.at[a]).start()
    small = [lcopy(a, b, ns.at[k]) for k, (a, b) in enumerate(((n0, N0), (n1, N1), (n2, N2), (n3, N3), (n4, N4), (n5, N5), (n6, N6), (bq, BQ)))]
    for cp in small:
        cp.start()

    bar = pltpu.get_barrier_semaphore()
    for o in range(1, NT):
        pl.semaphore_signal(bar, inc=1, device_id={'tp': (z + o) % NT}, device_id_type=pl.DeviceIdType.MESH)
    for o in range(1, NL):
        pl.semaphore_signal(bar, inc=1, device_id={'pp': (s + o) % NL}, device_id_type=pl.DeviceIdType.MESH)
    pl.semaphore_signal(bar, inc=1, device_id={'dp': 1 - xg}, device_id_type=pl.DeviceIdType.MESH)
    pl.semaphore_wait(bar, NT + NL - 1)

    def w_part(l, a, q):
        return W_BUF[a].at[l, rows(q * W_PART[a], W_PART[a])]

    def sib_copies():
        out = [rcopy(W_IN[a], W_BUF[a].at[s], ws.at[a], wr.at[s, NA * a], pp=sib) for a in ALL]
        return out + [rcopy(VEC.at[s], VEC.at[s], ws.at[NA], wr.at[s, NA * NA], pp=sib)]

    def y_copies():
        out = []
        for a in ALL:
            for k in range(2):
                q = 2 * xg + k
                out.append(rcopy(W_IN[a].at[rows(q * W_PART[a], W_PART[a])], w_part(s, a, q), wy.at[k, a], wr.at[s, NA * a + q], pp=oy + k))
        return out + [rcopy(VEC.at[s], VEC.at[s], wy.at[k, NA], wr.at[s, NA * NA], pp=oy + k) for k in range(2)]

    def start_all(copies):
        for cp in copies:
            cp.start()

    for cp in small:
        cp.wait()
    for k, ref in enumerate((N0, N1, N2, N3, N4, N5, N6)):
        VEC[s, k:k + 1, :] = ref[...].astype(F32)
    VEC[s, 7:8, :3 * E2] = jnp.concatenate([BQ[k, h:h + 1, :].astype(F32) for k in range(3) for h in range(2)], axis=1)

    @pl.when(s != 1)
    def _():
        start_all(y_copies())
    start_all(sib_copies())

    def arrived(l, a, q):
        rcopy(w_part(l, a, q), w_part(l, a, q), ws.at[a], wr.at[l, NA * a + q], pp=sib).wait_recv()

    def mine(hop):
        return 2 * (xg if hop == 0 else 1 - xg) + c

    def pass_copies(l, a, hop):
        part, sem = w_part(l, a, mine(hop)), wr.at[l, NA * a + mine(hop)]
        out = [rcopy(part, part, wf.at[l % 2, hop, a], sem, pp=sib)]
        return out if hop else out + [rcopy(part, part, wf.at[l % 2, 2, a], sem, dp=1 - xg)]

    def relay(l, arrays, hop):
        @pl.when(l // 2 != ys_)
        def _():
            for a in arrays:
                arrived(l, a, mine(hop))
                start_all(pass_copies(l, a, hop))

    def settle(l, arrays, small):
        @pl.when(l == s)
        def _():
            for a in arrays:
                lcopy(W_IN[a], W_BUF[a].at[s], wl.at[a]).wait()

        @pl.when(l == sib)
        def _():
            for a in arrays:
                rcopy(W_IN[a], W_BUF[a].at[l], ws.at[a], wr.at[l, NA * a], pp=sib).wait_recv()

        @pl.when(l // 2 != ys_)
        def _():
            for a in arrays:
                for k in range(2):
                    arrived(l, a, 2 * k + 1 - c)
        if small:
            @pl.when(l != s)
            def _():
                rcopy(VEC.at[l], VEC.at[l], ws.at[NA], wr.at[l, NA * NA], pp=sib).wait_recv()

    tcopy.wait()
    for i in range(NC):
        cb, sb = TAB[0, :C, :], TAB[1, :C, :]
        cr, sr = TAB[0, C + i:C + i + 1, :], TAB[1, C + i:C + i + 1, :]
        COS[i * C:(i + 1) * C, :] = cb * cr - sb * sr
        SIN[i * C:(i + 1) * C, :] = sb * cr + cb * sr

    lane = lax.broadcasted_iota(jnp.int32, (C, E2), 1)
    head_lane = lane // E
    in_head = lane % E
    rot_half = E // 8
    low = in_head < rot_half
    sub_head = lax.broadcasted_iota(jnp.int32, (E2, C), 0) // E
    lower = lax.broadcasted_iota(jnp.int32, (C, C), 0) <= lax.broadcasted_iota(jnp.int32, (C, C), 1)
    c1 = E ** -0.5 * LOG2E

    def tabs(i):
        cs, sn = COS[i * C:(i + 1) * C, :], SIN[i * C:(i + 1) * C, :]
        return cs, jnp.where(low, -sn, 0.0), jnp.where(low, 0.0, sn)

    def rotate(v, t):
        cs, sa, sb = t
        return v * cs + pltpu.roll(v, E2 - rot_half, 1) * sa + pltpu.roll(v, rot_half, 1) * sb

    def unrotate(v, t):
        cs, sa, sb = t
        return v * cs + pltpu.roll(v * sa, rot_half, 1) + pltpu.roll(v * sb, E2 - rot_half, 1)

    def end_copy(p, t):
        return rcopy(PS.at[t * SR:(t + 1) * SR], RA.at[p % 2, t * SR:(t + 1) * SR], sab.at[t], ra_s.at[p % 2, t], tp=hub)

    def peer_copy(p, t):
        return rcopy(PS.at[t * SR:(t + 1) * SR], RB.at[p % 2, t * SR:(t + 1) * SR], sab.at[t], rb_s.at[p % 2, t], tp=peer)

    def back_copy(p, di, t):
        return rcopy(H.at[di, t * SR:(t + 1) * SR], H.at[di, t * SR:(t + 1) * SR], sc.at[t], rc_s.at[p % 2, t], tp=leaf)

    def pf_row(i, back):
        return (NC if back and i == NC - 1 else i) * C

    def ar_send(p, i, back=False):
        @pl.when(is_end)
        def _():
            for t in range(i * SUB, (i + 1) * SUB):
                @pl.when(p > 0)
                def _():
                    end_copy(p, t).wait_send()
                f0 = pf_row(i, back) + (t - i * SUB) * SR
                PS[t * SR:(t + 1) * SR, :] = PF[f0:f0 + SR, :].astype(BF16)
                end_copy(p, t).start()

    def ar_mid(p, i, u, back=False):
        t = i * SUB + u
        r = slice(t * SR, (t + 1) * SR)
        f0 = pf_row(i, back) + u * SR

        @pl.when(inner)
        def _():
            end_copy(p, t).wait_recv()
            @pl.when(p > 0)
            def _():
                peer_copy(p, t).wait_send()
            PS[r, :] = (PF[f0:f0 + SR, :] + RA[p % 2, r, :].astype(F32)).astype(BF16)
            peer_copy(p, t).start()

    def ar_last(p, ri, di, i, u):
        t = i * SUB + u
        r = slice(t * SR, (t + 1) * SR)

        @pl.when(inner)
        def _():
            lv = jnp.minimum(p, NL - 1)
            bias = (VEC[lv, 4:5, :] + VEC[lv, 5:6, :]) * jnp.where(p < NL, 1.0, 0.0)
            peer_copy(p, t).wait_recv()
            @pl.when(p > 0)
            def _():
                back_copy(p, di, t).wait_send()
            both = PS[r, :].astype(F32) + RB[p % 2, r, :].astype(F32)
            H[di, r, :] = (H[ri, r, :].astype(F32) + both + bias).astype(BF16)
            back_copy(p, di, t).start()

    def ar_wait(p, di, i):
        @pl.when(is_end)
        def _():
            for t in range(i * SUB, (i + 1) * SUB):
                back_copy(p, di, t).wait_recv()

    def stats(hf):
        cen = hf - row_mean(hf)
        rstd = lax.rsqrt(row_mean(cen * cen) + LN_EPS)
        return cen * rstd, rstd

    LB = 64
    GR = 32

    def norms(l, i):
        g1, b1, g2, b2 = (VEC[l, k:k + 1, :] for k in range(NA))

        def step(b, carry):
            hf = H[l, rows(i * C + b * LB, LB), :].astype(F32)
            xhat, unused = stats(hf)
            AS[rows(b * LB, LB), :] = (xhat * g1 + b1).astype(BF16)
            MS[rows(b * LB, LB), :] = (xhat * g2 + b2).astype(BF16)
            return carry
        lax.fori_loop(0, C // LB, step, 0)

    def by_kind():
        return [(h * 3 + k) * E for k in range(3) for h in range(2)]

    def wq(l):
        return jnp.concatenate([WQ[l, r:r + E, :] for r in by_kind()], axis=0)

    def forward(l, i):
        r0, r1 = i * C, (i + 1) * C
        norms(l, i)
        qkv = nt(AS[...], wq(l)) + VEC[l, 7:8, :3 * E2]
        qkv = qkv.astype(BF16).astype(F32)
        t = tabs(i)
        q = rotate(qkv[:, :E2], t).astype(BF16)
        kf = rotate(qkv[:, E2:2 * E2], t)
        vf = qkv[:, 2 * E2:3 * E2]
        Q[l, r0:r1, :] = q
        K[l, r0:r1, :] = kf.astype(BF16)
        V[l, r0:r1, :] = vf.astype(BF16)
        KT[l, :, r0:r1] = jnp.transpose(kf).astype(BF16)
        VT[:, r0:r1] = jnp.transpose(vf).astype(BF16)
        yield
        RBK = C // 2
        outs = []
        for h in range(2):
            qm = jnp.where(head_lane == h, Q[l, r0:r1, :].astype(F32), 0.0).astype(BF16)
            ST[:r1, :] = nt(K[l, :r1, :], qm)
            ST[r0:r1, :] = jnp.where(lower, ST[r0:r1, :], -1e30)

            def top(b, m):
                return jnp.maximum(m, jnp.max(ST[rows(b * RBK, RBK), :].reshape(RBK // 8, 8, C), axis=0))
            m = jnp.max(lax.fori_loop(0, r1 // RBK, top, jnp.full((8, C), -3e38, F32)), axis=0, keepdims=True)
            mc = m * c1

            def expo(b, tot):
                e = jnp.exp2(ST[rows(b * RBK, RBK), :] * c1 - mc)
                ST[rows(b * RBK, RBK), :] = e
                return tot + fold(e)
            tot = col_sum(lax.fori_loop(0, r1 // RBK, expo, jnp.zeros((8, C), F32)))
            inv = 1.0 / tot

            def put(b, carry):
                PX[i][l, h, rows(b * RBK, RBK), :] = (ST[rows(b * RBK, RBK), :] * inv).astype(BF16)
                return carry
            lax.fori_loop(0, r1 // RBK, put, 0)
            outs.append(nn(VT[:, :r1], PX[i][l, h]))
            if h == 0:
                yield
        ctx = jnp.transpose(jnp.where(sub_head == 0, outs[0], outs[1])).astype(BF16)
        CTX[l, r0:r1, :] = ctx
        yield
        if i == 0:
            @pl.when(l == 0)
            def _():
                for hop in range(2):
                    relay(l, REST, hop)
            settle(l, REST, False)
        PF[r0:r1, :] = nn(ctx, WO[l])
        PRE[...] = nn(MS[...], WU[l])
        bup = VEC[l, 6:7, :]
        GB = 32

        def act(b, carry):
            u = PRE[rows(b * GB, GB), :] + bup
            cdf = 0.5 * (1.0 + lax.erf(u * RSQRT2))
            pdf = jnp.exp2(u * u * (-0.5 * LOG2E)) * INV_SQRT_2PI
            HID[l, rows(r0 + b * GB, GB), :] = (u * cdf).astype(BF16)
            GP[l, rows(r0 + b * GB, GB), :] = cdf + u * pdf
            return carry
        lax.fori_loop(0, C // GB, act, 0)
        PF[r0:r1, :] += nn(HID[l, r0:r1, :], WD[l])
        yield

    def backward(l, dl, i, last):
        r0, r1 = i * C, (i + 1) * C
        par = l % 2
        first = i == NC - 1

        def acc(ref, val):
            if first:
                ref[par] = val
            else:
                ref[par] += val

        def acc_row(k, val, w=D):
            GV[l, k:k + 1, :w] += val

        norms(l, i)
        dy = H[dl, r0:r1, :]
        acc_row(4, col_sum(dy.astype(F32)))
        PRE[...] = nt(dy, WD[l])
        GB = 32

        def act(b, tot):
            d = PRE[rows(b * GB, GB), :] * GP[l, rows(r0 + b * GB, GB), :]
            DPB[rows(b * GB, GB), :] = d.astype(BF16)
            return tot + fold(d)
        dbu = lax.fori_loop(0, C // GB, act, jnp.zeros((8, F), F32))
        acc_row(5, col_sum(dbu))
        acc(GD, tn(HID[l, r0:r1, :], dy))
        yield
        acc(GU, tn(MS[...], DPB[...]))
        f0 = pf_row(i, True)
        PF[f0:f0 + C, :] = nt(DPB[...], WU[l])
        yield
        dctx = nt(dy, WO[l]).astype(BF16)
        ctx = CTX[l, r0:r1, :]
        acc(GO, tn(ctx, dy))
        prod = dctx.astype(F32) * ctx.astype(F32)
        q = Q[l, r0:r1, :].astype(F32)
        dcf = dctx.astype(F32)
        RBK = C // 2
        dqt = []
        for h in range(2):
            sel = head_lane == h
            qm = jnp.where(sel, q, 0.0).astype(BF16)
            dcm = jnp.where(sel, dcf, 0.0).astype(BF16)
            dsum = jnp.transpose(jnp.where(sel, prod, 0.0))
            drow = col_sum(dsum)
            ST[:r1, :] = nt(V[l, :r1, :], dcm)

            def sub(b, carry):
                pr = PX[i][l, h, rows(b * RBK, RBK), :].astype(F32)
                DS[rows(b * RBK, RBK), :] = (pr * (ST[rows(b * RBK, RBK), :] - drow)).astype(BF16)
                return carry
            lax.fori_loop(0, r1 // RBK, sub, 0)
            dk = nn(DS[:r1, :], qm)
            dv = nn(PX[i][l, h], dcm)
            if first and h == 0:
                DK[:r1, :] = dk
                DV[:r1, :] = dv
            else:
                DK[:r1, :] += dk
                DV[:r1, :] += dv
            dqt.append(nn(KT[l, :, :r1], DS[:r1, :]))
            yield
        scale = E ** -0.5
        t = tabs(i)
        dq = unrotate(jnp.transpose(jnp.where(sub_head == 0, dqt[0], dqt[1])) * scale, t)
        dk = unrotate(DK[r0:r1, :] * scale, t)
        dv = DV[r0:r1, :]
        dqkv = jnp.concatenate([dq, dk, dv], axis=1)
        acc_row(6, col_sum(dqkv), 3 * E2)
        dqkv = dqkv.astype(BF16)
        dwq = tn(dqkv, AS[...])
        for k, r in enumerate(by_kind()):
            if first:
                GQ[par, r:r + E, :] = dwq[k * E:(k + 1) * E]
            else:
                GQ[par, r:r + E, :] += dwq[k * E:(k + 1) * E]
        PRE[...] = nn(dqkv, wq(l))
        yield
        g1, g2 = VEC[l, 0:1, :], VEC[l, 2:3, :]

        def lnb(b, tots):
            hf = H[l, rows(r0 + b * LB, LB), :].astype(F32)
            xhat, rstd = stats(hf)
            da = PRE[rows(b * LB, LB), :]
            dm = PF[rows(f0 + b * LB, LB), :]
            dx = da * g1 + dm * g2
            m1 = row_mean(dx)
            m2 = row_mean(dx * xhat)
            if not last:
                PF[rows(f0 + b * LB, LB), :] = rstd * (dx - m1 - xhat * m2)
            terms = (da * xhat, da, dm * xhat, dm)
            return tuple(a + fold(v) for a, v in zip(tots, terms))
        tots = lax.fori_loop(0, C // LB, lnb, tuple(jnp.zeros((8, D), F32) for _ in range(NA)))
        for k in range(NA):
            acc_row(k, col_sum(tots[k]))
        yield

    def g_half(a, k):
        return rows(k * G_HALF[a], G_HALF[a])

    def r1_view(l, a):
        return GP.at[l + 1, R1_OFF[a]:R1_OFF[a] + G_HALF[a], :G_COLS[a]]

    def g1_copy(l, a):
        return rcopy(G_BUF[a].at[l % 2, g_half(a, 1 - c)], r1_view(l, a), g1s.at[a], g1r.at[l % 2, a], pp=sib)

    def g2_copy(l, a):
        return rcopy(HID.at[l, R1_OFF[a]:R1_OFF[a] + G_HALF[a], :G_COLS[a]], R2[a].at[l % 2], g2s.at[l % 2, a], g2r.at[l % 2, a], pp=2 * (l // 2) + c)

    def g3_local(l, a):
        return lcopy(r1_view(l, a), G_OUT[a].at[g_half(a, c)], g3s.at[l % 2, a])

    def g3_remote(l, a):
        return rcopy(r1_view(l, a), G_OUT[a].at[g_half(a, c)], g3s.at[l % 2, a], g3r.at[a], pp=sib)

    def v1_copies(l):
        return [rcopy(GV.at[l], ZR.at[l, z], v1s.at[l, o - 1], v1r.at[l, z], tp=(z + o) % NT) for o in range(1, NT)]

    def grads_mid(l, arrays):
        for a in arrays:
            g1_copy(l, a).wait_recv()
            n = G_HALF[a]

            def add(b, carry):
                rr = rows(R1_OFF[a] + b * GR, GR)
                tot = G_BUF[a][l % 2, rows(c * n + b * GR, GR), :] + GP[l + 1, rr, :G_COLS[a]]
                GP[l + 1, rr, :G_COLS[a]] = tot
                HID[l, rr, :G_COLS[a]] = tot.astype(BF16)
                return carry
            lax.fori_loop(0, n // GR, add, 0)

            @pl.when(l // 2 != ys_)
            def _():
                g2_copy(l, a).start()

    def grads_last(l):
        @pl.when(l // 2 == ys_)
        def _():
            for a in MLP + ATT:
                g2_copy(l, a).wait_recv()

                def add(b, carry):
                    rr = rows(R1_OFF[a] + b * GR, GR)
                    GP[l + 1, rr, :G_COLS[a]] += R2[a][l % 2, rows(b * GR, GR), :].astype(F32)
                    return carry
                lax.fori_loop(0, G_HALF[a] // GR, add, 0)

                @pl.when(l == s)
                def _():
                    g3_local(l, a).start()

                @pl.when(l != s)
                def _():
                    g3_remote(l, a).start()

    def grads_sent(l):
        for a in range(NA):
            @pl.when(l // 2 != ys_)
            def _():
                g2_copy(l, a).wait_send()

            @pl.when(l == s)
            def _():
                g3_local(l, a).wait()

            @pl.when((l // 2 == ys_) & (l != s))
            def _():
                g3_remote(l, a).wait_send()

    def v2_copy(l):
        return rcopy(GZ.at[l], PR.at[s], v2s.at[l], v2r.at[s], pp=l)

    def vec_mid(l):
        ZR[l, z] = GV[l]
        for o in range(1, NT):
            q = (z + o) % NT
            rcopy(GV.at[l], ZR.at[l, q], v1s.at[l, o - 1], v1r.at[l, q], tp=q).wait_recv()
        tot = ZR[l, 0] + ZR[l, 1] + ZR[l, 2] + ZR[l, 3]
        row = lax.broadcasted_iota(jnp.int32, (8, D), 0)
        GZ[l] = jnp.where(row < 4, tot, GV[l])

        @pl.when(l == s)
        def _():
            PR[s] = GZ[l]

        @pl.when(l != s)
        def _():
            v2_copy(l).start()

    GV[...] = jnp.zeros_like(GV)
    for hop in range(2):
        relay(0, FIRST, hop)
    settle(0, FIRST, True)
    xcopy.wait()

    def run(phases, at, handle, after=lambda k: None):
        for k, unused in enumerate(phases):
            after(k)
            for op, lag, u in at.get(k, ()):
                handle(op, lag, u)

    def fwd_layer(l, carry):
        for i in range(NC):
            @pl.when(l > 0)
            def _():
                ar_wait(l - 1, l, i)

            def handle(op, lag, u):
                m = i - lag

                def go(p, j):
                    if op == 'mid':
                        ar_mid(p, j, u)
                    else:
                        ar_last(p, p, p + 1, j, u)
                if m >= 0:
                    go(l, m)
                else:
                    @pl.when(l > 0)
                    def _():
                        go(l - 1, m + NC)
            run(forward(l, i), FWD_AT, handle)
            ar_send(l, i)
            if i == 1:
                @pl.when(l == 0)
                def _():
                    gcopy.wait()
                    H[NL + 1] = GP[NL].astype(BF16)

                    @pl.when(s == 1)
                    def _():
                        start_all(y_copies())
            if i > 0:
                @pl.when(l < NL - 1)
                def _():
                    if i < NC - 1:
                        relay(l + 1, ALL, i - 1)
                    else:
                        settle(l + 1, FIRST, True)
        return carry
    lax.fori_loop(0, NL, fwd_layer, 0)

    y_local = lcopy(H.at[NL], y.at[ys_, c], ys.at[0])
    y_sib = rcopy(H.at[NL], y.at[ys_, c], ys.at[1], yr.at[s], pp=sib)
    y_far = rcopy(H.at[NL], y.at[ys_, c], ys.at[2], yr.at[s], pp=oy + c)
    y_fwd = rcopy(y.at[1 - ys_, c], y.at[1 - ys_, c], ys.at[3], yr.at[oy + c], pp=sib)

    def y_arrived(q):
        rcopy(H.at[NL], y.at[q // 2, q % 2], ys.at[1], yr.at[q], pp=sib).wait_recv()

    def ri(l):
        return jnp.where(l == NL - 1, NL + 1, l + 1)

    def bwd_layer(lb, carry):
        l = NL - 1 - lb
        p = NL + lb
        for n in range(NC):
            i = NC - 1 - n

            @pl.when(lb > 0)
            def _():
                ar_wait(p - 1, l + 1, i)

            def handle(op, lag, u):
                m = n - lag

                def go(q, lq, j):
                    if op == 'mid':
                        ar_mid(q, j, u, True)
                    else:
                        ar_last(q, ri(lq), lq, j, u)
                if m >= 0:
                    @pl.when(l > 0)
                    def _():
                        go(p, l, NC - 1 - m)
                else:
                    @pl.when(lb > 0)
                    def _():
                        go(p - 1, l + 1, -1 - m)

                    @pl.when(lb == 0)
                    def _():
                        if op == 'mid':
                            ar_mid(NL - 1, m + NC, u)
                        else:
                            ar_last(NL - 1, NL - 1, NL, m + NC, u)

            def after(k):
                if k == 0 and n == 0:
                    @pl.when(lb > 0)
                    def _():
                        grads_mid(l + 1, ATT)
                        for a in ALL:
                            g1_copy(l + 1, a).wait_send()
                if k == 1 and n == NC - 1:
                    for a in MLP:
                        g1_copy(l, a).start()
            run(backward(l, ri(l), i, False), BWD_AT, handle, after)

            @pl.when(l > 0)
            def _():
                ar_send(p, i, True)
            if n == 0:
                @pl.when(lb == 2)
                def _():
                    y_arrived(oy + c)
                    y_fwd.start()
            if n == 1:
                @pl.when(lb > 0)
                def _():
                    vec_mid(l + 1)
            if n == 2:
                @pl.when(lb == 0)
                def _():
                    for j in range(NC):
                        ar_wait(NL - 1, NL, j)
                    start_all((y_local, y_sib, y_far))

                @pl.when(lb > 1)
                def _():
                    grads_last(l + 2)

        for a in ATT:
            g1_copy(l, a).start()
        start_all(v1_copies(l))
        grads_mid(l, MLP)
        return carry
    lax.fori_loop(0, NL, bwd_layer, 0)

    grads_mid(0, ATT)
    grads_last(1)
    vec_mid(0)
    grads_last(0)

    for o in range(1, NL):
        q = (s + o) % NL
        rcopy(GZ.at[0], PR.at[q], v2s.at[0], v2r.at[q], pp=q).wait_recv()
    PRE[0:8, 0:D] = PR[0] + PR[1] + PR[2] + PR[3]
    vout = lcopy(PRE.at[0:8, 0:D], ovec, osem.at[0])
    vout.start()
    for l in range(NL):
        for cp in v1_copies(l):
            cp.wait_send()
    for l in range(NL):
        @pl.when(l != s)
        def _():
            v2_copy(l).wait_send()
    for a in range(NA):
        rcopy(G_OUT[a].at[g_half(a, 1 - c)], G_OUT[a].at[g_half(a, 1 - c)], g3s.at[a], g3r.at[a], pp=sib).wait_recv()
    y_local.wait()
    for cp in (y_sib, y_far, y_fwd):
        cp.wait_send()
    y_arrived(sib)
    y_arrived(oy + 1 - c)
    for a in range(NA):
        g1_copy(0, a).wait_send()
    for l in range(NL):
        grads_sent(l)
    for cp in sib_copies():
        cp.wait_send()
    for cp in y_copies():
        cp.wait_send()
    for k in range(2):
        for a in ALL:
            for hop in range(2):
                for cp in pass_copies(oy + k, a, hop):
                    cp.wait_send()

    @pl.when(is_end)
    def _():
        for t in range(NC * SUB):
            end_copy(0, t).wait_send()

    @pl.when(inner)
    def _():
        for t in range(NC * SUB):
            peer_copy(0, t).wait_send()
            back_copy(0, 1, t).wait_send()
    vout.wait()


def finish(y, gq, go, gu, gd, gv, yo, qo, oo, uo, do, n0, n1, n2, n3, n4, n5, n6, bq, yb, qb, ob, ub, db, got, put):
    trips = [(gd, db, do), (gu, ub, uo), (go, ob, oo), (gq, qb, qo)]
    trips += [tuple(ref.at[m, r] for ref in (y, yb, yo)) for m in range(y.shape[0]) for r in range(y.shape[1])]
    loads = [pltpu.make_async_copy(a, b, got.at[k]) for k, (a, b, o) in enumerate(trips)]
    stores = [pltpu.make_async_copy(b, o, put.at[k]) for k, (a, b, o) in enumerate(trips)]
    for cp in loads:
        cp.start()
    for row, refs in enumerate(((n0,), (n1,), (n2,), (n3,), (n4, n5), (n6,))):
        for ref in refs:
            ref[...] = gv[row:row + 1, :]
    e = bq.shape[2]
    for k in range(3):
        for h in range(2):
            bq[k, h:h + 1, :] = gv[6:7, (2 * k + h) * e:(2 * k + h + 1) * e]
    for cp, out in zip(loads, stores):
        cp.wait()
        out.start()
    for cp in stores:
        cp.wait()


def finish_step(y, gq, go, gu, gd, gv, e):
    hbm, vmem = pl.BlockSpec(memory_space=pl.ANY), pl.BlockSpec(memory_space=pltpu.VMEM)
    big = [jax.ShapeDtypeStruct(a.shape, a.dtype) for a in (y, gq, go, gu, gd)]
    row = jax.ShapeDtypeStruct((1, gv.shape[1]), F32)
    return pl.pallas_call(
        finish,
        out_shape=big + [row] * 7 + [jax.ShapeDtypeStruct((3, 2, e), F32)],
        in_specs=[hbm] * 5 + [vmem],
        out_specs=[hbm] * 5 + [vmem] * 8,
        scratch_shapes=[pltpu.VMEM(a.shape, a.dtype) for a in big] + [pltpu.SemaphoreType.DMA((8,))] * 2,
        name='neox_out',
    )(y, gq, go, gu, gd, gv)


def group_step(dims, *args):
    x = args[0]
    S, D, E, C, F = dims
    E2 = 2 * E
    hbm = pl.BlockSpec(memory_space=pl.ANY)
    out_shape = [
        jax.ShapeDtypeStruct(x.shape, BF16),
        jax.ShapeDtypeStruct((3 * E2, D), F32),
        jax.ShapeDtypeStruct((E2, D), F32),
        jax.ShapeDtypeStruct((D, F), F32),
        jax.ShapeDtypeStruct((F, D), F32),
        jax.ShapeDtypeStruct((8, D), F32),
    ]

    def vm(*shape, dtype=BF16):
        return pltpu.VMEM(shape, dtype)
    dma = pltpu.SemaphoreType.DMA
    scratch = [
        vm(NL, 3 * E2, D), vm(NL, E2, D), vm(NL, D, F), vm(NL, F, D), vm(NL, 8, D, dtype=F32),
        vm(NL + 2, S, D),
        vm(NL, S, E2), vm(NL, S, E2), vm(NL, S, E2), vm(NL, E2, S), vm(E2, S), vm(NL, S, E2),
        *[vm(NL, 2, (i + 1) * C, C) for i in range(NC)],
        vm(NL, S, F), vm(NL + 1, S, F, dtype=F32),
        vm(2, S, D), vm(2, S, D), vm(S, D), vm(S + C, D, dtype=F32),
        vm(2, 3 * E2, D, dtype=F32), vm(2, E2, D, dtype=F32), vm(2, D, F, dtype=F32), vm(2, F, D, dtype=F32),
        vm(2, 3 * E, D), vm(2, E, D), vm(2, D // 2, F), vm(2, F // 2, D),
        vm(S, E2, dtype=F32), vm(S, E2, dtype=F32),
        vm(2, C + 8, E2, dtype=F32), vm(S, E2, dtype=F32), vm(S, E2, dtype=F32),
        vm(NL, 8, D, dtype=F32), vm(NL, NT, 8, D, dtype=F32), vm(NL, 8, D, dtype=F32), vm(NL, 8, D, dtype=F32),
        vm(C, D), vm(C, D), vm(C, max(D, F), dtype=F32), vm(C, F), vm(S, C), vm(S, C, dtype=F32),
        *[vm(1, D, dtype=F32)] * 4, vm(1, D), vm(1, D), vm(1, F), vm(3, 2, E),
        dma((NA,)), dma((NA + 1,)), dma((2, NA + 1)), dma((NL, NA * NA + 1)), dma((2, 3, NA)), dma((2,)), dma((1,)),
        dma((NC * SUB,)), dma((NC * SUB,)), dma((2, NC * SUB)), dma((2, NC * SUB)), dma((2, NC * SUB)),
        dma((NL,)), dma((NL,)), dma((NA,)), dma((2, NA)), dma((2, NA)), dma((2, NA)), dma((2, NA)), dma((NA,)),
        dma((NL, NT - 1)), dma((NL, NT)), dma((NL,)), dma((NL,)), dma((1,)), dma((8,)),
    ]
    return pl.pallas_call(
        functools.partial(body, dims),
        out_shape=out_shape,
        in_specs=[hbm] * len(args),
        out_specs=[hbm] * 6,
        scratch_shapes=scratch,
        compiler_params=pltpu.CompilerParams(collective_id=0, has_side_effects=True, vmem_limit_bytes=67043328),
        name='neox_group',
    )(*args)


def solution(mesh):
    def device_fn(x_in, g_out, ln1_gain, ln1_bias, w_qkv, b_qkv, w_out, b_out, ln2_gain, ln2_bias, w_up, b_up, w_down, b_down):
        n_micro, n_rows, S, D = x_in.shape
        heads, E = w_qkv.shape[2], w_qkv.shape[4]
        F = w_up.shape[2]
        C = S // NC
        wqkv = jnp.transpose(w_qkv[0], (1, 2, 3, 0)).reshape(heads * 3 * E, D)
        bqkv = jnp.transpose(b_qkv[0], (1, 0, 2))
        tab = jnp.asarray(rotary_base(C, NC, E, heads))
        part = group_step((S, D, E, C, F), x_in, g_out, wqkv, w_out[0].reshape(heads * E, D), w_up[0], w_down[0], ln1_gain, ln1_bias, ln2_gain, ln2_bias, b_out, b_down, b_up, bqkv, tab)
        y, gq, go, gup, gdn, n1g, n1b, n2g, n2b, gbo, gbd, gbu, gbq = finish_step(*part, E)
        gq = jnp.transpose(gq.reshape(heads, 3, E, D), (3, 0, 1, 2))[None]
        gbq = jnp.transpose(gbq, (1, 0, 2))[None]
        return (y, n1g, n1b, gq, gbq, go.reshape(1, heads, E, D), gbo, n2g, n2b, gup[None], gbu, gdn[None], gbd)

    return jax.shard_map(device_fn, mesh=mesh, in_specs=(P('dp'), P('dp')) + STAGE_SPECS, out_specs=(P('dp'),) + GRAD_SPECS, check_vma=False)
```

```python
import functools
import math

import jax
import jax.numpy as jnp
import numpy as np
from jax import lax
from jax.experimental import pallas as pl
from jax.experimental.pallas import tpu as pltpu
from jax.sharding import PartitionSpec as P

ROPE_BASE = 10000.0
LN_EPS = 1e-5
STAGE_SPECS = (P('pp'), P('pp'), P('pp', None, 'tp'), P('pp', 'tp'), P('pp', 'tp'), P('pp'), P('pp'), P('pp'), P('pp', None, 'tp'), P('pp', 'tp'), P('pp', 'tp'), P('pp'))
OWN = ('dp', 'pp')
GRAD_SPECS = (P(OWN), P(OWN), P(OWN, None, 'tp'), P(OWN, 'tp'), P(OWN, 'tp'), P(OWN), P(OWN), P(OWN), P(OWN, None, 'tp'), P(OWN, 'tp'), P(OWN, 'tp'), P(OWN))


F32 = jnp.float32
BF16 = jnp.bfloat16
NL = 4
NT = 4
NC = 4
NA = 4
SUB = 2
FWD_AT = {0: (('mid', 1, 0), ('last', 2, 0)), 2: (('mid', 1, 1), ('last', 2, 1))}
BWD_AT = {0: (('last', 2, 0),), 1: (('mid', 1, 0),), 3: (('last', 2, 1),), 4: (('mid', 1, 1),)}
LOG2E = 1.4426950408889634
RSQRT2 = 0.7071067811865476
INV_SQRT_2PI = 0.3989422804014327


def nn(a, b):
    return lax.dot_general(a, b, (((1,), (0,)), ((), ())), preferred_element_type=F32)


def nt(a, b):
    return lax.dot_general(a, b, (((1,), (1,)), ((), ())), preferred_element_type=F32)


def tn(a, b):
    return lax.dot_general(a, b, (((0,), (0,)), ((), ())), preferred_element_type=F32)


def col_sum(v):
    return jnp.sum(v, axis=0, keepdims=True)


def row_mean(v):
    return jnp.mean(v, axis=-1, keepdims=True)


def fold(v):
    return jnp.sum(v.reshape(v.shape[0] // 8, 8, v.shape[1]), axis=0)


def rotary_base(chunk, n_chunks, head_dim, n_heads):
    rot_dim = head_dim // 4
    half = rot_dim // 2
    inv_freq = np.zeros((head_dim,), np.float64)
    inv_freq[:rot_dim] = np.tile(ROPE_BASE ** (-(np.arange(half) * 2.0) / rot_dim), 2)
    inv_freq = np.tile(inv_freq, n_heads)
    pos = np.concatenate([np.arange(chunk), np.arange(8) * (np.arange(8) < n_chunks) * chunk]).astype(np.float64)
    ang = pos[:, None] * inv_freq[None, :]
    return np.stack([np.cos(ang), np.sin(ang)]).astype(np.float32)


def body(dims, x, g, wqkv, wo, wup, wdn, n0, n1, n2, n3, n4, n5, n6, bq, tab,
         y, oqkv, oo, oup, odn, ovec,
         WQ, WO, WU, WD, VEC, H, Q, K, V, KT, VT, CTX, P0, P1, P2, P3, HID, GP, RA, RB, PS, PF,
         GQ, GO, GU, GD, R2Q, R2O, R2U, R2D, DK, DV, TAB, COS, SIN, GV, ZR, GZ, PR,
         AS, MS, PRE, DPB, DS, ST, N0, N1, N2, N3, N4, N5, N6, BQ,
         wl, ws, wy, wr, wf, xs, gs, sab, sc, ra_s, rb_s, rc_s, ys, yr, g1s, g1r, g2s, g2r, g3s, g3r, v1s, v1r, v2s, v2r, osem, ns):
    S, D, E, C, F = dims
    E2 = 2 * E
    SR = C // SUB
    z = lax.axis_index('tp')
    s = lax.axis_index('pp')
    ys_ = s // 2
    c = s % 2
    sib = s + 1 - 2 * c
    oy = 2 * (1 - ys_)
    is_end = z * (NT - 1 - z) == 0
    inner = z * (NT - 1 - z) > 0
    hub = 1 + z // 3
    leaf = jnp.where(z == 1, 0, 3)
    peer = 3 - z
    PX = (P0, P1, P2, P3)
    W_IN = (wqkv, wo, wup, wdn)
    W_BUF = (WQ, WO, WU, WD)
    G_HALF = (3 * E, E, D // 2, F // 2)
    ALL, FIRST, REST = tuple(range(NA)), (0,), (1, 2, 3)
    ATT, MLP = ALL[:2], ALL[2:]
    G_BUF = (GQ, GO, GU, GD)
    G_OUT = (oqkv, oo, oup, odn)
    G_COLS = (D, D, F, D)
    R1_OFF = (0, 3 * E, 4 * E, 4 * E + D // 2)
    R2 = (R2Q, R2O, R2U, R2D)

    def rcopy(src, dst, ss, rs, **dev):
        return pltpu.make_async_remote_copy(src_ref=src, dst_ref=dst, send_sem=ss, recv_sem=rs, device_id=dev, device_id_type=pl.DeviceIdType.MESH)

    def lcopy(src, dst, sem):
        return pltpu.make_async_copy(src, dst, sem)

    def rows(start, n):
        return pl.ds(pl.multiple_of(start, n), n)

    xcopy = lcopy(x.at[ys_, c], H.at[0], xs.at[0])
    xcopy.start()
    gcopy = lcopy(g.at[ys_, c], GP.at[NL], gs.at[0])
    gcopy.start()
    tcopy = lcopy(tab, TAB, xs.at[1])
    tcopy.start()
    for a in range(NA):
        lcopy(W_IN[a], W_BUF[a].at[s], wl.at[a]).start()
    small = [lcopy(a, b, ns.at[k]) for k, (a, b) in enumerate(((n0, N0), (n1, N1), (n2, N2), (n3, N3), (n4, N4), (n5, N5), (n6, N6), (bq, BQ)))]
    for cp in small:
        cp.start()

    bar = pltpu.get_barrier_semaphore()
    for o in range(1, NT):
        pl.semaphore_signal(bar, inc=1, device_id={'tp': (z + o) % NT}, device_id_type=pl.DeviceIdType.MESH)
    for o in range(1, NL):
        pl.semaphore_signal(bar, inc=1, device_id={'pp': (s + o) % NL}, device_id_type=pl.DeviceIdType.MESH)
    pl.semaphore_wait(bar, NT + NL - 2)

    def half(ref, a, k):
        return ref.at[rows(k * G_HALF[a], G_HALF[a])]

    def sib_copies():
        out = [rcopy(W_IN[a], W_BUF[a].at[s], ws.at[a], wr.at[s, 2 * a], pp=sib) for a in ALL]
        return out + [rcopy(VEC.at[s], VEC.at[s], ws.at[NA], wr.at[s, 2 * NA], pp=sib)]

    def y_copies():
        out = [rcopy(half(W_IN[a], a, k), half(W_BUF[a].at[s], a, k), wy.at[k, a], wr.at[s, 2 * a + k], pp=oy + k) for a in ALL for k in range(2)]
        return out[:2] + [rcopy(VEC.at[s], VEC.at[s], wy.at[k, NA], wr.at[s, 2 * NA], pp=oy + k) for k in range(2)] + out[2:]

    def start_all(copies):
        for cp in copies:
            cp.start()

    for cp in small:
        cp.wait()
    for k, ref in enumerate((N0, N1, N2, N3, N4, N5, N6)):
        VEC[s, k:k + 1, :] = ref[...].astype(F32)
    VEC[s, 7:8, :3 * E2] = jnp.concatenate([BQ[k, h:h + 1, :].astype(F32) for k in range(3) for h in range(2)], axis=1)

    @pl.when(s != 1)
    def _():
        start_all(y_copies())
    start_all(sib_copies())

    def pass_copy(l, a, k):
        part = half(W_BUF[a].at[l], a, k)
        return rcopy(part, part, wf.at[l % 2, a], wr.at[l, 2 * a + k], pp=sib)

    def relay(l, arrays):
        @pl.when(l // 2 != ys_)
        def _():
            for a in arrays:
                pass_copy(l, a, c).wait_recv()
                pass_copy(l, a, c).start()

    def settle(l, arrays, small):
        @pl.when(l == s)
        def _():
            for a in arrays:
                lcopy(W_IN[a], W_BUF[a].at[s], wl.at[a]).wait()

        @pl.when(l == sib)
        def _():
            for a in arrays:
                rcopy(W_IN[a], W_BUF[a].at[l], ws.at[a], wr.at[l, 2 * a], pp=sib).wait_recv()

        @pl.when(l // 2 != ys_)
        def _():
            for a in arrays:
                pass_copy(l, a, 1 - c).wait_recv()
        if small:
            @pl.when(l != s)
            def _():
                rcopy(VEC.at[l], VEC.at[l], ws.at[NA], wr.at[l, 2 * NA], pp=sib).wait_recv()

    tcopy.wait()
    for i in range(NC):
        cb, sb = TAB[0, :C, :], TAB[1, :C, :]
        cr, sr = TAB[0, C + i:C + i + 1, :], TAB[1, C + i:C + i + 1, :]
        COS[i * C:(i + 1) * C, :] = cb * cr - sb * sr
        SIN[i * C:(i + 1) * C, :] = sb * cr + cb * sr

    lane = lax.broadcasted_iota(jnp.int32, (C, E2), 1)
    head_lane = lane // E
    in_head = lane % E
    rot_half = E // 8
    low = in_head < rot_half
    sub_head = lax.broadcasted_iota(jnp.int32, (E2, C), 0) // E
    lower = lax.broadcasted_iota(jnp.int32, (C, C), 0) <= lax.broadcasted_iota(jnp.int32, (C, C), 1)
    c1 = E ** -0.5 * LOG2E

    def tabs(i):
        cs, sn = COS[i * C:(i + 1) * C, :], SIN[i * C:(i + 1) * C, :]
        return cs, jnp.where(low, -sn, 0.0), jnp.where(low, 0.0, sn)

    def rotate(v, t):
        cs, sa, sb = t
        return v * cs + pltpu.roll(v, E2 - rot_half, 1) * sa + pltpu.roll(v, rot_half, 1) * sb

    def unrotate(v, t):
        cs, sa, sb = t
        return v * cs + pltpu.roll(v * sa, rot_half, 1) + pltpu.roll(v * sb, E2 - rot_half, 1)

    def end_copy(p, t):
        return rcopy(PS.at[t * SR:(t + 1) * SR], RA.at[p % 2, t * SR:(t + 1) * SR], sab.at[t], ra_s.at[p % 2, t], tp=hub)

    def peer_copy(p, t):
        return rcopy(PS.at[t * SR:(t + 1) * SR], RB.at[p % 2, t * SR:(t + 1) * SR], sab.at[t], rb_s.at[p % 2, t], tp=peer)

    def back_copy(p, di, t):
        return rcopy(H.at[di, t * SR:(t + 1) * SR], H.at[di, t * SR:(t + 1) * SR], sc.at[t], rc_s.at[p % 2, t], tp=leaf)

    def pf_row(i, back):
        return (NC if back and i == NC - 1 else i) * C

    def ar_send(p, i, back=False):
        @pl.when(is_end)
        def _():
            for t in range(i * SUB, (i + 1) * SUB):
                @pl.when(p > 0)
                def _():
                    end_copy(p, t).wait_send()
                f0 = pf_row(i, back) + (t - i * SUB) * SR
                PS[t * SR:(t + 1) * SR, :] = PF[f0:f0 + SR, :].astype(BF16)
                end_copy(p, t).start()

    def ar_mid(p, i, u, back=False):
        t = i * SUB + u
        r = slice(t * SR, (t + 1) * SR)
        f0 = pf_row(i, back) + u * SR

        @pl.when(inner)
        def _():
            end_copy(p, t).wait_recv()
            @pl.when(p > 0)
            def _():
                peer_copy(p, t).wait_send()
            PS[r, :] = (PF[f0:f0 + SR, :] + RA[p % 2, r, :].astype(F32)).astype(BF16)
            peer_copy(p, t).start()

    def ar_last(p, ri, di, i, u):
        t = i * SUB + u
        r = slice(t * SR, (t + 1) * SR)

        @pl.when(inner)
        def _():
            lv = jnp.minimum(p, NL - 1)
            bias = (VEC[lv, 4:5, :] + VEC[lv, 5:6, :]) * jnp.where(p < NL, 1.0, 0.0)
            peer_copy(p, t).wait_recv()
            @pl.when(p > 0)
            def _():
                back_copy(p, di, t).wait_send()
            both = PS[r, :].astype(F32) + RB[p % 2, r, :].astype(F32)
            H[di, r, :] = (H[ri, r, :].astype(F32) + both + bias).astype(BF16)
            back_copy(p, di, t).start()

    def ar_wait(p, di, i):
        @pl.when(is_end)
        def _():
            for t in range(i * SUB, (i + 1) * SUB):
                back_copy(p, di, t).wait_recv()

    def stats(hf):
        cen = hf - row_mean(hf)
        rstd = lax.rsqrt(row_mean(cen * cen) + LN_EPS)
        return cen * rstd, rstd

    LB = 32
    GR = 32

    def norms(l, i):
        g1, b1, g2, b2 = (VEC[l, k:k + 1, :] for k in range(NA))

        def step(b, carry):
            hf = H[l, rows(i * C + b * LB, LB), :].astype(F32)
            xhat, unused = stats(hf)
            AS[rows(b * LB, LB), :] = (xhat * g1 + b1).astype(BF16)
            MS[rows(b * LB, LB), :] = (xhat * g2 + b2).astype(BF16)
            return carry
        lax.fori_loop(0, C // LB, step, 0, unroll=True)

    def by_kind():
        return [(h * 3 + k) * E for k in range(3) for h in range(2)]

    def wq(l):
        return jnp.concatenate([WQ[l, r:r + E, :] for r in by_kind()], axis=0)

    def forward(l, i):
        r0, r1 = i * C, (i + 1) * C
        norms(l, i)
        qkv = nt(AS[...], wq(l)) + VEC[l, 7:8, :3 * E2]
        qkv = qkv.astype(BF16).astype(F32)
        t = tabs(i)
        q = rotate(qkv[:, :E2], t).astype(BF16)
        kf = rotate(qkv[:, E2:2 * E2], t)
        vf = qkv[:, 2 * E2:3 * E2]
        Q[l, r0:r1, :] = q
        K[l, r0:r1, :] = kf.astype(BF16)
        V[l, r0:r1, :] = vf.astype(BF16)
        KT[l, :, r0:r1] = jnp.transpose(kf).astype(BF16)
        VT[:, r0:r1] = jnp.transpose(vf).astype(BF16)
        yield
        RBK = C // 2
        outs = []
        for h in range(2):
            qm = jnp.where(head_lane == h, Q[l, r0:r1, :].astype(F32), 0.0).astype(BF16)
            ST[:r1, :] = nt(K[l, :r1, :], qm)
            ST[r0:r1, :] = jnp.where(lower, ST[r0:r1, :], -1e30)

            def top(b, m):
                return jnp.maximum(m, jnp.max(ST[rows(b * RBK, RBK), :].reshape(RBK // 8, 8, C), axis=0))
            m = jnp.max(lax.fori_loop(0, r1 // RBK, top, jnp.full((8, C), -3e38, F32), unroll=True), axis=0, keepdims=True)
            mc = m * c1

            def expo(b, tot):
                e = jnp.exp2(ST[rows(b * RBK, RBK), :] * c1 - mc)
                ST[rows(b * RBK, RBK), :] = e
                return tot + fold(e)
            tot = col_sum(lax.fori_loop(0, r1 // RBK, expo, jnp.zeros((8, C), F32), unroll=True))
            inv = 1.0 / tot

            def put(b, carry):
                PX[i][l, h, rows(b * RBK, RBK), :] = (ST[rows(b * RBK, RBK), :] * inv).astype(BF16)
                return carry
            lax.fori_loop(0, r1 // RBK, put, 0, unroll=True)
            outs.append(nn(VT[:, :r1], PX[i][l, h]))
            if h == 0:
                yield
        ctx = jnp.transpose(jnp.where(sub_head == 0, outs[0], outs[1])).astype(BF16)
        CTX[l, r0:r1, :] = ctx
        yield
        if i == 0:
            @pl.when(l == 0)
            def _():
                relay(l, REST)
            settle(l, REST, False)
        PF[r0:r1, :] = nn(ctx, WO[l])
        PRE[...] = nn(MS[...], WU[l])
        bup = VEC[l, 6:7, :]
        GB = 32

        def act(b, carry):
            u = PRE[rows(b * GB, GB), :] + bup
            cdf = 0.5 * (1.0 + lax.erf(u * RSQRT2))
            pdf = jnp.exp2(u * u * (-0.5 * LOG2E)) * INV_SQRT_2PI
            HID[l, rows(r0 + b * GB, GB), :] = (u * cdf).astype(BF16)
            GP[l, rows(r0 + b * GB, GB), :] = cdf + u * pdf
            return carry
        lax.fori_loop(0, C // GB, act, 0, unroll=True)
        PF[r0:r1, :] += nn(HID[l, r0:r1, :], WD[l])
        yield

    def backward(l, dl, i, last):
        r0, r1 = i * C, (i + 1) * C
        par = l % 2
        first = i == NC - 1

        def acc(ref, val):
            if first:
                ref[par] = val
            else:
                ref[par] += val

        def acc_row(k, val, w=D):
            GV[l, k:k + 1, :w] += val

        norms(l, i)
        dy = H[dl, r0:r1, :]
        acc_row(4, col_sum(dy.astype(F32)))
        PRE[...] = nt(dy, WD[l])
        GB = 32

        def act(b, tot):
            d = PRE[rows(b * GB, GB), :] * GP[l, rows(r0 + b * GB, GB), :]
            DPB[rows(b * GB, GB), :] = d.astype(BF16)
            return tot + fold(d)
        dbu = lax.fori_loop(0, C // GB, act, jnp.zeros((8, F), F32), unroll=True)
        acc_row(5, col_sum(dbu))
        acc(GD, tn(HID[l, r0:r1, :], dy))
        yield
        acc(GU, tn(MS[...], DPB[...]))
        f0 = pf_row(i, True)
        PF[f0:f0 + C, :] = nt(DPB[...], WU[l])
        yield
        dctx = nt(dy, WO[l]).astype(BF16)
        ctx = CTX[l, r0:r1, :]
        acc(GO, tn(ctx, dy))
        prod = dctx.astype(F32) * ctx.astype(F32)
        q = Q[l, r0:r1, :].astype(F32)
        dcf = dctx.astype(F32)
        RBK = C // 2
        dqt = []
        for h in range(2):
            sel = head_lane == h
            qm = jnp.where(sel, q, 0.0).astype(BF16)
            dcm = jnp.where(sel, dcf, 0.0).astype(BF16)
            dsum = jnp.transpose(jnp.where(sel, prod, 0.0))
            drow = col_sum(dsum)
            ST[:r1, :] = nt(V[l, :r1, :], dcm)

            def sub(b, carry):
                pr = PX[i][l, h, rows(b * RBK, RBK), :].astype(F32)
                DS[rows(b * RBK, RBK), :] = (pr * (ST[rows(b * RBK, RBK), :] - drow)).astype(BF16)
                return carry
            lax.fori_loop(0, r1 // RBK, sub, 0, unroll=True)
            dk = nn(DS[:r1, :], qm)
            dv = nn(PX[i][l, h], dcm)
            if first and h == 0:
                DK[:r1, :] = dk
                DV[:r1, :] = dv
            else:
                DK[:r1, :] += dk
                DV[:r1, :] += dv
            dqt.append(nn(KT[l, :, :r1], DS[:r1, :]))
            yield
        scale = E ** -0.5
        t = tabs(i)
        dq = unrotate(jnp.transpose(jnp.where(sub_head == 0, dqt[0], dqt[1])) * scale, t)
        dk = unrotate(DK[r0:r1, :] * scale, t)
        dv = DV[r0:r1, :]
        dqkv = jnp.concatenate([dq, dk, dv], axis=1)
        acc_row(6, col_sum(dqkv), 3 * E2)
        dqkv = dqkv.astype(BF16)
        dwq = tn(dqkv, AS[...])
        for k, r in enumerate(by_kind()):
            if first:
                GQ[par, r:r + E, :] = dwq[k * E:(k + 1) * E]
            else:
                GQ[par, r:r + E, :] += dwq[k * E:(k + 1) * E]
        PRE[...] = nn(dqkv, wq(l))
        yield
        g1, g2 = VEC[l, 0:1, :], VEC[l, 2:3, :]

        def lnb(b, tots):
            hf = H[l, rows(r0 + b * LB, LB), :].astype(F32)
            xhat, rstd = stats(hf)
            da = PRE[rows(b * LB, LB), :]
            dm = PF[rows(f0 + b * LB, LB), :]
            dx = da * g1 + dm * g2
            m1 = row_mean(dx)
            m2 = row_mean(dx * xhat)
            if not last:
                PF[rows(f0 + b * LB, LB), :] = rstd * (dx - m1 - xhat * m2)
            terms = (da * xhat, da, dm * xhat, dm)
            return tuple(a + fold(v) for a, v in zip(tots, terms))
        tots = lax.fori_loop(0, C // LB, lnb, tuple(jnp.zeros((8, D), F32) for _ in range(NA)), unroll=True)
        for k in range(NA):
            acc_row(k, col_sum(tots[k]))
        yield

    def g_half(a, k):
        return rows(k * G_HALF[a], G_HALF[a])

    def r1_view(l, a):
        return GP.at[l + 1, R1_OFF[a]:R1_OFF[a] + G_HALF[a], :G_COLS[a]]

    def g1_copy(l, a):
        return rcopy(G_BUF[a].at[l % 2, g_half(a, 1 - c)], r1_view(l, a), g1s.at[a], g1r.at[l % 2, a], pp=sib)

    def g2_copy(l, a):
        return rcopy(HID.at[l, R1_OFF[a]:R1_OFF[a] + G_HALF[a], :G_COLS[a]], R2[a].at[l % 2], g2s.at[l % 2, a], g2r.at[l % 2, a], pp=2 * (l // 2) + c)

    def g3_local(l, a):
        return lcopy(r1_view(l, a), G_OUT[a].at[g_half(a, c)], g3s.at[l % 2, a])

    def g3_remote(l, a):
        return rcopy(r1_view(l, a), G_OUT[a].at[g_half(a, c)], g3s.at[l % 2, a], g3r.at[a], pp=sib)

    def v1_copies(l):
        return [rcopy(GV.at[l], ZR.at[l, z], v1s.at[l, o - 1], v1r.at[l, z], tp=(z + o) % NT) for o in range(1, NT)]

    def grads_mid(l, arrays):
        for a in arrays:
            g1_copy(l, a).wait_recv()
            n = G_HALF[a]

            def add(b, carry):
                rr = rows(R1_OFF[a] + b * GR, GR)
                tot = G_BUF[a][l % 2, rows(c * n + b * GR, GR), :] + GP[l + 1, rr, :G_COLS[a]]
                GP[l + 1, rr, :G_COLS[a]] = tot
                HID[l, rr, :G_COLS[a]] = tot.astype(BF16)
                return carry
            lax.fori_loop(0, n // GR, add, 0)

            @pl.when(l // 2 != ys_)
            def _():
                g2_copy(l, a).start()

    def grads_last(l):
        @pl.when(l // 2 == ys_)
        def _():
            for a in MLP + ATT:
                g2_copy(l, a).wait_recv()

                def add(b, carry):
                    rr = rows(R1_OFF[a] + b * GR, GR)
                    GP[l + 1, rr, :G_COLS[a]] += R2[a][l % 2, rows(b * GR, GR), :].astype(F32)
                    return carry
                lax.fori_loop(0, G_HALF[a] // GR, add, 0)

                @pl.when(l == s)
                def _():
                    g3_local(l, a).start()

                @pl.when(l != s)
                def _():
                    g3_remote(l, a).start()

    def grads_sent(l):
        for a in range(NA):
            @pl.when(l // 2 != ys_)
            def _():
                g2_copy(l, a).wait_send()

            @pl.when(l == s)
            def _():
                g3_local(l, a).wait()

            @pl.when((l // 2 == ys_) & (l != s))
            def _():
                g3_remote(l, a).wait_send()

    def v2_copy(l):
        return rcopy(GZ.at[l], PR.at[s], v2s.at[l], v2r.at[s], pp=l)

    def vec_mid(l):
        ZR[l, z] = GV[l]
        for o in range(1, NT):
            q = (z + o) % NT
            rcopy(GV.at[l], ZR.at[l, q], v1s.at[l, o - 1], v1r.at[l, q], tp=q).wait_recv()
        tot = ZR[l, 0] + ZR[l, 1] + ZR[l, 2] + ZR[l, 3]
        row = lax.broadcasted_iota(jnp.int32, (8, D), 0)
        GZ[l] = jnp.where(row < 4, tot, GV[l])

        @pl.when(l == s)
        def _():
            PR[s] = GZ[l]

        @pl.when(l != s)
        def _():
            v2_copy(l).start()

    GV[...] = jnp.zeros_like(GV)
    relay(0, FIRST)
    settle(0, FIRST, True)
    xcopy.wait()

    def run(phases, at, handle, after=lambda k: None):
        for k, unused in enumerate(phases):
            after(k)
            for op, lag, u in at.get(k, ()):
                handle(op, lag, u)

    def fwd_layer(l, carry):
        for i in range(NC):
            @pl.when(l > 0)
            def _():
                ar_wait(l - 1, l, i)

            def handle(op, lag, u):
                m = i - lag

                def go(p, j):
                    if op == 'mid':
                        ar_mid(p, j, u)
                    else:
                        ar_last(p, p, p + 1, j, u)
                if m >= 0:
                    go(l, m)
                else:
                    @pl.when(l > 0)
                    def _():
                        go(l - 1, m + NC)
            run(forward(l, i), FWD_AT, handle)
            ar_send(l, i)
            if i == 1:
                @pl.when(l == 0)
                def _():
                    gcopy.wait()
                    H[NL + 1] = GP[NL].astype(BF16)

                    @pl.when(s == 1)
                    def _():
                        start_all(y_copies())
            if i > 1:
                @pl.when(l < NL - 1)
                def _():
                    if i < NC - 1:
                        relay(l + 1, ALL)
                    else:
                        settle(l + 1, FIRST, True)
        return carry
    lax.fori_loop(0, NL, fwd_layer, 0)

    y_local = lcopy(H.at[NL], y.at[ys_, c], ys.at[0])
    y_sib = rcopy(H.at[NL], y.at[ys_, c], ys.at[1], yr.at[s], pp=sib)
    y_far = rcopy(H.at[NL], y.at[ys_, c], ys.at[2], yr.at[s], pp=oy + c)
    y_fwd = rcopy(y.at[1 - ys_, c], y.at[1 - ys_, c], ys.at[3], yr.at[oy + c], pp=sib)

    def y_arrived(q):
        rcopy(H.at[NL], y.at[q // 2, q % 2], ys.at[1], yr.at[q], pp=sib).wait_recv()

    def ri(l):
        return jnp.where(l == NL - 1, NL + 1, l + 1)

    def bwd_layer(lb, carry):
        l = NL - 1 - lb
        p = NL + lb
        for n in range(NC):
            i = NC - 1 - n

            @pl.when(lb > 0)
            def _():
                ar_wait(p - 1, l + 1, i)

            def handle(op, lag, u):
                m = n - lag

                def go(q, lq, j):
                    if op == 'mid':
                        ar_mid(q, j, u, True)
                    else:
                        ar_last(q, ri(lq), lq, j, u)
                if m >= 0:
                    @pl.when(l > 0)
                    def _():
                        go(p, l, NC - 1 - m)
                else:
                    @pl.when(lb > 0)
                    def _():
                        go(p - 1, l + 1, -1 - m)

                    @pl.when(lb == 0)
                    def _():
                        if op == 'mid':
                            ar_mid(NL - 1, m + NC, u)
                        else:
                            ar_last(NL - 1, NL - 1, NL, m + NC, u)

            def after(k):
                if k == 0 and n == 0:
                    @pl.when(lb > 0)
                    def _():
                        grads_mid(l + 1, ATT)
                        for a in ALL:
                            g1_copy(l + 1, a).wait_send()
                if k == 1 and n == NC - 1:
                    for a in MLP:
                        g1_copy(l, a).start()
            run(backward(l, ri(l), i, False), BWD_AT, handle, after)

            @pl.when(l > 0)
            def _():
                ar_send(p, i, True)
            if n == 0:
                @pl.when(lb == 2)
                def _():
                    y_arrived(oy + c)
                    y_fwd.start()
            if n == 1:
                @pl.when(lb > 0)
                def _():
                    vec_mid(l + 1)
            if n == 2:
                @pl.when(lb == 0)
                def _():
                    for j in range(NC):
                        ar_wait(NL - 1, NL, j)
                    start_all((y_local, y_sib, y_far))

                @pl.when(lb > 1)
                def _():
                    grads_last(l + 2)

        for a in ATT:
            g1_copy(l, a).start()
        start_all(v1_copies(l))
        grads_mid(l, MLP)
        return carry
    lax.fori_loop(0, NL, bwd_layer, 0)

    grads_mid(0, ATT)
    grads_last(1)
    vec_mid(0)
    grads_last(0)

    for o in range(1, NL):
        q = (s + o) % NL
        rcopy(GZ.at[0], PR.at[q], v2s.at[0], v2r.at[q], pp=q).wait_recv()
    PRE[0:8, 0:D] = PR[0] + PR[1] + PR[2] + PR[3]
    vout = lcopy(PRE.at[0:8, 0:D], ovec, osem.at[0])
    vout.start()
    for l in range(NL):
        for cp in v1_copies(l):
            cp.wait_send()
    for l in range(NL):
        @pl.when(l != s)
        def _():
            v2_copy(l).wait_send()
    for a in range(NA):
        rcopy(G_OUT[a].at[g_half(a, 1 - c)], G_OUT[a].at[g_half(a, 1 - c)], g3s.at[a], g3r.at[a], pp=sib).wait_recv()
    y_local.wait()
    for cp in (y_sib, y_far, y_fwd):
        cp.wait_send()
    y_arrived(sib)
    y_arrived(oy + 1 - c)
    for a in range(NA):
        g1_copy(0, a).wait_send()
    for l in range(NL):
        grads_sent(l)
    for cp in sib_copies():
        cp.wait_send()
    for cp in y_copies():
        cp.wait_send()
    for k in range(2):
        for a in ALL:
            pass_copy(oy + k, a, c).wait_send()

    @pl.when(is_end)
    def _():
        for t in range(NC * SUB):
            end_copy(0, t).wait_send()

    @pl.when(inner)
    def _():
        for t in range(NC * SUB):
            peer_copy(0, t).wait_send()
            back_copy(0, 1, t).wait_send()
    vout.wait()


def finish(y, gq, go, gu, gd, gv, yo, qo, oo, uo, do, n0, n1, n2, n3, n4, n5, n6, bq, yb, qb, ob, ub, db, got, put):
    trips = [(gd, db, do), (gu, ub, uo), (go, ob, oo), (gq, qb, qo)]
    trips += [tuple(ref.at[m, r] for ref in (y, yb, yo)) for m in range(y.shape[0]) for r in range(y.shape[1])]
    loads = [pltpu.make_async_copy(a, b, got.at[k]) for k, (a, b, o) in enumerate(trips)]
    stores = [pltpu.make_async_copy(b, o, put.at[k]) for k, (a, b, o) in enumerate(trips)]
    for cp in loads:
        cp.start()
    for row, refs in enumerate(((n0,), (n1,), (n2,), (n3,), (n4, n5), (n6,))):
        for ref in refs:
            ref[...] = gv[row:row + 1, :]
    e = bq.shape[2]
    for k in range(3):
        for h in range(2):
            bq[k, h:h + 1, :] = gv[6:7, (2 * k + h) * e:(2 * k + h + 1) * e]
    for cp, out in zip(loads, stores):
        cp.wait()
        out.start()
    for cp in stores:
        cp.wait()


def finish_step(y, gq, go, gu, gd, gv, e):
    hbm, vmem = pl.BlockSpec(memory_space=pl.ANY), pl.BlockSpec(memory_space=pltpu.VMEM)
    big = [jax.ShapeDtypeStruct(a.shape, a.dtype) for a in (y, gq, go, gu, gd)]
    row = jax.ShapeDtypeStruct((1, gv.shape[1]), F32)
    return pl.pallas_call(
        finish,
        out_shape=big + [row] * 7 + [jax.ShapeDtypeStruct((3, 2, e), F32)],
        in_specs=[hbm] * 5 + [vmem],
        out_specs=[hbm] * 5 + [vmem] * 8,
        scratch_shapes=[pltpu.VMEM(a.shape, a.dtype) for a in big] + [pltpu.SemaphoreType.DMA((8,))] * 2,
        name='neox_out',
    )(y, gq, go, gu, gd, gv)


def group_step(dims, *args):
    x = args[0]
    S, D, E, C, F = dims
    E2 = 2 * E
    hbm = pl.BlockSpec(memory_space=pl.ANY)
    out_shape = [
        jax.ShapeDtypeStruct(x.shape, BF16),
        jax.ShapeDtypeStruct((3 * E2, D), F32),
        jax.ShapeDtypeStruct((E2, D), F32),
        jax.ShapeDtypeStruct((D, F), F32),
        jax.ShapeDtypeStruct((F, D), F32),
        jax.ShapeDtypeStruct((8, D), F32),
    ]

    def vm(*shape, dtype=BF16):
        return pltpu.VMEM(shape, dtype)
    dma = pltpu.SemaphoreType.DMA
    scratch = [
        vm(NL, 3 * E2, D), vm(NL, E2, D), vm(NL, D, F), vm(NL, F, D), vm(NL, 8, D, dtype=F32),
        vm(NL + 2, S, D),
        vm(NL, S, E2), vm(NL, S, E2), vm(NL, S, E2), vm(NL, E2, S), vm(E2, S), vm(NL, S, E2),
        *[vm(NL, 2, (i + 1) * C, C) for i in range(NC)],
        vm(NL, S, F), vm(NL + 1, S, F, dtype=F32),
        vm(2, S, D), vm(2, S, D), vm(S, D), vm(S + C, D, dtype=F32),
        vm(2, 3 * E2, D, dtype=F32), vm(2, E2, D, dtype=F32), vm(2, D, F, dtype=F32), vm(2, F, D, dtype=F32),
        vm(2, 3 * E, D), vm(2, E, D), vm(2, D // 2, F), vm(2, F // 2, D),
        vm(S, E2, dtype=F32), vm(S, E2, dtype=F32),
        vm(2, C + 8, E2, dtype=F32), vm(S, E2, dtype=F32), vm(S, E2, dtype=F32),
        vm(NL, 8, D, dtype=F32), vm(NL, NT, 8, D, dtype=F32), vm(NL, 8, D, dtype=F32), vm(NL, 8, D, dtype=F32),
        vm(C, D), vm(C, D), vm(C, max(D, F), dtype=F32), vm(C, F), vm(S, C), vm(S, C, dtype=F32),
        *[vm(1, D, dtype=F32)] * 4, vm(1, D), vm(1, D), vm(1, F), vm(3, 2, E),
        dma((NA,)), dma((NA + 1,)), dma((2, NA + 1)), dma((NL, 2 * NA + 1)), dma((2, NA)), dma((2,)), dma((1,)),
        dma((NC * SUB,)), dma((NC * SUB,)), dma((2, NC * SUB)), dma((2, NC * SUB)), dma((2, NC * SUB)),
        dma((NL,)), dma((NL,)), dma((NA,)), dma((2, NA)), dma((2, NA)), dma((2, NA)), dma((2, NA)), dma((NA,)),
        dma((NL, NT - 1)), dma((NL, NT)), dma((NL,)), dma((NL,)), dma((1,)), dma((8,)),
    ]
    return pl.pallas_call(
        functools.partial(body, dims),
        out_shape=out_shape,
        in_specs=[hbm] * len(args),
        out_specs=[hbm] * 6,
        scratch_shapes=scratch,
        compiler_params=pltpu.CompilerParams(collective_id=0, has_side_effects=True, vmem_limit_bytes=67043328),
        name='neox_group',
    )(*args)


def solution(mesh):
    def device_fn(x_in, g_out, ln1_gain, ln1_bias, w_qkv, b_qkv, w_out, b_out, ln2_gain, ln2_bias, w_up, b_up, w_down, b_down):
        n_micro, n_rows, S, D = x_in.shape
        heads, E = w_qkv.shape[2], w_qkv.shape[4]
        F = w_up.shape[2]
        C = S // NC
        wqkv = jnp.transpose(w_qkv[0], (1, 2, 3, 0)).reshape(heads * 3 * E, D)
        bqkv = jnp.transpose(b_qkv[0], (1, 0, 2))
        tab = jnp.asarray(rotary_base(C, NC, E, heads))
        part = group_step((S, D, E, C, F), x_in, g_out, wqkv, w_out[0].reshape(heads * E, D), w_up[0], w_down[0], ln1_gain, ln1_bias, ln2_gain, ln2_bias, b_out, b_down, b_up, bqkv, tab)
        y, gq, go, gup, gdn, n1g, n1b, n2g, n2b, gbo, gbd, gbu, gbq = finish_step(*part, E)
        gq = jnp.transpose(gq.reshape(heads, 3, E, D), (3, 0, 1, 2))[None]
        gbq = jnp.transpose(gbq, (1, 0, 2))[None]
        return (y, n1g, n1b, gq, gbq, go.reshape(1, heads, E, D), gbo, n2g, n2b, gup[None], gbu, gdn[None], gbd)

    return jax.shard_map(device_fn, mesh=mesh, in_specs=(P('dp'), P('dp')) + STAGE_SPECS, out_specs=(P('dp'),) + GRAD_SPECS, check_vma=False)
```

```python
import functools
import math

import jax
import jax.numpy as jnp
import numpy as np
from jax import lax
from jax.experimental import pallas as pl
from jax.experimental.pallas import tpu as pltpu
from jax.sharding import PartitionSpec as P

ROPE_BASE = 10000.0
LN_EPS = 1e-5
STAGE_SPECS = (P('pp'), P('pp'), P('pp', None, 'tp'), P('pp', 'tp'), P('pp', 'tp'), P('pp'), P('pp'), P('pp'), P('pp', None, 'tp'), P('pp', 'tp'), P('pp', 'tp'), P('pp'))
OWN = ('dp', 'pp')
GRAD_SPECS = (P(OWN), P(OWN), P(OWN, None, 'tp'), P(OWN, 'tp'), P(OWN, 'tp'), P(OWN), P(OWN), P(OWN), P(OWN, None, 'tp'), P(OWN, 'tp'), P(OWN, 'tp'), P(OWN))


F32 = jnp.float32
BF16 = jnp.bfloat16
NL = 4
NT = 4
NC = 4
NA = 4
CORES = 2
SUB = 2
FWD_AT = {0: (('mid', 1, 0), ('last', 2, 0)), 2: (('mid', 1, 1), ('last', 2, 1))}
BWD_AT = {0: (('last', 2, 0),), 1: (('mid', 1, 0),), 3: (('last', 2, 1),), 4: (('mid', 1, 1),)}
LOG2E = 1.4426950408889634
RSQRT2 = 0.7071067811865476
INV_SQRT_2PI = 0.3989422804014327


def nn(a, b):
    return lax.dot_general(a, b, (((1,), (0,)), ((), ())), preferred_element_type=F32)


def nt(a, b):
    return lax.dot_general(a, b, (((1,), (1,)), ((), ())), preferred_element_type=F32)


def tn(a, b):
    return lax.dot_general(a, b, (((0,), (0,)), ((), ())), preferred_element_type=F32)


def col_sum(v):
    return jnp.sum(v, axis=0, keepdims=True)


def row_mean(v):
    return jnp.mean(v, axis=-1, keepdims=True)


def fold(v):
    return jnp.sum(v.reshape(v.shape[0] // 8, 8, v.shape[1]), axis=0)


def rotary_base(chunk, n_chunks, head_dim, n_heads):
    rot_dim = head_dim // 4
    half = rot_dim // CORES
    inv_freq = np.zeros((head_dim,), np.float64)
    inv_freq[:rot_dim] = np.tile(ROPE_BASE ** (-(np.arange(half) * 2.0) / rot_dim), 2)
    inv_freq = np.tile(inv_freq, n_heads)
    pos = np.concatenate([np.arange(chunk), np.arange(8) * (np.arange(8) < n_chunks) * chunk]).astype(np.float64)
    ang = pos[:, None] * inv_freq[None, :]
    return np.stack([np.cos(ang), np.sin(ang)]).astype(np.float32)


def body(dims, x, g, wqkv, wo, wup, wdn, n0, n1, n2, n3, n4, n5, n6, bq, tab,
         y, oqkv, oo, oup, odn, ovec,
         WQ, WO, WU, WD, VEC, H, Q, K, V, KT, VT, CTX, P0, P1, P2, P3, HID, GP, RA, RB, PS, PF,
         GQ, GO, GU, GD, R2Q, R2O, R2U, R2D, DK, DV, TAB, COS, SIN, GV, ZR, GZ, PR,
         AS, MS, PRE, DPB, DS, ST, N0, N1, N2, N3, N4, N5, N6, BQ,
         wl, ws, wy, wr, wf, w0s, w0r, xs, gs, sab, sc, ra_s, rb_s, rc_s, ys, yr, g1s, g1r, g2s, g2r, g3s, g3r, v1s, v1r, v2s, v2r, osem, ns):
    S, D, E, C, F = dims
    E2 = 2 * E
    SR = C // SUB
    z = lax.axis_index('tp')
    xg = lax.axis_index('dp')
    s = lax.axis_index('pp')
    ys_ = s // CORES
    c = s % CORES
    sib = s + 1 - 2 * c
    oy = 2 * (1 - ys_)
    is_end = z * (NT - 1 - z) == 0
    inner = z * (NT - 1 - z) > 0
    hub = 1 + z // 3
    leaf = jnp.where(z == 1, 0, 3)
    peer = 3 - z
    PX = (P0, P1, P2, P3)
    W_IN = (wqkv, wo, wup, wdn)
    W_BUF = (WQ, WO, WU, WD)
    G_HALF = (3 * E, E, D // CORES, F // CORES)
    ALL, FIRST, REST = tuple(range(NA)), (0,), (1, 2, 3)
    ATT, MLP = ALL[:2], ALL[2:]
    G_BUF = (GQ, GO, GU, GD)
    G_OUT = (oqkv, oo, oup, odn)
    G_COLS = (D, D, F, D)
    R1_OFF = (0, 3 * E, 4 * E, 4 * E + D // CORES)
    R2 = (R2Q, R2O, R2U, R2D)

    def rcopy(src, dst, ss, rs, **dev):
        return pltpu.make_async_remote_copy(src_ref=src, dst_ref=dst, send_sem=ss, recv_sem=rs, device_id=dev, device_id_type=pl.DeviceIdType.MESH)

    def lcopy(src, dst, sem):
        return pltpu.make_async_copy(src, dst, sem)

    def rows(start, n):
        return pl.ds(pl.multiple_of(start, n), n)

    xcopy = lcopy(x.at[ys_, c], H.at[0], xs.at[0])
    xcopy.start()
    gcopy = lcopy(g.at[ys_, c], GP.at[NL], gs.at[0])
    gcopy.start()
    tcopy = lcopy(tab, TAB, xs.at[1])
    tcopy.start()
    for a in range(NA):
        lcopy(W_IN[a], W_BUF[a].at[s], wl.at[a]).start()
    small = [lcopy(a, b, ns.at[k]) for k, (a, b) in enumerate(((n0, N0), (n1, N1), (n2, N2), (n3, N3), (n4, N4), (n5, N5), (n6, N6), (bq, BQ)))]
    for cp in small:
        cp.start()

    bar = pltpu.get_barrier_semaphore()
    for o in range(1, NT):
        pl.semaphore_signal(bar, inc=1, device_id={'tp': (z + o) % NT}, device_id_type=pl.DeviceIdType.MESH)
    for o in range(1, NL):
        pl.semaphore_signal(bar, inc=1, device_id={'pp': (s + o) % NL}, device_id_type=pl.DeviceIdType.MESH)
    pl.semaphore_signal(bar, inc=1, device_id={'dp': 1 - xg}, device_id_type=pl.DeviceIdType.MESH)
    pl.semaphore_wait(bar, NT + NL - 1)

    def half(ref, a, k):
        return ref.at[rows(k * G_HALF[a], G_HALF[a])]

    def sib_copies():
        out = [rcopy(W_IN[a], W_BUF[a].at[s], ws.at[a], wr.at[s, 2 * a], pp=sib) for a in ALL]
        return out + [rcopy(VEC.at[s], VEC.at[s], ws.at[NA], wr.at[s, 2 * NA], pp=sib)]

    def y_copies():
        out = [rcopy(half(W_IN[a], a, k), half(W_BUF[a].at[s], a, k), wy.at[k, a], wr.at[s, 2 * a + k], pp=oy + k) for a in ALL for k in range(CORES)]
        return out[:2] + [rcopy(VEC.at[s], VEC.at[s], wy.at[k, NA], wr.at[s, 2 * NA], pp=oy + k) for k in range(CORES)] + out[2:]

    def quarter(ref, a, q):
        return ref.at[rows(q * (G_HALF[a] // CORES), G_HALF[a] // CORES)]

    def first_copies():
        out = []
        for a in ALL:
            for k in range(CORES):
                q = 2 * xg + k
                out.append(rcopy(quarter(W_IN[a], a, q), quarter(W_BUF[a].at[0], a, q), wy.at[k, a], w0r.at[a, q], pp=oy + k))
        return out + [rcopy(VEC.at[s], VEC.at[s], wy.at[k, NA], wr.at[s, 2 * NA], pp=oy + k) for k in range(CORES)]

    def mine(hop):
        return 2 * (xg if hop == 0 else 1 - xg) + c

    def hop_copies(a, hop):
        part, sem = quarter(W_BUF[a].at[0], a, mine(hop)), w0r.at[a, mine(hop)]
        out = [rcopy(part, part, w0s.at[hop, a], sem, pp=sib)]
        return out if hop else out + [rcopy(part, part, w0s.at[2, a], sem, dp=1 - xg)]

    def hop_on(a, hop):
        copies = hop_copies(a, hop)
        copies[0].wait_recv()
        start_all(copies)

    def hop_end(a):
        for k in range(CORES):
            part = quarter(W_BUF[a].at[0], a, 2 * k + 1 - c)
            rcopy(part, part, w0s.at[0, a], w0r.at[a, 2 * k + 1 - c], pp=sib).wait_recv()

    def start_all(copies):
        for cp in copies:
            cp.start()

    for cp in small:
        cp.wait()
    for k, ref in enumerate((N0, N1, N2, N3, N4, N5, N6)):
        VEC[s, k:k + 1, :] = ref[...].astype(F32)
    VEC[s, 7:8, :3 * E2] = jnp.concatenate([BQ[k, h:h + 1, :].astype(F32) for k in range(3) for h in range(CORES)], axis=1)

    @pl.when(s == 0)
    def _():
        start_all(first_copies())

    @pl.when(s > 1)
    def _():
        start_all(y_copies())
    start_all(sib_copies())

    def pass_copy(l, a, k):
        part = half(W_BUF[a].at[l], a, k)
        return rcopy(part, part, wf.at[l % CORES, a], wr.at[l, 2 * a + k], pp=sib)

    def relay(l, arrays):
        @pl.when(l // CORES != ys_)
        def _():
            for a in arrays:
                pass_copy(l, a, c).wait_recv()
                pass_copy(l, a, c).start()

    def settle(l, arrays, small):
        @pl.when(l == s)
        def _():
            for a in arrays:
                lcopy(W_IN[a], W_BUF[a].at[s], wl.at[a]).wait()

        @pl.when(l == sib)
        def _():
            for a in arrays:
                rcopy(W_IN[a], W_BUF[a].at[l], ws.at[a], wr.at[l, 2 * a], pp=sib).wait_recv()

        @pl.when((l // CORES != ys_) & (l > 0))
        def _():
            for a in arrays:
                pass_copy(l, a, 1 - c).wait_recv()
        if small:
            @pl.when(l != s)
            def _():
                rcopy(VEC.at[l], VEC.at[l], ws.at[NA], wr.at[l, 2 * NA], pp=sib).wait_recv()

    tcopy.wait()
    for i in range(NC):
        cb, sb = TAB[0, :C, :], TAB[1, :C, :]
        cr, sr = TAB[0, C + i:C + i + 1, :], TAB[1, C + i:C + i + 1, :]
        COS[i * C:(i + 1) * C, :] = cb * cr - sb * sr
        SIN[i * C:(i + 1) * C, :] = sb * cr + cb * sr

    lane = lax.broadcasted_iota(jnp.int32, (C, E2), 1)
    head_lane = lane // E
    in_head = lane % E
    rot_half = E // 8
    low = in_head < rot_half
    sub_head = lax.broadcasted_iota(jnp.int32, (E2, C), 0) // E
    lower = lax.broadcasted_iota(jnp.int32, (C, C), 0) <= lax.broadcasted_iota(jnp.int32, (C, C), 1)
    c1 = E ** -0.5 * LOG2E

    def tabs(i):
        cs, sn = COS[i * C:(i + 1) * C, :], SIN[i * C:(i + 1) * C, :]
        return cs, jnp.where(low, -sn, 0.0), jnp.where(low, 0.0, sn)

    def rotate(v, t):
        cs, sa, sb = t
        return v * cs + pltpu.roll(v, E2 - rot_half, 1) * sa + pltpu.roll(v, rot_half, 1) * sb

    def unrotate(v, t):
        cs, sa, sb = t
        return v * cs + pltpu.roll(v * sa, rot_half, 1) + pltpu.roll(v * sb, E2 - rot_half, 1)

    def end_copy(p, t):
        return rcopy(PS.at[t * SR:(t + 1) * SR], RA.at[p % CORES, t * SR:(t + 1) * SR], sab.at[t], ra_s.at[p % CORES, t], tp=hub)

    def peer_copy(p, t):
        return rcopy(PS.at[t * SR:(t + 1) * SR], RB.at[p % CORES, t * SR:(t + 1) * SR], sab.at[t], rb_s.at[p % CORES, t], tp=peer)

    def back_copy(p, di, t):
        return rcopy(H.at[di, t * SR:(t + 1) * SR], H.at[di, t * SR:(t + 1) * SR], sc.at[t], rc_s.at[p % CORES, t], tp=leaf)

    def pf_row(i, back):
        return (NC if back and i == NC - 1 else i) * C

    def ar_send(p, i, back=False):
        @pl.when(is_end)
        def _():
            for t in range(i * SUB, (i + 1) * SUB):
                @pl.when(p > 0)
                def _():
                    end_copy(p, t).wait_send()
                f0 = pf_row(i, back) + (t - i * SUB) * SR
                PS[t * SR:(t + 1) * SR, :] = PF[f0:f0 + SR, :].astype(BF16)
                end_copy(p, t).start()

    def ar_mid(p, i, u, back=False):
        t = i * SUB + u
        r = slice(t * SR, (t + 1) * SR)
        f0 = pf_row(i, back) + u * SR

        @pl.when(inner)
        def _():
            end_copy(p, t).wait_recv()
            @pl.when(p > 0)
            def _():
                peer_copy(p, t).wait_send()
            PS[r, :] = (PF[f0:f0 + SR, :] + RA[p % CORES, r, :].astype(F32)).astype(BF16)
            peer_copy(p, t).start()

    def ar_last(p, ri, di, i, u):
        t = i * SUB + u
        r = slice(t * SR, (t + 1) * SR)

        @pl.when(inner)
        def _():
            lv = jnp.minimum(p, NL - 1)
            bias = (VEC[lv, 4:5, :] + VEC[lv, 5:6, :]) * jnp.where(p < NL, 1.0, 0.0)
            peer_copy(p, t).wait_recv()
            @pl.when(p > 0)
            def _():
                back_copy(p, di, t).wait_send()
            both = PS[r, :].astype(F32) + RB[p % CORES, r, :].astype(F32)
            H[di, r, :] = (H[ri, r, :].astype(F32) + both + bias).astype(BF16)
            back_copy(p, di, t).start()

    def ar_wait(p, di, i):
        @pl.when(is_end)
        def _():
            for t in range(i * SUB, (i + 1) * SUB):
                back_copy(p, di, t).wait_recv()

    def stats(hf):
        cen = hf - row_mean(hf)
        rstd = lax.rsqrt(row_mean(cen * cen) + LN_EPS)
        return cen * rstd, rstd

    LB = 32
    GR = 32

    def norms(l, i):
        g1, b1, g2, b2 = (VEC[l, k:k + 1, :] for k in range(NA))

        def step(b, carry):
            hf = H[l, rows(i * C + b * LB, LB), :].astype(F32)
            xhat, unused = stats(hf)
            AS[rows(b * LB, LB), :] = (xhat * g1 + b1).astype(BF16)
            MS[rows(b * LB, LB), :] = (xhat * g2 + b2).astype(BF16)
            return carry
        lax.fori_loop(0, C // LB, step, 0, unroll=True)

    def by_kind():
        return [(h * 3 + k) * E for k in range(3) for h in range(CORES)]

    def wq(l):
        return jnp.concatenate([WQ[l, r:r + E, :] for r in by_kind()], axis=0)

    def forward(l, i):
        r0, r1 = i * C, (i + 1) * C
        norms(l, i)
        qkv = nt(AS[...], wq(l)) + VEC[l, 7:8, :3 * E2]
        qkv = qkv.astype(BF16).astype(F32)
        t = tabs(i)
        q = rotate(qkv[:, :E2], t).astype(BF16)
        kf = rotate(qkv[:, E2:2 * E2], t)
        vf = qkv[:, 2 * E2:3 * E2]
        Q[l, r0:r1, :] = q
        K[l, r0:r1, :] = kf.astype(BF16)
        V[l, r0:r1, :] = vf.astype(BF16)
        KT[l, :, r0:r1] = jnp.transpose(kf).astype(BF16)
        VT[:, r0:r1] = jnp.transpose(vf).astype(BF16)
        yield
        RBK = C // CORES
        outs = []
        for h in range(CORES):
            qm = jnp.where(head_lane == h, Q[l, r0:r1, :].astype(F32), 0.0).astype(BF16)
            ST[:r1, :] = nt(K[l, :r1, :], qm)
            ST[r0:r1, :] = jnp.where(lower, ST[r0:r1, :], -1e30)

            def top(b, m):
                return jnp.maximum(m, jnp.max(ST[rows(b * RBK, RBK), :].reshape(RBK // 8, 8, C), axis=0))
            m = jnp.max(lax.fori_loop(0, r1 // RBK, top, jnp.full((8, C), -3e38, F32), unroll=True), axis=0, keepdims=True)
            mc = m * c1

            def expo(b, tot):
                e = jnp.exp2(ST[rows(b * RBK, RBK), :] * c1 - mc)
                ST[rows(b * RBK, RBK), :] = e
                return tot + fold(e)
            tot = col_sum(lax.fori_loop(0, r1 // RBK, expo, jnp.zeros((8, C), F32), unroll=True))
            inv = 1.0 / tot

            def put(b, carry):
                PX[i][l, h, rows(b * RBK, RBK), :] = (ST[rows(b * RBK, RBK), :] * inv).astype(BF16)
                return carry
            lax.fori_loop(0, r1 // RBK, put, 0, unroll=True)
            outs.append(nn(VT[:, :r1], PX[i][l, h]))
            if h == 0:
                yield
        ctx = jnp.transpose(jnp.where(sub_head == 0, outs[0], outs[1])).astype(BF16)
        CTX[l, r0:r1, :] = ctx
        yield
        if i == 0:
            @pl.when((l == 0) & (ys_ == 1))
            def _():
                hop_on(3, 0)
                hop_on(2, 1)
                hop_on(3, 1)
                for a in REST:
                    hop_end(a)
            settle(l, REST, False)
        PF[r0:r1, :] = nn(ctx, WO[l])
        PRE[...] = nn(MS[...], WU[l])
        bup = VEC[l, 6:7, :]
        GB = 32

        def act(b, carry):
            u = PRE[rows(b * GB, GB), :] + bup
            cdf = 0.5 * (1.0 + lax.erf(u * RSQRT2))
            pdf = jnp.exp2(u * u * (-0.5 * LOG2E)) * INV_SQRT_2PI
            HID[l, rows(r0 + b * GB, GB), :] = (u * cdf).astype(BF16)
            GP[l, rows(r0 + b * GB, GB), :] = cdf + u * pdf
            return carry
        lax.fori_loop(0, C // GB, act, 0, unroll=True)
        PF[r0:r1, :] += nn(HID[l, r0:r1, :], WD[l])
        yield

    def backward(l, dl, i, last):
        r0, r1 = i * C, (i + 1) * C
        par = l % CORES
        first = i == NC - 1

        def acc(ref, val):
            if first:
                ref[par] = val
            else:
                ref[par] += val

        def acc_row(k, val, w=D):
            GV[l, k:k + 1, :w] += val

        norms(l, i)
        dy = H[dl, r0:r1, :]
        acc_row(4, col_sum(dy.astype(F32)))
        PRE[...] = nt(dy, WD[l])
        GB = 32

        def act(b, tot):
            d = PRE[rows(b * GB, GB), :] * GP[l, rows(r0 + b * GB, GB), :]
            DPB[rows(b * GB, GB), :] = d.astype(BF16)
            return tot + fold(d)
        dbu = lax.fori_loop(0, C // GB, act, jnp.zeros((8, F), F32), unroll=True)
        acc_row(5, col_sum(dbu))
        acc(GD, tn(HID[l, r0:r1, :], dy))
        yield
        acc(GU, tn(MS[...], DPB[...]))
        f0 = pf_row(i, True)
        PF[f0:f0 + C, :] = nt(DPB[...], WU[l])
        yield
        dctx = nt(dy, WO[l]).astype(BF16)
        ctx = CTX[l, r0:r1, :]
        acc(GO, tn(ctx, dy))
        prod = dctx.astype(F32) * ctx.astype(F32)
        q = Q[l, r0:r1, :].astype(F32)
        dcf = dctx.astype(F32)
        RBK = C // CORES
        dqt = []
        for h in range(CORES):
            sel = head_lane == h
            qm = jnp.where(sel, q, 0.0).astype(BF16)
            dcm = jnp.where(sel, dcf, 0.0).astype(BF16)
            dsum = jnp.transpose(jnp.where(sel, prod, 0.0))
            drow = col_sum(dsum)
            ST[:r1, :] = nt(V[l, :r1, :], dcm)

            def sub(b, carry):
                pr = PX[i][l, h, rows(b * RBK, RBK), :].astype(F32)
                DS[rows(b * RBK, RBK), :] = (pr * (ST[rows(b * RBK, RBK), :] - drow)).astype(BF16)
                return carry
            lax.fori_loop(0, r1 // RBK, sub, 0, unroll=True)
            dk = nn(DS[:r1, :], qm)
            dv = nn(PX[i][l, h], dcm)
            if first and h == 0:
                DK[:r1, :] = dk
                DV[:r1, :] = dv
            else:
                DK[:r1, :] += dk
                DV[:r1, :] += dv
            dqt.append(nn(KT[l, :, :r1], DS[:r1, :]))
            yield
        scale = E ** -0.5
        t = tabs(i)
        dq = unrotate(jnp.transpose(jnp.where(sub_head == 0, dqt[0], dqt[1])) * scale, t)
        dk = unrotate(DK[r0:r1, :] * scale, t)
        dv = DV[r0:r1, :]
        dqkv = jnp.concatenate([dq, dk, dv], axis=1)
        acc_row(6, col_sum(dqkv), 3 * E2)
        dqkv = dqkv.astype(BF16)
        dwq = tn(dqkv, AS[...])
        for k, r in enumerate(by_kind()):
            if first:
                GQ[par, r:r + E, :] = dwq[k * E:(k + 1) * E]
            else:
                GQ[par, r:r + E, :] += dwq[k * E:(k + 1) * E]
        PRE[...] = nn(dqkv, wq(l))
        yield
        g1, g2 = VEC[l, 0:1, :], VEC[l, 2:3, :]

        def lnb(b, tots):
            hf = H[l, rows(r0 + b * LB, LB), :].astype(F32)
            xhat, rstd = stats(hf)
            da = PRE[rows(b * LB, LB), :]
            dm = PF[rows(f0 + b * LB, LB), :]
            dx = da * g1 + dm * g2
            m1 = row_mean(dx)
            m2 = row_mean(dx * xhat)
            if not last:
                PF[rows(f0 + b * LB, LB), :] = rstd * (dx - m1 - xhat * m2)
            terms = (da * xhat, da, dm * xhat, dm)
            return tuple(a + fold(v) for a, v in zip(tots, terms))
        tots = lax.fori_loop(0, C // LB, lnb, tuple(jnp.zeros((8, D), F32) for _ in range(NA)), unroll=True)
        for k in range(NA):
            acc_row(k, col_sum(tots[k]))
        yield

    def g_half(a, k):
        return rows(k * G_HALF[a], G_HALF[a])

    def r1_view(l, a):
        return GP.at[l + 1, R1_OFF[a]:R1_OFF[a] + G_HALF[a], :G_COLS[a]]

    def g1_copy(l, a):
        return rcopy(G_BUF[a].at[l % CORES, g_half(a, 1 - c)], r1_view(l, a), g1s.at[a], g1r.at[l % CORES, a], pp=sib)

    def g2_copy(l, a):
        return rcopy(HID.at[l, R1_OFF[a]:R1_OFF[a] + G_HALF[a], :G_COLS[a]], R2[a].at[l % CORES], g2s.at[l % CORES, a], g2r.at[l % CORES, a], pp=2 * (l // CORES) + c)

    def g3_local(l, a):
        return lcopy(r1_view(l, a), G_OUT[a].at[g_half(a, c)], g3s.at[l % CORES, a])

    def g3_remote(l, a):
        return rcopy(r1_view(l, a), G_OUT[a].at[g_half(a, c)], g3s.at[l % CORES, a], g3r.at[a], pp=sib)

    def v1_copies(l):
        return [rcopy(GV.at[l], ZR.at[l, z], v1s.at[l, o - 1], v1r.at[l, z], tp=(z + o) % NT) for o in range(1, NT)]

    def grads_mid(l, arrays):
        for a in arrays:
            g1_copy(l, a).wait_recv()
            n = G_HALF[a]

            def add(b, carry):
                rr = rows(R1_OFF[a] + b * GR, GR)
                tot = G_BUF[a][l % CORES, rows(c * n + b * GR, GR), :] + GP[l + 1, rr, :G_COLS[a]]
                GP[l + 1, rr, :G_COLS[a]] = tot
                HID[l, rr, :G_COLS[a]] = tot.astype(BF16)
                return carry
            lax.fori_loop(0, n // GR, add, 0)

            @pl.when(l // CORES != ys_)
            def _():
                g2_copy(l, a).start()

    def grads_last(l):
        @pl.when(l // CORES == ys_)
        def _():
            for a in MLP + ATT:
                g2_copy(l, a).wait_recv()

                def add(b, carry):
                    rr = rows(R1_OFF[a] + b * GR, GR)
                    GP[l + 1, rr, :G_COLS[a]] += R2[a][l % CORES, rows(b * GR, GR), :].astype(F32)
                    return carry
                lax.fori_loop(0, G_HALF[a] // GR, add, 0)

                @pl.when(l == s)
                def _():
                    g3_local(l, a).start()

                @pl.when(l != s)
                def _():
                    g3_remote(l, a).start()

    def grads_sent(l):
        for a in range(NA):
            @pl.when(l // CORES != ys_)
            def _():
                g2_copy(l, a).wait_send()

            @pl.when(l == s)
            def _():
                g3_local(l, a).wait()

            @pl.when((l // CORES == ys_) & (l != s))
            def _():
                g3_remote(l, a).wait_send()

    def v2_copy(l):
        return rcopy(GZ.at[l], PR.at[s], v2s.at[l], v2r.at[s], pp=l)

    def vec_mid(l):
        ZR[l, z] = GV[l]
        for o in range(1, NT):
            q = (z + o) % NT
            rcopy(GV.at[l], ZR.at[l, q], v1s.at[l, o - 1], v1r.at[l, q], tp=q).wait_recv()
        tot = ZR[l, 0] + ZR[l, 1] + ZR[l, 2] + ZR[l, 3]
        row = lax.broadcasted_iota(jnp.int32, (8, D), 0)
        GZ[l] = jnp.where(row < 4, tot, GV[l])

        @pl.when(l == s)
        def _():
            PR[s] = GZ[l]

        @pl.when(l != s)
        def _():
            v2_copy(l).start()

    GV[...] = jnp.zeros_like(GV)
    @pl.when(ys_ == 1)
    def _():
        for a, hop in ((0, 0), (1, 0), (0, 1), (2, 0), (1, 1)):
            hop_on(a, hop)
        hop_end(0)
    settle(0, FIRST, True)
    xcopy.wait()

    def run(phases, at, handle, after=lambda k: None):
        for k, unused in enumerate(phases):
            after(k)
            for op, lag, u in at.get(k, ()):
                handle(op, lag, u)

    def fwd_layer(l, carry):
        for i in range(NC):
            @pl.when(l > 0)
            def _():
                ar_wait(l - 1, l, i)

            def handle(op, lag, u):
                m = i - lag

                def go(p, j):
                    if op == 'mid':
                        ar_mid(p, j, u)
                    else:
                        ar_last(p, p, p + 1, j, u)
                if m >= 0:
                    go(l, m)
                else:
                    @pl.when(l > 0)
                    def _():
                        go(l - 1, m + NC)
            run(forward(l, i), FWD_AT, handle)
            ar_send(l, i)
            if i == 1:
                @pl.when(l == 0)
                def _():
                    gcopy.wait()
                    H[NL + 1] = GP[NL].astype(BF16)

                    @pl.when(s == 1)
                    def _():
                        start_all(y_copies())
            if i == 2:
                @pl.when((l > 0) & (l < NL - 1))
                def _():
                    relay(l + 1, ALL)
            if i == NC - 1:
                @pl.when(l == 0)
                def _():
                    relay(l + 1, ALL)

                @pl.when(l < NL - 1)
                def _():
                    settle(l + 1, FIRST, True)
        return carry
    lax.fori_loop(0, NL, fwd_layer, 0)

    y_local = lcopy(H.at[NL], y.at[ys_, c], ys.at[0])
    y_sib = rcopy(H.at[NL], y.at[ys_, c], ys.at[1], yr.at[s], pp=sib)
    y_far = rcopy(H.at[NL], y.at[ys_, c], ys.at[2], yr.at[s], pp=oy + c)
    y_fwd = rcopy(y.at[1 - ys_, c], y.at[1 - ys_, c], ys.at[3], yr.at[oy + c], pp=sib)

    def y_arrived(q):
        rcopy(H.at[NL], y.at[q // CORES, q % CORES], ys.at[1], yr.at[q], pp=sib).wait_recv()

    def ri(l):
        return jnp.where(l == NL - 1, NL + 1, l + 1)

    def bwd_layer(lb, carry):
        l = NL - 1 - lb
        p = NL + lb
        for n in range(NC):
            i = NC - 1 - n

            @pl.when(lb > 0)
            def _():
                ar_wait(p - 1, l + 1, i)

            def handle(op, lag, u):
                m = n - lag

                def go(q, lq, j):
                    if op == 'mid':
                        ar_mid(q, j, u, True)
                    else:
                        ar_last(q, ri(lq), lq, j, u)
                if m >= 0:
                    @pl.when(l > 0)
                    def _():
                        go(p, l, NC - 1 - m)
                else:
                    @pl.when(lb > 0)
                    def _():
                        go(p - 1, l + 1, -1 - m)

                    @pl.when(lb == 0)
                    def _():
                        if op == 'mid':
                            ar_mid(NL - 1, m + NC, u)
                        else:
                            ar_last(NL - 1, NL - 1, NL, m + NC, u)

            def after(k):
                if k == 0 and n == 0:
                    @pl.when(lb > 0)
                    def _():
                        grads_mid(l + 1, ATT)
                        for a in ALL:
                            g1_copy(l + 1, a).wait_send()
                if k == 1 and n == NC - 1:
                    for a in MLP:
                        g1_copy(l, a).start()
            run(backward(l, ri(l), i, False), BWD_AT, handle, after)

            @pl.when(l > 0)
            def _():
                ar_send(p, i, True)
            if n == 1:
                @pl.when(lb > 0)
                def _():
                    vec_mid(l + 1)
            if n == 2:
                @pl.when(lb == 0)
                def _():
                    for j in range(NC):
                        ar_wait(NL - 1, NL, j)
                    start_all((y_local, y_sib, y_far))

                @pl.when(lb > 1)
                def _():
                    grads_last(l + 2)

        for a in ATT:
            g1_copy(l, a).start()
        start_all(v1_copies(l))
        grads_mid(l, MLP)
        return carry
    lax.fori_loop(0, NL, bwd_layer, 0)

    grads_mid(0, ATT)
    y_arrived(oy + c)
    y_fwd.start()
    grads_last(1)
    vec_mid(0)
    grads_last(0)

    for o in range(1, NL):
        q = (s + o) % NL
        rcopy(GZ.at[0], PR.at[q], v2s.at[0], v2r.at[q], pp=q).wait_recv()
    PRE[0:8, 0:D] = PR[0] + PR[1] + PR[2] + PR[3]
    vout = lcopy(PRE.at[0:8, 0:D], ovec, osem.at[0])
    vout.start()
    for l in range(NL):
        for cp in v1_copies(l):
            cp.wait_send()
    for l in range(NL):
        @pl.when(l != s)
        def _():
            v2_copy(l).wait_send()
    for a in range(NA):
        rcopy(G_OUT[a].at[g_half(a, 1 - c)], G_OUT[a].at[g_half(a, 1 - c)], g3s.at[a], g3r.at[a], pp=sib).wait_recv()
    y_local.wait()
    for cp in (y_sib, y_far, y_fwd):
        cp.wait_send()
    y_arrived(sib)
    y_arrived(oy + 1 - c)
    for a in range(NA):
        g1_copy(0, a).wait_send()
    for l in range(NL):
        grads_sent(l)
    for cp in sib_copies():
        cp.wait_send()
    @pl.when(s == 0)
    def _():
        for cp in first_copies():
            cp.wait_send()

    @pl.when(s > 0)
    def _():
        for cp in y_copies():
            cp.wait_send()
    for a in ALL:
        pass_copy(oy + 1, a, c).wait_send()

        @pl.when(ys_ == 0)
        def _():
            pass_copy(oy, a, c).wait_send()

        @pl.when(ys_ == 1)
        def _():
            for hop in range(CORES):
                for cp in hop_copies(a, hop):
                    cp.wait_send()

    @pl.when(is_end)
    def _():
        for t in range(NC * SUB):
            end_copy(0, t).wait_send()

    @pl.when(inner)
    def _():
        for t in range(NC * SUB):
            peer_copy(0, t).wait_send()
            back_copy(0, 1, t).wait_send()
    vout.wait()


def finish(y, gq, go, gu, gd, gv, yo, qo, oo, uo, do, n0, n1, n2, n3, n4, n5, n6, bq, yb, qb, ob, ub, db, got, put):
    trips = [(gd, db, do), (gu, ub, uo), (go, ob, oo), (gq, qb, qo)]
    trips += [tuple(ref.at[m, r] for ref in (y, yb, yo)) for m in range(y.shape[0]) for r in range(y.shape[1])]
    loads = [pltpu.make_async_copy(a, b, got.at[k]) for k, (a, b, o) in enumerate(trips)]
    stores = [pltpu.make_async_copy(b, o, put.at[k]) for k, (a, b, o) in enumerate(trips)]
    for cp in loads:
        cp.start()
    for row, refs in enumerate(((n0,), (n1,), (n2,), (n3,), (n4, n5), (n6,))):
        for ref in refs:
            ref[...] = gv[row:row + 1, :]
    e = bq.shape[2]
    for k in range(3):
        for h in range(CORES):
            bq[k, h:h + 1, :] = gv[6:7, (2 * k + h) * e:(2 * k + h + 1) * e]
    for cp, out in zip(loads, stores):
        cp.wait()
        out.start()
    for cp in stores:
        cp.wait()


def finish_step(y, gq, go, gu, gd, gv, e):
    hbm, vmem = pl.BlockSpec(memory_space=pl.ANY), pl.BlockSpec(memory_space=pltpu.VMEM)
    big = [jax.ShapeDtypeStruct(a.shape, a.dtype) for a in (y, gq, go, gu, gd)]
    row = jax.ShapeDtypeStruct((1, gv.shape[1]), F32)
    return pl.pallas_call(
        finish,
        out_shape=big + [row] * 7 + [jax.ShapeDtypeStruct((3, 2, e), F32)],
        in_specs=[hbm] * 5 + [vmem],
        out_specs=[hbm] * 5 + [vmem] * 8,
        scratch_shapes=[pltpu.VMEM(a.shape, a.dtype) for a in big] + [pltpu.SemaphoreType.DMA((8,))] * 2,
        name='neox_out',
    )(y, gq, go, gu, gd, gv)


def group_step(dims, *args):
    x = args[0]
    S, D, E, C, F = dims
    E2 = 2 * E
    hbm = pl.BlockSpec(memory_space=pl.ANY)
    out_shape = [
        jax.ShapeDtypeStruct(x.shape, BF16),
        jax.ShapeDtypeStruct((3 * E2, D), F32),
        jax.ShapeDtypeStruct((E2, D), F32),
        jax.ShapeDtypeStruct((D, F), F32),
        jax.ShapeDtypeStruct((F, D), F32),
        jax.ShapeDtypeStruct((8, D), F32),
    ]

    def vm(*shape, dtype=BF16):
        return pltpu.VMEM(shape, dtype)
    dma = pltpu.SemaphoreType.DMA
    scratch = [
        vm(NL, 3 * E2, D), vm(NL, E2, D), vm(NL, D, F), vm(NL, F, D), vm(NL, 8, D, dtype=F32),
        vm(NL + 2, S, D),
        vm(NL, S, E2), vm(NL, S, E2), vm(NL, S, E2), vm(NL, E2, S), vm(E2, S), vm(NL, S, E2),
        *[vm(NL, 2, (i + 1) * C, C) for i in range(NC)],
        vm(NL, S, F), vm(NL + 1, S, F, dtype=F32),
        vm(CORES, S, D), vm(CORES, S, D), vm(S, D), vm(S + C, D, dtype=F32),
        vm(CORES, 3 * E2, D, dtype=F32), vm(CORES, E2, D, dtype=F32), vm(CORES, D, F, dtype=F32), vm(CORES, F, D, dtype=F32),
        vm(CORES, 3 * E, D), vm(CORES, E, D), vm(CORES, D // CORES, F), vm(CORES, F // CORES, D),
        vm(S, E2, dtype=F32), vm(S, E2, dtype=F32),
        vm(CORES, C + 8, E2, dtype=F32), vm(S, E2, dtype=F32), vm(S, E2, dtype=F32),
        vm(NL, 8, D, dtype=F32), vm(NL, NT, 8, D, dtype=F32), vm(NL, 8, D, dtype=F32), vm(NL, 8, D, dtype=F32),
        vm(C, D), vm(C, D), vm(C, max(D, F), dtype=F32), vm(C, F), vm(S, C), vm(S, C, dtype=F32),
        *[vm(1, D, dtype=F32)] * 4, vm(1, D), vm(1, D), vm(1, F), vm(3, 2, E),
        dma((NA,)), dma((NA + 1,)), dma((CORES, NA + 1)), dma((NL, 2 * NA + 1)), dma((CORES, NA)), dma((3, NA)), dma((NA, 4)), dma((CORES,)), dma((1,)),
        dma((NC * SUB,)), dma((NC * SUB,)), dma((CORES, NC * SUB)), dma((CORES, NC * SUB)), dma((CORES, NC * SUB)),
        dma((NL,)), dma((NL,)), dma((NA,)), dma((CORES, NA)), dma((CORES, NA)), dma((CORES, NA)), dma((CORES, NA)), dma((NA,)),
        dma((NL, NT - 1)), dma((NL, NT)), dma((NL,)), dma((NL,)), dma((1,)), dma((8,)),
    ]
    return pl.pallas_call(
        functools.partial(body, dims),
        out_shape=out_shape,
        in_specs=[hbm] * len(args),
        out_specs=[hbm] * 6,
        scratch_shapes=scratch,
        compiler_params=pltpu.CompilerParams(collective_id=0, has_side_effects=True, vmem_limit_bytes=67043328),
        name='neox_group',
    )(*args)


def solution(mesh):
    def device_fn(x_in, g_out, ln1_gain, ln1_bias, w_qkv, b_qkv, w_out, b_out, ln2_gain, ln2_bias, w_up, b_up, w_down, b_down):
        n_micro, n_rows, S, D = x_in.shape
        heads, E = w_qkv.shape[2], w_qkv.shape[4]
        F = w_up.shape[2]
        C = S // NC
        wqkv = jnp.transpose(w_qkv[0], (1, 2, 3, 0)).reshape(heads * 3 * E, D)
        bqkv = jnp.transpose(b_qkv[0], (1, 0, 2))
        tab = jnp.asarray(rotary_base(C, NC, E, heads))
        part = group_step((S, D, E, C, F), x_in, g_out, wqkv, w_out[0].reshape(heads * E, D), w_up[0], w_down[0], ln1_gain, ln1_bias, ln2_gain, ln2_bias, b_out, b_down, b_up, bqkv, tab)
        y, gq, go, gup, gdn, n1g, n1b, n2g, n2b, gbo, gbd, gbu, gbq = finish_step(*part, E)
        gq = jnp.transpose(gq.reshape(heads, 3, E, D), (3, 0, 1, 2))[None]
        gbq = jnp.transpose(gbq, (1, 0, 2))[None]
        return (y, n1g, n1b, gq, gbq, go.reshape(1, heads, E, D), gbo, n2g, n2b, gup[None], gbu, gdn[None], gbd)

    return jax.shard_map(device_fn, mesh=mesh, in_specs=(P('dp'), P('dp')) + STAGE_SPECS, out_specs=(P('dp'),) + GRAD_SPECS, check_vma=False)
```

```python
import functools
import math

import jax
import jax.numpy as jnp
import numpy as np
from jax import lax
from jax.experimental import pallas as pl
from jax.experimental.pallas import tpu as pltpu
from jax.sharding import PartitionSpec as P

ROPE_BASE = 10000.0
LN_EPS = 1e-5
STAGE_SPECS = (P('pp'), P('pp'), P('pp', None, 'tp'), P('pp', 'tp'), P('pp', 'tp'), P('pp'), P('pp'), P('pp'), P('pp', None, 'tp'), P('pp', 'tp'), P('pp', 'tp'), P('pp'))
OWN = ('dp', 'pp')
GRAD_SPECS = (P(OWN), P(OWN), P(OWN, None, 'tp'), P(OWN, 'tp'), P(OWN, 'tp'), P(OWN), P(OWN), P(OWN), P(OWN, None, 'tp'), P(OWN, 'tp'), P(OWN, 'tp'), P(OWN))


F32 = jnp.float32
BF16 = jnp.bfloat16
NL = 4
NT = 4
NC = 4
NA = 4
CORES = 2
SUB = 4
FWD_AT = {k: (('mid', 1, k), ('last', 2, k)) for k in range(SUB)}
BWD_AT = {k: (('last', 2, k),) * (k < SUB) + (('mid', 1, k - 1),) * (k > 0) for k in range(SUB + 1)}
LOG2E = 1.4426950408889634
RSQRT2 = 0.7071067811865476
INV_SQRT_2PI = 0.3989422804014327


def nn(a, b):
    return lax.dot_general(a, b, (((1,), (0,)), ((), ())), preferred_element_type=F32)


def nt(a, b):
    return lax.dot_general(a, b, (((1,), (1,)), ((), ())), preferred_element_type=F32)


def tn(a, b):
    return lax.dot_general(a, b, (((0,), (0,)), ((), ())), preferred_element_type=F32)


def col_sum(v):
    return jnp.sum(v, axis=0, keepdims=True)


def row_mean(v):
    return jnp.mean(v, axis=-1, keepdims=True)


def fold(v):
    return jnp.sum(v.reshape(v.shape[0] // 8, 8, v.shape[1]), axis=0)


def rotary_base(chunk, n_chunks, head_dim, n_heads):
    rot_dim = head_dim // 4
    half = rot_dim // CORES
    inv_freq = np.zeros((head_dim,), np.float64)
    inv_freq[:rot_dim] = np.tile(ROPE_BASE ** (-(np.arange(half) * 2.0) / rot_dim), 2)
    inv_freq = np.tile(inv_freq, n_heads)
    pos = np.concatenate([np.arange(chunk), np.arange(8) * (np.arange(8) < n_chunks) * chunk]).astype(np.float64)
    ang = pos[:, None] * inv_freq[None, :]
    return np.stack([np.cos(ang), np.sin(ang)]).astype(np.float32)


def body(dims, x, g, wqkv, wo, wup, wdn, n0, n1, n2, n3, n4, n5, n6, bq, tab,
         y, oqkv, oo, oup, odn, ovec,
         WQ, WO, WU, WD, VEC, H, Q, K, V, KT, VT, CTX, P0, P1, P2, P3, HID, GP, RA, RB, PS, PF,
         GQ, GO, GU, GD, R2Q, R2O, R2U, R2D, DK, DV, TAB, COS, SIN, GV, ZR, GZ, PR,
         AS, MS, PRE, DPB, DS, ST, N0, N1, N2, N3, N4, N5, N6, BQ,
         wl, ws, wy, wr, wf, w0s, w0r, xs, gs, sab, sc, ra_s, rb_s, rc_s, ys, yr, g1s, g1r, g2s, g2r, g3s, g3r, v1s, v1r, v2s, v2r, osem, ns):
    S, D, E, C, F = dims
    E2 = 2 * E
    SR = C // SUB
    z = lax.axis_index('tp')
    xg = lax.axis_index('dp')
    s = lax.axis_index('pp')
    ys_ = s // CORES
    c = s % CORES
    sib = s + 1 - 2 * c
    oy = 2 * (1 - ys_)
    is_end = z * (NT - 1 - z) == 0
    inner = z * (NT - 1 - z) > 0
    hub = 1 + z // 3
    leaf = jnp.where(z == 1, 0, 3)
    peer = 3 - z
    PX = (P0, P1, P2, P3)
    W_IN = (wqkv, wo, wup, wdn)
    W_BUF = (WQ, WO, WU, WD)
    G_HALF = (3 * E, E, D // CORES, F // CORES)
    ALL, FIRST, REST = tuple(range(NA)), (0,), (1, 2, 3)
    ATT, MLP = ALL[:2], ALL[2:]
    G_BUF = (GQ, GO, GU, GD)
    G_OUT = (oqkv, oo, oup, odn)
    G_COLS = (D, D, F, D)
    R1_OFF = (0, 3 * E, 4 * E, 4 * E + D // CORES)
    R2 = (R2Q, R2O, R2U, R2D)

    def rcopy(src, dst, ss, rs, **dev):
        return pltpu.make_async_remote_copy(src_ref=src, dst_ref=dst, send_sem=ss, recv_sem=rs, device_id=dev, device_id_type=pl.DeviceIdType.MESH)

    def lcopy(src, dst, sem):
        return pltpu.make_async_copy(src, dst, sem)

    def rows(start, n):
        return pl.ds(pl.multiple_of(start, n), n)

    xcopy = lcopy(x.at[ys_, c], H.at[0], xs.at[0])
    xcopy.start()
    gcopy = lcopy(g.at[ys_, c], GP.at[NL], gs.at[0])
    gcopy.start()
    tcopy = lcopy(tab, TAB, xs.at[1])
    tcopy.start()
    for a in range(NA):
        lcopy(W_IN[a], W_BUF[a].at[s], wl.at[a]).start()
    small = [lcopy(a, b, ns.at[k]) for k, (a, b) in enumerate(((n0, N0), (n1, N1), (n2, N2), (n3, N3), (n4, N4), (n5, N5), (n6, N6), (bq, BQ)))]
    for cp in small:
        cp.start()

    bar = pltpu.get_barrier_semaphore()
    for o in range(1, NT):
        pl.semaphore_signal(bar, inc=1, device_id={'tp': (z + o) % NT}, device_id_type=pl.DeviceIdType.MESH)
    for o in range(1, NL):
        pl.semaphore_signal(bar, inc=1, device_id={'pp': (s + o) % NL}, device_id_type=pl.DeviceIdType.MESH)
    pl.semaphore_signal(bar, inc=1, device_id={'dp': 1 - xg}, device_id_type=pl.DeviceIdType.MESH)
    pl.semaphore_wait(bar, NT + NL - 1)

    def half(ref, a, k):
        return ref.at[rows(k * G_HALF[a], G_HALF[a])]

    def sib_copies():
        out = [rcopy(W_IN[a], W_BUF[a].at[s], ws.at[a], wr.at[s, 2 * a], pp=sib) for a in ALL]
        return out + [rcopy(VEC.at[s], VEC.at[s], ws.at[NA], wr.at[s, 2 * NA], pp=sib)]

    def y_copies():
        out = [rcopy(half(W_IN[a], a, k), half(W_BUF[a].at[s], a, k), wy.at[k, a], wr.at[s, 2 * a + k], pp=oy + k) for a in ALL for k in range(CORES)]
        return out[:2] + [rcopy(VEC.at[s], VEC.at[s], wy.at[k, NA], wr.at[s, 2 * NA], pp=oy + k) for k in range(CORES)] + out[2:]

    def quarter(ref, a, q):
        return ref.at[rows(q * (G_HALF[a] // CORES), G_HALF[a] // CORES)]

    def first_copies():
        out = []
        for a in ALL:
            for k in range(CORES):
                q = 2 * xg + k
                out.append(rcopy(quarter(W_IN[a], a, q), quarter(W_BUF[a].at[0], a, q), wy.at[k, a], w0r.at[a, q], pp=oy + k))
        return out + [rcopy(VEC.at[s], VEC.at[s], wy.at[k, NA], wr.at[s, 2 * NA], pp=oy + k) for k in range(CORES)]

    def mine(hop):
        return 2 * (xg if hop == 0 else 1 - xg) + c

    def hop_copies(a, hop):
        part, sem = quarter(W_BUF[a].at[0], a, mine(hop)), w0r.at[a, mine(hop)]
        out = [rcopy(part, part, w0s.at[hop, a], sem, pp=sib)]
        return out if hop else out + [rcopy(part, part, w0s.at[2, a], sem, dp=1 - xg)]

    def hop_on(a, hop):
        copies = hop_copies(a, hop)
        copies[0].wait_recv()
        start_all(copies)

    def hop_end(a):
        for k in range(CORES):
            part = quarter(W_BUF[a].at[0], a, 2 * k + 1 - c)
            rcopy(part, part, w0s.at[0, a], w0r.at[a, 2 * k + 1 - c], pp=sib).wait_recv()

    def start_all(copies):
        for cp in copies:
            cp.start()

    for cp in small:
        cp.wait()
    for k, ref in enumerate((N0, N1, N2, N3, N4, N5, N6)):
        VEC[s, k:k + 1, :] = ref[...].astype(F32)
    VEC[s, 7:8, :3 * E2] = jnp.concatenate([BQ[k, h:h + 1, :].astype(F32) for k in range(3) for h in range(CORES)], axis=1)

    @pl.when(s == 0)
    def _():
        start_all(first_copies())

    @pl.when(s > 1)
    def _():
        start_all(y_copies())
    start_all(sib_copies())

    def pass_copy(l, a, k):
        part = half(W_BUF[a].at[l], a, k)
        return rcopy(part, part, wf.at[l % CORES, a], wr.at[l, 2 * a + k], pp=sib)

    def relay(l, arrays):
        @pl.when(l // CORES != ys_)
        def _():
            for a in arrays:
                pass_copy(l, a, c).wait_recv()
                pass_copy(l, a, c).start()

    def settle(l, arrays, small):
        @pl.when(l == s)
        def _():
            for a in arrays:
                lcopy(W_IN[a], W_BUF[a].at[s], wl.at[a]).wait()

        @pl.when(l == sib)
        def _():
            for a in arrays:
                rcopy(W_IN[a], W_BUF[a].at[l], ws.at[a], wr.at[l, 2 * a], pp=sib).wait_recv()

        @pl.when((l // CORES != ys_) & (l > 0))
        def _():
            for a in arrays:
                pass_copy(l, a, 1 - c).wait_recv()
        if small:
            @pl.when(l != s)
            def _():
                rcopy(VEC.at[l], VEC.at[l], ws.at[NA], wr.at[l, 2 * NA], pp=sib).wait_recv()

    tcopy.wait()
    for i in range(NC):
        cb, sb = TAB[0, :C, :], TAB[1, :C, :]
        cr, sr = TAB[0, C + i:C + i + 1, :], TAB[1, C + i:C + i + 1, :]
        COS[i * C:(i + 1) * C, :] = cb * cr - sb * sr
        SIN[i * C:(i + 1) * C, :] = sb * cr + cb * sr

    lane = lax.broadcasted_iota(jnp.int32, (C, E2), 1)
    head_lane = lane // E
    in_head = lane % E
    rot_half = E // 8
    low = in_head < rot_half
    sub_head = lax.broadcasted_iota(jnp.int32, (E2, C), 0) // E
    lower = lax.broadcasted_iota(jnp.int32, (C, C), 0) <= lax.broadcasted_iota(jnp.int32, (C, C), 1)
    c1 = E ** -0.5 * LOG2E

    def tabs(i):
        cs, sn = COS[i * C:(i + 1) * C, :], SIN[i * C:(i + 1) * C, :]
        return cs, jnp.where(low, -sn, 0.0), jnp.where(low, 0.0, sn)

    def rotate(v, t):
        cs, sa, sb = t
        return v * cs + pltpu.roll(v, E2 - rot_half, 1) * sa + pltpu.roll(v, rot_half, 1) * sb

    def unrotate(v, t):
        cs, sa, sb = t
        return v * cs + pltpu.roll(v * sa, rot_half, 1) + pltpu.roll(v * sb, E2 - rot_half, 1)

    def end_copy(p, t):
        return rcopy(PS.at[t * SR:(t + 1) * SR], RA.at[p % CORES, t * SR:(t + 1) * SR], sab.at[t], ra_s.at[p % CORES, t], tp=hub)

    def peer_copy(p, t):
        return rcopy(PS.at[t * SR:(t + 1) * SR], RB.at[p % CORES, t * SR:(t + 1) * SR], sab.at[t], rb_s.at[p % CORES, t], tp=peer)

    def back_copy(p, di, t):
        return rcopy(H.at[di, t * SR:(t + 1) * SR], H.at[di, t * SR:(t + 1) * SR], sc.at[t], rc_s.at[p % CORES, t], tp=leaf)

    def pf_row(i, back):
        return (NC if back and i == NC - 1 else i) * C

    def ar_send(p, i, back=False):
        @pl.when(is_end)
        def _():
            for t in range(i * SUB, (i + 1) * SUB):
                @pl.when(p > 0)
                def _():
                    end_copy(p, t).wait_send()
                f0 = pf_row(i, back) + (t - i * SUB) * SR
                PS[t * SR:(t + 1) * SR, :] = PF[f0:f0 + SR, :].astype(BF16)
                end_copy(p, t).start()

    def ar_mid(p, i, u, back=False):
        t = i * SUB + u
        r = slice(t * SR, (t + 1) * SR)
        f0 = pf_row(i, back) + u * SR

        @pl.when(inner)
        def _():
            end_copy(p, t).wait_recv()
            @pl.when(p > 0)
            def _():
                peer_copy(p, t).wait_send()
            PS[r, :] = (PF[f0:f0 + SR, :] + RA[p % CORES, r, :].astype(F32)).astype(BF16)
            peer_copy(p, t).start()

    def ar_last(p, ri, di, i, u):
        t = i * SUB + u
        r = slice(t * SR, (t + 1) * SR)

        @pl.when(inner)
        def _():
            lv = jnp.minimum(p, NL - 1)
            bias = (VEC[lv, 4:5, :] + VEC[lv, 5:6, :]) * jnp.where(p < NL, 1.0, 0.0)
            peer_copy(p, t).wait_recv()
            @pl.when(p > 0)
            def _():
                back_copy(p, di, t).wait_send()
            both = PS[r, :].astype(F32) + RB[p % CORES, r, :].astype(F32)
            H[di, r, :] = (H[ri, r, :].astype(F32) + both + bias).astype(BF16)
            back_copy(p, di, t).start()

    def ar_wait(p, di, i):
        @pl.when(is_end)
        def _():
            for t in range(i * SUB, (i + 1) * SUB):
                back_copy(p, di, t).wait_recv()

    def stats(hf):
        cen = hf - row_mean(hf)
        rstd = lax.rsqrt(row_mean(cen * cen) + LN_EPS)
        return cen * rstd, rstd

    LB = 32
    GR = 32

    def norms(l, i):
        g1, b1, g2, b2 = (VEC[l, k:k + 1, :] for k in range(NA))

        def step(b, carry):
            hf = H[l, rows(i * C + b * LB, LB), :].astype(F32)
            xhat, unused = stats(hf)
            AS[rows(b * LB, LB), :] = (xhat * g1 + b1).astype(BF16)
            MS[rows(b * LB, LB), :] = (xhat * g2 + b2).astype(BF16)
            return carry
        lax.fori_loop(0, C // LB, step, 0, unroll=True)

    def by_kind():
        return [(h * 3 + k) * E for k in range(3) for h in range(CORES)]

    def wq(l):
        return jnp.concatenate([WQ[l, r:r + E, :] for r in by_kind()], axis=0)

    def forward(l, i):
        r0, r1 = i * C, (i + 1) * C
        norms(l, i)
        qkv = nt(AS[...], wq(l)) + VEC[l, 7:8, :3 * E2]
        qkv = qkv.astype(BF16).astype(F32)
        t = tabs(i)
        q = rotate(qkv[:, :E2], t).astype(BF16)
        kf = rotate(qkv[:, E2:2 * E2], t)
        vf = qkv[:, 2 * E2:3 * E2]
        Q[l, r0:r1, :] = q
        K[l, r0:r1, :] = kf.astype(BF16)
        V[l, r0:r1, :] = vf.astype(BF16)
        KT[l, :, r0:r1] = jnp.transpose(kf).astype(BF16)
        VT[:, r0:r1] = jnp.transpose(vf).astype(BF16)
        yield

        def far(*hops):
            if i == 0:
                @pl.when((l == 0) & (ys_ == 1))
                def _():
                    for a, hop in hops:
                        hop_on(a, hop)
        far((2, 0), (1, 1))
        RBK = C // CORES
        outs = []
        for h in range(CORES):
            qm = jnp.where(head_lane == h, Q[l, r0:r1, :].astype(F32), 0.0).astype(BF16)
            ST[:r1, :] = nt(K[l, :r1, :], qm)
            ST[r0:r1, :] = jnp.where(lower, ST[r0:r1, :], -1e30)

            def top(b, m):
                return jnp.maximum(m, jnp.max(ST[rows(b * RBK, RBK), :].reshape(RBK // 8, 8, C), axis=0))
            m = jnp.max(lax.fori_loop(0, r1 // RBK, top, jnp.full((8, C), -3e38, F32), unroll=True), axis=0, keepdims=True)
            mc = m * c1

            def expo(b, tot):
                e = jnp.exp2(ST[rows(b * RBK, RBK), :] * c1 - mc)
                ST[rows(b * RBK, RBK), :] = e
                return tot + fold(e)
            tot = col_sum(lax.fori_loop(0, r1 // RBK, expo, jnp.zeros((8, C), F32), unroll=True))
            inv = 1.0 / tot

            def put(b, carry):
                PX[i][l, h, rows(b * RBK, RBK), :] = (ST[rows(b * RBK, RBK), :] * inv).astype(BF16)
                return carry
            lax.fori_loop(0, r1 // RBK, put, 0, unroll=True)
            outs.append(nn(VT[:, :r1], PX[i][l, h]))
            if h == 0:
                yield
                far((3, 0))
        ctx = jnp.transpose(jnp.where(sub_head == 0, outs[0], outs[1])).astype(BF16)
        CTX[l, r0:r1, :] = ctx
        yield
        if i == 0:
            far((2, 1), (3, 1))

            @pl.when((l == 0) & (ys_ == 1))
            def _():
                for a in REST:
                    hop_end(a)
            settle(l, REST, False)
        PF[r0:r1, :] = nn(ctx, WO[l])
        PRE[...] = nn(MS[...], WU[l])
        bup = VEC[l, 6:7, :]
        GB = 32

        def act(b, carry):
            u = PRE[rows(b * GB, GB), :] + bup
            cdf = 0.5 * (1.0 + lax.erf(u * RSQRT2))
            pdf = jnp.exp2(u * u * (-0.5 * LOG2E)) * INV_SQRT_2PI
            HID[l, rows(r0 + b * GB, GB), :] = (u * cdf).astype(BF16)
            GP[l, rows(r0 + b * GB, GB), :] = cdf + u * pdf
            return carry
        lax.fori_loop(0, C // GB, act, 0, unroll=True)
        PF[r0:r1, :] += nn(HID[l, r0:r1, :], WD[l])
        yield

    def backward(l, dl, i, last):
        r0, r1 = i * C, (i + 1) * C
        par = l % CORES
        first = i == NC - 1

        def acc(ref, val):
            if first:
                ref[par] = val
            else:
                ref[par] += val

        def acc_row(k, val, w=D):
            GV[l, k:k + 1, :w] += val

        norms(l, i)
        dy = H[dl, r0:r1, :]
        acc_row(4, col_sum(dy.astype(F32)))
        PRE[...] = nt(dy, WD[l])
        GB = 32

        def act(b, tot):
            d = PRE[rows(b * GB, GB), :] * GP[l, rows(r0 + b * GB, GB), :]
            DPB[rows(b * GB, GB), :] = d.astype(BF16)
            return tot + fold(d)
        dbu = lax.fori_loop(0, C // GB, act, jnp.zeros((8, F), F32), unroll=True)
        acc_row(5, col_sum(dbu))
        acc(GD, tn(HID[l, r0:r1, :], dy))
        yield
        acc(GU, tn(MS[...], DPB[...]))
        f0 = pf_row(i, True)
        PF[f0:f0 + C, :] = nt(DPB[...], WU[l])
        yield
        dctx = nt(dy, WO[l]).astype(BF16)
        ctx = CTX[l, r0:r1, :]
        acc(GO, tn(ctx, dy))
        prod = dctx.astype(F32) * ctx.astype(F32)
        q = Q[l, r0:r1, :].astype(F32)
        dcf = dctx.astype(F32)
        RBK = C // CORES
        dqt = []
        for h in range(CORES):
            sel = head_lane == h
            qm = jnp.where(sel, q, 0.0).astype(BF16)
            dcm = jnp.where(sel, dcf, 0.0).astype(BF16)
            dsum = jnp.transpose(jnp.where(sel, prod, 0.0))
            drow = col_sum(dsum)
            ST[:r1, :] = nt(V[l, :r1, :], dcm)

            def sub(b, carry):
                pr = PX[i][l, h, rows(b * RBK, RBK), :].astype(F32)
                DS[rows(b * RBK, RBK), :] = (pr * (ST[rows(b * RBK, RBK), :] - drow)).astype(BF16)
                return carry
            lax.fori_loop(0, r1 // RBK, sub, 0, unroll=True)
            dk = nn(DS[:r1, :], qm)
            dv = nn(PX[i][l, h], dcm)
            if first and h == 0:
                DK[:r1, :] = dk
                DV[:r1, :] = dv
            else:
                DK[:r1, :] += dk
                DV[:r1, :] += dv
            dqt.append(nn(KT[l, :, :r1], DS[:r1, :]))
            yield
        scale = E ** -0.5
        t = tabs(i)
        dq = unrotate(jnp.transpose(jnp.where(sub_head == 0, dqt[0], dqt[1])) * scale, t)
        dk = unrotate(DK[r0:r1, :] * scale, t)
        dv = DV[r0:r1, :]
        dqkv = jnp.concatenate([dq, dk, dv], axis=1)
        acc_row(6, col_sum(dqkv), 3 * E2)
        dqkv = dqkv.astype(BF16)
        dwq = tn(dqkv, AS[...])
        for k, r in enumerate(by_kind()):
            if first:
                GQ[par, r:r + E, :] = dwq[k * E:(k + 1) * E]
            else:
                GQ[par, r:r + E, :] += dwq[k * E:(k + 1) * E]
        PRE[...] = nn(dqkv, wq(l))
        yield
        g1, g2 = VEC[l, 0:1, :], VEC[l, 2:3, :]

        def lnb(b, tots):
            hf = H[l, rows(r0 + b * LB, LB), :].astype(F32)
            xhat, rstd = stats(hf)
            da = PRE[rows(b * LB, LB), :]
            dm = PF[rows(f0 + b * LB, LB), :]
            dx = da * g1 + dm * g2
            m1 = row_mean(dx)
            m2 = row_mean(dx * xhat)
            if not last:
                PF[rows(f0 + b * LB, LB), :] = rstd * (dx - m1 - xhat * m2)
            terms = (da * xhat, da, dm * xhat, dm)
            return tuple(a + fold(v) for a, v in zip(tots, terms))
        tots = lax.fori_loop(0, C // LB, lnb, tuple(jnp.zeros((8, D), F32) for _ in range(NA)), unroll=True)
        for k in range(NA):
            acc_row(k, col_sum(tots[k]))
        yield

    def g_half(a, k):
        return rows(k * G_HALF[a], G_HALF[a])

    def r1_view(l, a):
        return GP.at[l + 1, R1_OFF[a]:R1_OFF[a] + G_HALF[a], :G_COLS[a]]

    def g1_copy(l, a):
        return rcopy(G_BUF[a].at[l % CORES, g_half(a, 1 - c)], r1_view(l, a), g1s.at[a], g1r.at[l % CORES, a], pp=sib)

    def g2_copy(l, a):
        return rcopy(HID.at[l, R1_OFF[a]:R1_OFF[a] + G_HALF[a], :G_COLS[a]], R2[a].at[l % CORES], g2s.at[l % CORES, a], g2r.at[l % CORES, a], pp=2 * (l // CORES) + c)

    def g3_local(l, a):
        return lcopy(r1_view(l, a), G_OUT[a].at[g_half(a, c)], g3s.at[l % CORES, a])

    def g3_remote(l, a):
        return rcopy(r1_view(l, a), G_OUT[a].at[g_half(a, c)], g3s.at[l % CORES, a], g3r.at[a], pp=sib)

    def v1_copies(l):
        return [rcopy(GV.at[l], ZR.at[l, z], v1s.at[l, o - 1], v1r.at[l, z], tp=(z + o) % NT) for o in range(1, NT)]

    def grads_mid(l, arrays):
        for a in arrays:
            g1_copy(l, a).wait_recv()
            n = G_HALF[a]

            def add(b, carry):
                rr = rows(R1_OFF[a] + b * GR, GR)
                tot = G_BUF[a][l % CORES, rows(c * n + b * GR, GR), :] + GP[l + 1, rr, :G_COLS[a]]
                GP[l + 1, rr, :G_COLS[a]] = tot
                HID[l, rr, :G_COLS[a]] = tot.astype(BF16)
                return carry
            lax.fori_loop(0, n // GR, add, 0)

            @pl.when(l // CORES != ys_)
            def _():
                g2_copy(l, a).start()

    def grads_last(l):
        @pl.when(l // CORES == ys_)
        def _():
            for a in MLP + ATT:
                g2_copy(l, a).wait_recv()

                def add(b, carry):
                    rr = rows(R1_OFF[a] + b * GR, GR)
                    GP[l + 1, rr, :G_COLS[a]] += R2[a][l % CORES, rows(b * GR, GR), :].astype(F32)
                    return carry
                lax.fori_loop(0, G_HALF[a] // GR, add, 0)

                @pl.when(l == s)
                def _():
                    g3_local(l, a).start()

                @pl.when(l != s)
                def _():
                    g3_remote(l, a).start()

    def grads_sent(l):
        for a in range(NA):
            @pl.when(l // CORES != ys_)
            def _():
                g2_copy(l, a).wait_send()

            @pl.when(l == s)
            def _():
                g3_local(l, a).wait()

            @pl.when((l // CORES == ys_) & (l != s))
            def _():
                g3_remote(l, a).wait_send()

    def v2_copy(l):
        return rcopy(GZ.at[l], PR.at[s], v2s.at[l], v2r.at[s], pp=l)

    def vec_mid(l):
        ZR[l, z] = GV[l]
        for o in range(1, NT):
            q = (z + o) % NT
            rcopy(GV.at[l], ZR.at[l, q], v1s.at[l, o - 1], v1r.at[l, q], tp=q).wait_recv()
        tot = ZR[l, 0] + ZR[l, 1] + ZR[l, 2] + ZR[l, 3]
        row = lax.broadcasted_iota(jnp.int32, (8, D), 0)
        GZ[l] = jnp.where(row < 4, tot, GV[l])

        @pl.when(l == s)
        def _():
            PR[s] = GZ[l]

        @pl.when(l != s)
        def _():
            v2_copy(l).start()

    GV[...] = jnp.zeros_like(GV)
    @pl.when(ys_ == 1)
    def _():
        for a, hop in ((0, 0), (1, 0), (0, 1)):
            hop_on(a, hop)
        hop_end(0)
    settle(0, FIRST, True)
    xcopy.wait()

    def run(phases, at, handle, after=lambda k: None):
        for k, unused in enumerate(phases):
            after(k)
            for op, lag, u in at.get(k, ()):
                handle(op, lag, u)

    def fwd_layer(l, carry):
        for i in range(NC):
            @pl.when(l > 0)
            def _():
                ar_wait(l - 1, l, i)

            def handle(op, lag, u):
                m = i - lag

                def go(p, j):
                    if op == 'mid':
                        ar_mid(p, j, u)
                    else:
                        ar_last(p, p, p + 1, j, u)
                if m >= 0:
                    go(l, m)
                else:
                    @pl.when(l > 0)
                    def _():
                        go(l - 1, m + NC)
            run(forward(l, i), FWD_AT, handle)
            ar_send(l, i)
            if i == 1:
                @pl.when(l == 0)
                def _():
                    gcopy.wait()
                    H[NL + 1] = GP[NL].astype(BF16)

                    @pl.when(s == 1)
                    def _():
                        start_all(y_copies())
            if i == 2:
                @pl.when((l > 0) & (l < NL - 1))
                def _():
                    relay(l + 1, ALL)
            if i == NC - 1:
                @pl.when(l == 0)
                def _():
                    relay(l + 1, ALL)

                @pl.when(l < NL - 1)
                def _():
                    settle(l + 1, FIRST, True)
        return carry
    lax.fori_loop(0, NL, fwd_layer, 0)

    y_local = lcopy(H.at[NL], y.at[ys_, c], ys.at[0])
    y_sib = rcopy(H.at[NL], y.at[ys_, c], ys.at[1], yr.at[s], pp=sib)
    y_far = rcopy(H.at[NL], y.at[ys_, c], ys.at[2], yr.at[s], pp=oy + c)
    y_fwd = rcopy(y.at[1 - ys_, c], y.at[1 - ys_, c], ys.at[3], yr.at[oy + c], pp=sib)

    def y_arrived(q):
        rcopy(H.at[NL], y.at[q // CORES, q % CORES], ys.at[1], yr.at[q], pp=sib).wait_recv()

    def ri(l):
        return jnp.where(l == NL - 1, NL + 1, l + 1)

    def bwd_layer(lb, carry):
        l = NL - 1 - lb
        p = NL + lb
        for n in range(NC):
            i = NC - 1 - n

            @pl.when(lb > 0)
            def _():
                ar_wait(p - 1, l + 1, i)

            def handle(op, lag, u):
                m = n - lag

                def go(q, lq, j):
                    if op == 'mid':
                        ar_mid(q, j, u, True)
                    else:
                        ar_last(q, ri(lq), lq, j, u)
                if m >= 0:
                    @pl.when(l > 0)
                    def _():
                        go(p, l, NC - 1 - m)
                else:
                    @pl.when(lb > 0)
                    def _():
                        go(p - 1, l + 1, -1 - m)

                    @pl.when(lb == 0)
                    def _():
                        if op == 'mid':
                            ar_mid(NL - 1, m + NC, u)
                        else:
                            ar_last(NL - 1, NL - 1, NL, m + NC, u)

            def after(k):
                if k == 0 and n == 0:
                    @pl.when(lb > 0)
                    def _():
                        grads_mid(l + 1, ATT)
                        for a in ALL:
                            g1_copy(l + 1, a).wait_send()
                if n == NC - 1 and k == 1:
                    for a in MLP:
                        g1_copy(l, a).start()
                if n == NC - 1 and k == 3:
                    grads_mid(l, MLP)
            run(backward(l, ri(l), i, False), BWD_AT, handle, after)

            @pl.when(l > 0)
            def _():
                ar_send(p, i, True)
            if n == 1:
                @pl.when(lb > 0)
                def _():
                    vec_mid(l + 1)
            if n == 2:
                @pl.when(lb == 0)
                def _():
                    for j in range(NC):
                        ar_wait(NL - 1, NL, j)
                    start_all((y_local, y_sib, y_far))

                @pl.when(lb > 1)
                def _():
                    grads_last(l + 2)

        for a in ATT:
            g1_copy(l, a).start()
        start_all(v1_copies(l))
        return carry
    lax.fori_loop(0, NL, bwd_layer, 0)

    grads_mid(0, ATT)
    y_arrived(oy + c)
    y_fwd.start()
    grads_last(1)
    vec_mid(0)
    grads_last(0)

    for o in range(1, NL):
        q = (s + o) % NL
        rcopy(GZ.at[0], PR.at[q], v2s.at[0], v2r.at[q], pp=q).wait_recv()
    PRE[0:8, 0:D] = PR[0] + PR[1] + PR[2] + PR[3]
    vout = lcopy(PRE.at[0:8, 0:D], ovec, osem.at[0])
    vout.start()
    for l in range(NL):
        for cp in v1_copies(l):
            cp.wait_send()
    for l in range(NL):
        @pl.when(l != s)
        def _():
            v2_copy(l).wait_send()
    for a in range(NA):
        rcopy(G_OUT[a].at[g_half(a, 1 - c)], G_OUT[a].at[g_half(a, 1 - c)], g3s.at[a], g3r.at[a], pp=sib).wait_recv()
    y_local.wait()
    for cp in (y_sib, y_far, y_fwd):
        cp.wait_send()
    y_arrived(sib)
    y_arrived(oy + 1 - c)
    for a in range(NA):
        g1_copy(0, a).wait_send()
    for l in range(NL):
        grads_sent(l)
    for cp in sib_copies():
        cp.wait_send()
    @pl.when(s == 0)
    def _():
        for cp in first_copies():
            cp.wait_send()

    @pl.when(s > 0)
    def _():
        for cp in y_copies():
            cp.wait_send()
    for a in ALL:
        pass_copy(oy + 1, a, c).wait_send()

        @pl.when(ys_ == 0)
        def _():
            pass_copy(oy, a, c).wait_send()

        @pl.when(ys_ == 1)
        def _():
            for hop in range(CORES):
                for cp in hop_copies(a, hop):
                    cp.wait_send()

    @pl.when(is_end)
    def _():
        for t in range(NC * SUB):
            end_copy(0, t).wait_send()

    @pl.when(inner)
    def _():
        for t in range(NC * SUB):
            peer_copy(0, t).wait_send()
            back_copy(0, 1, t).wait_send()
    vout.wait()


def finish(y, gq, go, gu, gd, gv, yo, qo, oo, uo, do, n0, n1, n2, n3, n4, n5, n6, bq,
           yb, qb, ob, ub, db, vb, r0, r1, r2, r3, r4, r5, r6, rq, got, put, small):
    trips = [(gd, db, do), (gu, ub, uo), (go, ob, oo), (gq, qb, qo)]
    trips += [tuple(ref.at[m, r] for ref in (y, yb, yo)) for m in range(y.shape[0]) for r in range(y.shape[1])]
    loads = [pltpu.make_async_copy(a, b, got.at[k]) for k, (a, b, o) in enumerate(trips)]
    stores = [pltpu.make_async_copy(b, o, put.at[k]) for k, (a, b, o) in enumerate(trips)]
    vecs = pltpu.make_async_copy(gv, vb, small.at[len(trips)])
    vecs.start()
    for cp in loads:
        cp.start()
    vecs.wait()
    for row, refs in enumerate(((r0,), (r1,), (r2,), (r3,), (r4, r5), (r6,))):
        for ref in refs:
            ref[...] = vb[row:row + 1, :]
    e = rq.shape[2]
    for k in range(3):
        for h in range(CORES):
            rq[k, h:h + 1, :] = vb[6:7, (CORES * k + h) * e:(CORES * k + h + 1) * e]
    tiny = [pltpu.make_async_copy(a, b, small.at[k]) for k, (a, b) in enumerate(((r0, n0), (r1, n1), (r2, n2), (r3, n3), (r4, n4), (r5, n5), (r6, n6), (rq, bq)))]
    for cp in tiny:
        cp.start()
    for cp, out in zip(loads, stores):
        cp.wait()
        out.start()
    for cp in tiny + stores:
        cp.wait()


def finish_step(y, gq, go, gu, gd, gv, e):
    hbm = pl.BlockSpec(memory_space=pl.ANY)
    row = jax.ShapeDtypeStruct((1, gv.shape[1]), F32)
    outs = [jax.ShapeDtypeStruct(a.shape, a.dtype) for a in (y, gq, go, gu, gd)] + [row] * 7 + [jax.ShapeDtypeStruct((3, CORES, e), F32)]
    bufs = outs[:5] + [gv] + outs[5:]
    return pl.pallas_call(
        finish,
        out_shape=outs,
        in_specs=[hbm] * 6,
        out_specs=[hbm] * len(outs),
        scratch_shapes=[pltpu.VMEM(a.shape, a.dtype) for a in bufs] + [pltpu.SemaphoreType.DMA((9,))] * 3,
        name='neox_out',
    )(y, gq, go, gu, gd, gv)


def group_step(dims, *args):
    x = args[0]
    S, D, E, C, F = dims
    E2 = 2 * E
    hbm = pl.BlockSpec(memory_space=pl.ANY)
    out_shape = [
        jax.ShapeDtypeStruct(x.shape, BF16),
        jax.ShapeDtypeStruct((3 * E2, D), F32),
        jax.ShapeDtypeStruct((E2, D), F32),
        jax.ShapeDtypeStruct((D, F), F32),
        jax.ShapeDtypeStruct((F, D), F32),
        jax.ShapeDtypeStruct((8, D), F32),
    ]

    def vm(*shape, dtype=BF16):
        return pltpu.VMEM(shape, dtype)
    dma = pltpu.SemaphoreType.DMA
    scratch = [
        vm(NL, 3 * E2, D), vm(NL, E2, D), vm(NL, D, F), vm(NL, F, D), vm(NL, 8, D, dtype=F32),
        vm(NL + 2, S, D),
        vm(NL, S, E2), vm(NL, S, E2), vm(NL, S, E2), vm(NL, E2, S), vm(E2, S), vm(NL, S, E2),
        *[vm(NL, 2, (i + 1) * C, C) for i in range(NC)],
        vm(NL, S, F), vm(NL + 1, S, F, dtype=F32),
        vm(CORES, S, D), vm(CORES, S, D), vm(S, D), vm(S + C, D, dtype=F32),
        vm(CORES, 3 * E2, D, dtype=F32), vm(CORES, E2, D, dtype=F32), vm(CORES, D, F, dtype=F32), vm(CORES, F, D, dtype=F32),
        vm(CORES, 3 * E, D), vm(CORES, E, D), vm(CORES, D // CORES, F), vm(CORES, F // CORES, D),
        vm(S, E2, dtype=F32), vm(S, E2, dtype=F32),
        vm(CORES, C + 8, E2, dtype=F32), vm(S, E2, dtype=F32), vm(S, E2, dtype=F32),
        vm(NL, 8, D, dtype=F32), vm(NL, NT, 8, D, dtype=F32), vm(NL, 8, D, dtype=F32), vm(NL, 8, D, dtype=F32),
        vm(C, D), vm(C, D), vm(C, max(D, F), dtype=F32), vm(C, F), vm(S, C), vm(S, C, dtype=F32),
        *[vm(1, D, dtype=F32)] * 4, vm(1, D), vm(1, D), vm(1, F), vm(3, 2, E),
        dma((NA,)), dma((NA + 1,)), dma((CORES, NA + 1)), dma((NL, 2 * NA + 1)), dma((CORES, NA)), dma((3, NA)), dma((NA, 4)), dma((CORES,)), dma((1,)),
        dma((NC * SUB,)), dma((NC * SUB,)), dma((CORES, NC * SUB)), dma((CORES, NC * SUB)), dma((CORES, NC * SUB)),
        dma((NL,)), dma((NL,)), dma((NA,)), dma((CORES, NA)), dma((CORES, NA)), dma((CORES, NA)), dma((CORES, NA)), dma((NA,)),
        dma((NL, NT - 1)), dma((NL, NT)), dma((NL,)), dma((NL,)), dma((1,)), dma((8,)),
    ]
    return pl.pallas_call(
        functools.partial(body, dims),
        out_shape=out_shape,
        in_specs=[hbm] * len(args),
        out_specs=[hbm] * 6,
        scratch_shapes=scratch,
        compiler_params=pltpu.CompilerParams(collective_id=0, has_side_effects=True, vmem_limit_bytes=67043328),
        name='neox_group',
    )(*args)


def solution(mesh):
    def device_fn(x_in, g_out, ln1_gain, ln1_bias, w_qkv, b_qkv, w_out, b_out, ln2_gain, ln2_bias, w_up, b_up, w_down, b_down):
        n_micro, n_rows, S, D = x_in.shape
        heads, E = w_qkv.shape[2], w_qkv.shape[4]
        F = w_up.shape[2]
        C = S // NC
        wqkv = jnp.transpose(w_qkv[0], (1, 2, 3, 0)).reshape(heads * 3 * E, D)
        bqkv = jnp.transpose(b_qkv[0], (1, 0, 2))
        tab = jnp.asarray(rotary_base(C, NC, E, heads))
        part = group_step((S, D, E, C, F), x_in, g_out, wqkv, w_out[0].reshape(heads * E, D), w_up[0], w_down[0], ln1_gain, ln1_bias, ln2_gain, ln2_bias, b_out, b_down, b_up, bqkv, tab)
        y, gq, go, gup, gdn, n1g, n1b, n2g, n2b, gbo, gbd, gbu, gbq = finish_step(*part, E)
        gq = jnp.transpose(gq.reshape(heads, 3, E, D), (3, 0, 1, 2))[None]
        gbq = jnp.transpose(gbq, (1, 0, 2))[None]
        return (y, n1g, n1b, gq, gbq, go.reshape(1, heads, E, D), gbo, n2g, n2b, gup[None], gbu, gdn[None], gbd)

    return jax.shard_map(device_fn, mesh=mesh, in_specs=(P('dp'), P('dp')) + STAGE_SPECS, out_specs=(P('dp'),) + GRAD_SPECS, check_vma=False)
```

```python
import functools
import math

import jax
import jax.numpy as jnp
import numpy as np
from jax import lax
from jax.experimental import pallas as pl
from jax.experimental.pallas import tpu as pltpu
from jax.sharding import PartitionSpec as P

ROPE_BASE = 10000.0
LN_EPS = 1e-5
STAGE_SPECS = (P('pp'), P('pp'), P('pp', None, 'tp'), P('pp', 'tp'), P('pp', 'tp'), P('pp'), P('pp'), P('pp'), P('pp', None, 'tp'), P('pp', 'tp'), P('pp', 'tp'), P('pp'))
OWN = ('dp', 'pp')
GRAD_SPECS = (P(OWN), P(OWN), P(OWN, None, 'tp'), P(OWN, 'tp'), P(OWN, 'tp'), P(OWN), P(OWN), P(OWN), P(OWN, None, 'tp'), P(OWN, 'tp'), P(OWN, 'tp'), P(OWN))


F32 = jnp.float32
BF16 = jnp.bfloat16
NL = 4
NT = 4
NC = 4
NA = 4
CORES = 2
SUB = 2
FWD_AT = {0: (('mid', 1, 0), ('last', 2, 0)), 2: (('mid', 1, 1), ('last', 2, 1))}
BWD_AT = {0: (('last', 2, 0),), 1: (('mid', 1, 0),), 3: (('last', 2, 1),), 4: (('mid', 1, 1),)}
LOG2E = 1.4426950408889634
RSQRT2 = 0.7071067811865476
INV_SQRT_2PI = 0.3989422804014327


def nn(a, b):
    return lax.dot_general(a, b, (((1,), (0,)), ((), ())), preferred_element_type=F32)


def nt(a, b):
    return lax.dot_general(a, b, (((1,), (1,)), ((), ())), preferred_element_type=F32)


def tn(a, b):
    return lax.dot_general(a, b, (((0,), (0,)), ((), ())), preferred_element_type=F32)


def col_sum(v):
    return jnp.sum(v, axis=0, keepdims=True)


def row_mean(v):
    return jnp.mean(v, axis=-1, keepdims=True)


def fold(v):
    return jnp.sum(v.reshape(v.shape[0] // 8, 8, v.shape[1]), axis=0)


def rotary_base(chunk, n_chunks, head_dim, n_heads):
    rot_dim = head_dim // 4
    half = rot_dim // CORES
    inv_freq = np.zeros((head_dim,), np.float64)
    inv_freq[:rot_dim] = np.tile(ROPE_BASE ** (-(np.arange(half) * 2.0) / rot_dim), 2)
    inv_freq = np.tile(inv_freq, n_heads)
    pos = np.concatenate([np.arange(chunk), np.arange(8) * (np.arange(8) < n_chunks) * chunk]).astype(np.float64)
    ang = pos[:, None] * inv_freq[None, :]
    return np.stack([np.cos(ang), np.sin(ang)]).astype(np.float32)


def body(dims, x, g, wqkv, wo, wup, wdn, n0, n1, n2, n3, n4, n5, n6, bq, tab,
         y, oqkv, oo, oup, odn, ovec,
         WQ, WO, WU, WD, VEC, H, Q, K, V, KT, VT, CTX, P0, P1, P2, P3, HID, GP, RA, RB, PS, PF,
         GQ, GO, GU, GD, R2Q, R2O, R2U, R2D, DK, DV, TAB, COS, SIN, GV, ZR, GZ, PR,
         AS, MS, PRE, DPB, DS, ST, N0, N1, N2, N3, N4, N5, N6, BQ,
         wl, ws, wy, wr, wf, w0s, w0r, xs, gs, sab, sc, ra_s, rb_s, rc_s, ys, yr, g1s, g1r, g2s, g2r, g3s, g3r, v1s, v1r, v2s, v2r, osem, ns):
    S, D, E, C, F = dims
    E2 = 2 * E
    SR = C // SUB
    z = lax.axis_index('tp')
    xg = lax.axis_index('dp')
    s = lax.axis_index('pp')
    ys_ = s // CORES
    c = s % CORES
    sib = s + 1 - 2 * c
    oy = 2 * (1 - ys_)
    is_end = z * (NT - 1 - z) == 0
    inner = z * (NT - 1 - z) > 0
    hub = 1 + z // 3
    leaf = jnp.where(z == 1, 0, 3)
    peer = 3 - z
    PX = (P0, P1, P2, P3)
    W_IN = (wqkv, wo, wup, wdn)
    W_BUF = (WQ, WO, WU, WD)
    G_HALF = (3 * E, E, D // CORES, F // CORES)
    ALL, FIRST, REST = tuple(range(NA)), (0,), (1, 2, 3)
    ATT, MLP = ALL[:2], ALL[2:]
    G_BUF = (GQ, GO, GU, GD)
    G_OUT = (oqkv, oo, oup, odn)
    G_COLS = (D, D, F, D)
    R1_OFF = (0, 3 * E, 4 * E, 4 * E + D // CORES)
    R2 = (R2Q, R2O, R2U, R2D)

    def rcopy(src, dst, ss, rs, **dev):
        return pltpu.make_async_remote_copy(src_ref=src, dst_ref=dst, send_sem=ss, recv_sem=rs, device_id=dev, device_id_type=pl.DeviceIdType.MESH)

    def lcopy(src, dst, sem):
        return pltpu.make_async_copy(src, dst, sem)

    def rows(start, n):
        return pl.ds(pl.multiple_of(start, n), n)

    xcopy = lcopy(x.at[ys_, c], H.at[0], xs.at[0])
    xcopy.start()
    gcopy = lcopy(g.at[ys_, c], GP.at[NL], gs.at[0])
    gcopy.start()
    tcopy = lcopy(tab, TAB, xs.at[1])
    tcopy.start()
    for a in range(NA):
        lcopy(W_IN[a], W_BUF[a].at[s], wl.at[a]).start()
    small = [lcopy(a, b, ns.at[k]) for k, (a, b) in enumerate(((n0, N0), (n1, N1), (n2, N2), (n3, N3), (n4, N4), (n5, N5), (n6, N6), (bq, BQ)))]
    for cp in small:
        cp.start()

    bar = pltpu.get_barrier_semaphore()
    for o in range(1, NT):
        pl.semaphore_signal(bar, inc=1, device_id={'tp': (z + o) % NT}, device_id_type=pl.DeviceIdType.MESH)
    for o in range(1, NL):
        pl.semaphore_signal(bar, inc=1, device_id={'pp': (s + o) % NL}, device_id_type=pl.DeviceIdType.MESH)
    pl.semaphore_signal(bar, inc=1, device_id={'dp': 1 - xg}, device_id_type=pl.DeviceIdType.MESH)
    pl.semaphore_wait(bar, NT + NL - 1)

    def half(ref, a, k):
        return ref.at[rows(k * G_HALF[a], G_HALF[a])]

    def sib_copies():
        out = [rcopy(W_IN[a], W_BUF[a].at[s], ws.at[a], wr.at[s, 2 * a], pp=sib) for a in ALL]
        return out + [rcopy(VEC.at[s], VEC.at[s], ws.at[NA], wr.at[s, 2 * NA], pp=sib)]

    def y_copies():
        out = [rcopy(half(W_IN[a], a, k), half(W_BUF[a].at[s], a, k), wy.at[k, a], wr.at[s, 2 * a + k], pp=oy + k) for a in ALL for k in range(CORES)]
        return out[:2] + [rcopy(VEC.at[s], VEC.at[s], wy.at[k, NA], wr.at[s, 2 * NA], pp=oy + k) for k in range(CORES)] + out[2:]

    def quarter(ref, a, q):
        return ref.at[rows(q * (G_HALF[a] // CORES), G_HALF[a] // CORES)]

    def first_copies():
        out = []
        for a in ALL:
            for k in range(CORES):
                q = 2 * xg + k
                out.append(rcopy(quarter(W_IN[a], a, q), quarter(W_BUF[a].at[0], a, q), wy.at[k, a], w0r.at[a, q], pp=oy + k))
        return out + [rcopy(VEC.at[s], VEC.at[s], wy.at[k, NA], wr.at[s, 2 * NA], pp=oy + k) for k in range(CORES)]

    def mine(hop):
        return 2 * (xg if hop == 0 else 1 - xg) + c

    def hop_copies(a, hop):
        part, sem = quarter(W_BUF[a].at[0], a, mine(hop)), w0r.at[a, mine(hop)]
        out = [rcopy(part, part, w0s.at[hop, a], sem, pp=sib)]
        return out if hop else out + [rcopy(part, part, w0s.at[2, a], sem, dp=1 - xg)]

    def hop_on(a, hop):
        copies = hop_copies(a, hop)
        copies[0].wait_recv()
        start_all(copies)

    def hop_end(a):
        for k in range(CORES):
            part = quarter(W_BUF[a].at[0], a, 2 * k + 1 - c)
            rcopy(part, part, w0s.at[0, a], w0r.at[a, 2 * k + 1 - c], pp=sib).wait_recv()

    def start_all(copies):
        for cp in copies:
            cp.start()

    for cp in small:
        cp.wait()
    for k, ref in enumerate((N0, N1, N2, N3, N4, N5, N6)):
        VEC[s, k:k + 1, :] = ref[...].astype(F32)
    VEC[s, 7:8, :3 * E2] = jnp.concatenate([BQ[k, h:h + 1, :].astype(F32) for k in range(3) for h in range(CORES)], axis=1)

    @pl.when(s == 0)
    def _():
        start_all(first_copies())

    @pl.when(s > 1)
    def _():
        start_all(y_copies())
    start_all(sib_copies())

    def pass_copy(l, a, k):
        part = half(W_BUF[a].at[l], a, k)
        return rcopy(part, part, wf.at[l % CORES, a], wr.at[l, 2 * a + k], pp=sib)

    def relay(l, arrays):
        @pl.when(l // CORES != ys_)
        def _():
            for a in arrays:
                pass_copy(l, a, c).wait_recv()
                pass_copy(l, a, c).start()

    def settle(l, arrays, small):
        @pl.when(l == s)
        def _():
            for a in arrays:
                lcopy(W_IN[a], W_BUF[a].at[s], wl.at[a]).wait()

        @pl.when(l == sib)
        def _():
            for a in arrays:
                rcopy(W_IN[a], W_BUF[a].at[l], ws.at[a], wr.at[l, 2 * a], pp=sib).wait_recv()

        @pl.when((l // CORES != ys_) & (l > 0))
        def _():
            for a in arrays:
                pass_copy(l, a, 1 - c).wait_recv()
        if small:
            @pl.when(l != s)
            def _():
                rcopy(VEC.at[l], VEC.at[l], ws.at[NA], wr.at[l, 2 * NA], pp=sib).wait_recv()

    tcopy.wait()
    for i in range(NC):
        cb, sb = TAB[0, :C, :], TAB[1, :C, :]
        cr, sr = TAB[0, C + i:C + i + 1, :], TAB[1, C + i:C + i + 1, :]
        COS[i * C:(i + 1) * C, :] = cb * cr - sb * sr
        SIN[i * C:(i + 1) * C, :] = sb * cr + cb * sr

    lane = lax.broadcasted_iota(jnp.int32, (C, E2), 1)
    head_lane = lane // E
    in_head = lane % E
    rot_half = E // 8
    low = in_head < rot_half
    sub_head = lax.broadcasted_iota(jnp.int32, (E2, C), 0) // E
    lower = lax.broadcasted_iota(jnp.int32, (C, C), 0) <= lax.broadcasted_iota(jnp.int32, (C, C), 1)
    c1 = E ** -0.5 * LOG2E

    def tabs(i):
        cs, sn = COS[i * C:(i + 1) * C, :], SIN[i * C:(i + 1) * C, :]
        return cs, jnp.where(low, -sn, 0.0), jnp.where(low, 0.0, sn)

    def rotate(v, t):
        cs, sa, sb = t
        return v * cs + pltpu.roll(v, E2 - rot_half, 1) * sa + pltpu.roll(v, rot_half, 1) * sb

    def unrotate(v, t):
        cs, sa, sb = t
        return v * cs + pltpu.roll(v * sa, rot_half, 1) + pltpu.roll(v * sb, E2 - rot_half, 1)

    def end_copy(p, t):
        return rcopy(PS.at[t * SR:(t + 1) * SR], RA.at[p % CORES, t * SR:(t + 1) * SR], sab.at[t], ra_s.at[p % CORES, t], tp=hub)

    def peer_copy(p, t):
        return rcopy(PS.at[t * SR:(t + 1) * SR], RB.at[p % CORES, t * SR:(t + 1) * SR], sab.at[t], rb_s.at[p % CORES, t], tp=peer)

    def back_copy(p, di, t):
        return rcopy(H.at[di, t * SR:(t + 1) * SR], H.at[di, t * SR:(t + 1) * SR], sc.at[t], rc_s.at[p % CORES, t], tp=leaf)

    def pf_row(i, back):
        return (NC if back and i == NC - 1 else i) * C

    def ar_send(p, i, back=False):
        @pl.when(is_end)
        def _():
            for t in range(i * SUB, (i + 1) * SUB):
                @pl.when(p > 0)
                def _():
                    end_copy(p, t).wait_send()
                f0 = pf_row(i, back) + (t - i * SUB) * SR
                PS[t * SR:(t + 1) * SR, :] = PF[f0:f0 + SR, :].astype(BF16)
                end_copy(p, t).start()

    def ar_mid(p, i, u, back=False):
        t = i * SUB + u
        r = slice(t * SR, (t + 1) * SR)
        f0 = pf_row(i, back) + u * SR

        @pl.when(inner)
        def _():
            end_copy(p, t).wait_recv()
            @pl.when(p > 0)
            def _():
                peer_copy(p, t).wait_send()
            PS[r, :] = (PF[f0:f0 + SR, :] + RA[p % CORES, r, :].astype(F32)).astype(BF16)
            peer_copy(p, t).start()

    def ar_last(p, ri, di, i, u):
        t = i * SUB + u
        r = slice(t * SR, (t + 1) * SR)

        @pl.when(inner)
        def _():
            lv = jnp.minimum(p, NL - 1)
            bias = (VEC[lv, 4:5, :] + VEC[lv, 5:6, :]) * jnp.where(p < NL, 1.0, 0.0)
            peer_copy(p, t).wait_recv()
            @pl.when(p > 0)
            def _():
                back_copy(p, di, t).wait_send()
            both = PS[r, :].astype(F32) + RB[p % CORES, r, :].astype(F32)
            H[di, r, :] = (H[ri, r, :].astype(F32) + both + bias).astype(BF16)
            back_copy(p, di, t).start()

    def ar_wait(p, di, i):
        @pl.when(is_end)
        def _():
            for t in range(i * SUB, (i + 1) * SUB):
                back_copy(p, di, t).wait_recv()

    def stats(hf):
        cen = hf - row_mean(hf)
        rstd = lax.rsqrt(row_mean(cen * cen) + LN_EPS)
        return cen * rstd, rstd

    LB = 32
    GR = 32

    def norms(l, i):
        g1, b1, g2, b2 = (VEC[l, k:k + 1, :] for k in range(NA))

        def step(b, carry):
            hf = H[l, rows(i * C + b * LB, LB), :].astype(F32)
            xhat, unused = stats(hf)
            AS[rows(b * LB, LB), :] = (xhat * g1 + b1).astype(BF16)
            MS[rows(b * LB, LB), :] = (xhat * g2 + b2).astype(BF16)
            return carry
        lax.fori_loop(0, C // LB, step, 0, unroll=True)

    def by_kind():
        return [(h * 3 + k) * E for k in range(3) for h in range(CORES)]

    def wq(l):
        return jnp.concatenate([WQ[l, r:r + E, :] for r in by_kind()], axis=0)

    def forward(l, i):
        r0, r1 = i * C, (i + 1) * C
        norms(l, i)
        qkv = nt(AS[...], wq(l)) + VEC[l, 7:8, :3 * E2]
        qkv = qkv.astype(BF16).astype(F32)
        t = tabs(i)
        q = rotate(qkv[:, :E2], t).astype(BF16)
        kf = rotate(qkv[:, E2:2 * E2], t)
        vf = qkv[:, 2 * E2:3 * E2]
        Q[l, r0:r1, :] = q
        K[l, r0:r1, :] = kf.astype(BF16)
        V[l, r0:r1, :] = vf.astype(BF16)
        KT[l, :, r0:r1] = jnp.transpose(kf).astype(BF16)
        VT[:, r0:r1] = jnp.transpose(vf).astype(BF16)
        yield

        def far(*hops):
            if i == 0:
                @pl.when((l == 0) & (ys_ == 1))
                def _():
                    for a, hop in hops:
                        hop_on(a, hop)
        far((2, 0), (1, 1))
        RBK = C // CORES
        outs = []
        for h in range(CORES):
            qm = jnp.where(head_lane == h, Q[l, r0:r1, :].astype(F32), 0.0).astype(BF16)
            ST[:r1, :] = nt(K[l, :r1, :], qm)
            ST[r0:r1, :] = jnp.where(lower, ST[r0:r1, :], -1e30)

            def top(b, m):
                return jnp.maximum(m, jnp.max(ST[rows(b * RBK, RBK), :].reshape(RBK // 8, 8, C), axis=0))
            m = jnp.max(lax.fori_loop(0, r1 // RBK, top, jnp.full((8, C), -3e38, F32), unroll=True), axis=0, keepdims=True)
            mc = m * c1

            def expo(b, tot):
                e = jnp.exp2(ST[rows(b * RBK, RBK), :] * c1 - mc)
                ST[rows(b * RBK, RBK), :] = e
                return tot + fold(e)
            tot = col_sum(lax.fori_loop(0, r1 // RBK, expo, jnp.zeros((8, C), F32), unroll=True))
            inv = 1.0 / tot

            def put(b, carry):
                PX[i][l, h, rows(b * RBK, RBK), :] = (ST[rows(b * RBK, RBK), :] * inv).astype(BF16)
                return carry
            lax.fori_loop(0, r1 // RBK, put, 0, unroll=True)
            outs.append(nn(VT[:, :r1], PX[i][l, h]))
            if h == 0:
                yield
                far((3, 0))
        ctx = jnp.transpose(jnp.where(sub_head == 0, outs[0], outs[1])).astype(BF16)
        CTX[l, r0:r1, :] = ctx
        yield
        if i == 0:
            far((2, 1), (3, 1))

            @pl.when((l == 0) & (ys_ == 1))
            def _():
                for a in REST:
                    hop_end(a)
            settle(l, REST, False)
        PF[r0:r1, :] = nn(ctx, WO[l])
        PRE[...] = nn(MS[...], WU[l])
        bup = VEC[l, 6:7, :]
        GB = 32

        def act(b, carry):
            u = PRE[rows(b * GB, GB), :] + bup
            cdf = 0.5 * (1.0 + lax.erf(u * RSQRT2))
            pdf = jnp.exp2(u * u * (-0.5 * LOG2E)) * INV_SQRT_2PI
            HID[l, rows(r0 + b * GB, GB), :] = (u * cdf).astype(BF16)
            GP[l, rows(r0 + b * GB, GB), :] = cdf + u * pdf
            return carry
        lax.fori_loop(0, C // GB, act, 0, unroll=True)
        PF[r0:r1, :] += nn(HID[l, r0:r1, :], WD[l])
        yield

    def backward(l, dl, i, last):
        r0, r1 = i * C, (i + 1) * C
        par = l % CORES
        first = i == NC - 1

        def acc(ref, val):
            if first:
                ref[par] = val
            else:
                ref[par] += val

        def acc_row(k, val, w=D):
            GV[l, k:k + 1, :w] += val

        norms(l, i)
        dy = H[dl, r0:r1, :]
        acc_row(4, col_sum(dy.astype(F32)))
        PRE[...] = nt(dy, WD[l])
        GB = 32

        def act(b, tot):
            d = PRE[rows(b * GB, GB), :] * GP[l, rows(r0 + b * GB, GB), :]
            DPB[rows(b * GB, GB), :] = d.astype(BF16)
            return tot + fold(d)
        dbu = lax.fori_loop(0, C // GB, act, jnp.zeros((8, F), F32), unroll=True)
        acc_row(5, col_sum(dbu))
        acc(GD, tn(HID[l, r0:r1, :], dy))
        yield
        acc(GU, tn(MS[...], DPB[...]))
        f0 = pf_row(i, True)
        PF[f0:f0 + C, :] = nt(DPB[...], WU[l])
        yield
        dctx = nt(dy, WO[l]).astype(BF16)
        ctx = CTX[l, r0:r1, :]
        acc(GO, tn(ctx, dy))
        prod = dctx.astype(F32) * ctx.astype(F32)
        q = Q[l, r0:r1, :].astype(F32)
        dcf = dctx.astype(F32)
        RBK = C // CORES
        dqt = []
        for h in range(CORES):
            sel = head_lane == h
            qm = jnp.where(sel, q, 0.0).astype(BF16)
            dcm = jnp.where(sel, dcf, 0.0).astype(BF16)
            dsum = jnp.transpose(jnp.where(sel, prod, 0.0))
            drow = col_sum(dsum)
            ST[:r1, :] = nt(V[l, :r1, :], dcm)

            def sub(b, carry):
                pr = PX[i][l, h, rows(b * RBK, RBK), :].astype(F32)
                DS[rows(b * RBK, RBK), :] = (pr * (ST[rows(b * RBK, RBK), :] - drow)).astype(BF16)
                return carry
            lax.fori_loop(0, r1 // RBK, sub, 0, unroll=True)
            dk = nn(DS[:r1, :], qm)
            dv = nn(PX[i][l, h], dcm)
            if first and h == 0:
                DK[:r1, :] = dk
                DV[:r1, :] = dv
            else:
                DK[:r1, :] += dk
                DV[:r1, :] += dv
            dqt.append(nn(KT[l, :, :r1], DS[:r1, :]))
            yield
        scale = E ** -0.5
        t = tabs(i)
        dq = unrotate(jnp.transpose(jnp.where(sub_head == 0, dqt[0], dqt[1])) * scale, t)
        dk = unrotate(DK[r0:r1, :] * scale, t)
        dv = DV[r0:r1, :]
        dqkv = jnp.concatenate([dq, dk, dv], axis=1)
        acc_row(6, col_sum(dqkv), 3 * E2)
        dqkv = dqkv.astype(BF16)
        dwq = tn(dqkv, AS[...])
        for k, r in enumerate(by_kind()):
            if first:
                GQ[par, r:r + E, :] = dwq[k * E:(k + 1) * E]
            else:
                GQ[par, r:r + E, :] += dwq[k * E:(k + 1) * E]
        PRE[...] = nn(dqkv, wq(l))
        yield
        g1, g2 = VEC[l, 0:1, :], VEC[l, 2:3, :]

        def lnb(b, tots):
            hf = H[l, rows(r0 + b * LB, LB), :].astype(F32)
            xhat, rstd = stats(hf)
            da = PRE[rows(b * LB, LB), :]
            dm = PF[rows(f0 + b * LB, LB), :]
            dx = da * g1 + dm * g2
            m1 = row_mean(dx)
            m2 = row_mean(dx * xhat)
            if not last:
                PF[rows(f0 + b * LB, LB), :] = rstd * (dx - m1 - xhat * m2)
            terms = (da * xhat, da, dm * xhat, dm)
            return tuple(a + fold(v) for a, v in zip(tots, terms))
        tots = lax.fori_loop(0, C // LB, lnb, tuple(jnp.zeros((8, D), F32) for _ in range(NA)), unroll=True)
        for k in range(NA):
            acc_row(k, col_sum(tots[k]))
        yield

    def g_half(a, k):
        return rows(k * G_HALF[a], G_HALF[a])

    def r1_view(l, a):
        return GP.at[l + 1, R1_OFF[a]:R1_OFF[a] + G_HALF[a], :G_COLS[a]]

    def g1_copy(l, a):
        return rcopy(G_BUF[a].at[l % CORES, g_half(a, 1 - c)], r1_view(l, a), g1s.at[a], g1r.at[l % CORES, a], pp=sib)

    def g2_copy(l, a):
        return rcopy(HID.at[l, R1_OFF[a]:R1_OFF[a] + G_HALF[a], :G_COLS[a]], R2[a].at[l % CORES], g2s.at[l % CORES, a], g2r.at[l % CORES, a], pp=2 * (l // CORES) + c)

    def g3_local(l, a):
        return lcopy(r1_view(l, a), G_OUT[a].at[g_half(a, c)], g3s.at[l % CORES, a])

    def g3_remote(l, a):
        return rcopy(r1_view(l, a), G_OUT[a].at[g_half(a, c)], g3s.at[l % CORES, a], g3r.at[a], pp=sib)

    def v1_copies(l):
        return [rcopy(GV.at[l], ZR.at[l, z], v1s.at[l, o - 1], v1r.at[l, z], tp=(z + o) % NT) for o in range(1, NT)]

    def grads_mid(l, arrays):
        for a in arrays:
            g1_copy(l, a).wait_recv()
            n = G_HALF[a]

            def add(b, carry):
                rr = rows(R1_OFF[a] + b * GR, GR)
                tot = G_BUF[a][l % CORES, rows(c * n + b * GR, GR), :] + GP[l + 1, rr, :G_COLS[a]]
                GP[l + 1, rr, :G_COLS[a]] = tot
                HID[l, rr, :G_COLS[a]] = tot.astype(BF16)
                return carry
            lax.fori_loop(0, n // GR, add, 0)

            @pl.when(l // CORES != ys_)
            def _():
                g2_copy(l, a).start()

    def grads_last(l):
        @pl.when(l // CORES == ys_)
        def _():
            for a in MLP + ATT:
                g2_copy(l, a).wait_recv()

                def add(b, carry):
                    rr = rows(R1_OFF[a] + b * GR, GR)
                    GP[l + 1, rr, :G_COLS[a]] += R2[a][l % CORES, rows(b * GR, GR), :].astype(F32)
                    return carry
                lax.fori_loop(0, G_HALF[a] // GR, add, 0)

                @pl.when(l == s)
                def _():
                    g3_local(l, a).start()

                @pl.when(l != s)
                def _():
                    g3_remote(l, a).start()

    def grads_sent(l):
        for a in range(NA):
            @pl.when(l // CORES != ys_)
            def _():
                g2_copy(l, a).wait_send()

            @pl.when(l == s)
            def _():
                g3_local(l, a).wait()

            @pl.when((l // CORES == ys_) & (l != s))
            def _():
                g3_remote(l, a).wait_send()

    def v2_copy(l):
        return rcopy(GZ.at[l], PR.at[s], v2s.at[l], v2r.at[s], pp=l)

    def vec_mid(l):
        ZR[l, z] = GV[l]
        for o in range(1, NT):
            q = (z + o) % NT
            rcopy(GV.at[l], ZR.at[l, q], v1s.at[l, o - 1], v1r.at[l, q], tp=q).wait_recv()
        tot = ZR[l, 0] + ZR[l, 1] + ZR[l, 2] + ZR[l, 3]
        row = lax.broadcasted_iota(jnp.int32, (8, D), 0)
        GZ[l] = jnp.where(row < 4, tot, GV[l])

        @pl.when(l == s)
        def _():
            PR[s] = GZ[l]

        @pl.when(l != s)
        def _():
            v2_copy(l).start()

    GV[...] = jnp.zeros_like(GV)
    @pl.when(ys_ == 1)
    def _():
        for a, hop in ((0, 0), (1, 0), (0, 1)):
            hop_on(a, hop)
        hop_end(0)
    settle(0, FIRST, True)
    xcopy.wait()

    def run(phases, at, handle, after=lambda k: None):
        for k, unused in enumerate(phases):
            after(k)
            for op, lag, u in at.get(k, ()):
                handle(op, lag, u)

    def fwd_layer(l, carry):
        for i in range(NC):
            @pl.when(l > 0)
            def _():
                ar_wait(l - 1, l, i)

            def handle(op, lag, u):
                m = i - lag

                def go(p, j):
                    if op == 'mid':
                        ar_mid(p, j, u)
                    else:
                        ar_last(p, p, p + 1, j, u)
                if m >= 0:
                    go(l, m)
                else:
                    @pl.when(l > 0)
                    def _():
                        go(l - 1, m + NC)
            run(forward(l, i), FWD_AT, handle)
            ar_send(l, i)
            if i == 1:
                @pl.when(l == 0)
                def _():
                    gcopy.wait()
                    H[NL + 1] = GP[NL].astype(BF16)

                    @pl.when(s == 1)
                    def _():
                        start_all(y_copies())
            if i == 2:
                @pl.when((l > 0) & (l < NL - 1))
                def _():
                    relay(l + 1, ALL)
            if i == NC - 1:
                @pl.when(l == 0)
                def _():
                    relay(l + 1, ALL)

                @pl.when(l < NL - 1)
                def _():
                    settle(l + 1, FIRST, True)
        return carry
    lax.fori_loop(0, NL, fwd_layer, 0)

    y_local = lcopy(H.at[NL], y.at[ys_, c], ys.at[0])
    y_sib = rcopy(H.at[NL], y.at[ys_, c], ys.at[1], yr.at[s], pp=sib)
    y_far = rcopy(H.at[NL], y.at[ys_, c], ys.at[2], yr.at[s], pp=oy + c)
    y_fwd = rcopy(y.at[1 - ys_, c], y.at[1 - ys_, c], ys.at[3], yr.at[oy + c], pp=sib)

    def y_arrived(q):
        rcopy(H.at[NL], y.at[q // CORES, q % CORES], ys.at[1], yr.at[q], pp=sib).wait_recv()

    def ri(l):
        return jnp.where(l == NL - 1, NL + 1, l + 1)

    def bwd_layer(lb, carry):
        l = NL - 1 - lb
        p = NL + lb
        for n in range(NC):
            i = NC - 1 - n

            @pl.when(lb > 0)
            def _():
                ar_wait(p - 1, l + 1, i)

            def handle(op, lag, u):
                m = n - lag

                def go(q, lq, j):
                    if op == 'mid':
                        ar_mid(q, j, u, True)
                    else:
                        ar_last(q, ri(lq), lq, j, u)
                if m >= 0:
                    @pl.when(l > 0)
                    def _():
                        go(p, l, NC - 1 - m)
                else:
                    @pl.when(lb > 0)
                    def _():
                        go(p - 1, l + 1, -1 - m)

                    @pl.when(lb == 0)
                    def _():
                        if op == 'mid':
                            ar_mid(NL - 1, m + NC, u)
                        else:
                            ar_last(NL - 1, NL - 1, NL, m + NC, u)

            def after(k):
                if k == 0 and n == 0:
                    @pl.when(lb > 0)
                    def _():
                        grads_mid(l + 1, ATT)
                        for a in ALL:
                            g1_copy(l + 1, a).wait_send()
                if n == NC - 1 and k == 1:
                    for a in MLP:
                        g1_copy(l, a).start()
                if n == NC - 1 and k == 3:
                    grads_mid(l, MLP)
            run(backward(l, ri(l), i, False), BWD_AT, handle, after)

            @pl.when(l > 0)
            def _():
                ar_send(p, i, True)
            if n == 1:
                @pl.when(lb > 0)
                def _():
                    vec_mid(l + 1)
            if n == 2:
                @pl.when(lb == 0)
                def _():
                    for j in range(NC):
                        ar_wait(NL - 1, NL, j)
                    start_all((y_local, y_sib, y_far))

                @pl.when(lb > 1)
                def _():
                    grads_last(l + 2)

        for a in ATT:
            g1_copy(l, a).start()
        start_all(v1_copies(l))
        return carry
    lax.fori_loop(0, NL, bwd_layer, 0)

    grads_mid(0, ATT)
    y_arrived(oy + c)
    y_fwd.start()
    grads_last(1)
    vec_mid(0)
    grads_last(0)

    for o in range(1, NL):
        q = (s + o) % NL
        rcopy(GZ.at[0], PR.at[q], v2s.at[0], v2r.at[q], pp=q).wait_recv()
    PRE[0:8, 0:D] = PR[0] + PR[1] + PR[2] + PR[3]
    vout = lcopy(PRE.at[0:8, 0:D], ovec, osem.at[0])
    vout.start()
    for l in range(NL):
        for cp in v1_copies(l):
            cp.wait_send()
    for l in range(NL):
        @pl.when(l != s)
        def _():
            v2_copy(l).wait_send()
    for a in range(NA):
        rcopy(G_OUT[a].at[g_half(a, 1 - c)], G_OUT[a].at[g_half(a, 1 - c)], g3s.at[a], g3r.at[a], pp=sib).wait_recv()
    y_local.wait()
    for cp in (y_sib, y_far, y_fwd):
        cp.wait_send()
    y_arrived(sib)
    y_arrived(oy + 1 - c)
    for a in range(NA):
        g1_copy(0, a).wait_send()
    for l in range(NL):
        grads_sent(l)
    for cp in sib_copies():
        cp.wait_send()
    @pl.when(s == 0)
    def _():
        for cp in first_copies():
            cp.wait_send()

    @pl.when(s > 0)
    def _():
        for cp in y_copies():
            cp.wait_send()
    for a in ALL:
        pass_copy(oy + 1, a, c).wait_send()

        @pl.when(ys_ == 0)
        def _():
            pass_copy(oy, a, c).wait_send()

        @pl.when(ys_ == 1)
        def _():
            for hop in range(CORES):
                for cp in hop_copies(a, hop):
                    cp.wait_send()

    @pl.when(is_end)
    def _():
        for t in range(NC * SUB):
            end_copy(0, t).wait_send()

    @pl.when(inner)
    def _():
        for t in range(NC * SUB):
            peer_copy(0, t).wait_send()
            back_copy(0, 1, t).wait_send()
    vout.wait()


def finish(y, gq, go, gu, gd, gv, yo, qo, oo, uo, do, n0, n1, n2, n3, n4, n5, n6, bq,
           yb, qb, ob, ub, db, vb, r0, r1, r2, r3, r4, r5, r6, rq, got, put, small):
    trips = [(gd, db, do), (gu, ub, uo), (go, ob, oo), (gq, qb, qo)]
    trips += [tuple(ref.at[m, r] for ref in (y, yb, yo)) for m in range(y.shape[0]) for r in range(y.shape[1])]
    loads = [pltpu.make_async_copy(a, b, got.at[k]) for k, (a, b, o) in enumerate(trips)]
    stores = [pltpu.make_async_copy(b, o, put.at[k]) for k, (a, b, o) in enumerate(trips)]
    vecs = pltpu.make_async_copy(gv, vb, small.at[len(trips)])
    vecs.start()
    for cp in loads:
        cp.start()
    vecs.wait()
    for row, refs in enumerate(((r0,), (r1,), (r2,), (r3,), (r4, r5), (r6,))):
        for ref in refs:
            ref[...] = vb[row:row + 1, :]
    e = rq.shape[2]
    for k in range(3):
        for h in range(CORES):
            rq[k, h:h + 1, :] = vb[6:7, (CORES * k + h) * e:(CORES * k + h + 1) * e]
    tiny = [pltpu.make_async_copy(a, b, small.at[k]) for k, (a, b) in enumerate(((r0, n0), (r1, n1), (r2, n2), (r3, n3), (r4, n4), (r5, n5), (r6, n6), (rq, bq)))]
    for cp in tiny:
        cp.start()
    for cp, out in zip(loads, stores):
        cp.wait()
        out.start()
    for cp in tiny + stores:
        cp.wait()


def finish_step(y, gq, go, gu, gd, gv, e):
    hbm = pl.BlockSpec(memory_space=pl.ANY)
    row = jax.ShapeDtypeStruct((1, gv.shape[1]), F32)
    outs = [jax.ShapeDtypeStruct(a.shape, a.dtype) for a in (y, gq, go, gu, gd)] + [row] * 7 + [jax.ShapeDtypeStruct((3, CORES, e), F32)]
    bufs = outs[:5] + [gv] + outs[5:]
    return pl.pallas_call(
        finish,
        out_shape=outs,
        in_specs=[hbm] * 6,
        out_specs=[hbm] * len(outs),
        scratch_shapes=[pltpu.VMEM(a.shape, a.dtype) for a in bufs] + [pltpu.SemaphoreType.DMA((9,))] * 3,
        name='neox_out',
    )(y, gq, go, gu, gd, gv)


def group_step(dims, *args):
    x = args[0]
    S, D, E, C, F = dims
    E2 = 2 * E
    hbm = pl.BlockSpec(memory_space=pl.ANY)
    out_shape = [
        jax.ShapeDtypeStruct(x.shape, BF16),
        jax.ShapeDtypeStruct((3 * E2, D), F32),
        jax.ShapeDtypeStruct((E2, D), F32),
        jax.ShapeDtypeStruct((D, F), F32),
        jax.ShapeDtypeStruct((F, D), F32),
        jax.ShapeDtypeStruct((8, D), F32),
    ]

    def vm(*shape, dtype=BF16):
        return pltpu.VMEM(shape, dtype)
    dma = pltpu.SemaphoreType.DMA
    scratch = [
        vm(NL, 3 * E2, D), vm(NL, E2, D), vm(NL, D, F), vm(NL, F, D), vm(NL, 8, D, dtype=F32),
        vm(NL + 2, S, D),
        vm(NL, S, E2), vm(NL, S, E2), vm(NL, S, E2), vm(NL, E2, S), vm(E2, S), vm(NL, S, E2),
        *[vm(NL, 2, (i + 1) * C, C) for i in range(NC)],
        vm(NL, S, F), vm(NL + 1, S, F, dtype=F32),
        vm(CORES, S, D), vm(CORES, S, D), vm(S, D), vm(S + C, D, dtype=F32),
        vm(CORES, 3 * E2, D, dtype=F32), vm(CORES, E2, D, dtype=F32), vm(CORES, D, F, dtype=F32), vm(CORES, F, D, dtype=F32),
        vm(CORES, 3 * E, D), vm(CORES, E, D), vm(CORES, D // CORES, F), vm(CORES, F // CORES, D),
        vm(S, E2, dtype=F32), vm(S, E2, dtype=F32),
        vm(CORES, C + 8, E2, dtype=F32), vm(S, E2, dtype=F32), vm(S, E2, dtype=F32),
        vm(NL, 8, D, dtype=F32), vm(NL, NT, 8, D, dtype=F32), vm(NL, 8, D, dtype=F32), vm(NL, 8, D, dtype=F32),
        vm(C, D), vm(C, D), vm(C, max(D, F), dtype=F32), vm(C, F), vm(S, C), vm(S, C, dtype=F32),
        *[vm(1, D, dtype=F32)] * 4, vm(1, D), vm(1, D), vm(1, F), vm(3, 2, E),
        dma((NA,)), dma((NA + 1,)), dma((CORES, NA + 1)), dma((NL, 2 * NA + 1)), dma((CORES, NA)), dma((3, NA)), dma((NA, 4)), dma((CORES,)), dma((1,)),
        dma((NC * SUB,)), dma((NC * SUB,)), dma((CORES, NC * SUB)), dma((CORES, NC * SUB)), dma((CORES, NC * SUB)),
        dma((NL,)), dma((NL,)), dma((NA,)), dma((CORES, NA)), dma((CORES, NA)), dma((CORES, NA)), dma((CORES, NA)), dma((NA,)),
        dma((NL, NT - 1)), dma((NL, NT)), dma((NL,)), dma((NL,)), dma((1,)), dma((8,)),
    ]
    return pl.pallas_call(
        functools.partial(body, dims),
        out_shape=out_shape,
        in_specs=[hbm] * len(args),
        out_specs=[hbm] * 6,
        scratch_shapes=scratch,
        compiler_params=pltpu.CompilerParams(collective_id=0, has_side_effects=True, vmem_limit_bytes=67043328),
        name='neox_group',
    )(*args)


def solution(mesh):
    def device_fn(x_in, g_out, ln1_gain, ln1_bias, w_qkv, b_qkv, w_out, b_out, ln2_gain, ln2_bias, w_up, b_up, w_down, b_down):
        n_micro, n_rows, S, D = x_in.shape
        heads, E = w_qkv.shape[2], w_qkv.shape[4]
        F = w_up.shape[2]
        C = S // NC
        wqkv = jnp.transpose(w_qkv[0], (1, 2, 3, 0)).reshape(heads * 3 * E, D)
        bqkv = jnp.transpose(b_qkv[0], (1, 0, 2))
        tab = jnp.asarray(rotary_base(C, NC, E, heads))
        part = group_step((S, D, E, C, F), x_in, g_out, wqkv, w_out[0].reshape(heads * E, D), w_up[0], w_down[0], ln1_gain, ln1_bias, ln2_gain, ln2_bias, b_out, b_down, b_up, bqkv, tab)
        y, gq, go, gup, gdn, n1g, n1b, n2g, n2b, gbo, gbd, gbu, gbq = finish_step(*part, E)
        gq = jnp.transpose(gq.reshape(heads, 3, E, D), (3, 0, 1, 2))[None]
        gbq = jnp.transpose(gbq, (1, 0, 2))[None]
        return (y, n1g, n1b, gq, gbq, go.reshape(1, heads, E, D), gbo, n2g, n2b, gup[None], gbu, gdn[None], gbd)

    return jax.shard_map(device_fn, mesh=mesh, in_specs=(P('dp'), P('dp')) + STAGE_SPECS, out_specs=(P('dp'),) + GRAD_SPECS, check_vma=False)
```

```python
import functools
import math

import jax
import jax.numpy as jnp
import numpy as np
from jax import lax
from jax.experimental import pallas as pl
from jax.experimental.pallas import tpu as pltpu
from jax.sharding import PartitionSpec as P

ROPE_BASE = 10000.0
LN_EPS = 1e-5
STAGE_SPECS = (P('pp'), P('pp'), P('pp', None, 'tp'), P('pp', 'tp'), P('pp', 'tp'), P('pp'), P('pp'), P('pp'), P('pp', None, 'tp'), P('pp', 'tp'), P('pp', 'tp'), P('pp'))
OWN = ('dp', 'pp')
GRAD_SPECS = (P(OWN), P(OWN), P(OWN, None, 'tp'), P(OWN, 'tp'), P(OWN, 'tp'), P(OWN), P(OWN), P(OWN), P(OWN, None, 'tp'), P(OWN, 'tp'), P(OWN, 'tp'), P(OWN))


F32 = jnp.float32
BF16 = jnp.bfloat16
NL = 4
NT = 4
NC = 4
NA = 4
CORES = 2
SUB = 4
FWD_AT = {k: (('mid', 1, k), ('last', 2, k)) for k in range(SUB)}
BWD_AT = {k: (('last', 2, k),) * (k < SUB) + (('mid', 1, k - 1),) * (k > 0) for k in range(SUB + 1)}
LOG2E = 1.4426950408889634
RSQRT2 = 0.7071067811865476
INV_SQRT_2PI = 0.3989422804014327


def nn(a, b):
    return lax.dot_general(a, b, (((1,), (0,)), ((), ())), preferred_element_type=F32)


def nt(a, b):
    return lax.dot_general(a, b, (((1,), (1,)), ((), ())), preferred_element_type=F32)


def tn(a, b):
    return lax.dot_general(a, b, (((0,), (0,)), ((), ())), preferred_element_type=F32)


def col_sum(v):
    return jnp.sum(v, axis=0, keepdims=True)


def row_mean(v):
    return jnp.mean(v, axis=-1, keepdims=True)


def fold(v):
    return jnp.sum(v.reshape(v.shape[0] // 8, 8, v.shape[1]), axis=0)


def rotary_base(chunk, n_chunks, head_dim, n_heads):
    rot_dim = head_dim // 4
    half = rot_dim // CORES
    inv_freq = np.zeros((head_dim,), np.float64)
    inv_freq[:rot_dim] = np.tile(ROPE_BASE ** (-(np.arange(half) * 2.0) / rot_dim), 2)
    inv_freq = np.tile(inv_freq, n_heads)
    pos = np.concatenate([np.arange(chunk), np.arange(8) * (np.arange(8) < n_chunks) * chunk]).astype(np.float64)
    ang = pos[:, None] * inv_freq[None, :]
    return np.stack([np.cos(ang), np.sin(ang)]).astype(np.float32)


def body(dims, x, g, wqkv, wo, wup, wdn, n0, n1, n2, n3, n4, n5, n6, bq, tab,
         y, oqkv, oo, oup, odn, ovec,
         WQ, WO, WU, WD, VEC, H, Q, K, V, KT, VT, CTX, P0, P1, P2, P3, HID, GP, RA, RB, PS, PF,
         GQ, GO, GU, GD, R2Q, R2O, R2U, R2D, DK, DV, TAB, COS, SIN, GV, ZR, GZ, PR,
         AS, MS, PRE, DPB, DS, ST, N0, N1, N2, N3, N4, N5, N6, BQ,
         wl, ws, wy, wr, wf, w0s, w0r, xs, gs, sab, sc, ra_s, rb_s, rc_s, ys, yr, g1s, g1r, g2s, g2r, g3s, g3r, v1s, v1r, v2s, v2r, osem, ns):
    S, D, E, C, F = dims
    E2 = 2 * E
    SR = C // SUB
    z = lax.axis_index('tp')
    xg = lax.axis_index('dp')
    s = lax.axis_index('pp')
    ys_ = s // CORES
    c = s % CORES
    sib = s + 1 - 2 * c
    oy = 2 * (1 - ys_)
    is_end = z * (NT - 1 - z) == 0
    inner = z * (NT - 1 - z) > 0
    hub = 1 + z // 3
    leaf = jnp.where(z == 1, 0, 3)
    peer = 3 - z
    PX = (P0, P1, P2, P3)
    W_IN = (wqkv, wo, wup, wdn)
    W_BUF = (WQ, WO, WU, WD)
    G_HALF = (3 * E, E, D // CORES, F // CORES)
    ALL, FIRST, REST = tuple(range(NA)), (0,), (1, 2, 3)
    ATT, MLP = ALL[:2], ALL[2:]
    G_BUF = (GQ, GO, GU, GD)
    G_OUT = (oqkv, oo, oup, odn)
    G_COLS = (D, D, F, D)
    R1_OFF = (0, 3 * E, 4 * E, 4 * E + D // CORES)
    R2 = (R2Q, R2O, R2U, R2D)

    def rcopy(src, dst, ss, rs, **dev):
        return pltpu.make_async_remote_copy(src_ref=src, dst_ref=dst, send_sem=ss, recv_sem=rs, device_id=dev, device_id_type=pl.DeviceIdType.MESH)

    def lcopy(src, dst, sem):
        return pltpu.make_async_copy(src, dst, sem)

    def rows(start, n):
        return pl.ds(pl.multiple_of(start, n), n)

    xcopy = lcopy(x.at[ys_, c], H.at[0], xs.at[0])
    xcopy.start()
    gcopy = lcopy(g.at[ys_, c], GP.at[NL], gs.at[0])
    gcopy.start()
    tcopy = lcopy(tab, TAB, xs.at[1])
    tcopy.start()
    for a in range(NA):
        lcopy(W_IN[a], W_BUF[a].at[s], wl.at[a]).start()
    small = [lcopy(a, b, ns.at[k]) for k, (a, b) in enumerate(((n0, N0), (n1, N1), (n2, N2), (n3, N3), (n4, N4), (n5, N5), (n6, N6), (bq, BQ)))]
    for cp in small:
        cp.start()

    bar = pltpu.get_barrier_semaphore()
    for o in range(1, NT):
        pl.semaphore_signal(bar, inc=1, device_id={'tp': (z + o) % NT}, device_id_type=pl.DeviceIdType.MESH)
    for o in range(1, NL):
        pl.semaphore_signal(bar, inc=1, device_id={'pp': (s + o) % NL}, device_id_type=pl.DeviceIdType.MESH)
    pl.semaphore_signal(bar, inc=1, device_id={'dp': 1 - xg}, device_id_type=pl.DeviceIdType.MESH)
    pl.semaphore_wait(bar, NT + NL - 1)

    def half(ref, a, k):
        return ref.at[rows(k * G_HALF[a], G_HALF[a])]

    def sib_copies():
        out = [rcopy(W_IN[a], W_BUF[a].at[s], ws.at[a], wr.at[s, 2 * a], pp=sib) for a in ALL]
        return out + [rcopy(VEC.at[s], VEC.at[s], ws.at[NA], wr.at[s, 2 * NA], pp=sib)]

    def y_copies():
        out = [rcopy(half(W_IN[a], a, k), half(W_BUF[a].at[s], a, k), wy.at[k, a], wr.at[s, 2 * a + k], pp=oy + k) for a in ALL for k in range(CORES)]
        return out[:2] + [rcopy(VEC.at[s], VEC.at[s], wy.at[k, NA], wr.at[s, 2 * NA], pp=oy + k) for k in range(CORES)] + out[2:]

    def quarter(ref, a, q):
        return ref.at[rows(q * (G_HALF[a] // CORES), G_HALF[a] // CORES)]

    def first_copies():
        out = []
        for a in ALL:
            for k in range(CORES):
                q = 2 * xg + k
                out.append(rcopy(quarter(W_IN[a], a, q), quarter(W_BUF[a].at[0], a, q), wy.at[k, a], w0r.at[a, q], pp=oy + k))
        return out + [rcopy(VEC.at[s], VEC.at[s], wy.at[k, NA], wr.at[s, 2 * NA], pp=oy + k) for k in range(CORES)]

    def mine(hop):
        return 2 * (xg if hop == 0 else 1 - xg) + c

    def hop_copies(a, hop):
        part, sem = quarter(W_BUF[a].at[0], a, mine(hop)), w0r.at[a, mine(hop)]
        out = [rcopy(part, part, w0s.at[hop, a], sem, pp=sib)]
        return out if hop else out + [rcopy(part, part, w0s.at[2, a], sem, dp=1 - xg)]

    def hop_on(a, hop):
        copies = hop_copies(a, hop)
        copies[0].wait_recv()
        start_all(copies)

    def hop_end(a):
        for k in range(CORES):
            part = quarter(W_BUF[a].at[0], a, 2 * k + 1 - c)
            rcopy(part, part, w0s.at[0, a], w0r.at[a, 2 * k + 1 - c], pp=sib).wait_recv()

    def start_all(copies):
        for cp in copies:
            cp.start()

    for cp in small:
        cp.wait()
    for k, ref in enumerate((N0, N1, N2, N3, N4, N5, N6)):
        VEC[s, k:k + 1, :] = ref[...].astype(F32)
    VEC[s, 7:8, :3 * E2] = jnp.concatenate([BQ[k, h:h + 1, :].astype(F32) for k in range(3) for h in range(CORES)], axis=1)

    @pl.when(s == 0)
    def _():
        start_all(first_copies())

    @pl.when(s > 1)
    def _():
        start_all(y_copies())
    start_all(sib_copies())

    def pass_copy(l, a, k):
        part = half(W_BUF[a].at[l], a, k)
        return rcopy(part, part, wf.at[l % CORES, a], wr.at[l, 2 * a + k], pp=sib)

    def relay(l, arrays):
        @pl.when(l // CORES != ys_)
        def _():
            for a in arrays:
                pass_copy(l, a, c).wait_recv()
                pass_copy(l, a, c).start()

    def settle(l, arrays, small):
        @pl.when(l == s)
        def _():
            for a in arrays:
                lcopy(W_IN[a], W_BUF[a].at[s], wl.at[a]).wait()

        @pl.when(l == sib)
        def _():
            for a in arrays:
                rcopy(W_IN[a], W_BUF[a].at[l], ws.at[a], wr.at[l, 2 * a], pp=sib).wait_recv()

        @pl.when((l // CORES != ys_) & (l > 0))
        def _():
            for a in arrays:
                pass_copy(l, a, 1 - c).wait_recv()
        if small:
            @pl.when(l != s)
            def _():
                rcopy(VEC.at[l], VEC.at[l], ws.at[NA], wr.at[l, 2 * NA], pp=sib).wait_recv()

    tcopy.wait()
    for i in range(NC):
        cb, sb = TAB[0, :C, :], TAB[1, :C, :]
        cr, sr = TAB[0, C + i:C + i + 1, :], TAB[1, C + i:C + i + 1, :]
        COS[i * C:(i + 1) * C, :] = cb * cr - sb * sr
        SIN[i * C:(i + 1) * C, :] = sb * cr + cb * sr

    lane = lax.broadcasted_iota(jnp.int32, (C, E2), 1)
    head_lane = lane // E
    in_head = lane % E
    rot_half = E // 8
    low = in_head < rot_half
    sub_head = lax.broadcasted_iota(jnp.int32, (E2, C), 0) // E
    lower = lax.broadcasted_iota(jnp.int32, (C, C), 0) <= lax.broadcasted_iota(jnp.int32, (C, C), 1)
    c1 = E ** -0.5 * LOG2E

    def tabs(i):
        cs, sn = COS[i * C:(i + 1) * C, :], SIN[i * C:(i + 1) * C, :]
        return cs, jnp.where(low, -sn, 0.0), jnp.where(low, 0.0, sn)

    def rotate(v, t):
        cs, sa, sb = t
        return v * cs + pltpu.roll(v, E2 - rot_half, 1) * sa + pltpu.roll(v, rot_half, 1) * sb

    def unrotate(v, t):
        cs, sa, sb = t
        return v * cs + pltpu.roll(v * sa, rot_half, 1) + pltpu.roll(v * sb, E2 - rot_half, 1)

    def end_copy(p, t):
        return rcopy(PS.at[t * SR:(t + 1) * SR], RA.at[p % CORES, t * SR:(t + 1) * SR], sab.at[t], ra_s.at[p % CORES, t], tp=hub)

    def peer_copy(p, t):
        return rcopy(PS.at[t * SR:(t + 1) * SR], RB.at[p % CORES, t * SR:(t + 1) * SR], sab.at[t], rb_s.at[p % CORES, t], tp=peer)

    def back_copy(p, di, t):
        return rcopy(H.at[di, t * SR:(t + 1) * SR], H.at[di, t * SR:(t + 1) * SR], sc.at[t], rc_s.at[p % CORES, t], tp=leaf)

    def pf_row(i, back):
        return (NC if back and i == NC - 1 else i) * C

    def ar_send(p, i, back=False):
        @pl.when(is_end)
        def _():
            for t in range(i * SUB, (i + 1) * SUB):
                @pl.when(p > 0)
                def _():
                    end_copy(p, t).wait_send()
                f0 = pf_row(i, back) + (t - i * SUB) * SR
                PS[t * SR:(t + 1) * SR, :] = PF[f0:f0 + SR, :].astype(BF16)
                end_copy(p, t).start()

    def ar_mid(p, i, u, back=False):
        t = i * SUB + u
        r = slice(t * SR, (t + 1) * SR)
        f0 = pf_row(i, back) + u * SR

        @pl.when(inner)
        def _():
            end_copy(p, t).wait_recv()
            @pl.when(p > 0)
            def _():
                peer_copy(p, t).wait_send()
            PS[r, :] = (PF[f0:f0 + SR, :] + RA[p % CORES, r, :].astype(F32)).astype(BF16)
            peer_copy(p, t).start()

    def ar_last(p, ri, di, i, u):
        t = i * SUB + u
        r = slice(t * SR, (t + 1) * SR)

        @pl.when(inner)
        def _():
            lv = jnp.minimum(p, NL - 1)
            bias = (VEC[lv, 4:5, :] + VEC[lv, 5:6, :]) * jnp.where(p < NL, 1.0, 0.0)
            peer_copy(p, t).wait_recv()
            @pl.when(p > 0)
            def _():
                back_copy(p, di, t).wait_send()
            both = PS[r, :].astype(F32) + RB[p % CORES, r, :].astype(F32)
            H[di, r, :] = (H[ri, r, :].astype(F32) + both + bias).astype(BF16)
            back_copy(p, di, t).start()

    def ar_wait(p, di, i):
        @pl.when(is_end)
        def _():
            for t in range(i * SUB, (i + 1) * SUB):
                back_copy(p, di, t).wait_recv()

    def stats(hf):
        cen = hf - row_mean(hf)
        rstd = lax.rsqrt(row_mean(cen * cen) + LN_EPS)
        return cen * rstd, rstd

    LB = 32
    GR = 32

    def norms(l, i):
        g1, b1, g2, b2 = (VEC[l, k:k + 1, :] for k in range(NA))

        def step(b, carry):
            hf = H[l, rows(i * C + b * LB, LB), :].astype(F32)
            xhat, unused = stats(hf)
            AS[rows(b * LB, LB), :] = (xhat * g1 + b1).astype(BF16)
            MS[rows(b * LB, LB), :] = (xhat * g2 + b2).astype(BF16)
            return carry
        lax.fori_loop(0, C // LB, step, 0, unroll=True)

    def by_kind():
        return [(h * 3 + k) * E for k in range(3) for h in range(CORES)]

    def wq(l):
        return jnp.concatenate([WQ[l, r:r + E, :] for r in by_kind()], axis=0)

    def forward(l, i):
        r0, r1 = i * C, (i + 1) * C
        norms(l, i)
        qkv = nt(AS[...], wq(l)) + VEC[l, 7:8, :3 * E2]
        qkv = qkv.astype(BF16).astype(F32)
        t = tabs(i)
        q = rotate(qkv[:, :E2], t).astype(BF16)
        kf = rotate(qkv[:, E2:2 * E2], t)
        vf = qkv[:, 2 * E2:3 * E2]
        Q[l, r0:r1, :] = q
        K[l, r0:r1, :] = kf.astype(BF16)
        V[l, r0:r1, :] = vf.astype(BF16)
        KT[l, :, r0:r1] = jnp.transpose(kf).astype(BF16)
        VT[:, r0:r1] = jnp.transpose(vf).astype(BF16)
        yield

        def far(*hops):
            if i == 0:
                @pl.when((l == 0) & (ys_ == 1))
                def _():
                    for a, hop in hops:
                        hop_on(a, hop)
        far((2, 0), (1, 1))
        RBK = C // CORES
        outs = []
        for h in range(CORES):
            qm = jnp.where(head_lane == h, Q[l, r0:r1, :].astype(F32), 0.0).astype(BF16)
            ST[:r1, :] = nt(K[l, :r1, :], qm)
            ST[r0:r1, :] = jnp.where(lower, ST[r0:r1, :], -1e30)

            def top(b, m):
                return jnp.maximum(m, jnp.max(ST[rows(b * RBK, RBK), :].reshape(RBK // 8, 8, C), axis=0))
            m = jnp.max(lax.fori_loop(0, r1 // RBK, top, jnp.full((8, C), -3e38, F32), unroll=True), axis=0, keepdims=True)
            mc = m * c1

            def expo(b, tot):
                e = jnp.exp2(ST[rows(b * RBK, RBK), :] * c1 - mc)
                ST[rows(b * RBK, RBK), :] = e
                return tot + fold(e)
            tot = col_sum(lax.fori_loop(0, r1 // RBK, expo, jnp.zeros((8, C), F32), unroll=True))
            inv = 1.0 / tot

            def put(b, carry):
                PX[i][l, h, rows(b * RBK, RBK), :] = (ST[rows(b * RBK, RBK), :] * inv).astype(BF16)
                return carry
            lax.fori_loop(0, r1 // RBK, put, 0, unroll=True)
            outs.append(nn(VT[:, :r1], PX[i][l, h]))
            if h == 0:
                yield
                far((3, 0))
        ctx = jnp.transpose(jnp.where(sub_head == 0, outs[0], outs[1])).astype(BF16)
        CTX[l, r0:r1, :] = ctx
        yield
        if i == 0:
            far((2, 1), (3, 1))

            @pl.when((l == 0) & (ys_ == 1))
            def _():
                for a in REST:
                    hop_end(a)
            settle(l, REST, False)
        PF[r0:r1, :] = nn(ctx, WO[l])
        PRE[...] = nn(MS[...], WU[l])
        bup = VEC[l, 6:7, :]
        GB = 32

        def act(b, carry):
            u = PRE[rows(b * GB, GB), :] + bup
            cdf = 0.5 * (1.0 + lax.erf(u * RSQRT2))
            pdf = jnp.exp2(u * u * (-0.5 * LOG2E)) * INV_SQRT_2PI
            HID[l, rows(r0 + b * GB, GB), :] = (u * cdf).astype(BF16)
            GP[l, rows(r0 + b * GB, GB), :] = cdf + u * pdf
            return carry
        lax.fori_loop(0, C // GB, act, 0, unroll=True)
        PF[r0:r1, :] += nn(HID[l, r0:r1, :], WD[l])
        yield

    def backward(l, dl, i, last):
        r0, r1 = i * C, (i + 1) * C
        par = l % CORES
        first = i == NC - 1

        def acc(ref, val):
            if first:
                ref[par] = val
            else:
                ref[par] += val

        def acc_row(k, val, w=D):
            GV[l, k:k + 1, :w] += val

        norms(l, i)
        dy = H[dl, r0:r1, :]
        acc_row(4, col_sum(dy.astype(F32)))
        PRE[...] = nt(dy, WD[l])
        GB = 32

        def act(b, tot):
            d = PRE[rows(b * GB, GB), :] * GP[l, rows(r0 + b * GB, GB), :]
            DPB[rows(b * GB, GB), :] = d.astype(BF16)
            return tot + fold(d)
        dbu = lax.fori_loop(0, C // GB, act, jnp.zeros((8, F), F32), unroll=True)
        acc_row(5, col_sum(dbu))
        acc(GD, tn(HID[l, r0:r1, :], dy))
        yield
        acc(GU, tn(MS[...], DPB[...]))
        f0 = pf_row(i, True)
        PF[f0:f0 + C, :] = nt(DPB[...], WU[l])
        yield
        dctx = nt(dy, WO[l]).astype(BF16)
        ctx = CTX[l, r0:r1, :]
        acc(GO, tn(ctx, dy))
        prod = dctx.astype(F32) * ctx.astype(F32)
        q = Q[l, r0:r1, :].astype(F32)
        dcf = dctx.astype(F32)
        RBK = C // CORES
        dqt = []
        for h in range(CORES):
            sel = head_lane == h
            qm = jnp.where(sel, q, 0.0).astype(BF16)
            dcm = jnp.where(sel, dcf, 0.0).astype(BF16)
            dsum = jnp.transpose(jnp.where(sel, prod, 0.0))
            drow = col_sum(dsum)
            ST[:r1, :] = nt(V[l, :r1, :], dcm)

            def sub(b, carry):
                pr = PX[i][l, h, rows(b * RBK, RBK), :].astype(F32)
                DS[rows(b * RBK, RBK), :] = (pr * (ST[rows(b * RBK, RBK), :] - drow)).astype(BF16)
                return carry
            lax.fori_loop(0, r1 // RBK, sub, 0, unroll=True)
            dk = nn(DS[:r1, :], qm)
            dv = nn(PX[i][l, h], dcm)
            if first and h == 0:
                DK[:r1, :] = dk
                DV[:r1, :] = dv
            else:
                DK[:r1, :] += dk
                DV[:r1, :] += dv
            dqt.append(nn(KT[l, :, :r1], DS[:r1, :]))
            yield
        scale = E ** -0.5
        t = tabs(i)
        dq = unrotate(jnp.transpose(jnp.where(sub_head == 0, dqt[0], dqt[1])) * scale, t)
        dk = unrotate(DK[r0:r1, :] * scale, t)
        dv = DV[r0:r1, :]
        dqkv = jnp.concatenate([dq, dk, dv], axis=1)
        acc_row(6, col_sum(dqkv), 3 * E2)
        dqkv = dqkv.astype(BF16)
        dwq = tn(dqkv, AS[...])
        for k, r in enumerate(by_kind()):
            if first:
                GQ[par, r:r + E, :] = dwq[k * E:(k + 1) * E]
            else:
                GQ[par, r:r + E, :] += dwq[k * E:(k + 1) * E]
        PRE[...] = nn(dqkv, wq(l))
        yield
        g1, g2 = VEC[l, 0:1, :], VEC[l, 2:3, :]

        def lnb(b, tots):
            hf = H[l, rows(r0 + b * LB, LB), :].astype(F32)
            xhat, rstd = stats(hf)
            da = PRE[rows(b * LB, LB), :]
            dm = PF[rows(f0 + b * LB, LB), :]
            dx = da * g1 + dm * g2
            m1 = row_mean(dx)
            m2 = row_mean(dx * xhat)
            if not last:
                PF[rows(f0 + b * LB, LB), :] = rstd * (dx - m1 - xhat * m2)
            terms = (da * xhat, da, dm * xhat, dm)
            return tuple(a + fold(v) for a, v in zip(tots, terms))
        tots = lax.fori_loop(0, C // LB, lnb, tuple(jnp.zeros((8, D), F32) for _ in range(NA)), unroll=True)
        for k in range(NA):
            acc_row(k, col_sum(tots[k]))
        yield

    def g_half(a, k):
        return rows(k * G_HALF[a], G_HALF[a])

    def r1_view(l, a):
        return GP.at[l + 1, R1_OFF[a]:R1_OFF[a] + G_HALF[a], :G_COLS[a]]

    def g1_copy(l, a):
        return rcopy(G_BUF[a].at[l % CORES, g_half(a, 1 - c)], r1_view(l, a), g1s.at[a], g1r.at[l % CORES, a], pp=sib)

    def g2_copy(l, a):
        return rcopy(HID.at[l, R1_OFF[a]:R1_OFF[a] + G_HALF[a], :G_COLS[a]], R2[a].at[l % CORES], g2s.at[l % CORES, a], g2r.at[l % CORES, a], pp=2 * (l // CORES) + c)

    def g3_local(l, a):
        return lcopy(r1_view(l, a), G_OUT[a].at[g_half(a, c)], g3s.at[l % CORES, a])

    def g3_remote(l, a):
        return rcopy(r1_view(l, a), G_OUT[a].at[g_half(a, c)], g3s.at[l % CORES, a], g3r.at[a], pp=sib)

    def v1_copies(l):
        return [rcopy(GV.at[l], ZR.at[l, z], v1s.at[l, o - 1], v1r.at[l, z], tp=(z + o) % NT) for o in range(1, NT)]

    def grads_mid(l, arrays):
        for a in arrays:
            g1_copy(l, a).wait_recv()
            n = G_HALF[a]

            def add(b, carry):
                rr = rows(R1_OFF[a] + b * GR, GR)
                tot = G_BUF[a][l % CORES, rows(c * n + b * GR, GR), :] + GP[l + 1, rr, :G_COLS[a]]
                GP[l + 1, rr, :G_COLS[a]] = tot
                HID[l, rr, :G_COLS[a]] = tot.astype(BF16)
                return carry
            lax.fori_loop(0, n // GR, add, 0)

            @pl.when(l // CORES != ys_)
            def _():
                g2_copy(l, a).start()

    def grads_last(l):
        @pl.when(l // CORES == ys_)
        def _():
            for a in MLP + ATT:
                g2_copy(l, a).wait_recv()

                def add(b, carry):
                    rr = rows(R1_OFF[a] + b * GR, GR)
                    GP[l + 1, rr, :G_COLS[a]] += R2[a][l % CORES, rows(b * GR, GR), :].astype(F32)
                    return carry
                lax.fori_loop(0, G_HALF[a] // GR, add, 0)

                @pl.when(l == s)
                def _():
                    g3_local(l, a).start()

                @pl.when(l != s)
                def _():
                    g3_remote(l, a).start()

    def grads_sent(l):
        for a in range(NA):
            @pl.when(l // CORES != ys_)
            def _():
                g2_copy(l, a).wait_send()

            @pl.when(l == s)
            def _():
                g3_local(l, a).wait()

            @pl.when((l // CORES == ys_) & (l != s))
            def _():
                g3_remote(l, a).wait_send()

    def v2_copy(l):
        return rcopy(GZ.at[l], PR.at[s], v2s.at[l], v2r.at[s], pp=l)

    def vec_mid(l):
        ZR[l, z] = GV[l]
        for o in range(1, NT):
            q = (z + o) % NT
            rcopy(GV.at[l], ZR.at[l, q], v1s.at[l, o - 1], v1r.at[l, q], tp=q).wait_recv()
        tot = ZR[l, 0] + ZR[l, 1] + ZR[l, 2] + ZR[l, 3]
        row = lax.broadcasted_iota(jnp.int32, (8, D), 0)
        GZ[l] = jnp.where(row < 4, tot, GV[l])

        @pl.when(l == s)
        def _():
            PR[s] = GZ[l]

        @pl.when(l != s)
        def _():
            v2_copy(l).start()

    GV[...] = jnp.zeros_like(GV)
    @pl.when(ys_ == 1)
    def _():
        for a, hop in ((0, 0), (1, 0), (0, 1)):
            hop_on(a, hop)
        hop_end(0)
    settle(0, FIRST, True)
    xcopy.wait()

    def run(phases, at, handle, after=lambda k: None):
        for k, unused in enumerate(phases):
            after(k)
            for op, lag, u in at.get(k, ()):
                handle(op, lag, u)

    def fwd_layer(l, carry):
        for i in range(NC):
            @pl.when(l > 0)
            def _():
                ar_wait(l - 1, l, i)

            def handle(op, lag, u):
                m = i - lag

                def go(p, j):
                    if op == 'mid':
                        ar_mid(p, j, u)
                    else:
                        ar_last(p, p, p + 1, j, u)
                if m >= 0:
                    go(l, m)
                else:
                    @pl.when(l > 0)
                    def _():
                        go(l - 1, m + NC)
            run(forward(l, i), FWD_AT, handle)
            ar_send(l, i)
            if i == 1:
                @pl.when(l == 0)
                def _():
                    gcopy.wait()
                    H[NL + 1] = GP[NL].astype(BF16)

                    @pl.when(s == 1)
                    def _():
                        start_all(y_copies())
            if i == 2:
                @pl.when((l > 0) & (l < NL - 1))
                def _():
                    relay(l + 1, ALL)
            if i == NC - 1:
                @pl.when(l == 0)
                def _():
                    relay(l + 1, ALL)

                @pl.when(l < NL - 1)
                def _():
                    settle(l + 1, FIRST, True)
        return carry
    lax.fori_loop(0, NL, fwd_layer, 0)

    y_local = lcopy(H.at[NL], y.at[ys_, c], ys.at[0])
    y_sib = rcopy(H.at[NL], y.at[ys_, c], ys.at[1], yr.at[s], pp=sib)
    y_far = rcopy(H.at[NL], y.at[ys_, c], ys.at[2], yr.at[s], pp=oy + c)
    y_fwd = rcopy(y.at[1 - ys_, c], y.at[1 - ys_, c], ys.at[3], yr.at[oy + c], pp=sib)

    def y_arrived(q):
        rcopy(H.at[NL], y.at[q // CORES, q % CORES], ys.at[1], yr.at[q], pp=sib).wait_recv()

    def ri(l):
        return jnp.where(l == NL - 1, NL + 1, l + 1)

    def bwd_layer(lb, carry):
        l = NL - 1 - lb
        p = NL + lb
        for n in range(NC):
            i = NC - 1 - n

            @pl.when(lb > 0)
            def _():
                ar_wait(p - 1, l + 1, i)

            def handle(op, lag, u):
                m = n - lag

                def go(q, lq, j):
                    if op == 'mid':
                        ar_mid(q, j, u, True)
                    else:
                        ar_last(q, ri(lq), lq, j, u)
                if m >= 0:
                    @pl.when(l > 0)
                    def _():
                        go(p, l, NC - 1 - m)
                else:
                    @pl.when(lb > 0)
                    def _():
                        go(p - 1, l + 1, -1 - m)

                    @pl.when(lb == 0)
                    def _():
                        if op == 'mid':
                            ar_mid(NL - 1, m + NC, u)
                        else:
                            ar_last(NL - 1, NL - 1, NL, m + NC, u)

            def after(k):
                if k == 0 and n == 0:
                    @pl.when(lb > 0)
                    def _():
                        grads_mid(l + 1, ATT)
                        for a in ALL:
                            g1_copy(l + 1, a).wait_send()
                if n == NC - 1 and k == 1:
                    for a in MLP:
                        g1_copy(l, a).start()
                if n == NC - 1 and k == 3:
                    @pl.when(l == 0)
                    def _():
                        grads_mid(l, MLP)
            run(backward(l, ri(l), i, False), BWD_AT, handle, after)

            @pl.when(l > 0)
            def _():
                ar_send(p, i, True)
            if n == 1:
                @pl.when(lb > 0)
                def _():
                    vec_mid(l + 1)
            if n == 2:
                @pl.when(lb == 0)
                def _():
                    for j in range(NC):
                        ar_wait(NL - 1, NL, j)
                    start_all((y_local, y_sib, y_far))

                @pl.when(lb > 1)
                def _():
                    grads_last(l + 2)

        for a in ATT:
            g1_copy(l, a).start()
        start_all(v1_copies(l))

        @pl.when(l > 0)
        def _():
            grads_mid(l, MLP)
        return carry
    lax.fori_loop(0, NL, bwd_layer, 0)

    grads_mid(0, ATT)
    y_arrived(oy + c)
    y_fwd.start()
    grads_last(1)
    vec_mid(0)
    grads_last(0)

    for o in range(1, NL):
        q = (s + o) % NL
        rcopy(GZ.at[0], PR.at[q], v2s.at[0], v2r.at[q], pp=q).wait_recv()
    PRE[0:8, 0:D] = PR[0] + PR[1] + PR[2] + PR[3]
    vout = lcopy(PRE.at[0:8, 0:D], ovec, osem.at[0])
    vout.start()
    for l in range(NL):
        for cp in v1_copies(l):
            cp.wait_send()
    for l in range(NL):
        @pl.when(l != s)
        def _():
            v2_copy(l).wait_send()
    for a in range(NA):
        rcopy(G_OUT[a].at[g_half(a, 1 - c)], G_OUT[a].at[g_half(a, 1 - c)], g3s.at[a], g3r.at[a], pp=sib).wait_recv()
    y_local.wait()
    for cp in (y_sib, y_far, y_fwd):
        cp.wait_send()
    y_arrived(sib)
    y_arrived(oy + 1 - c)
    for a in range(NA):
        g1_copy(0, a).wait_send()
    for l in range(NL):
        grads_sent(l)
    for cp in sib_copies():
        cp.wait_send()
    @pl.when(s == 0)
    def _():
        for cp in first_copies():
            cp.wait_send()

    @pl.when(s > 0)
    def _():
        for cp in y_copies():
            cp.wait_send()
    for a in ALL:
        pass_copy(oy + 1, a, c).wait_send()

        @pl.when(ys_ == 0)
        def _():
            pass_copy(oy, a, c).wait_send()

        @pl.when(ys_ == 1)
        def _():
            for hop in range(CORES):
                for cp in hop_copies(a, hop):
                    cp.wait_send()

    @pl.when(is_end)
    def _():
        for t in range(NC * SUB):
            end_copy(0, t).wait_send()

    @pl.when(inner)
    def _():
        for t in range(NC * SUB):
            peer_copy(0, t).wait_send()
            back_copy(0, 1, t).wait_send()
    vout.wait()


def finish(y, gq, go, gu, gd, gv, yo, qo, oo, uo, do, n0, n1, n2, n3, n4, n5, n6, bq,
           yb, qb, ob, ub, db, vb, r0, r1, r2, r3, r4, r5, r6, rq, got, put, small):
    trips = [(gd, db, do), (gu, ub, uo), (go, ob, oo), (gq, qb, qo)]
    trips += [tuple(ref.at[m, r] for ref in (y, yb, yo)) for m in range(y.shape[0]) for r in range(y.shape[1])]
    loads = [pltpu.make_async_copy(a, b, got.at[k]) for k, (a, b, o) in enumerate(trips)]
    stores = [pltpu.make_async_copy(b, o, put.at[k]) for k, (a, b, o) in enumerate(trips)]
    vecs = pltpu.make_async_copy(gv, vb, small.at[len(trips)])
    vecs.start()
    for cp in loads:
        cp.start()
    vecs.wait()
    for row, refs in enumerate(((r0,), (r1,), (r2,), (r3,), (r4, r5), (r6,))):
        for ref in refs:
            ref[...] = vb[row:row + 1, :]
    e = rq.shape[2]
    for k in range(3):
        for h in range(CORES):
            rq[k, h:h + 1, :] = vb[6:7, (CORES * k + h) * e:(CORES * k + h + 1) * e]
    tiny = [pltpu.make_async_copy(a, b, small.at[k]) for k, (a, b) in enumerate(((r0, n0), (r1, n1), (r2, n2), (r3, n3), (r4, n4), (r5, n5), (r6, n6), (rq, bq)))]
    for cp in tiny:
        cp.start()
    for cp, out in zip(loads, stores):
        cp.wait()
        out.start()
    for cp in tiny + stores:
        cp.wait()


def finish_step(y, gq, go, gu, gd, gv, e):
    hbm = pl.BlockSpec(memory_space=pl.ANY)
    row = jax.ShapeDtypeStruct((1, gv.shape[1]), F32)
    outs = [jax.ShapeDtypeStruct(a.shape, a.dtype) for a in (y, gq, go, gu, gd)] + [row] * 7 + [jax.ShapeDtypeStruct((3, CORES, e), F32)]
    bufs = outs[:5] + [gv] + outs[5:]
    return pl.pallas_call(
        finish,
        out_shape=outs,
        in_specs=[hbm] * 6,
        out_specs=[hbm] * len(outs),
        scratch_shapes=[pltpu.VMEM(a.shape, a.dtype) for a in bufs] + [pltpu.SemaphoreType.DMA((9,))] * 3,
        name='neox_out',
    )(y, gq, go, gu, gd, gv)


def group_step(dims, *args):
    x = args[0]
    S, D, E, C, F = dims
    E2 = 2 * E
    hbm = pl.BlockSpec(memory_space=pl.ANY)
    out_shape = [
        jax.ShapeDtypeStruct(x.shape, BF16),
        jax.ShapeDtypeStruct((3 * E2, D), F32),
        jax.ShapeDtypeStruct((E2, D), F32),
        jax.ShapeDtypeStruct((D, F), F32),
        jax.ShapeDtypeStruct((F, D), F32),
        jax.ShapeDtypeStruct((8, D), F32),
    ]

    def vm(*shape, dtype=BF16):
        return pltpu.VMEM(shape, dtype)
    dma = pltpu.SemaphoreType.DMA
    scratch = [
        vm(NL, 3 * E2, D), vm(NL, E2, D), vm(NL, D, F), vm(NL, F, D), vm(NL, 8, D, dtype=F32),
        vm(NL + 2, S, D),
        vm(NL, S, E2), vm(NL, S, E2), vm(NL, S, E2), vm(NL, E2, S), vm(E2, S), vm(NL, S, E2),
        *[vm(NL, 2, (i + 1) * C, C) for i in range(NC)],
        vm(NL, S, F), vm(NL + 1, S, F, dtype=F32),
        vm(CORES, S, D), vm(CORES, S, D), vm(S, D), vm(S + C, D, dtype=F32),
        vm(CORES, 3 * E2, D, dtype=F32), vm(CORES, E2, D, dtype=F32), vm(CORES, D, F, dtype=F32), vm(CORES, F, D, dtype=F32),
        vm(CORES, 3 * E, D), vm(CORES, E, D), vm(CORES, D // CORES, F), vm(CORES, F // CORES, D),
        vm(S, E2, dtype=F32), vm(S, E2, dtype=F32),
        vm(CORES, C + 8, E2, dtype=F32), vm(S, E2, dtype=F32), vm(S, E2, dtype=F32),
        vm(NL, 8, D, dtype=F32), vm(NL, NT, 8, D, dtype=F32), vm(NL, 8, D, dtype=F32), vm(NL, 8, D, dtype=F32),
        vm(C, D), vm(C, D), vm(C, max(D, F), dtype=F32), vm(C, F), vm(S, C), vm(S, C, dtype=F32),
        *[vm(1, D, dtype=F32)] * 4, vm(1, D), vm(1, D), vm(1, F), vm(3, 2, E),
        dma((NA,)), dma((NA + 1,)), dma((CORES, NA + 1)), dma((NL, 2 * NA + 1)), dma((CORES, NA)), dma((3, NA)), dma((NA, 4)), dma((CORES,)), dma((1,)),
        dma((NC * SUB,)), dma((NC * SUB,)), dma((CORES, NC * SUB)), dma((CORES, NC * SUB)), dma((CORES, NC * SUB)),
        dma((NL,)), dma((NL,)), dma((NA,)), dma((CORES, NA)), dma((CORES, NA)), dma((CORES, NA)), dma((CORES, NA)), dma((NA,)),
        dma((NL, NT - 1)), dma((NL, NT)), dma((NL,)), dma((NL,)), dma((1,)), dma((8,)),
    ]
    return pl.pallas_call(
        functools.partial(body, dims),
        out_shape=out_shape,
        in_specs=[hbm] * len(args),
        out_specs=[hbm] * 6,
        scratch_shapes=scratch,
        compiler_params=pltpu.CompilerParams(collective_id=0, has_side_effects=True, vmem_limit_bytes=67043328),
        name='neox_group',
    )(*args)


def solution(mesh):
    def device_fn(x_in, g_out, ln1_gain, ln1_bias, w_qkv, b_qkv, w_out, b_out, ln2_gain, ln2_bias, w_up, b_up, w_down, b_down):
        n_micro, n_rows, S, D = x_in.shape
        heads, E = w_qkv.shape[2], w_qkv.shape[4]
        F = w_up.shape[2]
        C = S // NC
        wqkv = jnp.transpose(w_qkv[0], (1, 2, 3, 0)).reshape(heads * 3 * E, D)
        bqkv = jnp.transpose(b_qkv[0], (1, 0, 2))
        tab = jnp.asarray(rotary_base(C, NC, E, heads))
        part = group_step((S, D, E, C, F), x_in, g_out, wqkv, w_out[0].reshape(heads * E, D), w_up[0], w_down[0], ln1_gain, ln1_bias, ln2_gain, ln2_bias, b_out, b_down, b_up, bqkv, tab)
        y, gq, go, gup, gdn, n1g, n1b, n2g, n2b, gbo, gbd, gbu, gbq = finish_step(*part, E)
        gq = jnp.transpose(gq.reshape(heads, 3, E, D), (3, 0, 1, 2))[None]
        gbq = jnp.transpose(gbq, (1, 0, 2))[None]
        return (y, n1g, n1b, gq, gbq, go.reshape(1, heads, E, D), gbo, n2g, n2b, gup[None], gbu, gdn[None], gbd)

    return jax.shard_map(device_fn, mesh=mesh, in_specs=(P('dp'), P('dp')) + STAGE_SPECS, out_specs=(P('dp'),) + GRAD_SPECS, check_vma=False)
```

```python
import functools
import math

import jax
import jax.numpy as jnp
import numpy as np
from jax import lax
from jax.experimental import pallas as pl
from jax.experimental.pallas import tpu as pltpu
from jax.sharding import PartitionSpec as P

ROPE_BASE = 10000.0
LN_EPS = 1e-5
STAGE_SPECS = (P('pp'), P('pp'), P('pp', None, 'tp'), P('pp', 'tp'), P('pp', 'tp'), P('pp'), P('pp'), P('pp'), P('pp', None, 'tp'), P('pp', 'tp'), P('pp', 'tp'), P('pp'))
OWN = ('dp', 'pp')
GRAD_SPECS = (P(OWN), P(OWN), P(OWN, None, 'tp'), P(OWN, 'tp'), P(OWN, 'tp'), P(OWN), P(OWN), P(OWN), P(OWN, None, 'tp'), P(OWN, 'tp'), P(OWN, 'tp'), P(OWN))


F32 = jnp.float32
BF16 = jnp.bfloat16
NL = 4
NT = 4
NC = 4
NA = 4
CORES = 2
SUB = 2
FWD_AT = {0: (('mid', 1, 0), ('last', 2, 0)), 2: (('mid', 1, 1), ('last', 2, 1))}
BWD_AT = {0: (('last', 2, 0),), 1: (('mid', 1, 0),), 3: (('last', 2, 1),), 4: (('mid', 1, 1),)}
LOG2E = 1.4426950408889634
RSQRT2 = 0.7071067811865476
INV_SQRT_2PI = 0.3989422804014327


def nn(a, b):
    return lax.dot_general(a, b, (((1,), (0,)), ((), ())), preferred_element_type=F32)


def nt(a, b):
    return lax.dot_general(a, b, (((1,), (1,)), ((), ())), preferred_element_type=F32)


def tn(a, b):
    return lax.dot_general(a, b, (((0,), (0,)), ((), ())), preferred_element_type=F32)


def col_sum(v):
    return jnp.sum(v, axis=0, keepdims=True)


def row_mean(v):
    return jnp.mean(v, axis=-1, keepdims=True)


def fold(v):
    return jnp.sum(v.reshape(v.shape[0] // 8, 8, v.shape[1]), axis=0)


def rotary_base(chunk, n_chunks, head_dim, n_heads):
    rot_dim = head_dim // 4
    half = rot_dim // CORES
    inv_freq = np.zeros((head_dim,), np.float64)
    inv_freq[:rot_dim] = np.tile(ROPE_BASE ** (-(np.arange(half) * 2.0) / rot_dim), 2)
    inv_freq = np.tile(inv_freq, n_heads)
    pos = np.concatenate([np.arange(chunk), np.arange(8) * (np.arange(8) < n_chunks) * chunk]).astype(np.float64)
    ang = pos[:, None] * inv_freq[None, :]
    return np.stack([np.cos(ang), np.sin(ang)]).astype(np.float32)


def body(dims, x, g, wqkv, wo, wup, wdn, n0, n1, n2, n3, n4, n5, n6, bq, tab,
         y, oqkv, oo, oup, odn, ovec,
         WQ, WO, WU, WD, VEC, H, Q, K, V, KT, VT, CTX, P0, P1, P2, P3, HID, GP, RA, RB, PS, PF,
         GQ, GO, GU, GD, R2Q, R2O, R2U, R2D, DK, DV, TAB, COS, SIN, GV, ZR, GZ, PR,
         AS, MS, PRE, DPB, DS, ST, N0, N1, N2, N3, N4, N5, N6, BQ,
         wl, ws, wy, wr, wf, w0s, w0r, xs, gs, sab, sc, ra_s, rb_s, rc_s, ys, yr, g1s, g1r, g2s, g2r, g3s, g3r, v1s, v1r, v2s, v2r, osem, ns):
    S, D, E, C, F = dims
    E2 = 2 * E
    SR = C // SUB
    z = lax.axis_index('tp')
    xg = lax.axis_index('dp')
    s = lax.axis_index('pp')
    ys_ = s // CORES
    c = s % CORES
    sib = s + 1 - 2 * c
    oy = 2 * (1 - ys_)
    is_end = z * (NT - 1 - z) == 0
    inner = z * (NT - 1 - z) > 0
    hub = 1 + z // 3
    leaf = jnp.where(z == 1, 0, 3)
    peer = 3 - z
    PX = (P0, P1, P2, P3)
    W_IN = (wqkv, wo, wup, wdn)
    W_BUF = (WQ, WO, WU, WD)
    G_HALF = (3 * E, E, D // CORES, F // CORES)
    ALL, FIRST, REST = tuple(range(NA)), (0,), (1, 2, 3)
    ATT, MLP = ALL[:2], ALL[2:]
    G_BUF = (GQ, GO, GU, GD)
    G_OUT = (oqkv, oo, oup, odn)
    G_COLS = (D, D, F, D)
    R1_OFF = (0, 3 * E, 4 * E, 4 * E + D // CORES)
    R2 = (R2Q, R2O, R2U, R2D)

    def rcopy(src, dst, ss, rs, **dev):
        return pltpu.make_async_remote_copy(src_ref=src, dst_ref=dst, send_sem=ss, recv_sem=rs, device_id=dev, device_id_type=pl.DeviceIdType.MESH)

    def lcopy(src, dst, sem):
        return pltpu.make_async_copy(src, dst, sem)

    def rows(start, n):
        return pl.ds(pl.multiple_of(start, n), n)

    xcopy = lcopy(x.at[ys_, c], H.at[0], xs.at[0])
    xcopy.start()
    gcopy = lcopy(g.at[ys_, c], GP.at[NL], gs.at[0])
    gcopy.start()
    tcopy = lcopy(tab, TAB, xs.at[1])
    tcopy.start()
    for a in range(NA):
        lcopy(W_IN[a], W_BUF[a].at[s], wl.at[a]).start()
    small = [lcopy(a, b, ns.at[k]) for k, (a, b) in enumerate(((n0, N0), (n1, N1), (n2, N2), (n3, N3), (n4, N4), (n5, N5), (n6, N6), (bq, BQ)))]
    for cp in small:
        cp.start()

    bar = pltpu.get_barrier_semaphore()
    for o in range(1, NT):
        pl.semaphore_signal(bar, inc=1, device_id={'tp': (z + o) % NT}, device_id_type=pl.DeviceIdType.MESH)
    for o in range(1, NL):
        pl.semaphore_signal(bar, inc=1, device_id={'pp': (s + o) % NL}, device_id_type=pl.DeviceIdType.MESH)
    pl.semaphore_signal(bar, inc=1, device_id={'dp': 1 - xg}, device_id_type=pl.DeviceIdType.MESH)
    pl.semaphore_wait(bar, NT + NL - 1)

    def half(ref, a, k):
        return ref.at[rows(k * G_HALF[a], G_HALF[a])]

    def sib_copies():
        out = [rcopy(W_IN[a], W_BUF[a].at[s], ws.at[a], wr.at[s, 2 * a], pp=sib) for a in ALL]
        return out + [rcopy(VEC.at[s], VEC.at[s], ws.at[NA], wr.at[s, 2 * NA], pp=sib)]

    def y_copies():
        out = [rcopy(half(W_IN[a], a, k), half(W_BUF[a].at[s], a, k), wy.at[k, a], wr.at[s, 2 * a + k], pp=oy + k) for a in ALL for k in range(CORES)]
        return out[:2] + [rcopy(VEC.at[s], VEC.at[s], wy.at[k, NA], wr.at[s, 2 * NA], pp=oy + k) for k in range(CORES)] + out[2:]

    def quarter(ref, a, q):
        return ref.at[rows(q * (G_HALF[a] // CORES), G_HALF[a] // CORES)]

    def first_copies():
        out = []
        for a in ALL:
            for k in range(CORES):
                q = 2 * xg + k
                out.append(rcopy(quarter(W_IN[a], a, q), quarter(W_BUF[a].at[0], a, q), wy.at[k, a], w0r.at[a, q], pp=oy + k))
        return out + [rcopy(VEC.at[s], VEC.at[s], wy.at[k, NA], wr.at[s, 2 * NA], pp=oy + k) for k in range(CORES)]

    def mine(hop):
        return 2 * (xg if hop == 0 else 1 - xg) + c

    def hop_copies(a, hop):
        part, sem = quarter(W_BUF[a].at[0], a, mine(hop)), w0r.at[a, mine(hop)]
        out = [rcopy(part, part, w0s.at[hop, a], sem, pp=sib)]
        return out if hop else out + [rcopy(part, part, w0s.at[2, a], sem, dp=1 - xg)]

    def hop_on(a, hop):
        copies = hop_copies(a, hop)
        copies[0].wait_recv()
        start_all(copies)

    def hop_end(a):
        for k in range(CORES):
            part = quarter(W_BUF[a].at[0], a, 2 * k + 1 - c)
            rcopy(part, part, w0s.at[0, a], w0r.at[a, 2 * k + 1 - c], pp=sib).wait_recv()

    def start_all(copies):
        for cp in copies:
            cp.start()

    for cp in small:
        cp.wait()
    for k, ref in enumerate((N0, N1, N2, N3, N4, N5, N6)):
        VEC[s, k:k + 1, :] = ref[...].astype(F32)
    VEC[s, 7:8, :3 * E2] = jnp.concatenate([BQ[k, h:h + 1, :].astype(F32) for k in range(3) for h in range(CORES)], axis=1)

    @pl.when(s == 0)
    def _():
        start_all(first_copies())

    @pl.when(s > 1)
    def _():
        start_all(y_copies())
    start_all(sib_copies())

    def pass_copy(l, a, k):
        part = half(W_BUF[a].at[l], a, k)
        return rcopy(part, part, wf.at[l % CORES, a], wr.at[l, 2 * a + k], pp=sib)

    def relay(l, arrays):
        @pl.when(l // CORES != ys_)
        def _():
            for a in arrays:
                pass_copy(l, a, c).wait_recv()
                pass_copy(l, a, c).start()

    def settle(l, arrays, small):
        @pl.when(l == s)
        def _():
            for a in arrays:
                lcopy(W_IN[a], W_BUF[a].at[s], wl.at[a]).wait()

        @pl.when(l == sib)
        def _():
            for a in arrays:
                rcopy(W_IN[a], W_BUF[a].at[l], ws.at[a], wr.at[l, 2 * a], pp=sib).wait_recv()

        @pl.when((l // CORES != ys_) & (l > 0))
        def _():
            for a in arrays:
                pass_copy(l, a, 1 - c).wait_recv()
        if small:
            @pl.when(l != s)
            def _():
                rcopy(VEC.at[l], VEC.at[l], ws.at[NA], wr.at[l, 2 * NA], pp=sib).wait_recv()

    tcopy.wait()
    for i in range(NC):
        cb, sb = TAB[0, :C, :], TAB[1, :C, :]
        cr, sr = TAB[0, C + i:C + i + 1, :], TAB[1, C + i:C + i + 1, :]
        COS[i * C:(i + 1) * C, :] = cb * cr - sb * sr
        SIN[i * C:(i + 1) * C, :] = sb * cr + cb * sr

    lane = lax.broadcasted_iota(jnp.int32, (C, E2), 1)
    head_lane = lane // E
    in_head = lane % E
    rot_half = E // 8
    low = in_head < rot_half
    sub_head = lax.broadcasted_iota(jnp.int32, (E2, C), 0) // E
    lower = lax.broadcasted_iota(jnp.int32, (C, C), 0) <= lax.broadcasted_iota(jnp.int32, (C, C), 1)
    c1 = E ** -0.5 * LOG2E

    def tabs(i):
        cs, sn = COS[i * C:(i + 1) * C, :], SIN[i * C:(i + 1) * C, :]
        return cs, jnp.where(low, -sn, 0.0), jnp.where(low, 0.0, sn)

    def rotate(v, t):
        cs, sa, sb = t
        return v * cs + pltpu.roll(v, E2 - rot_half, 1) * sa + pltpu.roll(v, rot_half, 1) * sb

    def unrotate(v, t):
        cs, sa, sb = t
        return v * cs + pltpu.roll(v * sa, rot_half, 1) + pltpu.roll(v * sb, E2 - rot_half, 1)

    def end_copy(p, t):
        return rcopy(PS.at[t * SR:(t + 1) * SR], RA.at[p % CORES, t * SR:(t + 1) * SR], sab.at[t], ra_s.at[p % CORES, t], tp=hub)

    def peer_copy(p, t):
        return rcopy(PS.at[t * SR:(t + 1) * SR], RB.at[p % CORES, t * SR:(t + 1) * SR], sab.at[t], rb_s.at[p % CORES, t], tp=peer)

    def back_copy(p, di, t):
        return rcopy(H.at[di, t * SR:(t + 1) * SR], H.at[di, t * SR:(t + 1) * SR], sc.at[t], rc_s.at[p % CORES, t], tp=leaf)

    def pf_row(i, back):
        return (NC if back and i == NC - 1 else i) * C

    def ar_send(p, i, back=False):
        @pl.when(is_end)
        def _():
            for t in range(i * SUB, (i + 1) * SUB):
                @pl.when(p > 0)
                def _():
                    end_copy(p, t).wait_send()
                f0 = pf_row(i, back) + (t - i * SUB) * SR
                PS[t * SR:(t + 1) * SR, :] = PF[f0:f0 + SR, :].astype(BF16)
                end_copy(p, t).start()

    def ar_mid(p, i, u, back=False):
        t = i * SUB + u
        r = slice(t * SR, (t + 1) * SR)
        f0 = pf_row(i, back) + u * SR

        @pl.when(inner)
        def _():
            end_copy(p, t).wait_recv()
            @pl.when(p > 0)
            def _():
                peer_copy(p, t).wait_send()
            PS[r, :] = (PF[f0:f0 + SR, :] + RA[p % CORES, r, :].astype(F32)).astype(BF16)
            peer_copy(p, t).start()

    def ar_last(p, ri, di, i, u):
        t = i * SUB + u
        r = slice(t * SR, (t + 1) * SR)

        @pl.when(inner)
        def _():
            lv = jnp.minimum(p, NL - 1)
            bias = (VEC[lv, 4:5, :] + VEC[lv, 5:6, :]) * jnp.where(p < NL, 1.0, 0.0)
            peer_copy(p, t).wait_recv()
            @pl.when(p > 0)
            def _():
                back_copy(p, di, t).wait_send()
            both = PS[r, :].astype(F32) + RB[p % CORES, r, :].astype(F32)
            H[di, r, :] = (H[ri, r, :].astype(F32) + both + bias).astype(BF16)
            back_copy(p, di, t).start()

    def ar_wait(p, di, i):
        @pl.when(is_end)
        def _():
            for t in range(i * SUB, (i + 1) * SUB):
                back_copy(p, di, t).wait_recv()

    def stats(hf):
        cen = hf - row_mean(hf)
        rstd = lax.rsqrt(row_mean(cen * cen) + LN_EPS)
        return cen * rstd, rstd

    LB = 32
    GR = 32

    def norms(l, i):
        g1, b1, g2, b2 = (VEC[l, k:k + 1, :] for k in range(NA))

        def step(b, carry):
            hf = H[l, rows(i * C + b * LB, LB), :].astype(F32)
            xhat, unused = stats(hf)
            AS[rows(b * LB, LB), :] = (xhat * g1 + b1).astype(BF16)
            MS[rows(b * LB, LB), :] = (xhat * g2 + b2).astype(BF16)
            return carry
        lax.fori_loop(0, C // LB, step, 0, unroll=True)

    def by_kind():
        return [(h * 3 + k) * E for k in range(3) for h in range(CORES)]

    def wq(l):
        return jnp.concatenate([WQ[l, r:r + E, :] for r in by_kind()], axis=0)

    def forward(l, i):
        r0, r1 = i * C, (i + 1) * C
        norms(l, i)
        qkv = nt(AS[...], wq(l)) + VEC[l, 7:8, :3 * E2]
        qkv = qkv.astype(BF16).astype(F32)
        t = tabs(i)
        q = rotate(qkv[:, :E2], t).astype(BF16)
        kf = rotate(qkv[:, E2:2 * E2], t)
        vf = qkv[:, 2 * E2:3 * E2]
        Q[l, r0:r1, :] = q
        K[l, r0:r1, :] = kf.astype(BF16)
        V[l, r0:r1, :] = vf.astype(BF16)
        KT[l, :, r0:r1] = jnp.transpose(kf).astype(BF16)
        VT[:, r0:r1] = jnp.transpose(vf).astype(BF16)
        yield

        def far(*hops):
            if i == 0:
                @pl.when((l == 0) & (ys_ == 1))
                def _():
                    for a, hop in hops:
                        hop_on(a, hop)
        far((3, 0))
        RBK = C // CORES
        outs = []
        for h in range(CORES):
            qm = jnp.where(head_lane == h, Q[l, r0:r1, :].astype(F32), 0.0).astype(BF16)
            ST[:r1, :] = nt(K[l, :r1, :], qm)
            ST[r0:r1, :] = jnp.where(lower, ST[r0:r1, :], -1e30)

            def top(b, m):
                return jnp.maximum(m, jnp.max(ST[rows(b * RBK, RBK), :].reshape(RBK // 8, 8, C), axis=0))
            m = jnp.max(lax.fori_loop(0, r1 // RBK, top, jnp.full((8, C), -3e38, F32), unroll=True), axis=0, keepdims=True)
            mc = m * c1

            def expo(b, tot):
                e = jnp.exp2(ST[rows(b * RBK, RBK), :] * c1 - mc)
                ST[rows(b * RBK, RBK), :] = e
                return tot + fold(e)
            tot = col_sum(lax.fori_loop(0, r1 // RBK, expo, jnp.zeros((8, C), F32), unroll=True))
            inv = 1.0 / tot

            def put(b, carry):
                PX[i][l, h, rows(b * RBK, RBK), :] = (ST[rows(b * RBK, RBK), :] * inv).astype(BF16)
                return carry
            lax.fori_loop(0, r1 // RBK, put, 0, unroll=True)
            outs.append(nn(VT[:, :r1], PX[i][l, h]))
            if h == 0:
                yield
        ctx = jnp.transpose(jnp.where(sub_head == 0, outs[0], outs[1])).astype(BF16)
        CTX[l, r0:r1, :] = ctx
        yield
        if i == 0:
            far((2, 1), (3, 1))

            @pl.when((l == 0) & (ys_ == 1))
            def _():
                for a in REST:
                    hop_end(a)
            settle(l, REST, False)
        PF[r0:r1, :] = nn(ctx, WO[l])
        PRE[...] = nn(MS[...], WU[l])
        bup = VEC[l, 6:7, :]
        GB = 32

        def act(b, carry):
            u = PRE[rows(b * GB, GB), :] + bup
            cdf = 0.5 * (1.0 + lax.erf(u * RSQRT2))
            pdf = jnp.exp2(u * u * (-0.5 * LOG2E)) * INV_SQRT_2PI
            HID[l, rows(r0 + b * GB, GB), :] = (u * cdf).astype(BF16)
            GP[l, rows(r0 + b * GB, GB), :] = cdf + u * pdf
            return carry
        lax.fori_loop(0, C // GB, act, 0, unroll=True)
        PF[r0:r1, :] += nn(HID[l, r0:r1, :], WD[l])
        yield

    def backward(l, dl, i, last):
        r0, r1 = i * C, (i + 1) * C
        par = l % CORES
        first = i == NC - 1

        def acc(ref, val):
            if first:
                ref[par] = val
            else:
                ref[par] += val

        def acc_row(k, val, w=D):
            GV[l, k:k + 1, :w] += val

        norms(l, i)
        dy = H[dl, r0:r1, :]
        acc_row(4, col_sum(dy.astype(F32)))
        PRE[...] = nt(dy, WD[l])
        GB = 32

        def act(b, tot):
            d = PRE[rows(b * GB, GB), :] * GP[l, rows(r0 + b * GB, GB), :]
            DPB[rows(b * GB, GB), :] = d.astype(BF16)
            return tot + fold(d)
        dbu = lax.fori_loop(0, C // GB, act, jnp.zeros((8, F), F32), unroll=True)
        acc_row(5, col_sum(dbu))
        acc(GD, tn(HID[l, r0:r1, :], dy))
        yield
        acc(GU, tn(MS[...], DPB[...]))
        f0 = pf_row(i, True)
        PF[f0:f0 + C, :] = nt(DPB[...], WU[l])
        yield
        dctx = nt(dy, WO[l]).astype(BF16)
        ctx = CTX[l, r0:r1, :]
        acc(GO, tn(ctx, dy))
        prod = dctx.astype(F32) * ctx.astype(F32)
        q = Q[l, r0:r1, :].astype(F32)
        dcf = dctx.astype(F32)
        RBK = C // CORES
        dqt = []
        for h in range(CORES):
            sel = head_lane == h
            qm = jnp.where(sel, q, 0.0).astype(BF16)
            dcm = jnp.where(sel, dcf, 0.0).astype(BF16)
            dsum = jnp.transpose(jnp.where(sel, prod, 0.0))
            drow = col_sum(dsum)
            ST[:r1, :] = nt(V[l, :r1, :], dcm)

            def sub(b, carry):
                pr = PX[i][l, h, rows(b * RBK, RBK), :].astype(F32)
                DS[rows(b * RBK, RBK), :] = (pr * (ST[rows(b * RBK, RBK), :] - drow)).astype(BF16)
                return carry
            lax.fori_loop(0, r1 // RBK, sub, 0, unroll=True)
            dk = nn(DS[:r1, :], qm)
            dv = nn(PX[i][l, h], dcm)
            if first and h == 0:
                DK[:r1, :] = dk
                DV[:r1, :] = dv
            else:
                DK[:r1, :] += dk
                DV[:r1, :] += dv
            dqt.append(nn(KT[l, :, :r1], DS[:r1, :]))
            yield
        scale = E ** -0.5
        t = tabs(i)
        dq = unrotate(jnp.transpose(jnp.where(sub_head == 0, dqt[0], dqt[1])) * scale, t)
        dk = unrotate(DK[r0:r1, :] * scale, t)
        dv = DV[r0:r1, :]
        dqkv = jnp.concatenate([dq, dk, dv], axis=1)
        acc_row(6, col_sum(dqkv), 3 * E2)
        dqkv = dqkv.astype(BF16)
        dwq = tn(dqkv, AS[...])
        for k, r in enumerate(by_kind()):
            if first:
                GQ[par, r:r + E, :] = dwq[k * E:(k + 1) * E]
            else:
                GQ[par, r:r + E, :] += dwq[k * E:(k + 1) * E]
        PRE[...] = nn(dqkv, wq(l))
        yield
        g1, g2 = VEC[l, 0:1, :], VEC[l, 2:3, :]

        def lnb(b, tots):
            hf = H[l, rows(r0 + b * LB, LB), :].astype(F32)
            xhat, rstd = stats(hf)
            da = PRE[rows(b * LB, LB), :]
            dm = PF[rows(f0 + b * LB, LB), :]
            dx = da * g1 + dm * g2
            m1 = row_mean(dx)
            m2 = row_mean(dx * xhat)
            if not last:
                PF[rows(f0 + b * LB, LB), :] = rstd * (dx - m1 - xhat * m2)
            terms = (da * xhat, da, dm * xhat, dm)
            return tuple(a + fold(v) for a, v in zip(tots, terms))
        tots = lax.fori_loop(0, C // LB, lnb, tuple(jnp.zeros((8, D), F32) for _ in range(NA)), unroll=True)
        for k in range(NA):
            acc_row(k, col_sum(tots[k]))
        yield

    def g_half(a, k):
        return rows(k * G_HALF[a], G_HALF[a])

    def r1_view(l, a):
        return GP.at[l + 1, R1_OFF[a]:R1_OFF[a] + G_HALF[a], :G_COLS[a]]

    def g1_copy(l, a):
        return rcopy(G_BUF[a].at[l % CORES, g_half(a, 1 - c)], r1_view(l, a), g1s.at[a], g1r.at[l % CORES, a], pp=sib)

    def g2_copy(l, a):
        return rcopy(HID.at[l, R1_OFF[a]:R1_OFF[a] + G_HALF[a], :G_COLS[a]], R2[a].at[l % CORES], g2s.at[l % CORES, a], g2r.at[l % CORES, a], pp=2 * (l // CORES) + c)

    def g3_local(l, a):
        return lcopy(r1_view(l, a), G_OUT[a].at[g_half(a, c)], g3s.at[l % CORES, a])

    def g3_remote(l, a):
        return rcopy(r1_view(l, a), G_OUT[a].at[g_half(a, c)], g3s.at[l % CORES, a], g3r.at[a], pp=sib)

    def v1_copies(l):
        return [rcopy(GV.at[l], ZR.at[l, z], v1s.at[l, o - 1], v1r.at[l, z], tp=(z + o) % NT) for o in range(1, NT)]

    def grads_mid(l, arrays):
        for a in arrays:
            g1_copy(l, a).wait_recv()
            n = G_HALF[a]

            def add(b, carry):
                rr = rows(R1_OFF[a] + b * GR, GR)
                tot = G_BUF[a][l % CORES, rows(c * n + b * GR, GR), :] + GP[l + 1, rr, :G_COLS[a]]
                GP[l + 1, rr, :G_COLS[a]] = tot
                HID[l, rr, :G_COLS[a]] = tot.astype(BF16)
                return carry
            lax.fori_loop(0, n // GR, add, 0)

            @pl.when(l // CORES != ys_)
            def _():
                g2_copy(l, a).start()

    def grads_last(l):
        @pl.when(l // CORES == ys_)
        def _():
            for a in MLP + ATT:
                g2_copy(l, a).wait_recv()

                def add(b, carry):
                    rr = rows(R1_OFF[a] + b * GR, GR)
                    GP[l + 1, rr, :G_COLS[a]] += R2[a][l % CORES, rows(b * GR, GR), :].astype(F32)
                    return carry
                lax.fori_loop(0, G_HALF[a] // GR, add, 0)

                @pl.when(l == s)
                def _():
                    g3_local(l, a).start()

                @pl.when(l != s)
                def _():
                    g3_remote(l, a).start()

    def grads_sent(l):
        for a in range(NA):
            @pl.when(l // CORES != ys_)
            def _():
                g2_copy(l, a).wait_send()

            @pl.when(l == s)
            def _():
                g3_local(l, a).wait()

            @pl.when((l // CORES == ys_) & (l != s))
            def _():
                g3_remote(l, a).wait_send()

    def v2_copy(l):
        return rcopy(GZ.at[l], PR.at[s], v2s.at[l], v2r.at[s], pp=l)

    def vec_mid(l):
        ZR[l, z] = GV[l]
        for o in range(1, NT):
            q = (z + o) % NT
            rcopy(GV.at[l], ZR.at[l, q], v1s.at[l, o - 1], v1r.at[l, q], tp=q).wait_recv()
        tot = ZR[l, 0] + ZR[l, 1] + ZR[l, 2] + ZR[l, 3]
        row = lax.broadcasted_iota(jnp.int32, (8, D), 0)
        GZ[l] = jnp.where(row < 4, tot, GV[l])

        @pl.when(l == s)
        def _():
            PR[s] = GZ[l]

        @pl.when(l != s)
        def _():
            v2_copy(l).start()

    GV[...] = jnp.zeros_like(GV)
    @pl.when(ys_ == 1)
    def _():
        for a, hop in ((0, 0), (1, 0), (0, 1), (2, 0), (1, 1)):
            hop_on(a, hop)
        hop_end(0)
    settle(0, FIRST, True)
    xcopy.wait()

    def run(phases, at, handle, after=lambda k: None):
        for k, unused in enumerate(phases):
            after(k)
            for op, lag, u in at.get(k, ()):
                handle(op, lag, u)

    def fwd_layer(l, carry):
        for i in range(NC):
            @pl.when(l > 0)
            def _():
                ar_wait(l - 1, l, i)

            def handle(op, lag, u):
                m = i - lag

                def go(p, j):
                    if op == 'mid':
                        ar_mid(p, j, u)
                    else:
                        ar_last(p, p, p + 1, j, u)
                if m >= 0:
                    go(l, m)
                else:
                    @pl.when(l > 0)
                    def _():
                        go(l - 1, m + NC)
            run(forward(l, i), FWD_AT, handle)
            ar_send(l, i)
            if i == 1:
                @pl.when(l == 0)
                def _():
                    gcopy.wait()
                    H[NL + 1] = GP[NL].astype(BF16)

                    @pl.when(s == 1)
                    def _():
                        start_all(y_copies())
            if i == 2:
                @pl.when((l > 0) & (l < NL - 1))
                def _():
                    relay(l + 1, ALL)
            if i == NC - 1:
                @pl.when(l == 0)
                def _():
                    relay(l + 1, ALL)

                @pl.when(l < NL - 1)
                def _():
                    settle(l + 1, FIRST, True)
        return carry
    lax.fori_loop(0, NL, fwd_layer, 0)

    y_local = lcopy(H.at[NL], y.at[ys_, c], ys.at[0])
    y_sib = rcopy(H.at[NL], y.at[ys_, c], ys.at[1], yr.at[s], pp=sib)
    y_far = rcopy(H.at[NL], y.at[ys_, c], ys.at[2], yr.at[s], pp=oy + c)
    y_fwd = rcopy(y.at[1 - ys_, c], y.at[1 - ys_, c], ys.at[3], yr.at[oy + c], pp=sib)

    def y_arrived(q):
        rcopy(H.at[NL], y.at[q // CORES, q % CORES], ys.at[1], yr.at[q], pp=sib).wait_recv()

    def ri(l):
        return jnp.where(l == NL - 1, NL + 1, l + 1)

    def bwd_layer(lb, carry):
        l = NL - 1 - lb
        p = NL + lb
        for n in range(NC):
            i = NC - 1 - n

            @pl.when(lb > 0)
            def _():
                ar_wait(p - 1, l + 1, i)

            def handle(op, lag, u):
                m = n - lag

                def go(q, lq, j):
                    if op == 'mid':
                        ar_mid(q, j, u, True)
                    else:
                        ar_last(q, ri(lq), lq, j, u)
                if m >= 0:
                    @pl.when(l > 0)
                    def _():
                        go(p, l, NC - 1 - m)
                else:
                    @pl.when(lb > 0)
                    def _():
                        go(p - 1, l + 1, -1 - m)

                    @pl.when(lb == 0)
                    def _():
                        if op == 'mid':
                            ar_mid(NL - 1, m + NC, u)
                        else:
                            ar_last(NL - 1, NL - 1, NL, m + NC, u)

            def after(k):
                if k == 0 and n == 0:
                    @pl.when(lb > 0)
                    def _():
                        grads_mid(l + 1, ATT)
                        for a in ALL:
                            g1_copy(l + 1, a).wait_send()
                if n == NC - 1 and k == 1:
                    for a in MLP:
                        g1_copy(l, a).start()
            run(backward(l, ri(l), i, False), BWD_AT, handle, after)

            @pl.when(l > 0)
            def _():
                ar_send(p, i, True)
            if n == 1:
                @pl.when(lb > 0)
                def _():
                    vec_mid(l + 1)
            if n == 2:
                @pl.when(lb == 0)
                def _():
                    for j in range(NC):
                        ar_wait(NL - 1, NL, j)
                    start_all((y_local, y_sib, y_far))

                @pl.when(lb > 1)
                def _():
                    grads_last(l + 2)

        for a in ATT:
            g1_copy(l, a).start()
        start_all(v1_copies(l))
        grads_mid(l, MLP)
        return carry
    lax.fori_loop(0, NL, bwd_layer, 0)

    grads_mid(0, ATT)
    y_arrived(oy + c)
    y_fwd.start()
    grads_last(1)
    vec_mid(0)
    grads_last(0)

    for o in range(1, NL):
        q = (s + o) % NL
        rcopy(GZ.at[0], PR.at[q], v2s.at[0], v2r.at[q], pp=q).wait_recv()
    PRE[0:8, 0:D] = PR[0] + PR[1] + PR[2] + PR[3]
    vout = lcopy(PRE.at[0:8, 0:D], ovec, osem.at[0])
    vout.start()
    for l in range(NL):
        for cp in v1_copies(l):
            cp.wait_send()
    for l in range(NL):
        @pl.when(l != s)
        def _():
            v2_copy(l).wait_send()
    for a in range(NA):
        rcopy(G_OUT[a].at[g_half(a, 1 - c)], G_OUT[a].at[g_half(a, 1 - c)], g3s.at[a], g3r.at[a], pp=sib).wait_recv()
    y_local.wait()
    for cp in (y_sib, y_far, y_fwd):
        cp.wait_send()
    y_arrived(sib)
    y_arrived(oy + 1 - c)
    for a in range(NA):
        g1_copy(0, a).wait_send()
    for l in range(NL):
        grads_sent(l)
    for cp in sib_copies():
        cp.wait_send()
    @pl.when(s == 0)
    def _():
        for cp in first_copies():
            cp.wait_send()

    @pl.when(s > 0)
    def _():
        for cp in y_copies():
            cp.wait_send()
    for a in ALL:
        pass_copy(oy + 1, a, c).wait_send()

        @pl.when(ys_ == 0)
        def _():
            pass_copy(oy, a, c).wait_send()

        @pl.when(ys_ == 1)
        def _():
            for hop in range(CORES):
                for cp in hop_copies(a, hop):
                    cp.wait_send()

    @pl.when(is_end)
    def _():
        for t in range(NC * SUB):
            end_copy(0, t).wait_send()

    @pl.when(inner)
    def _():
        for t in range(NC * SUB):
            peer_copy(0, t).wait_send()
            back_copy(0, 1, t).wait_send()
    vout.wait()


def finish(y, gq, go, gu, gd, gv, yo, qo, oo, uo, do, n0, n1, n2, n3, n4, n5, n6, bq,
           yb, qb, ob, ub, db, vb, r0, r1, r2, r3, r4, r5, r6, rq, got, put, small):
    trips = [(gd, db, do), (gu, ub, uo), (go, ob, oo), (gq, qb, qo)]
    trips += [tuple(ref.at[m, r] for ref in (y, yb, yo)) for m in range(y.shape[0]) for r in range(y.shape[1])]
    loads = [pltpu.make_async_copy(a, b, got.at[k]) for k, (a, b, o) in enumerate(trips)]
    stores = [pltpu.make_async_copy(b, o, put.at[k]) for k, (a, b, o) in enumerate(trips)]
    vecs = pltpu.make_async_copy(gv, vb, small.at[len(trips)])
    vecs.start()
    for cp in loads:
        cp.start()
    vecs.wait()
    for row, refs in enumerate(((r0,), (r1,), (r2,), (r3,), (r4, r5), (r6,))):
        for ref in refs:
            ref[...] = vb[row:row + 1, :]
    e = rq.shape[2]
    for k in range(3):
        for h in range(CORES):
            rq[k, h:h + 1, :] = vb[6:7, (CORES * k + h) * e:(CORES * k + h + 1) * e]
    tiny = [pltpu.make_async_copy(a, b, small.at[k]) for k, (a, b) in enumerate(((r0, n0), (r1, n1), (r2, n2), (r3, n3), (r4, n4), (r5, n5), (r6, n6), (rq, bq)))]
    for cp in tiny:
        cp.start()
    for cp, out in zip(loads, stores):
        cp.wait()
        out.start()
    for cp in tiny + stores:
        cp.wait()


def finish_step(y, gq, go, gu, gd, gv, e):
    hbm = pl.BlockSpec(memory_space=pl.ANY)
    row = jax.ShapeDtypeStruct((1, gv.shape[1]), F32)
    outs = [jax.ShapeDtypeStruct(a.shape, a.dtype) for a in (y, gq, go, gu, gd)] + [row] * 7 + [jax.ShapeDtypeStruct((3, CORES, e), F32)]
    bufs = outs[:5] + [gv] + outs[5:]
    return pl.pallas_call(
        finish,
        out_shape=outs,
        in_specs=[hbm] * 6,
        out_specs=[hbm] * len(outs),
        scratch_shapes=[pltpu.VMEM(a.shape, a.dtype) for a in bufs] + [pltpu.SemaphoreType.DMA((9,))] * 3,
        name='neox_out',
    )(y, gq, go, gu, gd, gv)


def group_step(dims, *args):
    x = args[0]
    S, D, E, C, F = dims
    E2 = 2 * E
    hbm = pl.BlockSpec(memory_space=pl.ANY)
    out_shape = [
        jax.ShapeDtypeStruct(x.shape, BF16),
        jax.ShapeDtypeStruct((3 * E2, D), F32),
        jax.ShapeDtypeStruct((E2, D), F32),
        jax.ShapeDtypeStruct((D, F), F32),
        jax.ShapeDtypeStruct((F, D), F32),
        jax.ShapeDtypeStruct((8, D), F32),
    ]

    def vm(*shape, dtype=BF16):
        return pltpu.VMEM(shape, dtype)
    dma = pltpu.SemaphoreType.DMA
    scratch = [
        vm(NL, 3 * E2, D), vm(NL, E2, D), vm(NL, D, F), vm(NL, F, D), vm(NL, 8, D, dtype=F32),
        vm(NL + 2, S, D),
        vm(NL, S, E2), vm(NL, S, E2), vm(NL, S, E2), vm(NL, E2, S), vm(E2, S), vm(NL, S, E2),
        *[vm(NL, 2, (i + 1) * C, C) for i in range(NC)],
        vm(NL, S, F), vm(NL + 1, S, F, dtype=F32),
        vm(CORES, S, D), vm(CORES, S, D), vm(S, D), vm(S + C, D, dtype=F32),
        vm(CORES, 3 * E2, D, dtype=F32), vm(CORES, E2, D, dtype=F32), vm(CORES, D, F, dtype=F32), vm(CORES, F, D, dtype=F32),
        vm(CORES, 3 * E, D), vm(CORES, E, D), vm(CORES, D // CORES, F), vm(CORES, F // CORES, D),
        vm(S, E2, dtype=F32), vm(S, E2, dtype=F32),
        vm(CORES, C + 8, E2, dtype=F32), vm(S, E2, dtype=F32), vm(S, E2, dtype=F32),
        vm(NL, 8, D, dtype=F32), vm(NL, NT, 8, D, dtype=F32), vm(NL, 8, D, dtype=F32), vm(NL, 8, D, dtype=F32),
        vm(C, D), vm(C, D), vm(C, max(D, F), dtype=F32), vm(C, F), vm(S, C), vm(S, C, dtype=F32),
        *[vm(1, D, dtype=F32)] * 4, vm(1, D), vm(1, D), vm(1, F), vm(3, 2, E),
        dma((NA,)), dma((NA + 1,)), dma((CORES, NA + 1)), dma((NL, 2 * NA + 1)), dma((CORES, NA)), dma((3, NA)), dma((NA, 4)), dma((CORES,)), dma((1,)),
        dma((NC * SUB,)), dma((NC * SUB,)), dma((CORES, NC * SUB)), dma((CORES, NC * SUB)), dma((CORES, NC * SUB)),
        dma((NL,)), dma((NL,)), dma((NA,)), dma((CORES, NA)), dma((CORES, NA)), dma((CORES, NA)), dma((CORES, NA)), dma((NA,)),
        dma((NL, NT - 1)), dma((NL, NT)), dma((NL,)), dma((NL,)), dma((1,)), dma((8,)),
    ]
    return pl.pallas_call(
        functools.partial(body, dims),
        out_shape=out_shape,
        in_specs=[hbm] * len(args),
        out_specs=[hbm] * 6,
        scratch_shapes=scratch,
        compiler_params=pltpu.CompilerParams(collective_id=0, has_side_effects=True, vmem_limit_bytes=67043328),
        name='neox_group',
    )(*args)


def solution(mesh):
    def device_fn(x_in, g_out, ln1_gain, ln1_bias, w_qkv, b_qkv, w_out, b_out, ln2_gain, ln2_bias, w_up, b_up, w_down, b_down):
        n_micro, n_rows, S, D = x_in.shape
        heads, E = w_qkv.shape[2], w_qkv.shape[4]
        F = w_up.shape[2]
        C = S // NC
        wqkv = jnp.transpose(w_qkv[0], (1, 2, 3, 0)).reshape(heads * 3 * E, D)
        bqkv = jnp.transpose(b_qkv[0], (1, 0, 2))
        tab = jnp.asarray(rotary_base(C, NC, E, heads))
        part = group_step((S, D, E, C, F), x_in, g_out, wqkv, w_out[0].reshape(heads * E, D), w_up[0], w_down[0], ln1_gain, ln1_bias, ln2_gain, ln2_bias, b_out, b_down, b_up, bqkv, tab)
        y, gq, go, gup, gdn, n1g, n1b, n2g, n2b, gbo, gbd, gbu, gbq = finish_step(*part, E)
        gq = jnp.transpose(gq.reshape(heads, 3, E, D), (3, 0, 1, 2))[None]
        gbq = jnp.transpose(gbq, (1, 0, 2))[None]
        return (y, n1g, n1b, gq, gbq, go.reshape(1, heads, E, D), gbo, n2g, n2b, gup[None], gbu, gdn[None], gbd)

    return jax.shard_map(device_fn, mesh=mesh, in_specs=(P('dp'), P('dp')) + STAGE_SPECS, out_specs=(P('dp'),) + GRAD_SPECS, check_vma=False)
```

```python
import functools
import math

import jax
import jax.numpy as jnp
import numpy as np
from jax import lax
from jax.experimental import pallas as pl
from jax.experimental.pallas import tpu as pltpu
from jax.sharding import PartitionSpec as P

ROPE_BASE = 10000.0
LN_EPS = 1e-5
STAGE_SPECS = (P('pp'), P('pp'), P('pp', None, 'tp'), P('pp', 'tp'), P('pp', 'tp'), P('pp'), P('pp'), P('pp'), P('pp', None, 'tp'), P('pp', 'tp'), P('pp', 'tp'), P('pp'))
OWN = ('dp', 'pp')
GRAD_SPECS = (P(OWN), P(OWN), P(OWN, None, 'tp'), P(OWN, 'tp'), P(OWN, 'tp'), P(OWN), P(OWN), P(OWN), P(OWN, None, 'tp'), P(OWN, 'tp'), P(OWN, 'tp'), P(OWN))


F32 = jnp.float32
BF16 = jnp.bfloat16
NL = 4
NT = 4
NC = 4
NA = 4
CORES = 2
SUB = 2
FWD_AT = {0: (('mid', 1, 0), ('last', 2, 0)), 2: (('mid', 1, 1), ('last', 2, 1))}
BWD_AT = {0: (('last', 2, 0),), 1: (('mid', 1, 0),), 3: (('last', 2, 1),), 4: (('mid', 1, 1),)}
LOG2E = 1.4426950408889634
RSQRT2 = 0.7071067811865476
INV_SQRT_2PI = 0.3989422804014327


def nn(a, b):
    return lax.dot_general(a, b, (((1,), (0,)), ((), ())), preferred_element_type=F32)


def nt(a, b):
    return lax.dot_general(a, b, (((1,), (1,)), ((), ())), preferred_element_type=F32)


def tn(a, b):
    return lax.dot_general(a, b, (((0,), (0,)), ((), ())), preferred_element_type=F32)


def col_sum(v):
    return jnp.sum(v, axis=0, keepdims=True)


def row_mean(v):
    return jnp.mean(v, axis=-1, keepdims=True)


def fold(v):
    return jnp.sum(v.reshape(v.shape[0] // 8, 8, v.shape[1]), axis=0)


def rotary_base(chunk, n_chunks, head_dim, n_heads):
    rot_dim = head_dim // 4
    half = rot_dim // CORES
    inv_freq = np.zeros((head_dim,), np.float64)
    inv_freq[:rot_dim] = np.tile(ROPE_BASE ** (-(np.arange(half) * 2.0) / rot_dim), 2)
    inv_freq = np.tile(inv_freq, n_heads)
    pos = np.concatenate([np.arange(chunk), np.arange(8) * (np.arange(8) < n_chunks) * chunk]).astype(np.float64)
    ang = pos[:, None] * inv_freq[None, :]
    return np.stack([np.cos(ang), np.sin(ang)]).astype(np.float32)


def body(dims, x, g, wqkv, wo, wup, wdn, n0, n1, n2, n3, n4, n5, n6, bq, tab,
         y, oqkv, oo, oup, odn, ovec,
         WQ, WO, WU, WD, VEC, H, Q, K, V, KT, VT, CTX, P0, P1, P2, P3, HID, GP, RA, RB, PS, PF,
         GQ, GO, GU, GD, R2Q, R2O, R2U, R2D, DK, DV, TAB, GV, ZR, GZ, PR,
         AS, MS, PRE, DPB, DS, ST, N0, N1, N2, N3, N4, N5, N6, BQ, GX,
         wl, ws, wy, wr, wf, w0s, w0r, xs, gs, sab, sc, ra_s, rb_s, rc_s, ys, yr, g1s, g1r, g2s, g2r, g3s, g3r, v1s, v1r, v2s, v2r, osem, ns, gxs, gxr, gs2, gs3, ygs):
    S, D, E, C, F = dims
    E2 = 2 * E
    SR = C // SUB
    z = lax.axis_index('tp')
    xg = lax.axis_index('dp')
    s = lax.axis_index('pp')
    ys_ = s // CORES
    c = s % CORES
    sib = s + 1 - 2 * c
    oy = 2 * (1 - ys_)
    is_end = z * (NT - 1 - z) == 0
    inner = z * (NT - 1 - z) > 0
    edge = 1 - jnp.minimum(z * (NT - 1 - z), 1)
    hub = 1 + z // 3
    leaf = jnp.where(z == 1, 0, 3)
    peer = 3 - z
    PX = (P0, P1, P2, P3)
    W_IN = (wqkv, wo, wup, wdn)
    W_BUF = (WQ, WO, WU, WD)
    G_HALF = (3 * E, E, D // CORES, F // CORES)
    ALL = tuple(range(NA))
    FIRST, REST = ALL[:1], ALL[1:]
    ATT, MLP = ALL[:2], ALL[2:]
    G_BUF = (GQ, GO, GU, GD)
    G_OUT = (oqkv, oo, oup, odn)
    G_COLS = (D, D, F, D)
    R1_OFF = tuple(sum(G_HALF[:k]) for k in range(NA))
    R2 = (R2Q, R2O, R2U, R2D)

    def rcopy(src, dst, ss, rs, **dev):
        return pltpu.make_async_remote_copy(src_ref=src, dst_ref=dst, send_sem=ss, recv_sem=rs, device_id=dev, device_id_type=pl.DeviceIdType.MESH)

    def lcopy(src, dst, sem):
        return pltpu.make_async_copy(src, dst, sem)

    def rows(start, n):
        return pl.ds(pl.multiple_of(start, n), n)

    xcopy = lcopy(x.at[ys_, c], H.at[0], xs.at[0])
    xcopy.start()
    gcopy = lcopy(g.at[ys_, c], GP.at[NL], gs.at[0])
    gcopy.start()
    tcopy = lcopy(tab, TAB, xs.at[1])
    tcopy.start()
    for a in range(NA):
        lcopy(W_IN[a], W_BUF[a].at[s], wl.at[a]).start()
    small = [lcopy(a, b, ns.at[k]) for k, (a, b) in enumerate(((n0, N0), (n1, N1), (n2, N2), (n3, N3), (n4, N4), (n5, N5), (n6, N6), (bq, BQ)))]
    for cp in small:
        cp.start()

    bar = pltpu.get_barrier_semaphore()
    for o in range(1, NT):
        pl.semaphore_signal(bar, inc=1, device_id={'tp': (z + o) % NT}, device_id_type=pl.DeviceIdType.MESH)
    for o in range(1, NL):
        pl.semaphore_signal(bar, inc=1, device_id={'pp': (s + o) % NL}, device_id_type=pl.DeviceIdType.MESH)
    pl.semaphore_signal(bar, inc=1, device_id={'dp': 1 - xg}, device_id_type=pl.DeviceIdType.MESH)
    pl.semaphore_wait(bar, NT + NL - 1)

    def half(ref, a, k):
        return ref.at[rows(k * G_HALF[a], G_HALF[a])]

    def sib_copies():
        out = [rcopy(W_IN[a], W_BUF[a].at[s], ws.at[a], wr.at[s, 2 * a], pp=sib) for a in ALL]
        return out + [rcopy(VEC.at[s], VEC.at[s], ws.at[NA], wr.at[s, 2 * NA], pp=sib)]

    def y_copies():
        out = [rcopy(half(W_IN[a], a, k), half(W_BUF[a].at[s], a, k), wy.at[k, a], wr.at[s, 2 * a + k], pp=oy + k) for a in ALL for k in range(CORES)]
        return out[:2] + [rcopy(VEC.at[s], VEC.at[s], wy.at[k, NA], wr.at[s, 2 * NA], pp=oy + k) for k in range(CORES)] + out[2:]

    def quarter(ref, a, q):
        return ref.at[rows(q * (G_HALF[a] // CORES), G_HALF[a] // CORES)]

    def first_copies():
        out = []
        for a in ALL:
            for k in range(CORES):
                q = 2 * xg + k
                out.append(rcopy(quarter(W_IN[a], a, q), quarter(W_BUF[a].at[0], a, q), wy.at[k, a], w0r.at[a, q], pp=oy + k))
        return out + [rcopy(VEC.at[s], VEC.at[s], wy.at[k, NA], wr.at[s, 2 * NA], pp=oy + k) for k in range(CORES)]

    def mine(hop):
        return 2 * (xg if hop == 0 else 1 - xg) + c

    def hop_copies(a, hop):
        part, sem = quarter(W_BUF[a].at[0], a, mine(hop)), w0r.at[a, mine(hop)]
        out = [rcopy(part, part, w0s.at[hop, a], sem, pp=sib)]
        return out if hop else out + [rcopy(part, part, w0s.at[2, a], sem, dp=1 - xg)]

    def hop_on(a, hop):
        copies = hop_copies(a, hop)
        copies[0].wait_recv()
        start_all(copies)

    def hop_end(a):
        for k in range(CORES):
            part = quarter(W_BUF[a].at[0], a, 2 * k + 1 - c)
            rcopy(part, part, w0s.at[0, a], w0r.at[a, 2 * k + 1 - c], pp=sib).wait_recv()

    def start_all(copies):
        for cp in copies:
            cp.start()

    for cp in small:
        cp.wait()
    for k, ref in enumerate((N0, N1, N2, N3, N4, N5, N6)):
        VEC[s, k:k + 1, :] = ref[...].astype(F32)
    VEC[s, 7:8, :3 * E2] = jnp.concatenate([BQ[k, h:h + 1, :].astype(F32) for k in range(3) for h in range(CORES)], axis=1)

    @pl.when(s == 0)
    def _():
        start_all(first_copies())

    @pl.when(s > 1)
    def _():
        start_all(y_copies())
    start_all(sib_copies())

    def pass_copy(l, a, k):
        part = half(W_BUF[a].at[l], a, k)
        return rcopy(part, part, wf.at[l % CORES, a], wr.at[l, 2 * a + k], pp=sib)

    def relay(l, arrays):
        @pl.when(l // CORES != ys_)
        def _():
            for a in arrays:
                pass_copy(l, a, c).wait_recv()
                pass_copy(l, a, c).start()

    def settle(l, arrays, small):
        @pl.when(l == s)
        def _():
            for a in arrays:
                lcopy(W_IN[a], W_BUF[a].at[s], wl.at[a]).wait()

        @pl.when(l == sib)
        def _():
            for a in arrays:
                rcopy(W_IN[a], W_BUF[a].at[l], ws.at[a], wr.at[l, 2 * a], pp=sib).wait_recv()

        @pl.when((l // CORES != ys_) & (l > 0))
        def _():
            for a in arrays:
                pass_copy(l, a, 1 - c).wait_recv()
        if small:
            @pl.when(l != s)
            def _():
                rcopy(VEC.at[l], VEC.at[l], ws.at[NA], wr.at[l, 2 * NA], pp=sib).wait_recv()

    tcopy.wait()

    lane = lax.broadcasted_iota(jnp.int32, (C, E2), 1)
    head_lane = lane // E
    in_head = lane % E
    rot_half = E // 8
    low = in_head < rot_half
    sub_head = lax.broadcasted_iota(jnp.int32, (E2, C), 0) // E
    lower = lax.broadcasted_iota(jnp.int32, (C, C), 0) <= lax.broadcasted_iota(jnp.int32, (C, C), 1)
    c1 = E ** -0.5 * LOG2E

    def tabs(i):
        (cb, sb), (cr, sr) = ([TAB[k, r, :] for k in range(CORES)] for r in (slice(C), slice(C + i, C + i + 1)))
        cs, sn = cb * cr - sb * sr, sb * cr + cb * sr
        return cs, jnp.where(low, -sn, 0.0), jnp.where(low, 0.0, sn)

    def rotate(v, t):
        cs, sa, sb = t
        return v * cs + pltpu.roll(v, E2 - rot_half, 1) * sa + pltpu.roll(v, rot_half, 1) * sb

    def unrotate(v, t):
        cs, sa, sb = t
        return v * cs + pltpu.roll(v * sa, rot_half, 1) + pltpu.roll(v * sb, E2 - rot_half, 1)

    def end_copy(p, t):
        return rcopy(PS.at[t * SR:(t + 1) * SR], RA.at[p % CORES, t * SR:(t + 1) * SR], sab.at[t], ra_s.at[p % CORES, t], tp=hub)

    def peer_copy(p, t):
        return rcopy(PS.at[t * SR:(t + 1) * SR], RB.at[p % CORES, t * SR:(t + 1) * SR], sab.at[t], rb_s.at[p % CORES, t], tp=peer)

    def back_copy(p, di, t):
        return rcopy(H.at[di, t * SR:(t + 1) * SR], H.at[di, t * SR:(t + 1) * SR], sc.at[t], rc_s.at[p % CORES, t], tp=leaf)

    def pf_row(i, back):
        return (NC if back and i == NC - 1 else i) * C

    def ar_send(p, i, back=False):
        @pl.when(is_end)
        def _():
            for t in range(i * SUB, (i + 1) * SUB):
                @pl.when(p > 0)
                def _():
                    end_copy(p, t).wait_send()
                f0 = pf_row(i, back) + (t - i * SUB) * SR
                PS[t * SR:(t + 1) * SR, :] = PF[f0:f0 + SR, :].astype(BF16)
                end_copy(p, t).start()

    def out_bias(l):
        return VEC[l, 4:5, :] + VEC[l, 5:6, :]

    def ar_mid(p, i, u, back=False):
        t = i * SUB + u
        r = slice(t * SR, (t + 1) * SR)
        f0 = pf_row(i, back) + u * SR

        @pl.when(inner)
        def _():
            end_copy(p, t).wait_recv()
            @pl.when(p > 0)
            def _():
                peer_copy(p, t).wait_send()
            PS[r, :] = (PF[f0:f0 + SR, :] + RA[p % CORES, r, :].astype(F32)).astype(BF16)
            peer_copy(p, t).start()

    def ar_last(p, ri, di, i, u, back=False):
        t = i * SUB + u
        r = slice(t * SR, (t + 1) * SR)

        @pl.when(inner)
        def _():
            peer_copy(p, t).wait_recv()
            @pl.when(p > 0)
            def _():
                back_copy(p, di, t).wait_send()
            both = PS[r, :].astype(F32) + RB[p % CORES, r, :].astype(F32)
            own = H[ri, r, :].astype(F32)
            H[di, r, :] = (own + both if back else own + both + out_bias(p)).astype(BF16)
            back_copy(p, di, t).start()

    def ar_wait(p, di, i, on=1):
        @pl.when(on * edge > 0)
        def _():
            for t in range(i * SUB, (i + 1) * SUB):
                back_copy(p, di, t).wait_recv()

    GP1 = NL % 3

    def guest_copy(i):
        part = GX.at[i * C:(i + 1) * C]
        return rcopy(part, part, gxs.at[i], gxr.at[i], pp=c)

    def guest_send(i):
        r = slice(i * C, (i + 1) * C)
        once = jnp.where(z == 1, 1.0, 0.0)
        GX[r, :] = (PF[r, :] + once * (H[NL - 1, r, :].astype(F32) + out_bias(NL - 1))).astype(BF16)
        guest_copy(i).start()

    def guest_hop(t, dst, sem, arrive, to):
        return rcopy(GX.at[t * SR:(t + 1) * SR], dst.at[GP1, t * SR:(t + 1) * SR], sem.at[t], arrive.at[GP1, t], tp=to)

    def guest_to_hub(t):
        return guest_hop(t, RA, gs2, ra_s, hub)

    def guest_to_peer(t):
        return guest_hop(t, RB, gs2, rb_s, peer)

    def guest_to_leaf(t):
        return guest_hop(t, RB, gs3, rc_s, leaf)

    def parts(i):
        return [(t, slice(t * SR, (t + 1) * SR)) for t in range(i * SUB, (i + 1) * SUB)]

    def guest_in(i):
        guest_copy(i).wait_recv()

        @pl.when(is_end)
        def _():
            for t, r in parts(i):
                guest_to_hub(t).start()

    def guest_mid(i):
        @pl.when(inner)
        def _():
            for t, r in parts(i):
                guest_to_hub(t).wait_recv()
                GX[r, :] = (GX[r, :].astype(F32) + RA[GP1, r, :].astype(F32)).astype(BF16)
                guest_to_peer(t).start()

    def guest_last(i):
        @pl.when(inner)
        def _():
            for t, r in parts(i):
                guest_to_peer(t).wait_recv()
                guest_to_peer(t).wait_send()
                GX[r, :] = (GX[r, :].astype(F32) + RB[GP1, r, :].astype(F32)).astype(BF16)
                guest_to_leaf(t).start()

    def guest_back(i):
        @pl.when(is_end)
        def _():
            for t, r in parts(i):
                guest_to_leaf(t).wait_recv()

    def guest_out(act):
        for role, src in ((is_end, RB.at[GP1]), (inner, GX)):
            @pl.when(role)
            def _():
                dst = y.at[1, c]
                act(lcopy(src, dst, ygs.at[0]), rcopy(src, dst, ygs.at[1], yr.at[s + CORES], pp=sib), rcopy(src, dst, ygs.at[2], yr.at[s + CORES], pp=s + CORES))

    def stats(hf):
        cen = hf - row_mean(hf)
        rstd = lax.rsqrt(row_mean(cen * cen) + LN_EPS)
        return cen * rstd, rstd

    LB = 32
    GR = 32

    def norms(l, i):
        g1, b1, g2, b2 = (VEC[l, k:k + 1, :] for k in range(NA))

        def step(b, carry):
            hf = H[l, rows(i * C + b * LB, LB), :].astype(F32)
            xhat, unused = stats(hf)
            AS[rows(b * LB, LB), :] = (xhat * g1 + b1).astype(BF16)
            MS[rows(b * LB, LB), :] = (xhat * g2 + b2).astype(BF16)
            return carry
        lax.fori_loop(0, C // LB, step, 0, unroll=True)

    def by_kind():
        return [(h * 3 + k) * E for k in range(3) for h in range(CORES)]

    def wq(l):
        return jnp.concatenate([WQ[l, r:r + E, :] for r in by_kind()], axis=0)

    def forward(l, i):
        r0, r1 = i * C, (i + 1) * C
        norms(l, i)
        qkv = nt(AS[...], wq(l)) + VEC[l, 7:8, :3 * E2]
        qkv = qkv.astype(BF16).astype(F32)
        t = tabs(i)
        q = rotate(qkv[:, :E2], t).astype(BF16)
        kf = rotate(qkv[:, E2:2 * E2], t)
        vf = qkv[:, 2 * E2:3 * E2]
        Q[l, r0:r1, :] = q
        K[l, r0:r1, :] = kf.astype(BF16)
        V[l, r0:r1, :] = vf.astype(BF16)
        KT[l, :, r0:r1] = jnp.transpose(kf).astype(BF16)
        VT[:, r0:r1] = jnp.transpose(vf).astype(BF16)
        yield

        def far(*hops):
            if i == 0:
                @pl.when((l == 0) & (ys_ == 1))
                def _():
                    for a, hop in hops:
                        hop_on(a, hop)
        far((3, 0))
        RBK = C // CORES
        outs = []
        for h in range(CORES):
            qm = jnp.where(head_lane == h, Q[l, r0:r1, :].astype(F32), 0.0).astype(BF16)
            ST[:r1, :] = nt(K[l, :r1, :], qm)
            ST[r0:r1, :] = jnp.where(lower, ST[r0:r1, :], -1e30)

            def top(b, m):
                return jnp.maximum(m, jnp.max(ST[rows(b * RBK, RBK), :].reshape(RBK // 8, 8, C), axis=0))
            m = jnp.max(lax.fori_loop(0, r1 // RBK, top, jnp.full((8, C), -3e38, F32), unroll=True), axis=0, keepdims=True)
            mc = m * c1

            def expo(b, tot):
                e = jnp.exp2(ST[rows(b * RBK, RBK), :] * c1 - mc)
                ST[rows(b * RBK, RBK), :] = e
                return tot + fold(e)
            tot = col_sum(lax.fori_loop(0, r1 // RBK, expo, jnp.zeros((8, C), F32), unroll=True))
            inv = 1.0 / tot

            def put(b, carry):
                PX[i][l, h, rows(b * RBK, RBK), :] = (ST[rows(b * RBK, RBK), :] * inv).astype(BF16)
                return carry
            lax.fori_loop(0, r1 // RBK, put, 0, unroll=True)
            outs.append(nn(VT[:, :r1], PX[i][l, h]))
            if h == 0:
                yield
        ctx = jnp.transpose(jnp.where(sub_head == 0, outs[0], outs[1])).astype(BF16)
        CTX[l, r0:r1, :] = ctx
        yield
        if i == 0:
            far((2, 1), (3, 1))

            @pl.when((l == 0) & (ys_ == 1))
            def _():
                for a in REST:
                    hop_end(a)
            settle(l, REST, False)
        PF[r0:r1, :] = nn(ctx, WO[l])
        PRE[...] = nn(MS[...], WU[l])
        bup = VEC[l, 6:7, :]
        GB = 32

        def act(b, carry):
            u = PRE[rows(b * GB, GB), :] + bup
            cdf = 0.5 * (1.0 + lax.erf(u * RSQRT2))
            pdf = jnp.exp2(u * u * (-0.5 * LOG2E)) * INV_SQRT_2PI
            HID[l, rows(r0 + b * GB, GB), :] = (u * cdf).astype(BF16)
            GP[l, rows(r0 + b * GB, GB), :] = cdf + u * pdf
            return carry
        lax.fori_loop(0, C // GB, act, 0, unroll=True)
        PF[r0:r1, :] += nn(HID[l, r0:r1, :], WD[l])
        yield

    def backward(l, dl, i, last):
        r0, r1 = i * C, (i + 1) * C
        par = l % CORES
        first = i == NC - 1

        def acc(ref, val):
            if first:
                ref[par] = val
            else:
                ref[par] += val

        def acc_row(k, val, w=D):
            GV[l, k:k + 1, :w] += val

        norms(l, i)
        dy = H[dl, r0:r1, :]
        acc_row(4, col_sum(dy.astype(F32)))
        PRE[...] = nt(dy, WD[l])
        GB = 32

        def act(b, tot):
            d = PRE[rows(b * GB, GB), :] * GP[l, rows(r0 + b * GB, GB), :]
            DPB[rows(b * GB, GB), :] = d.astype(BF16)
            return tot + fold(d)
        dbu = lax.fori_loop(0, C // GB, act, jnp.zeros((8, F), F32), unroll=True)
        acc_row(5, col_sum(dbu))
        acc(GD, tn(HID[l, r0:r1, :], dy))
        yield
        acc(GU, tn(MS[...], DPB[...]))
        f0 = pf_row(i, True)
        PF[f0:f0 + C, :] = nt(DPB[...], WU[l])
        yield
        dctx = nt(dy, WO[l]).astype(BF16)
        ctx = CTX[l, r0:r1, :]
        acc(GO, tn(ctx, dy))
        prod = dctx.astype(F32) * ctx.astype(F32)
        q = Q[l, r0:r1, :].astype(F32)
        dcf = dctx.astype(F32)
        RBK = C // CORES
        dqt = []
        for h in range(CORES):
            sel = head_lane == h
            qm = jnp.where(sel, q, 0.0).astype(BF16)
            dcm = jnp.where(sel, dcf, 0.0).astype(BF16)
            dsum = jnp.transpose(jnp.where(sel, prod, 0.0))
            drow = col_sum(dsum)
            ST[:r1, :] = nt(V[l, :r1, :], dcm)

            def sub(b, carry):
                pr = PX[i][l, h, rows(b * RBK, RBK), :].astype(F32)
                DS[rows(b * RBK, RBK), :] = (pr * (ST[rows(b * RBK, RBK), :] - drow)).astype(BF16)
                return carry
            lax.fori_loop(0, r1 // RBK, sub, 0, unroll=True)
            dk = nn(DS[:r1, :], qm)
            dv = nn(PX[i][l, h], dcm)
            if first and h == 0:
                DK[:r1, :] = dk
                DV[:r1, :] = dv
            else:
                DK[:r1, :] += dk
                DV[:r1, :] += dv
            dqt.append(nn(KT[l, :, :r1], DS[:r1, :]))
            yield
        scale = E ** -0.5
        t = tabs(i)
        dq = unrotate(jnp.transpose(jnp.where(sub_head == 0, dqt[0], dqt[1])) * scale, t)
        dk = unrotate(DK[r0:r1, :] * scale, t)
        dv = DV[r0:r1, :]
        dqkv = jnp.concatenate([dq, dk, dv], axis=1)
        acc_row(6, col_sum(dqkv), 3 * E2)
        dqkv = dqkv.astype(BF16)
        dwq = tn(dqkv, AS[...])
        for k, r in enumerate(by_kind()):
            if first:
                GQ[par, r:r + E, :] = dwq[k * E:(k + 1) * E]
            else:
                GQ[par, r:r + E, :] += dwq[k * E:(k + 1) * E]
        PRE[...] = nn(dqkv, wq(l))
        yield
        g1, g2 = VEC[l, 0:1, :], VEC[l, 2:3, :]

        def lnb(b, tots):
            hf = H[l, rows(r0 + b * LB, LB), :].astype(F32)
            xhat, rstd = stats(hf)
            da = PRE[rows(b * LB, LB), :]
            dm = PF[rows(f0 + b * LB, LB), :]
            dx = da * g1 + dm * g2
            m1 = row_mean(dx)
            m2 = row_mean(dx * xhat)
            if not last:
                PF[rows(f0 + b * LB, LB), :] = rstd * (dx - m1 - xhat * m2)
            terms = (da * xhat, da, dm * xhat, dm)
            return tuple(a + fold(v) for a, v in zip(tots, terms))
        tots = lax.fori_loop(0, C // LB, lnb, tuple(jnp.zeros((8, D), F32) for _ in range(NA)), unroll=True)
        for k in range(NA):
            acc_row(k, col_sum(tots[k]))
        yield

    def g_half(a, k):
        return rows(k * G_HALF[a], G_HALF[a])

    def r1_view(l, a):
        return GP.at[l + 1, R1_OFF[a]:R1_OFF[a] + G_HALF[a], :G_COLS[a]]

    def g1_copy(l, a):
        return rcopy(G_BUF[a].at[l % CORES, g_half(a, 1 - c)], r1_view(l, a), g1s.at[a], g1r.at[l % CORES, a], pp=sib)

    def g2_copy(l, a):
        return rcopy(HID.at[l, R1_OFF[a]:R1_OFF[a] + G_HALF[a], :G_COLS[a]], R2[a].at[l % CORES], g2s.at[l % CORES, a], g2r.at[l % CORES, a], pp=2 * (l // CORES) + c)

    def g3_local(l, a):
        return lcopy(r1_view(l, a), G_OUT[a].at[g_half(a, c)], g3s.at[l % CORES, a])

    def g3_remote(l, a):
        return rcopy(r1_view(l, a), G_OUT[a].at[g_half(a, c)], g3s.at[l % CORES, a], g3r.at[a], pp=sib)

    def v1_copies(l):
        return [rcopy(GV.at[l], ZR.at[l, z], v1s.at[l, o - 1], v1r.at[l, z], tp=(z + o) % NT) for o in range(1, NT)]

    def grads_mid(l, arrays):
        for a in arrays:
            g1_copy(l, a).wait_recv()
            n = G_HALF[a]

            def add(b, carry):
                rr = rows(R1_OFF[a] + b * GR, GR)
                tot = G_BUF[a][l % CORES, rows(c * n + b * GR, GR), :] + GP[l + 1, rr, :G_COLS[a]]
                GP[l + 1, rr, :G_COLS[a]] = tot
                HID[l, rr, :G_COLS[a]] = tot.astype(BF16)
                return carry
            lax.fori_loop(0, n // GR, add, 0)

            @pl.when(l // CORES != ys_)
            def _():
                g2_copy(l, a).start()

    def grads_last(l):
        @pl.when(l // CORES == ys_)
        def _():
            for a in MLP + ATT:
                g2_copy(l, a).wait_recv()

                def add(b, carry):
                    rr = rows(R1_OFF[a] + b * GR, GR)
                    GP[l + 1, rr, :G_COLS[a]] += R2[a][l % CORES, rows(b * GR, GR), :].astype(F32)
                    return carry
                lax.fori_loop(0, G_HALF[a] // GR, add, 0)

                @pl.when(l == s)
                def _():
                    g3_local(l, a).start()

                @pl.when(l != s)
                def _():
                    g3_remote(l, a).start()

    def grads_sent(l):
        for a in range(NA):
            @pl.when(l // CORES != ys_)
            def _():
                g2_copy(l, a).wait_send()

            @pl.when(l == s)
            def _():
                g3_local(l, a).wait()

            @pl.when((l // CORES == ys_) & (l != s))
            def _():
                g3_remote(l, a).wait_send()

    def v2_copy(l):
        return rcopy(GZ.at[l], PR.at[s], v2s.at[l], v2r.at[s], pp=l)

    def vec_mid(l):
        ZR[l, z] = GV[l]
        for o in range(1, NT):
            q = (z + o) % NT
            rcopy(GV.at[l], ZR.at[l, q], v1s.at[l, o - 1], v1r.at[l, q], tp=q).wait_recv()
        tot = sum(ZR[l, k] for k in range(NT))
        row = lax.broadcasted_iota(jnp.int32, (8, D), 0)
        GZ[l] = jnp.where(row < 4, tot, GV[l])

        @pl.when(l == s)
        def _():
            PR[s] = GZ[l]

        @pl.when(l != s)
        def _():
            v2_copy(l).start()

    GV[...] = jnp.zeros_like(GV)
    @pl.when(ys_ == 1)
    def _():
        for a, hop in ((0, 0), (1, 0), (0, 1), (2, 0), (1, 1)):
            hop_on(a, hop)
        hop_end(0)
    settle(0, FIRST, True)
    xcopy.wait()

    def run(phases, at, handle, after=lambda k: None):
        for k, unused in enumerate(phases):
            after(k)
            for op, lag, u in at.get(k, ()):
                handle(op, lag, u)

    def fwd_layer(l, carry):
        for i in range(NC):
            ar_wait(l - 1, l, i, l)

            def handle(op, lag, u):
                m = i - lag

                def go(p, j):
                    if op == 'mid':
                        ar_mid(p, j, u)
                    else:
                        ar_last(p, p, p + 1, j, u)
                if m >= 0:
                    @pl.when(l * ys_ < NL - 1)
                    def _():
                        go(l, m)
                else:
                    @pl.when(l > 0)
                    def _():
                        go(l - 1, m + NC)
            run(forward(l, i), FWD_AT, handle)

            @pl.when(l * ys_ < NL - 1)
            def _():
                ar_send(l, i)

            @pl.when(l * ys_ == NL - 1)
            def _():
                guest_send(i)
            if i == 1:
                @pl.when(l == 0)
                def _():
                    gcopy.wait()
                    H[NL + 1] = GP[NL].astype(BF16)

                    @pl.when(s == 1)
                    def _():
                        start_all(y_copies())
            if i == 2:
                @pl.when((l > 0) & (l < NL - 1))
                def _():
                    relay(l + 1, ALL)
            if i == NC - 1:
                @pl.when(l == 0)
                def _():
                    relay(l + 1, ALL)

                @pl.when(l < NL - 1)
                def _():
                    settle(l + 1, FIRST, True)
        return carry
    lax.fori_loop(0, NL, fwd_layer, 0)

    y_local = lcopy(H.at[NL], y.at[ys_, c], ys.at[0])
    y_sib = rcopy(H.at[NL], y.at[ys_, c], ys.at[1], yr.at[s], pp=sib)
    y_far = rcopy(H.at[NL], y.at[ys_, c], ys.at[2], yr.at[s], pp=oy + c)
    y_fwd = rcopy(y.at[1 - ys_, c], y.at[1 - ys_, c], ys.at[3], yr.at[oy + c], pp=sib)
    y_own = rcopy(y.at[ys_, c], y.at[ys_, c], ys.at[2], yr.at[s], pp=sib)

    def y_arrived(q):
        rcopy(H.at[NL], y.at[q // CORES, q % CORES], ys.at[1], yr.at[q], pp=sib).wait_recv()

    def ri(l):
        return jnp.where(l == NL - 1, NL + 1, l + 1)

    def pass_of(lb):
        return NL - 1 + lb + (1 - ys_) * (1 + jnp.minimum(lb, 1))

    def bwd_layer(lb, carry):
        l = NL - 1 - lb
        p = pass_of(lb)
        before = pass_of(lb - 1)
        for n in range(NC):
            i = NC - 1 - n

            ar_wait(before, l + 1, i, lb)

            def handle(op, lag, u):
                m = n - lag

                def go(q, lq, j):
                    if op == 'mid':
                        ar_mid(q, j, u, True)
                    else:
                        ar_last(q, ri(lq), lq, j, u, True)
                if m >= 0:
                    @pl.when(l > 0)
                    def _():
                        go(p, l, NC - 1 - m)
                else:
                    @pl.when(lb > 0)
                    def _():
                        go(before, l + 1, -1 - m)

                    @pl.when(lb == NL * ys_)
                    def _():
                        if op == 'mid':
                            ar_mid(NL - 1, m + NC, u)
                        else:
                            ar_last(NL - 1, NL - 1, NL, m + NC, u)

            def guests(layer, what, j):
                @pl.when(lb == layer + NL * ys_)
                def _():
                    what(j)

            def after(k):
                if k == 0:
                    guests(1, guest_in, i)
                if k == 1:
                    guests(1 if n else 2, guest_last, i + 1 if n else 0)
                if k == NC:
                    guests(1, guest_mid, i)
                if k == 0 and n == 0:
                    @pl.when(lb > 0)
                    def _():
                        grads_mid(l + 1, ATT)
                        for a in ALL:
                            g1_copy(l + 1, a).wait_send()
                if n == NC - 1 and k == 1:
                    for a in MLP:
                        g1_copy(l, a).start()
            run(backward(l, ri(l), i, False), BWD_AT, handle, after)

            @pl.when(lb == 2 + NL * ys_)
            def _():
                guest_back(i)

            @pl.when(l > 0)
            def _():
                ar_send(p, i, True)
            if n == NC - 1:
                @pl.when(lb == 2 + NL * ys_)
                def _():
                    guest_out(lambda *copies: start_all(copies))
            if n == 1:
                @pl.when(lb > 0)
                def _():
                    vec_mid(l + 1)
            if n == 2:
                @pl.when(lb == NL * ys_)
                def _():
                    for j in range(NC):
                        ar_wait(NL - 1, NL, j)
                    start_all((y_local, y_sib, y_far))

                @pl.when(lb > 1)
                def _():
                    grads_last(l + 2)

        for a in ATT:
            g1_copy(l, a).start()
        start_all(v1_copies(l))
        grads_mid(l, MLP)
        return carry
    lax.fori_loop(0, NL, bwd_layer, 0)

    grads_mid(0, ATT)

    @pl.when(ys_ == 1)
    def _():
        y_arrived(oy + c)
        y_fwd.start()
        y_arrived(s)
        y_own.start()
    grads_last(1)
    vec_mid(0)
    grads_last(0)

    for o in range(1, NL):
        q = (s + o) % NL
        rcopy(GZ.at[0], PR.at[q], v2s.at[0], v2r.at[q], pp=q).wait_recv()
    PRE[:8, :D] = sum(PR[k] for k in range(NL))
    vout = lcopy(PRE.at[:8, :D], ovec, osem.at[0])
    vout.start()
    for l in range(NL):
        for cp in v1_copies(l):
            cp.wait_send()
    for l in range(NL):
        @pl.when(l != s)
        def _():
            v2_copy(l).wait_send()
    for a in range(NA):
        rcopy(G_OUT[a].at[g_half(a, 1 - c)], G_OUT[a].at[g_half(a, 1 - c)], g3s.at[a], g3r.at[a], pp=sib).wait_recv()

    def out_done(local, *sent):
        local.wait()
        for cp in sent:
            cp.wait_send()

    @pl.when(ys_ == 0)
    def _():
        out_done(y_local, y_sib, y_far)
        guest_out(out_done)

        @pl.when(is_end)
        def _():
            for t in range(NC * SUB):
                guest_to_hub(t).wait_send()

        @pl.when(inner)
        def _():
            for t in range(NC * SUB):
                guest_to_leaf(t).wait_send()

    @pl.when(ys_ == 1)
    def _():
        y_fwd.wait_send()
        y_own.wait_send()
        for i in range(NC):
            guest_copy(i).wait_send()
    y_arrived(sib)
    y_arrived(oy + 1 - c)
    for a in range(NA):
        g1_copy(0, a).wait_send()
    for l in range(NL):
        grads_sent(l)
    for cp in sib_copies():
        cp.wait_send()
    @pl.when(s == 0)
    def _():
        for cp in first_copies():
            cp.wait_send()

    @pl.when(s > 0)
    def _():
        for cp in y_copies():
            cp.wait_send()
    for a in ALL:
        pass_copy(oy + 1, a, c).wait_send()

        @pl.when(ys_ == 0)
        def _():
            pass_copy(oy, a, c).wait_send()

        @pl.when(ys_ == 1)
        def _():
            for hop in range(CORES):
                for cp in hop_copies(a, hop):
                    cp.wait_send()

    @pl.when(is_end)
    def _():
        for t in range(NC * SUB):
            end_copy(0, t).wait_send()

    @pl.when(inner)
    def _():
        for t in range(NC * SUB):
            peer_copy(0, t).wait_send()
            back_copy(0, 1, t).wait_send()
    vout.wait()


def finish(y, gq, go, gu, gd, gv, yo, qo, oo, uo, do, n0, n1, n2, n3, n4, n5, n6, bq,
           yb, qb, ob, ub, db, vb, r0, r1, r2, r3, r4, r5, r6, rq, got, put, small):
    trips = [(gd, db, do), (gu, ub, uo), (go, ob, oo), (gq, qb, qo)]
    trips += [tuple(ref.at[m, r] for ref in (y, yb, yo)) for m in range(y.shape[0]) for r in range(y.shape[1])]
    loads = [pltpu.make_async_copy(a, b, got.at[k]) for k, (a, b, o) in enumerate(trips)]
    stores = [pltpu.make_async_copy(b, o, put.at[k]) for k, (a, b, o) in enumerate(trips)]
    vecs = pltpu.make_async_copy(gv, vb, small.at[len(trips)])
    vecs.start()
    for cp in loads:
        cp.start()
    vecs.wait()
    for row, refs in enumerate(((r0,), (r1,), (r2,), (r3,), (r4, r5), (r6,))):
        for ref in refs:
            ref[...] = vb[row:row + 1, :]
    e = rq.shape[2]
    for k in range(3):
        for h in range(CORES):
            rq[k, h:h + 1, :] = vb[6:7, (CORES * k + h) * e:(CORES * k + h + 1) * e]
    tiny = [pltpu.make_async_copy(a, b, small.at[k]) for k, (a, b) in enumerate(((r0, n0), (r1, n1), (r2, n2), (r3, n3), (r4, n4), (r5, n5), (r6, n6), (rq, bq)))]
    for cp in tiny:
        cp.start()
    for cp, out in zip(loads, stores):
        cp.wait()
        out.start()
    for cp in tiny + stores:
        cp.wait()


def finish_step(y, gq, go, gu, gd, gv, e):
    hbm = pl.BlockSpec(memory_space=pl.ANY)
    row = jax.ShapeDtypeStruct((1, gv.shape[1]), F32)
    outs = [jax.ShapeDtypeStruct(a.shape, a.dtype) for a in (y, gq, go, gu, gd)] + [row] * 7 + [jax.ShapeDtypeStruct((3, CORES, e), F32)]
    bufs = outs[:5] + [gv] + outs[5:]
    return pl.pallas_call(
        finish,
        out_shape=outs,
        in_specs=[hbm] * 6,
        out_specs=[hbm] * len(outs),
        scratch_shapes=[pltpu.VMEM(a.shape, a.dtype) for a in bufs] + [pltpu.SemaphoreType.DMA((9,))] * 3,
        name='neox_out',
    )(y, gq, go, gu, gd, gv)


def group_step(dims, *args):
    x = args[0]
    S, D, E, C, F = dims
    E2 = 2 * E
    hbm = pl.BlockSpec(memory_space=pl.ANY)
    out_shape = [
        jax.ShapeDtypeStruct(x.shape, BF16),
        jax.ShapeDtypeStruct((3 * E2, D), F32),
        jax.ShapeDtypeStruct((E2, D), F32),
        jax.ShapeDtypeStruct((D, F), F32),
        jax.ShapeDtypeStruct((F, D), F32),
        jax.ShapeDtypeStruct((8, D), F32),
    ]

    def vm(*shape, dtype=BF16):
        return pltpu.VMEM(shape, dtype)
    dma = pltpu.SemaphoreType.DMA
    scratch = [
        vm(NL, 3 * E2, D), vm(NL, E2, D), vm(NL, D, F), vm(NL, F, D), vm(NL, 8, D, dtype=F32),
        vm(NL + 2, S, D),
        vm(NL, S, E2), vm(NL, S, E2), vm(NL, S, E2), vm(NL, E2, S), vm(E2, S), vm(NL, S, E2),
        *[vm(NL, 2, (i + 1) * C, C) for i in range(NC)],
        vm(NL, S, F), vm(NL + 1, S, F, dtype=F32),
        vm(CORES, S, D), vm(CORES, S, D), vm(S, D), vm(S + C, D, dtype=F32),
        *[vm(CORES, *k, dtype=F32) for k in ((3 * E2, D), (E2, D), (D, F), (F, D))],
        *[vm(CORES, *k) for k in ((3 * E, D), (E, D), (D // CORES, F), (F // CORES, D))],
        vm(S, E2, dtype=F32), vm(S, E2, dtype=F32),
        vm(CORES, C + 8, E2, dtype=F32),
        *[vm(*k, 8, D, dtype=F32) for k in ((NL,), (NL, NT), (NL,), (NL,))],
        vm(C, D), vm(C, D), vm(C, max(D, F), dtype=F32), vm(C, F), vm(S, C), vm(S, C, dtype=F32),
        *[vm(1, D, dtype=F32)] * 4, vm(1, D), vm(1, D), vm(1, F), vm(3, CORES, E), vm(S, D),
        dma((NA,)), dma((NA + 1,)), dma((CORES, NA + 1)), dma((NL, 2 * NA + 1)), dma((CORES, NA)), dma((3, NA)), dma((NA, 4)), dma((CORES,)), dma((1,)),
        dma((NC * SUB,)), dma((NC * SUB,)), dma((CORES, NC * SUB)), dma((CORES, NC * SUB)), dma((CORES, NC * SUB)),
        dma((NL,)), dma((NL,)), dma((NA,)), dma((CORES, NA)), dma((CORES, NA)), dma((CORES, NA)), dma((CORES, NA)), dma((NA,)),
        dma((NL, NT - 1)), dma((NL, NT)), dma((NL,)), dma((NL,)), dma((1,)), dma((8,)),
        dma((NC,)), dma((NC,)), dma((NC * SUB,)), dma((NC * SUB,)), dma((3,)),
    ]
    return pl.pallas_call(
        functools.partial(body, dims),
        out_shape=out_shape,
        in_specs=[hbm] * len(args),
        out_specs=[hbm] * 6,
        scratch_shapes=scratch,
        compiler_params=pltpu.CompilerParams(collective_id=0, has_side_effects=True, vmem_limit_bytes=67043328),
        name='neox_group',
    )(*args)


def solution(mesh):
    def device_fn(x_in, g_out, ln1_gain, ln1_bias, w_qkv, b_qkv, w_out, b_out, ln2_gain, ln2_bias, w_up, b_up, w_down, b_down):
        n_micro, n_rows, S, D = x_in.shape
        heads, E = w_qkv.shape[2], w_qkv.shape[4]
        F = w_up.shape[2]
        C = S // NC
        wqkv = jnp.transpose(w_qkv[0], (1, 2, 3, 0)).reshape(heads * 3 * E, D)
        bqkv = jnp.transpose(b_qkv[0], (1, 0, 2))
        tab = jnp.asarray(rotary_base(C, NC, E, heads))
        part = group_step((S, D, E, C, F), x_in, g_out, wqkv, w_out[0].reshape(heads * E, D), w_up[0], w_down[0], ln1_gain, ln1_bias, ln2_gain, ln2_bias, b_out, b_down, b_up, bqkv, tab)
        y, gq, go, gup, gdn, n1g, n1b, n2g, n2b, gbo, gbd, gbu, gbq = finish_step(*part, E)
        gq = jnp.transpose(gq.reshape(heads, 3, E, D), (3, 0, 1, 2))[None]
        gbq = jnp.transpose(gbq, (1, 0, 2))[None]
        return (y, n1g, n1b, gq, gbq, go.reshape(1, heads, E, D), gbo, n2g, n2b, gup[None], gbu, gdn[None], gbd)

    return jax.shard_map(device_fn, mesh=mesh, in_specs=(P('dp'), P('dp')) + STAGE_SPECS, out_specs=(P('dp'),) + GRAD_SPECS, check_vma=False)
```

```python
import functools
import math

import jax
import jax.numpy as jnp
import numpy as np
from jax import lax
from jax.experimental import pallas as pl
from jax.experimental.pallas import tpu as pltpu
from jax.sharding import PartitionSpec as P

ROPE_BASE = 10000.0
LN_EPS = 1e-5
STAGE_SPECS = (P('pp'), P('pp'), P('pp', None, 'tp'), P('pp', 'tp'), P('pp', 'tp'), P('pp'), P('pp'), P('pp'), P('pp', None, 'tp'), P('pp', 'tp'), P('pp', 'tp'), P('pp'))
OWN = ('dp', 'pp')
GRAD_SPECS = (P(OWN), P(OWN), P(OWN, None, 'tp'), P(OWN, 'tp'), P(OWN, 'tp'), P(OWN), P(OWN), P(OWN), P(OWN, None, 'tp'), P(OWN, 'tp'), P(OWN, 'tp'), P(OWN))


F32 = jnp.float32
BF16 = jnp.bfloat16
NL = 4
NT = 4
NC = 4
NA = 4
CORES = 2
SUB = 2
FWD_AT = {0: (('mid', 1, 0), ('last', 2, 0)), 2: (('mid', 1, 1), ('last', 2, 1))}
BWD_AT = {0: (('last', 2, 0),), 1: (('mid', 1, 0),), 3: (('last', 2, 1),), 4: (('mid', 1, 1),)}
LOG2E = 1.4426950408889634
RSQRT2 = 0.7071067811865476
INV_SQRT_2PI = 0.3989422804014327


def nn(a, b):
    return lax.dot_general(a, b, (((1,), (0,)), ((), ())), preferred_element_type=F32)


def nt(a, b):
    return lax.dot_general(a, b, (((1,), (1,)), ((), ())), preferred_element_type=F32)


def tn(a, b):
    return lax.dot_general(a, b, (((0,), (0,)), ((), ())), preferred_element_type=F32)


def loop(n, step, init, unroll=False):
    return lax.fori_loop(0, n, step, init, unroll=unroll)


def col_sum(v):
    return jnp.sum(v, axis=0, keepdims=True)


def row_mean(v):
    return jnp.mean(v, axis=-1, keepdims=True)


def fold(v):
    return jnp.sum(v.reshape(v.shape[0] // 8, 8, v.shape[1]), axis=0)


def rotary_base(chunk, n_chunks, head_dim, n_heads):
    rot_dim = head_dim // 4
    half = rot_dim // CORES
    inv_freq = np.zeros((head_dim,), np.float64)
    inv_freq[:rot_dim] = np.tile(ROPE_BASE ** (-(np.arange(half) * 2.0) / rot_dim), 2)
    inv_freq = np.tile(inv_freq, n_heads)
    pos = np.concatenate([np.arange(chunk), np.arange(8) * (np.arange(8) < n_chunks) * chunk]).astype(np.float64)
    ang = pos[:, None] * inv_freq[None, :]
    return np.stack([np.cos(ang), np.sin(ang)]).astype(np.float32)


def body(dims, x, g, wqkv, wo, wup, wdn, n0, n1, n2, n3, n4, n5, n6, bq, tab,
         y, oqkv, oo, oup, odn, ovec,
         WQ, WO, WU, WD, VEC, H, Q, K, V, KT, VT, CTX, P0, P1, P2, P3, HID, GP, RA, RB, PS, PF,
         GQ, GO, GU, GD, R2Q, R2O, R2U, R2D, DK, DV, TAB, GV, ZR, GZ, PR,
         AS, MS, PRE, DPB, DS, ST, N0, N1, N2, N3, N4, N5, N6, BQ, GX,
         wl, ws, wy, wr, wf, w0s, w0r, xs, gs, sab, sc, ra_s, rb_s, rc_s, ys, yr, g1s, g1r, g2s, g2r, g3s, g3r, v1s, v1r, v2s, v2r, osem, ns, gxs, gxr, gs2, gs3, ygs, ygr):
    S, D, E, C, F = dims
    E2 = 2 * E
    SR = C // SUB
    z = lax.axis_index('tp')
    xg = lax.axis_index('dp')
    s = lax.axis_index('pp')
    ys_ = s // CORES
    c = s % CORES
    sib = s + 1 - 2 * c
    oy = 2 * (1 - ys_)
    is_end = z * (NT - 1 - z) == 0
    inner = z * (NT - 1 - z) > 0
    edge = 1 - jnp.minimum(z * (NT - 1 - z), 1)
    hub = 1 + z // 3
    leaf = jnp.where(z == 1, 0, 3)
    peer = 3 - z
    PX = (P0, P1, P2, P3)
    W_IN = (wqkv, wo, wup, wdn)
    W_BUF = (WQ, WO, WU, WD)
    G_HALF = (3 * E, E, D // CORES, F // CORES)
    ALL = tuple(range(NA))
    FIRST, REST = ALL[:1], ALL[1:]
    ATT, MLP = ALL[:2], ALL[2:]
    G_BUF = (GQ, GO, GU, GD)
    G_OUT = (oqkv, oo, oup, odn)
    G_COLS = (D, D, F, D)
    R1_OFF = tuple(sum(G_HALF[:k]) for k in range(NA))
    R2 = (R2Q, R2O, R2U, R2D)

    def rcopy(src, dst, ss, rs, **dev):
        return pltpu.make_async_remote_copy(src_ref=src, dst_ref=dst, send_sem=ss, recv_sem=rs, device_id=dev, device_id_type=pl.DeviceIdType.MESH)

    def lcopy(src, dst, sem):
        return pltpu.make_async_copy(src, dst, sem)

    def rows(start, n):
        return pl.ds(pl.multiple_of(start, n), n)

    xcopy = lcopy(x.at[ys_, c], H.at[0], xs.at[0])
    xcopy.start()
    gcopy = lcopy(g.at[ys_, c], GP.at[NL], gs.at[0])
    gcopy.start()
    tcopy = lcopy(tab, TAB, xs.at[1])
    tcopy.start()
    for a in range(NA):
        lcopy(W_IN[a], W_BUF[a].at[s], wl.at[a]).start()
    small = [lcopy(a, b, ns.at[k]) for k, (a, b) in enumerate(((n0, N0), (n1, N1), (n2, N2), (n3, N3), (n4, N4), (n5, N5), (n6, N6), (bq, BQ)))]
    for cp in small:
        cp.start()

    bar = pltpu.get_barrier_semaphore()
    for o in range(1, NT):
        pl.semaphore_signal(bar, inc=1, device_id={'tp': (z + o) % NT}, device_id_type=pl.DeviceIdType.MESH)
    for o in range(1, NL):
        pl.semaphore_signal(bar, inc=1, device_id={'pp': (s + o) % NL}, device_id_type=pl.DeviceIdType.MESH)
    pl.semaphore_signal(bar, inc=1, device_id={'dp': 1 - xg}, device_id_type=pl.DeviceIdType.MESH)
    pl.semaphore_wait(bar, NT + NL - 1)

    def half(ref, a, k):
        return ref.at[rows(k * G_HALF[a], G_HALF[a])]

    def sib_copies():
        out = [rcopy(W_IN[a], W_BUF[a].at[s], ws.at[a], wr.at[s, 2 * a], pp=sib) for a in ALL]
        return out + [rcopy(VEC.at[s], VEC.at[s], ws.at[NA], wr.at[s, 2 * NA], pp=sib)]

    def y_copies():
        out = [rcopy(half(W_IN[a], a, k), half(W_BUF[a].at[s], a, k), wy.at[k, a], wr.at[s, 2 * a + k], pp=oy + k) for a in ALL for k in range(CORES)]
        return out[:2] + [rcopy(VEC.at[s], VEC.at[s], wy.at[k, NA], wr.at[s, 2 * NA], pp=oy + k) for k in range(CORES)] + out[2:]

    def quarter(ref, a, q):
        return ref.at[rows(q * (G_HALF[a] // CORES), G_HALF[a] // CORES)]

    def first_copies():
        out = []
        for a in ALL:
            for k in range(CORES):
                q = 2 * xg + k
                out.append(rcopy(quarter(W_IN[a], a, q), quarter(W_BUF[a].at[0], a, q), wy.at[k, a], w0r.at[a, q], pp=oy + k))
        return out + [rcopy(VEC.at[s], VEC.at[s], wy.at[k, NA], wr.at[s, 2 * NA], pp=oy + k) for k in range(CORES)]

    def mine(hop):
        return 2 * (xg if hop == 0 else 1 - xg) + c

    def hop_copies(a, hop):
        part, sem = quarter(W_BUF[a].at[0], a, mine(hop)), w0r.at[a, mine(hop)]
        out = [rcopy(part, part, w0s.at[hop, a], sem, pp=sib)]
        return out if hop else out + [rcopy(part, part, w0s.at[2, a], sem, dp=1 - xg)]

    def hop_on(a, hop):
        copies = hop_copies(a, hop)
        copies[0].wait_recv()
        start_all(copies)

    def hop_end(a):
        for k in range(CORES):
            part = quarter(W_BUF[a].at[0], a, 2 * k + 1 - c)
            rcopy(part, part, w0s.at[0, a], w0r.at[a, 2 * k + 1 - c], pp=sib).wait_recv()

    def start_all(copies):
        for cp in copies:
            cp.start()

    for cp in small:
        cp.wait()
    for k, ref in enumerate((N0, N1, N2, N3, N4, N5, N6)):
        VEC[s, k:k + 1, :] = ref[...].astype(F32)
    VEC[s, 7:8, :3 * E2] = jnp.concatenate([BQ[k, h:h + 1, :].astype(F32) for k in range(3) for h in range(CORES)], axis=1)

    @pl.when(s == 0)
    def _():
        start_all(first_copies())

    @pl.when(s > 1)
    def _():
        start_all(y_copies())
    start_all(sib_copies())

    def pass_copy(l, a, k):
        part = half(W_BUF[a].at[l], a, k)
        return rcopy(part, part, wf.at[l % CORES, a], wr.at[l, 2 * a + k], pp=sib)

    def relay(l, arrays):
        @pl.when(l // CORES != ys_)
        def _():
            for a in arrays:
                pass_copy(l, a, c).wait_recv()
                pass_copy(l, a, c).start()

    def settle(l, arrays, small):
        @pl.when(l == s)
        def _():
            for a in arrays:
                lcopy(W_IN[a], W_BUF[a].at[s], wl.at[a]).wait()

        @pl.when(l == sib)
        def _():
            for a in arrays:
                rcopy(W_IN[a], W_BUF[a].at[l], ws.at[a], wr.at[l, 2 * a], pp=sib).wait_recv()

        @pl.when((l // CORES != ys_) & (l > 0))
        def _():
            for a in arrays:
                pass_copy(l, a, 1 - c).wait_recv()
        if small:
            @pl.when(l != s)
            def _():
                rcopy(VEC.at[l], VEC.at[l], ws.at[NA], wr.at[l, 2 * NA], pp=sib).wait_recv()

    tcopy.wait()

    lane = lax.broadcasted_iota(jnp.int32, (C, E2), 1)
    head_lane = lane // E
    in_head = lane % E
    rot_half = E // 8
    low = in_head < rot_half
    sub_head = lax.broadcasted_iota(jnp.int32, (E2, C), 0) // E
    lower = lax.broadcasted_iota(jnp.int32, (C, C), 0) <= lax.broadcasted_iota(jnp.int32, (C, C), 1)
    c1 = E ** -0.5 * LOG2E

    def tabs(i):
        (cb, sb), (cr, sr) = ([TAB[k, r, :] for k in range(CORES)] for r in (slice(C), slice(C + i, C + i + 1)))
        cs, sn = cb * cr - sb * sr, sb * cr + cb * sr
        return cs, jnp.where(low, -sn, 0.0), jnp.where(low, 0.0, sn)

    def rotate(v, t):
        cs, sa, sb = t
        return v * cs + pltpu.roll(v, E2 - rot_half, 1) * sa + pltpu.roll(v, rot_half, 1) * sb

    def unrotate(v, t):
        cs, sa, sb = t
        return v * cs + pltpu.roll(v * sa, rot_half, 1) + pltpu.roll(v * sb, E2 - rot_half, 1)

    def end_copy(p, t):
        return rcopy(PS.at[t * SR:(t + 1) * SR], RA.at[p % CORES, t * SR:(t + 1) * SR], sab.at[t], ra_s.at[p % CORES, t], tp=hub)

    def peer_copy(p, t):
        return rcopy(PS.at[t * SR:(t + 1) * SR], RB.at[p % CORES, t * SR:(t + 1) * SR], sab.at[t], rb_s.at[p % CORES, t], tp=peer)

    def back_copy(p, di, t):
        return rcopy(H.at[di, t * SR:(t + 1) * SR], H.at[di, t * SR:(t + 1) * SR], sc.at[t], rc_s.at[p % CORES, t], tp=leaf)

    def pf_row(i, back):
        return (NC if back and i == NC - 1 else i) * C

    def ar_send(p, i, back=False):
        @pl.when(is_end)
        def _():
            for t in range(i * SUB, (i + 1) * SUB):
                @pl.when(p > 0)
                def _():
                    end_copy(p, t).wait_send()
                f0 = pf_row(i, back) + (t - i * SUB) * SR
                PS[t * SR:(t + 1) * SR, :] = PF[f0:f0 + SR, :].astype(BF16)
                end_copy(p, t).start()

    def out_bias(l):
        return VEC[l, 4:5, :] + VEC[l, 5:6, :]

    def ar_mid(p, i, u, back=False):
        t = i * SUB + u
        r = slice(t * SR, (t + 1) * SR)
        f0 = pf_row(i, back) + u * SR

        @pl.when(inner)
        def _():
            end_copy(p, t).wait_recv()
            @pl.when(p > 0)
            def _():
                peer_copy(p, t).wait_send()
            PS[r, :] = (PF[f0:f0 + SR, :] + RA[p % CORES, r, :].astype(F32)).astype(BF16)
            peer_copy(p, t).start()

    def ar_last(p, ri, di, i, u, back=False):
        t = i * SUB + u
        r = slice(t * SR, (t + 1) * SR)

        @pl.when(inner)
        def _():
            peer_copy(p, t).wait_recv()
            @pl.when(p > 0)
            def _():
                back_copy(p, di, t).wait_send()
            both = PS[r, :].astype(F32) + RB[p % CORES, r, :].astype(F32)
            own = H[ri, r, :].astype(F32)
            H[di, r, :] = (own + both if back else own + both + out_bias(p)).astype(BF16)
            back_copy(p, di, t).start()

    def ar_wait(p, di, i, on=1):
        @pl.when(on * edge > 0)
        def _():
            for t in range(i * SUB, (i + 1) * SUB):
                back_copy(p, di, t).wait_recv()

    GP1 = NL % 3
    HOME = NC // CORES

    def guest_copy(i):
        part = GX.at[i * C:(i + 1) * C]
        return rcopy(part, part, gxs.at[i], gxr.at[i], pp=c)

    def guest_send(i):
        r = slice(i * C, (i + 1) * C)
        once = jnp.where(z == 1, 1.0, 0.0)
        GX[r, :] = (PF[r, :] + once * (H[NL - 1, r, :].astype(F32) + out_bias(NL - 1))).astype(BF16)
        guest_copy(i).start()

    def guest_hop(t, dst, sem, arrive, to):
        return rcopy(GX.at[t * SR:(t + 1) * SR], dst.at[GP1, t * SR:(t + 1) * SR], sem.at[t], arrive.at[GP1, t], tp=to)

    def guest_to_hub(t):
        return guest_hop(t, RA, gs2, ra_s, hub)

    def guest_to_peer(t):
        return guest_hop(t, RB, gs2, rb_s, peer)

    def guest_to_leaf(t):
        return guest_hop(t, RB, gs3, rc_s, leaf)

    def parts(i):
        return [(t, slice(t * SR, (t + 1) * SR)) for t in range(i * SUB, (i + 1) * SUB)]

    def guest_in(i):
        guest_copy(i).wait_recv()

        @pl.when(is_end)
        def _():
            for t, r in parts(i):
                guest_to_hub(t).start()

    def guest_mid(i):
        @pl.when(inner)
        def _():
            for t, r in parts(i):
                guest_to_hub(t).wait_recv()
                GX[r, :] = (GX[r, :].astype(F32) + RA[GP1, r, :].astype(F32)).astype(BF16)
                guest_to_peer(t).start()

    def guest_last(i):
        @pl.when(inner)
        def _():
            for t, r in parts(i):
                guest_to_peer(t).wait_recv()
                guest_to_peer(t).wait_send()
                GX[r, :] = (GX[r, :].astype(F32) + RB[GP1, r, :].astype(F32)).astype(BF16)
                guest_to_leaf(t).start()

    def guest_back(i):
        @pl.when(is_end)
        def _():
            for t, r in parts(i):
                guest_to_leaf(t).wait_recv()

    def guest_out(act):
        low = slice(HOME * C, S)
        for role, src in ((is_end, RB.at[GP1, low]), (inner, GX.at[low])):
            @pl.when(role)
            def _():
                dst = y.at[1, c, low]
                act(lcopy(src, dst, ygs.at[0]), rcopy(src, dst, ygs.at[1], ygr.at[c], pp=sib), rcopy(src, dst, ygs.at[2], ygr.at[c], pp=s + CORES))

    def guest_home(q):
        return rcopy(y.at[1, q, HOME * C:S], y.at[1, q, HOME * C:S], ygs.at[0], ygr.at[q], pp=sib)

    def stats(hf):
        cen = hf - row_mean(hf)
        rstd = lax.rsqrt(row_mean(cen * cen) + LN_EPS)
        return cen * rstd, rstd

    LB = 32
    GR = 32

    def norms(l, i):
        g1, b1, g2, b2 = (VEC[l, k:k + 1, :] for k in range(NA))

        def step(b, carry):
            hf = H[l, rows(i * C + b * LB, LB), :].astype(F32)
            xhat, unused = stats(hf)
            AS[rows(b * LB, LB), :] = (xhat * g1 + b1).astype(BF16)
            MS[rows(b * LB, LB), :] = (xhat * g2 + b2).astype(BF16)
            return carry
        loop(C // LB, step, 0, unroll=True)

    def by_kind():
        return [(h * 3 + k) * E for k in range(3) for h in range(CORES)]

    def wq(l):
        return jnp.concatenate([WQ[l, r:r + E, :] for r in by_kind()], axis=0)

    def forward(l, i):
        r0, r1 = i * C, (i + 1) * C
        norms(l, i)
        qkv = nt(AS[...], wq(l)) + VEC[l, 7:8, :3 * E2]
        qkv = qkv.astype(BF16).astype(F32)
        t = tabs(i)
        q = rotate(qkv[:, :E2], t).astype(BF16)
        kf = rotate(qkv[:, E2:2 * E2], t)
        vf = qkv[:, 2 * E2:3 * E2]
        Q[l, r0:r1, :] = q
        K[l, r0:r1, :] = kf.astype(BF16)
        V[l, r0:r1, :] = vf.astype(BF16)
        KT[l, :, r0:r1] = jnp.transpose(kf).astype(BF16)
        VT[:, r0:r1] = jnp.transpose(vf).astype(BF16)
        yield

        def far(*hops):
            if i == 0:
                @pl.when((l == 0) & (ys_ == 1))
                def _():
                    for a, hop in hops:
                        hop_on(a, hop)
        far((3, 0))
        RBK = C // CORES
        outs = []
        for h in range(CORES):
            qm = jnp.where(head_lane == h, Q[l, r0:r1, :].astype(F32), 0.0).astype(BF16)
            ST[:r1, :] = nt(K[l, :r1, :], qm)
            ST[r0:r1, :] = jnp.where(lower, ST[r0:r1, :], -1e30)

            def top(b, m):
                return jnp.maximum(m, jnp.max(ST[rows(b * RBK, RBK), :].reshape(RBK // 8, 8, C), axis=0))
            m = jnp.max(loop(r1 // RBK, top, jnp.full((8, C), -3e38, F32), unroll=True), axis=0, keepdims=True)
            mc = m * c1

            def expo(b, tot):
                e = jnp.exp2(ST[rows(b * RBK, RBK), :] * c1 - mc)
                ST[rows(b * RBK, RBK), :] = e
                return tot + fold(e)
            tot = col_sum(loop(r1 // RBK, expo, jnp.zeros((8, C), F32), unroll=True))
            inv = 1.0 / tot

            def put(b, carry):
                PX[i][l, h, rows(b * RBK, RBK), :] = (ST[rows(b * RBK, RBK), :] * inv).astype(BF16)
                return carry
            loop(r1 // RBK, put, 0, unroll=True)
            outs.append(nn(VT[:, :r1], PX[i][l, h]))
            if h == 0:
                yield
        ctx = jnp.transpose(jnp.where(sub_head == 0, outs[0], outs[1])).astype(BF16)
        CTX[l, r0:r1, :] = ctx
        yield
        if i == 0:
            far((2, 1), (3, 1))

            @pl.when((l == 0) & (ys_ == 1))
            def _():
                for a in REST:
                    hop_end(a)
            settle(l, REST, False)
        PF[r0:r1, :] = nn(ctx, WO[l])
        PRE[...] = nn(MS[...], WU[l])
        bup = VEC[l, 6:7, :]
        GB = 32

        def act(b, carry):
            u = PRE[rows(b * GB, GB), :] + bup
            cdf = 0.5 * (1.0 + lax.erf(u * RSQRT2))
            pdf = jnp.exp2(u * u * (-0.5 * LOG2E)) * INV_SQRT_2PI
            HID[l, rows(r0 + b * GB, GB), :] = (u * cdf).astype(BF16)
            GP[l, rows(r0 + b * GB, GB), :] = cdf + u * pdf
            return carry
        loop(C // GB, act, 0, unroll=True)
        PF[r0:r1, :] += nn(HID[l, r0:r1, :], WD[l])
        yield

    def backward(l, dl, i, last):
        r0, r1 = i * C, (i + 1) * C
        par = l % CORES
        first = i == NC - 1

        def acc(ref, val):
            if first:
                ref[par] = val
            else:
                ref[par] += val

        def acc_row(k, val, w=D):
            GV[l, k:k + 1, :w] += val

        norms(l, i)
        dy = H[dl, r0:r1, :]
        acc_row(4, col_sum(dy.astype(F32)))
        PRE[...] = nt(dy, WD[l])
        GB = 32

        def act(b, tot):
            d = PRE[rows(b * GB, GB), :] * GP[l, rows(r0 + b * GB, GB), :]
            DPB[rows(b * GB, GB), :] = d.astype(BF16)
            return tot + fold(d)
        dbu = loop(C // GB, act, jnp.zeros((8, F), F32), unroll=True)
        acc_row(5, col_sum(dbu))
        acc(GD, tn(HID[l, r0:r1, :], dy))
        yield
        acc(GU, tn(MS[...], DPB[...]))
        f0 = pf_row(i, True)
        PF[f0:f0 + C, :] = nt(DPB[...], WU[l])
        yield
        dctx = nt(dy, WO[l]).astype(BF16)
        ctx = CTX[l, r0:r1, :]
        acc(GO, tn(ctx, dy))
        prod = dctx.astype(F32) * ctx.astype(F32)
        q = Q[l, r0:r1, :].astype(F32)
        dcf = dctx.astype(F32)
        RBK = C // CORES
        dqt = []
        for h in range(CORES):
            sel = head_lane == h
            qm = jnp.where(sel, q, 0.0).astype(BF16)
            dcm = jnp.where(sel, dcf, 0.0).astype(BF16)
            dsum = jnp.transpose(jnp.where(sel, prod, 0.0))
            drow = col_sum(dsum)
            ST[:r1, :] = nt(V[l, :r1, :], dcm)

            def sub(b, carry):
                pr = PX[i][l, h, rows(b * RBK, RBK), :].astype(F32)
                DS[rows(b * RBK, RBK), :] = (pr * (ST[rows(b * RBK, RBK), :] - drow)).astype(BF16)
                return carry
            loop(r1 // RBK, sub, 0, unroll=True)
            dk = nn(DS[:r1, :], qm)
            dv = nn(PX[i][l, h], dcm)
            if first and h == 0:
                DK[:r1, :] = dk
                DV[:r1, :] = dv
            else:
                DK[:r1, :] += dk
                DV[:r1, :] += dv
            dqt.append(nn(KT[l, :, :r1], DS[:r1, :]))
            yield
        scale = E ** -0.5
        t = tabs(i)
        dq = unrotate(jnp.transpose(jnp.where(sub_head == 0, dqt[0], dqt[1])) * scale, t)
        dk = unrotate(DK[r0:r1, :] * scale, t)
        dv = DV[r0:r1, :]
        dqkv = jnp.concatenate([dq, dk, dv], axis=1)
        acc_row(6, col_sum(dqkv), 3 * E2)
        dqkv = dqkv.astype(BF16)
        dwq = tn(dqkv, AS[...])
        for k, r in enumerate(by_kind()):
            if first:
                GQ[par, r:r + E, :] = dwq[k * E:(k + 1) * E]
            else:
                GQ[par, r:r + E, :] += dwq[k * E:(k + 1) * E]
        PRE[...] = nn(dqkv, wq(l))
        yield
        g1, g2 = VEC[l, 0:1, :], VEC[l, 2:3, :]

        def lnb(b, tots):
            hf = H[l, rows(r0 + b * LB, LB), :].astype(F32)
            xhat, rstd = stats(hf)
            da = PRE[rows(b * LB, LB), :]
            dm = PF[rows(f0 + b * LB, LB), :]
            dx = da * g1 + dm * g2
            m1 = row_mean(dx)
            m2 = row_mean(dx * xhat)
            if not last:
                PF[rows(f0 + b * LB, LB), :] = rstd * (dx - m1 - xhat * m2)
            terms = (da * xhat, da, dm * xhat, dm)
            return tuple(a + fold(v) for a, v in zip(tots, terms))
        tots = loop(C // LB, lnb, tuple(jnp.zeros((8, D), F32) for _ in range(NA)), unroll=True)
        for k in range(NA):
            acc_row(k, col_sum(tots[k]))
        yield

    def g_half(a, k):
        return rows(k * G_HALF[a], G_HALF[a])

    def r1_view(l, a):
        return GP.at[l + 1, R1_OFF[a]:R1_OFF[a] + G_HALF[a], :G_COLS[a]]

    def g1_copy(l, a):
        return rcopy(G_BUF[a].at[l % CORES, g_half(a, 1 - c)], r1_view(l, a), g1s.at[a], g1r.at[l % CORES, a], pp=sib)

    def g2_copy(l, a):
        return rcopy(HID.at[l, R1_OFF[a]:R1_OFF[a] + G_HALF[a], :G_COLS[a]], R2[a].at[l % CORES], g2s.at[l % CORES, a], g2r.at[l % CORES, a], pp=2 * (l // CORES) + c)

    def g3_local(l, a):
        return lcopy(r1_view(l, a), G_OUT[a].at[g_half(a, c)], g3s.at[l % CORES, a])

    def g3_remote(l, a):
        return rcopy(r1_view(l, a), G_OUT[a].at[g_half(a, c)], g3s.at[l % CORES, a], g3r.at[a], pp=sib)

    def v1_copies(l):
        return [rcopy(GV.at[l], ZR.at[l, z], v1s.at[l, o - 1], v1r.at[l, z], tp=(z + o) % NT) for o in range(1, NT)]

    def grads_mid(l, arrays):
        for a in arrays:
            g1_copy(l, a).wait_recv()
            n = G_HALF[a]

            def add(b, carry):
                rr = rows(R1_OFF[a] + b * GR, GR)
                tot = G_BUF[a][l % CORES, rows(c * n + b * GR, GR), :] + GP[l + 1, rr, :G_COLS[a]]
                GP[l + 1, rr, :G_COLS[a]] = tot
                HID[l, rr, :G_COLS[a]] = tot.astype(BF16)
                return carry
            loop(n // GR, add, 0)

            @pl.when(l // CORES != ys_)
            def _():
                g2_copy(l, a).start()

    def grads_last(l):
        @pl.when(l // CORES == ys_)
        def _():
            for a in MLP[::-1] + ATT:
                g2_copy(l, a).wait_recv()

                def add(b, carry):
                    rr = rows(R1_OFF[a] + b * GR, GR)
                    GP[l + 1, rr, :G_COLS[a]] += R2[a][l % CORES, rows(b * GR, GR), :].astype(F32)
                    return carry
                loop(G_HALF[a] // GR, add, 0)

                @pl.when(l == s)
                def _():
                    g3_local(l, a).start()

                @pl.when(l != s)
                def _():
                    g3_remote(l, a).start()

    def grads_sent(l):
        for a in range(NA):
            @pl.when(l // CORES != ys_)
            def _():
                g2_copy(l, a).wait_send()

            @pl.when(l == s)
            def _():
                g3_local(l, a).wait()

            @pl.when((l // CORES == ys_) & (l != s))
            def _():
                g3_remote(l, a).wait_send()

    def v2_copy(l):
        return rcopy(GZ.at[l], PR.at[s], v2s.at[l], v2r.at[s], pp=l)

    def vec_mid(l):
        ZR[l, z] = GV[l]
        for o in range(1, NT):
            q = (z + o) % NT
            rcopy(GV.at[l], ZR.at[l, q], v1s.at[l, o - 1], v1r.at[l, q], tp=q).wait_recv()
        tot = sum(ZR[l, k] for k in range(NT))
        row = lax.broadcasted_iota(jnp.int32, (8, D), 0)
        GZ[l] = jnp.where(row < 4, tot, GV[l])

        @pl.when(l == s)
        def _():
            PR[s] = GZ[l]

        @pl.when(l != s)
        def _():
            v2_copy(l).start()

    GV[...] = jnp.zeros_like(GV)
    @pl.when(ys_ == 1)
    def _():
        for a, hop in ((0, 0), (1, 0), (0, 1), (2, 0), (1, 1)):
            hop_on(a, hop)
        hop_end(0)
    settle(0, FIRST, True)
    xcopy.wait()

    def run(phases, at, handle, after=lambda k: None):
        for k, unused in enumerate(phases):
            after(k)
            for op, lag, u in at.get(k, ()):
                handle(op, lag, u)

    def fwd_layer(l, carry):
        for i in range(NC):
            ar_wait(l - 1, l, i, l)

            def handle(op, lag, u):
                m = i - lag

                def go(p, j):
                    if op == 'mid':
                        ar_mid(p, j, u)
                    else:
                        ar_last(p, p, p + 1, j, u)
                if m >= HOME:
                    @pl.when(l * ys_ < NL - 1)
                    def _():
                        go(l, m)
                elif m >= 0:
                    go(l, m)
                else:
                    @pl.when(l > 0)
                    def _():
                        go(l - 1, m + NC)
            run(forward(l, i), FWD_AT, handle)

            if i < HOME:
                ar_send(l, i)
            else:
                @pl.when(l * ys_ < NL - 1)
                def _():
                    ar_send(l, i)

                @pl.when(l * ys_ == NL - 1)
                def _():
                    guest_send(i)
            if i == 1:
                @pl.when(l == 0)
                def _():
                    gcopy.wait()
                    H[NL + 1] = GP[NL].astype(BF16)

                    @pl.when(s == 1)
                    def _():
                        start_all(y_copies())
            if i == 2:
                @pl.when((l > 0) & (l < NL - 1))
                def _():
                    relay(l + 1, ALL)
            if i == NC - 1:
                @pl.when(l == 0)
                def _():
                    relay(l + 1, ALL)

                @pl.when(l < NL - 1)
                def _():
                    settle(l + 1, FIRST, True)
        return carry
    loop(NL, fwd_layer, 0)

    def y_copies_of(q, n):
        src, dst, got = H.at[NL, :n], y.at[q // CORES, c, :n], yr.at[q]
        return lcopy(src, dst, ys.at[0]), rcopy(src, dst, ys.at[1], got, pp=sib), rcopy(src, dst, ys.at[2], got, pp=oy + c)

    def y_pass(q, n):
        part = y.at[q // CORES, c, :n]
        return rcopy(part, part, ys.at[3], yr.at[q], pp=sib)

    def y_arrived(q, n):
        part = y.at[q // CORES, q % CORES, :n]
        rcopy(part, part, ys.at[1], yr.at[q], pp=sib).wait_recv()

    def each_row(do):
        for row, n, other in ((0, S, HOME * C), (1, HOME * C, S)):
            @pl.when(ys_ == row)
            def _():
                do(row, n, other)

    def ri(l):
        return jnp.where(l == NL - 1, NL + 1, l + 1)

    def pass_of(lb):
        return NL + lb + (1 - ys_) * jnp.minimum(lb, 1)

    def bwd_layer(lb, carry):
        l = NL - 1 - lb
        p = pass_of(lb)
        before = pass_of(lb - 1)
        for n in range(NC):
            i = NC - 1 - n

            ar_wait(before, l + 1, i, lb)

            def handle(op, lag, u):
                m = n - lag

                def go(q, lq, j):
                    if op == 'mid':
                        ar_mid(q, j, u, True)
                    else:
                        ar_last(q, ri(lq), lq, j, u, True)
                if m >= 0:
                    @pl.when(l > 0)
                    def _():
                        go(p, l, NC - 1 - m)
                else:
                    @pl.when(lb > 0)
                    def _():
                        go(before, l + 1, -1 - m)

                    @pl.when(lb == NL * ys_)
                    def _():
                        if op == 'mid':
                            ar_mid(NL - 1, m + NC, u)
                        else:
                            ar_last(NL - 1, NL - 1, NL, m + NC, u)

            def guests(layer, what, j):
                @pl.when(lb == layer + NL * ys_)
                def _():
                    what(j)

            def after(k):
                if k == 0 and i >= HOME:
                    guests(1, guest_in, i)
                if k == 1 and NC > i + 1 >= HOME:
                    guests(1, guest_last, i + 1)
                if k == NC and i >= HOME:
                    guests(1, guest_mid, i)
                if k == 0 and n == 0:
                    @pl.when(lb > 0)
                    def _():
                        grads_mid(l + 1, ATT)
                        for a in ALL:
                            g1_copy(l + 1, a).wait_send()
                if n == NC - 1 and k < 2:
                    g1_copy(l, MLP[1 - k]).start()
                if n == NC - 1 and k in (3, 4):
                    @pl.when(l == 0)
                    def _():
                        grads_mid(l, (MLP[4 - k],))
            run(backward(l, ri(l), i, False), BWD_AT, handle, after)

            if i >= HOME:
                @pl.when(lb == 2 + NL * ys_)
                def _():
                    guest_back(i)

            @pl.when(l > 0)
            def _():
                ar_send(p, i, True)
            if n == NC - 1:
                @pl.when(lb == 2 + NL * ys_)
                def _():
                    guest_out(lambda *copies: start_all(copies))
            if n == 1:
                @pl.when(lb > 0)
                def _():
                    vec_mid(l + 1)
            if n == 2:
                @pl.when(lb == 0)
                def _():
                    def out(row, n, other):
                        for j in range(n // C):
                            ar_wait(NL - 1, NL, j)
                        start_all(y_copies_of(CORES * row + c, n))
                    each_row(out)

                @pl.when(lb > 1)
                def _():
                    grads_last(l + 2)

        for a in ATT:
            g1_copy(l, a).start()
        start_all(v1_copies(l))

        @pl.when(l > 0)
        def _():
            grads_mid(l, MLP)
        return carry
    loop(NL, bwd_layer, 0)

    grads_mid(0, ATT)

    def pass_on(row, n, other):
        y_arrived(CORES * (1 - row) + c, other)
        y_pass(CORES * (1 - row) + c, other).start()
        if row:
            guest_home(c).wait_recv()
            guest_home(c).start()
    each_row(pass_on)
    grads_last(1)
    vec_mid(0)
    grads_last(0)

    for o in range(1, NL):
        q = (s + o) % NL
        rcopy(GZ.at[0], PR.at[q], v2s.at[0], v2r.at[q], pp=q).wait_recv()
    PRE[:8, :D] = sum(PR[k] for k in range(NL))
    vout = lcopy(PRE.at[:8, :D], ovec, osem.at[0])
    vout.start()
    for l in range(NL):
        for cp in v1_copies(l):
            cp.wait_send()
    for l in range(NL):
        @pl.when(l != s)
        def _():
            v2_copy(l).wait_send()
    for a in range(NA):
        rcopy(G_OUT[a].at[g_half(a, 1 - c)], G_OUT[a].at[g_half(a, 1 - c)], g3s.at[a], g3r.at[a], pp=sib).wait_recv()

    def out_done(local, *sent):
        local.wait()
        for cp in sent:
            cp.wait_send()

    def all_out(row, n, other):
        out_done(*y_copies_of(CORES * row + c, n))
        y_pass(CORES * (1 - row) + c, other).wait_send()
        y_arrived(CORES * row + 1 - c, n)
        y_arrived(CORES * (1 - row) + 1 - c, other)
        guest_home(1 - c).wait_recv()
    each_row(all_out)

    @pl.when(ys_ == 0)
    def _():
        guest_out(out_done)

        @pl.when(is_end)
        def _():
            for t in range(HOME * SUB, NC * SUB):
                guest_to_hub(t).wait_send()

        @pl.when(inner)
        def _():
            for t in range(HOME * SUB, NC * SUB):
                guest_to_leaf(t).wait_send()

    @pl.when(ys_ == 1)
    def _():
        guest_home(c).wait_send()
        for i in range(HOME, NC):
            guest_copy(i).wait_send()
    for a in range(NA):
        g1_copy(0, a).wait_send()
    for l in range(NL):
        grads_sent(l)
    for cp in sib_copies():
        cp.wait_send()
    @pl.when(s == 0)
    def _():
        for cp in first_copies():
            cp.wait_send()

    @pl.when(s > 0)
    def _():
        for cp in y_copies():
            cp.wait_send()
    for a in ALL:
        pass_copy(oy + 1, a, c).wait_send()

        @pl.when(ys_ == 0)
        def _():
            pass_copy(oy, a, c).wait_send()

        @pl.when(ys_ == 1)
        def _():
            for hop in range(CORES):
                for cp in hop_copies(a, hop):
                    cp.wait_send()

    @pl.when(is_end)
    def _():
        for t in range(NC * SUB):
            end_copy(0, t).wait_send()

    @pl.when(inner)
    def _():
        for t in range(NC * SUB):
            peer_copy(0, t).wait_send()
            back_copy(0, 1, t).wait_send()
    vout.wait()


def finish(y, gq, go, gu, gd, gv, yo, qo, oo, uo, do, n0, n1, n2, n3, n4, n5, n6, bq,
           yb, qb, ob, ub, db, vb, r0, r1, r2, r3, r4, r5, r6, rq, got, put, small):
    trips = [(gd, db, do), (gu, ub, uo), (go, ob, oo), (gq, qb, qo)]
    trips += [tuple(ref.at[m, r] for ref in (y, yb, yo)) for m in range(y.shape[0]) for r in range(y.shape[1])]
    loads = [pltpu.make_async_copy(a, b, got.at[k]) for k, (a, b, o) in enumerate(trips)]
    stores = [pltpu.make_async_copy(b, o, put.at[k]) for k, (a, b, o) in enumerate(trips)]
    vecs = pltpu.make_async_copy(gv, vb, small.at[len(trips)])
    vecs.start()
    for cp in loads:
        cp.start()
    vecs.wait()
    for row, refs in enumerate(((r0,), (r1,), (r2,), (r3,), (r4, r5), (r6,))):
        for ref in refs:
            ref[...] = vb[row:row + 1, :]
    e = rq.shape[2]
    for k in range(3):
        for h in range(CORES):
            rq[k, h:h + 1, :] = vb[6:7, (CORES * k + h) * e:(CORES * k + h + 1) * e]
    tiny = [pltpu.make_async_copy(a, b, small.at[k]) for k, (a, b) in enumerate(((r0, n0), (r1, n1), (r2, n2), (r3, n3), (r4, n4), (r5, n5), (r6, n6), (rq, bq)))]
    for cp in tiny:
        cp.start()
    for cp, out in zip(loads, stores):
        cp.wait()
        out.start()
    for cp in tiny + stores:
        cp.wait()


def finish_step(y, gq, go, gu, gd, gv, e):
    hbm = pl.BlockSpec(memory_space=pl.ANY)
    row = jax.ShapeDtypeStruct((1, gv.shape[1]), F32)
    outs = [jax.ShapeDtypeStruct(a.shape, a.dtype) for a in (y, gq, go, gu, gd)] + [row] * 7 + [jax.ShapeDtypeStruct((3, CORES, e), F32)]
    bufs = outs[:5] + [gv] + outs[5:]
    return pl.pallas_call(
        finish,
        out_shape=outs,
        in_specs=[hbm] * 6,
        out_specs=[hbm] * len(outs),
        scratch_shapes=[pltpu.VMEM(a.shape, a.dtype) for a in bufs] + [pltpu.SemaphoreType.DMA((9,))] * 3,
        name='neox_out',
    )(y, gq, go, gu, gd, gv)


def group_step(dims, *args):
    x = args[0]
    S, D, E, C, F = dims
    E2 = 2 * E
    hbm = pl.BlockSpec(memory_space=pl.ANY)
    out_shape = [
        jax.ShapeDtypeStruct(x.shape, BF16),
        jax.ShapeDtypeStruct((3 * E2, D), F32),
        jax.ShapeDtypeStruct((E2, D), F32),
        jax.ShapeDtypeStruct((D, F), F32),
        jax.ShapeDtypeStruct((F, D), F32),
        jax.ShapeDtypeStruct((8, D), F32),
    ]

    def vm(*shape, dtype=BF16):
        return pltpu.VMEM(shape, dtype)
    dma = pltpu.SemaphoreType.DMA
    scratch = [
        vm(NL, 3 * E2, D), vm(NL, E2, D), vm(NL, D, F), vm(NL, F, D), vm(NL, 8, D, dtype=F32),
        vm(NL + 2, S, D),
        vm(NL, S, E2), vm(NL, S, E2), vm(NL, S, E2), vm(NL, E2, S), vm(E2, S), vm(NL, S, E2),
        *[vm(NL, 2, (i + 1) * C, C) for i in range(NC)],
        vm(NL, S, F), vm(NL + 1, S, F, dtype=F32),
        vm(CORES, S, D), vm(CORES, S, D), vm(S, D), vm(S + C, D, dtype=F32),
        *[vm(CORES, *k, dtype=F32) for k in ((3 * E2, D), (E2, D), (D, F), (F, D))],
        *[vm(CORES, *k) for k in ((3 * E, D), (E, D), (D // CORES, F), (F // CORES, D))],
        vm(S, E2, dtype=F32), vm(S, E2, dtype=F32),
        vm(CORES, C + 8, E2, dtype=F32),
        *[vm(*k, 8, D, dtype=F32) for k in ((NL,), (NL, NT), (NL,), (NL,))],
        vm(C, D), vm(C, D), vm(C, max(D, F), dtype=F32), vm(C, F), vm(S, C), vm(S, C, dtype=F32),
        *[vm(1, D, dtype=F32)] * 4, vm(1, D), vm(1, D), vm(1, F), vm(3, CORES, E), vm(S, D),
        dma((NA,)), dma((NA + 1,)), dma((CORES, NA + 1)), dma((NL, 2 * NA + 1)), dma((CORES, NA)), dma((3, NA)), dma((NA, 4)), dma((CORES,)), dma((1,)),
        dma((NC * SUB,)), dma((NC * SUB,)), dma((CORES, NC * SUB)), dma((CORES, NC * SUB)), dma((CORES, NC * SUB)),
        dma((NL,)), dma((NL,)), dma((NA,)), dma((CORES, NA)), dma((CORES, NA)), dma((CORES, NA)), dma((CORES, NA)), dma((NA,)),
        dma((NL, NT - 1)), dma((NL, NT)), dma((NL,)), dma((NL,)), dma((1,)), dma((8,)),
        dma((NC,)), dma((NC,)), dma((NC * SUB,)), dma((NC * SUB,)), dma((3,)), dma((CORES,)),
    ]
    return pl.pallas_call(
        functools.partial(body, dims),
        out_shape=out_shape,
        in_specs=[hbm] * len(args),
        out_specs=[hbm] * 6,
        scratch_shapes=scratch,
        compiler_params=pltpu.CompilerParams(collective_id=0, has_side_effects=True, vmem_limit_bytes=67043328),
        name='neox_group',
    )(*args)


def solution(mesh):
    def device_fn(x_in, g_out, ln1_gain, ln1_bias, w_qkv, b_qkv, w_out, b_out, ln2_gain, ln2_bias, w_up, b_up, w_down, b_down):
        n_micro, n_rows, S, D = x_in.shape
        heads, E = w_qkv.shape[2], w_qkv.shape[4]
        F = w_up.shape[2]
        C = S // NC
        wqkv = jnp.transpose(w_qkv[0], (1, 2, 3, 0)).reshape(heads * 3 * E, D)
        bqkv = jnp.transpose(b_qkv[0], (1, 0, 2))
        tab = jnp.asarray(rotary_base(C, NC, E, heads))
        part = group_step((S, D, E, C, F), x_in, g_out, wqkv, w_out[0].reshape(heads * E, D), w_up[0], w_down[0], ln1_gain, ln1_bias, ln2_gain, ln2_bias, b_out, b_down, b_up, bqkv, tab)
        y, gq, go, gup, gdn, n1g, n1b, n2g, n2b, gbo, gbd, gbu, gbq = finish_step(*part, E)
        gq = jnp.transpose(gq.reshape(heads, 3, E, D), (3, 0, 1, 2))[None]
        gbq = jnp.transpose(gbq, (1, 0, 2))[None]
        return (y, n1g, n1b, gq, gbq, go.reshape(1, heads, E, D), gbo, n2g, n2b, gup[None], gbu, gdn[None], gbd)

    return jax.shard_map(device_fn, mesh=mesh, in_specs=(P('dp'), P('dp')) + STAGE_SPECS, out_specs=(P('dp'),) + GRAD_SPECS, check_vma=False)
```

```python
import functools
import math

import jax
import jax.numpy as jnp
import numpy as np
from jax import lax
from jax.experimental import pallas as pl
from jax.experimental.pallas import tpu as pltpu
from jax.sharding import PartitionSpec as P

ROPE_BASE = 10000.0
LN_EPS = 1e-5
STAGE_SPECS = (P('pp'), P('pp'), P('pp', None, 'tp'), P('pp', 'tp'), P('pp', 'tp'), P('pp'), P('pp'), P('pp'), P('pp', None, 'tp'), P('pp', 'tp'), P('pp', 'tp'), P('pp'))
OWN = ('dp', 'pp')
GRAD_SPECS = (P(OWN), P(OWN), P(OWN, None, 'tp'), P(OWN, 'tp'), P(OWN, 'tp'), P(OWN), P(OWN), P(OWN), P(OWN, None, 'tp'), P(OWN, 'tp'), P(OWN, 'tp'), P(OWN))


F32 = jnp.float32
BF16 = jnp.bfloat16
NL = 4
NT = 4
NC = 4
NA = 4
CORES = 2
SUB = 4
FWD_AT = {k: (('mid', 1, k), ('last', 2, k)) for k in range(SUB)}
BWD_AT = {k: (('last', 2, k),) * (k < SUB) + (('mid', 1, k - 1),) * (k > 0) for k in range(SUB + 1)}
LOG2E = 1.4426950408889634
RSQRT2 = 0.7071067811865476
INV_SQRT_2PI = 0.3989422804014327


def nn(a, b):
    return lax.dot_general(a, b, (((1,), (0,)), ((), ())), preferred_element_type=F32)


def nt(a, b):
    return lax.dot_general(a, b, (((1,), (1,)), ((), ())), preferred_element_type=F32)


def tn(a, b):
    return lax.dot_general(a, b, (((0,), (0,)), ((), ())), preferred_element_type=F32)


def loop(n, step, init, unroll=False):
    return lax.fori_loop(0, n, step, init, unroll=unroll)


def col_sum(v):
    return jnp.sum(v, axis=0, keepdims=True)


def row_mean(v):
    return jnp.mean(v, axis=-1, keepdims=True)


def fold(v):
    return jnp.sum(v.reshape(v.shape[0] // 8, 8, v.shape[1]), axis=0)


def rotary_base(chunk, n_chunks, head_dim, n_heads):
    rot_dim = head_dim // 4
    half = rot_dim // CORES
    inv_freq = np.zeros((head_dim,), np.float64)
    inv_freq[:rot_dim] = np.tile(ROPE_BASE ** (-(np.arange(half) * 2.0) / rot_dim), 2)
    inv_freq = np.tile(inv_freq, n_heads)
    pos = np.concatenate([np.arange(chunk), np.arange(8) * (np.arange(8) < n_chunks) * chunk]).astype(np.float64)
    ang = pos[:, None] * inv_freq[None, :]
    return np.stack([np.cos(ang), np.sin(ang)]).astype(np.float32)


def body(dims, x, g, wqkv, wo, wup, wdn, n0, n1, n2, n3, n4, n5, n6, bq, tab,
         y, oqkv, oo, oup, odn, ovec,
         WQ, WO, WU, WD, VEC, H, Q, K, V, KT, VT, CTX, P0, P1, P2, P3, HID, GP, RA, RB, PS, PF,
         GQ, GO, GU, GD, R2Q, R2O, R2U, R2D, DK, DV, TAB, GV, ZR, GZ, PR,
         AS, MS, PRE, DPB, DS, ST, N0, N1, N2, N3, N4, N5, N6, BQ, GX,
         wl, ws, wy, wr, wf, w0s, w0r, xs, gs, sab, sc, ra_s, rb_s, rc_s, ys, yr, g1s, g1r, g2s, g2r, g3s, g3r, v1s, v1r, v2s, v2r, osem, ns, gxs, gxr, gs2, gs3, ygs, ygr):
    S, D, E, C, F = dims
    E2 = 2 * E
    SR = C // SUB
    z = lax.axis_index('tp')
    xg = lax.axis_index('dp')
    s = lax.axis_index('pp')
    ys_ = s // CORES
    c = s % CORES
    sib = s + 1 - 2 * c
    oy = 2 * (1 - ys_)
    is_end = z * (NT - 1 - z) == 0
    inner = z * (NT - 1 - z) > 0
    edge = 1 - jnp.minimum(z * (NT - 1 - z), 1)
    hub = 1 + z // 3
    leaf = jnp.where(z == 1, 0, 3)
    peer = 3 - z
    PX = (P0, P1, P2, P3)
    W_IN = (wqkv, wo, wup, wdn)
    W_BUF = (WQ, WO, WU, WD)
    G_HALF = (3 * E, E, D // CORES, F // CORES)
    ALL = tuple(range(NA))
    FIRST, REST = ALL[:1], ALL[1:]
    ATT, MLP = ALL[:2], ALL[2:]
    G_BUF = (GQ, GO, GU, GD)
    G_OUT = (oqkv, oo, oup, odn)
    G_COLS = (D, D, F, D)
    R1_OFF = tuple(sum(G_HALF[:k]) for k in range(NA))
    R2 = (R2Q, R2O, R2U, R2D)

    def rcopy(src, dst, ss, rs, **dev):
        return pltpu.make_async_remote_copy(src_ref=src, dst_ref=dst, send_sem=ss, recv_sem=rs, device_id=dev, device_id_type=pl.DeviceIdType.MESH)

    def lcopy(src, dst, sem):
        return pltpu.make_async_copy(src, dst, sem)

    def rows(start, n):
        return pl.ds(pl.multiple_of(start, n), n)

    xcopy = lcopy(x.at[ys_, c], H.at[0], xs.at[0])
    xcopy.start()
    gcopy = lcopy(g.at[ys_, c], GP.at[NL], gs.at[0])
    gcopy.start()
    tcopy = lcopy(tab, TAB, xs.at[1])
    tcopy.start()
    for a in range(NA):
        lcopy(W_IN[a], W_BUF[a].at[s], wl.at[a]).start()
    small = [lcopy(a, b, ns.at[k]) for k, (a, b) in enumerate(((n0, N0), (n1, N1), (n2, N2), (n3, N3), (n4, N4), (n5, N5), (n6, N6), (bq, BQ)))]
    for cp in small:
        cp.start()

    bar = pltpu.get_barrier_semaphore()
    for o in range(1, NT):
        pl.semaphore_signal(bar, inc=1, device_id={'tp': (z + o) % NT}, device_id_type=pl.DeviceIdType.MESH)
    for o in range(1, NL):
        pl.semaphore_signal(bar, inc=1, device_id={'pp': (s + o) % NL}, device_id_type=pl.DeviceIdType.MESH)
    pl.semaphore_signal(bar, inc=1, device_id={'dp': 1 - xg}, device_id_type=pl.DeviceIdType.MESH)
    pl.semaphore_wait(bar, NT + NL - 1)

    def half(ref, a, k):
        return ref.at[rows(k * G_HALF[a], G_HALF[a])]

    def sib_copies():
        out = [rcopy(W_IN[a], W_BUF[a].at[s], ws.at[a], wr.at[s, 2 * a], pp=sib) for a in ALL]
        return out + [rcopy(VEC.at[s], VEC.at[s], ws.at[NA], wr.at[s, 2 * NA], pp=sib)]

    def y_copies():
        out = [rcopy(half(W_IN[a], a, k), half(W_BUF[a].at[s], a, k), wy.at[k, a], wr.at[s, 2 * a + k], pp=oy + k) for a in ALL for k in range(CORES)]
        return out[:2] + [rcopy(VEC.at[s], VEC.at[s], wy.at[k, NA], wr.at[s, 2 * NA], pp=oy + k) for k in range(CORES)] + out[2:]

    def quarter(ref, a, q):
        return ref.at[rows(q * (G_HALF[a] // CORES), G_HALF[a] // CORES)]

    def first_copies():
        out = []
        for a in ALL:
            for k in range(CORES):
                q = 2 * xg + k
                out.append(rcopy(quarter(W_IN[a], a, q), quarter(W_BUF[a].at[0], a, q), wy.at[k, a], w0r.at[a, q], pp=oy + k))
        return out + [rcopy(VEC.at[s], VEC.at[s], wy.at[k, NA], wr.at[s, 2 * NA], pp=oy + k) for k in range(CORES)]

    def mine(hop):
        return 2 * (xg if hop == 0 else 1 - xg) + c

    def hop_copies(a, hop):
        part, sem = quarter(W_BUF[a].at[0], a, mine(hop)), w0r.at[a, mine(hop)]
        out = [rcopy(part, part, w0s.at[hop, a], sem, pp=sib)]
        return out if hop else out + [rcopy(part, part, w0s.at[2, a], sem, dp=1 - xg)]

    def hop_on(a, hop):
        copies = hop_copies(a, hop)
        copies[0].wait_recv()
        start_all(copies)

    def hop_end(a):
        for k in range(CORES):
            part = quarter(W_BUF[a].at[0], a, 2 * k + 1 - c)
            rcopy(part, part, w0s.at[0, a], w0r.at[a, 2 * k + 1 - c], pp=sib).wait_recv()

    def start_all(copies):
        for cp in copies:
            cp.start()

    for cp in small:
        cp.wait()
    for k, ref in enumerate((N0, N1, N2, N3, N4, N5, N6)):
        VEC[s, k:k + 1, :] = ref[...].astype(F32)
    VEC[s, 7:8, :3 * E2] = jnp.concatenate([BQ[k, h:h + 1, :].astype(F32) for k in range(3) for h in range(CORES)], axis=1)

    @pl.when(s == 0)
    def _():
        start_all(first_copies())

    @pl.when(s > 1)
    def _():
        start_all(y_copies())
    start_all(sib_copies())

    def pass_copy(l, a, k):
        part = half(W_BUF[a].at[l], a, k)
        return rcopy(part, part, wf.at[l % CORES, a], wr.at[l, 2 * a + k], pp=sib)

    def relay(l, arrays):
        @pl.when(l // CORES != ys_)
        def _():
            for a in arrays:
                pass_copy(l, a, c).wait_recv()
                pass_copy(l, a, c).start()

    def settle(l, arrays, small):
        @pl.when(l == s)
        def _():
            for a in arrays:
                lcopy(W_IN[a], W_BUF[a].at[s], wl.at[a]).wait()

        @pl.when(l == sib)
        def _():
            for a in arrays:
                rcopy(W_IN[a], W_BUF[a].at[l], ws.at[a], wr.at[l, 2 * a], pp=sib).wait_recv()

        @pl.when((l // CORES != ys_) & (l > 0))
        def _():
            for a in arrays:
                pass_copy(l, a, 1 - c).wait_recv()
        if small:
            @pl.when(l != s)
            def _():
                rcopy(VEC.at[l], VEC.at[l], ws.at[NA], wr.at[l, 2 * NA], pp=sib).wait_recv()

    tcopy.wait()

    lane = lax.broadcasted_iota(jnp.int32, (C, E2), 1)
    head_lane = lane // E
    in_head = lane % E
    rot_half = E // 8
    low = in_head < rot_half
    sub_head = lax.broadcasted_iota(jnp.int32, (E2, C), 0) // E
    lower = lax.broadcasted_iota(jnp.int32, (C, C), 0) <= lax.broadcasted_iota(jnp.int32, (C, C), 1)
    c1 = E ** -0.5 * LOG2E

    def tabs(i):
        (cb, sb), (cr, sr) = ([TAB[k, r, :] for k in range(CORES)] for r in (slice(C), slice(C + i, C + i + 1)))
        cs, sn = cb * cr - sb * sr, sb * cr + cb * sr
        return cs, jnp.where(low, -sn, 0.0), jnp.where(low, 0.0, sn)

    def rotate(v, t):
        cs, sa, sb = t
        return v * cs + pltpu.roll(v, E2 - rot_half, 1) * sa + pltpu.roll(v, rot_half, 1) * sb

    def unrotate(v, t):
        cs, sa, sb = t
        return v * cs + pltpu.roll(v * sa, rot_half, 1) + pltpu.roll(v * sb, E2 - rot_half, 1)

    def end_copy(p, t):
        return rcopy(PS.at[t * SR:(t + 1) * SR], RA.at[p % CORES, t * SR:(t + 1) * SR], sab.at[t], ra_s.at[p % CORES, t], tp=hub)

    def peer_copy(p, t):
        return rcopy(PS.at[t * SR:(t + 1) * SR], RB.at[p % CORES, t * SR:(t + 1) * SR], sab.at[t], rb_s.at[p % CORES, t], tp=peer)

    def back_copy(p, di, t):
        return rcopy(H.at[di, t * SR:(t + 1) * SR], H.at[di, t * SR:(t + 1) * SR], sc.at[t], rc_s.at[p % CORES, t], tp=leaf)

    def pf_row(i, back):
        return (NC if back and i == NC - 1 else i) * C

    def ar_send(p, i, back=False):
        @pl.when(is_end)
        def _():
            for t in range(i * SUB, (i + 1) * SUB):
                @pl.when(p > 0)
                def _():
                    end_copy(p, t).wait_send()
                f0 = pf_row(i, back) + (t - i * SUB) * SR
                PS[t * SR:(t + 1) * SR, :] = PF[f0:f0 + SR, :].astype(BF16)
                end_copy(p, t).start()

    def out_bias(l):
        return VEC[l, 4:5, :] + VEC[l, 5:6, :]

    def ar_mid(p, i, u, back=False):
        t = i * SUB + u
        r = slice(t * SR, (t + 1) * SR)
        f0 = pf_row(i, back) + u * SR

        @pl.when(inner)
        def _():
            end_copy(p, t).wait_recv()
            @pl.when(p > 0)
            def _():
                peer_copy(p, t).wait_send()
            PS[r, :] = (PF[f0:f0 + SR, :] + RA[p % CORES, r, :].astype(F32)).astype(BF16)
            peer_copy(p, t).start()

    def ar_last(p, ri, di, i, u, back=False):
        t = i * SUB + u
        r = slice(t * SR, (t + 1) * SR)

        @pl.when(inner)
        def _():
            peer_copy(p, t).wait_recv()
            @pl.when(p > 0)
            def _():
                back_copy(p, di, t).wait_send()
            both = PS[r, :].astype(F32) + RB[p % CORES, r, :].astype(F32)
            own = H[ri, r, :].astype(F32)
            H[di, r, :] = (own + both if back else own + both + out_bias(p)).astype(BF16)
            back_copy(p, di, t).start()

    def ar_wait(p, di, i, on=1):
        @pl.when(on * edge > 0)
        def _():
            for t in range(i * SUB, (i + 1) * SUB):
                back_copy(p, di, t).wait_recv()

    GP1 = NL % 3
    HOME = NC // CORES

    def guest_copy(i):
        part = GX.at[i * C:(i + 1) * C]
        return rcopy(part, part, gxs.at[i], gxr.at[i], pp=c)

    def guest_send(i):
        r = slice(i * C, (i + 1) * C)
        once = jnp.where(z == 1, 1.0, 0.0)
        GX[r, :] = (PF[r, :] + once * (H[NL - 1, r, :].astype(F32) + out_bias(NL - 1))).astype(BF16)
        guest_copy(i).start()

    def guest_hop(t, dst, sem, arrive, to):
        return rcopy(GX.at[t * SR:(t + 1) * SR], dst.at[GP1, t * SR:(t + 1) * SR], sem.at[t], arrive.at[GP1, t], tp=to)

    def guest_to_hub(t):
        return guest_hop(t, RA, gs2, ra_s, hub)

    def guest_to_peer(t):
        return guest_hop(t, RB, gs2, rb_s, peer)

    def guest_to_leaf(t):
        return guest_hop(t, RB, gs3, rc_s, leaf)

    def parts(i):
        return [(t, slice(t * SR, (t + 1) * SR)) for t in range(i * SUB, (i + 1) * SUB)]

    def guest_in(i):
        guest_copy(i).wait_recv()

        @pl.when(is_end)
        def _():
            for t, r in parts(i):
                guest_to_hub(t).start()

    def guest_mid(i):
        @pl.when(inner)
        def _():
            for t, r in parts(i):
                guest_to_hub(t).wait_recv()
                GX[r, :] = (GX[r, :].astype(F32) + RA[GP1, r, :].astype(F32)).astype(BF16)
                guest_to_peer(t).start()

    def guest_last(i):
        @pl.when(inner)
        def _():
            for t, r in parts(i):
                guest_to_peer(t).wait_recv()
                guest_to_peer(t).wait_send()
                GX[r, :] = (GX[r, :].astype(F32) + RB[GP1, r, :].astype(F32)).astype(BF16)
                guest_to_leaf(t).start()

    def guest_back(i):
        @pl.when(is_end)
        def _():
            for t, r in parts(i):
                guest_to_leaf(t).wait_recv()

    def guest_out(act):
        low = slice(HOME * C, S)
        for role, src in ((is_end, RB.at[GP1, low]), (inner, GX.at[low])):
            @pl.when(role)
            def _():
                dst = y.at[1, c, low]
                act(lcopy(src, dst, ygs.at[0]), rcopy(src, dst, ygs.at[1], ygr.at[c], pp=sib), rcopy(src, dst, ygs.at[2], ygr.at[c], pp=s + CORES))

    def guest_home(q):
        return rcopy(y.at[1, q, HOME * C:S], y.at[1, q, HOME * C:S], ygs.at[0], ygr.at[q], pp=sib)

    def stats(hf):
        cen = hf - row_mean(hf)
        rstd = lax.rsqrt(row_mean(cen * cen) + LN_EPS)
        return cen * rstd, rstd

    LB = 32
    GR = 32

    def norms(l, i):
        g1, b1, g2, b2 = (VEC[l, k:k + 1, :] for k in range(NA))

        def step(b, carry):
            hf = H[l, rows(i * C + b * LB, LB), :].astype(F32)
            xhat, unused = stats(hf)
            AS[rows(b * LB, LB), :] = (xhat * g1 + b1).astype(BF16)
            MS[rows(b * LB, LB), :] = (xhat * g2 + b2).astype(BF16)
            return carry
        loop(C // LB, step, 0, unroll=True)

    def by_kind():
        return [(h * 3 + k) * E for k in range(3) for h in range(CORES)]

    def wq(l):
        return jnp.concatenate([WQ[l, r:r + E, :] for r in by_kind()], axis=0)

    def forward(l, i):
        r0, r1 = i * C, (i + 1) * C
        norms(l, i)
        qkv = nt(AS[...], wq(l)) + VEC[l, 7:8, :3 * E2]
        qkv = qkv.astype(BF16).astype(F32)
        t = tabs(i)
        q = rotate(qkv[:, :E2], t).astype(BF16)
        kf = rotate(qkv[:, E2:2 * E2], t)
        vf = qkv[:, 2 * E2:3 * E2]
        Q[l, r0:r1, :] = q
        K[l, r0:r1, :] = kf.astype(BF16)
        V[l, r0:r1, :] = vf.astype(BF16)
        KT[l, :, r0:r1] = jnp.transpose(kf).astype(BF16)
        VT[:, r0:r1] = jnp.transpose(vf).astype(BF16)
        yield

        def far(*hops):
            if i == 0:
                @pl.when((l == 0) & (ys_ == 1))
                def _():
                    for a, hop in hops:
                        hop_on(a, hop)
        far((3, 0))
        RBK = C // CORES
        outs = []
        for h in range(CORES):
            qm = jnp.where(head_lane == h, Q[l, r0:r1, :].astype(F32), 0.0).astype(BF16)
            ST[:r1, :] = nt(K[l, :r1, :], qm)
            ST[r0:r1, :] = jnp.where(lower, ST[r0:r1, :], -1e30)

            def top(b, m):
                return jnp.maximum(m, jnp.max(ST[rows(b * RBK, RBK), :].reshape(RBK // 8, 8, C), axis=0))
            m = jnp.max(loop(r1 // RBK, top, jnp.full((8, C), -3e38, F32), unroll=True), axis=0, keepdims=True)
            mc = m * c1

            def expo(b, tot):
                e = jnp.exp2(ST[rows(b * RBK, RBK), :] * c1 - mc)
                ST[rows(b * RBK, RBK), :] = e
                return tot + fold(e)
            tot = col_sum(loop(r1 // RBK, expo, jnp.zeros((8, C), F32), unroll=True))
            inv = 1.0 / tot

            def put(b, carry):
                PX[i][l, h, rows(b * RBK, RBK), :] = (ST[rows(b * RBK, RBK), :] * inv).astype(BF16)
                return carry
            loop(r1 // RBK, put, 0, unroll=True)
            outs.append(nn(VT[:, :r1], PX[i][l, h]))
            if h == 0:
                yield
        ctx = jnp.transpose(jnp.where(sub_head == 0, outs[0], outs[1])).astype(BF16)
        CTX[l, r0:r1, :] = ctx
        yield
        if i == 0:
            far((2, 1), (3, 1))

            @pl.when((l == 0) & (ys_ == 1))
            def _():
                for a in REST:
                    hop_end(a)
            settle(l, REST, False)
        PF[r0:r1, :] = nn(ctx, WO[l])
        PRE[...] = nn(MS[...], WU[l])
        bup = VEC[l, 6:7, :]
        GB = 32

        def act(b, carry):
            u = PRE[rows(b * GB, GB), :] + bup
            cdf = 0.5 * (1.0 + lax.erf(u * RSQRT2))
            pdf = jnp.exp2(u * u * (-0.5 * LOG2E)) * INV_SQRT_2PI
            HID[l, rows(r0 + b * GB, GB), :] = (u * cdf).astype(BF16)
            GP[l, rows(r0 + b * GB, GB), :] = cdf + u * pdf
            return carry
        loop(C // GB, act, 0, unroll=True)
        PF[r0:r1, :] += nn(HID[l, r0:r1, :], WD[l])
        yield

    def backward(l, dl, i, last):
        r0, r1 = i * C, (i + 1) * C
        par = l % CORES
        first = i == NC - 1

        def acc(ref, val):
            if first:
                ref[par] = val
            else:
                ref[par] += val

        def acc_row(k, val, w=D):
            GV[l, k:k + 1, :w] += val

        norms(l, i)
        dy = H[dl, r0:r1, :]
        acc_row(4, col_sum(dy.astype(F32)))
        PRE[...] = nt(dy, WD[l])
        GB = 32

        def act(b, tot):
            d = PRE[rows(b * GB, GB), :] * GP[l, rows(r0 + b * GB, GB), :]
            DPB[rows(b * GB, GB), :] = d.astype(BF16)
            return tot + fold(d)
        dbu = loop(C // GB, act, jnp.zeros((8, F), F32), unroll=True)
        acc_row(5, col_sum(dbu))
        acc(GD, tn(HID[l, r0:r1, :], dy))
        yield
        acc(GU, tn(MS[...], DPB[...]))
        f0 = pf_row(i, True)
        PF[f0:f0 + C, :] = nt(DPB[...], WU[l])
        yield
        dctx = nt(dy, WO[l]).astype(BF16)
        ctx = CTX[l, r0:r1, :]
        acc(GO, tn(ctx, dy))
        prod = dctx.astype(F32) * ctx.astype(F32)
        q = Q[l, r0:r1, :].astype(F32)
        dcf = dctx.astype(F32)
        RBK = C // CORES
        dqt = []
        for h in range(CORES):
            sel = head_lane == h
            qm = jnp.where(sel, q, 0.0).astype(BF16)
            dcm = jnp.where(sel, dcf, 0.0).astype(BF16)
            dsum = jnp.transpose(jnp.where(sel, prod, 0.0))
            drow = col_sum(dsum)
            ST[:r1, :] = nt(V[l, :r1, :], dcm)

            def sub(b, carry):
                pr = PX[i][l, h, rows(b * RBK, RBK), :].astype(F32)
                DS[rows(b * RBK, RBK), :] = (pr * (ST[rows(b * RBK, RBK), :] - drow)).astype(BF16)
                return carry
            loop(r1 // RBK, sub, 0, unroll=True)
            dk = nn(DS[:r1, :], qm)
            dv = nn(PX[i][l, h], dcm)
            if first and h == 0:
                DK[:r1, :] = dk
                DV[:r1, :] = dv
            else:
                DK[:r1, :] += dk
                DV[:r1, :] += dv
            dqt.append(nn(KT[l, :, :r1], DS[:r1, :]))
            yield
        scale = E ** -0.5
        t = tabs(i)
        dq = unrotate(jnp.transpose(jnp.where(sub_head == 0, dqt[0], dqt[1])) * scale, t)
        dk = unrotate(DK[r0:r1, :] * scale, t)
        dv = DV[r0:r1, :]
        dqkv = jnp.concatenate([dq, dk, dv], axis=1)
        acc_row(6, col_sum(dqkv), 3 * E2)
        dqkv = dqkv.astype(BF16)
        dwq = tn(dqkv, AS[...])
        for k, r in enumerate(by_kind()):
            if first:
                GQ[par, r:r + E, :] = dwq[k * E:(k + 1) * E]
            else:
                GQ[par, r:r + E, :] += dwq[k * E:(k + 1) * E]
        PRE[...] = nn(dqkv, wq(l))
        yield
        g1, g2 = VEC[l, 0:1, :], VEC[l, 2:3, :]

        def lnb(b, tots):
            hf = H[l, rows(r0 + b * LB, LB), :].astype(F32)
            xhat, rstd = stats(hf)
            da = PRE[rows(b * LB, LB), :]
            dm = PF[rows(f0 + b * LB, LB), :]
            dx = da * g1 + dm * g2
            m1 = row_mean(dx)
            m2 = row_mean(dx * xhat)
            if not last:
                PF[rows(f0 + b * LB, LB), :] = rstd * (dx - m1 - xhat * m2)
            terms = (da * xhat, da, dm * xhat, dm)
            return tuple(a + fold(v) for a, v in zip(tots, terms))
        tots = loop(C // LB, lnb, tuple(jnp.zeros((8, D), F32) for _ in range(NA)), unroll=True)
        for k in range(NA):
            acc_row(k, col_sum(tots[k]))
        yield

    def g_half(a, k):
        return rows(k * G_HALF[a], G_HALF[a])

    def r1_view(l, a):
        return GP.at[l + 1, R1_OFF[a]:R1_OFF[a] + G_HALF[a], :G_COLS[a]]

    def g1_copy(l, a):
        return rcopy(G_BUF[a].at[l % CORES, g_half(a, 1 - c)], r1_view(l, a), g1s.at[a], g1r.at[l % CORES, a], pp=sib)

    def g2_copy(l, a):
        return rcopy(HID.at[l, R1_OFF[a]:R1_OFF[a] + G_HALF[a], :G_COLS[a]], R2[a].at[l % CORES], g2s.at[l % CORES, a], g2r.at[l % CORES, a], pp=2 * (l // CORES) + c)

    def g3_local(l, a):
        return lcopy(r1_view(l, a), G_OUT[a].at[g_half(a, c)], g3s.at[l % CORES, a])

    def g3_remote(l, a):
        return rcopy(r1_view(l, a), G_OUT[a].at[g_half(a, c)], g3s.at[l % CORES, a], g3r.at[a], pp=sib)

    def v1_copies(l):
        return [rcopy(GV.at[l], ZR.at[l, z], v1s.at[l, o - 1], v1r.at[l, z], tp=(z + o) % NT) for o in range(1, NT)]

    def grads_mid(l, arrays):
        for a in arrays:
            g1_copy(l, a).wait_recv()
            n = G_HALF[a]

            def add(b, carry):
                rr = rows(R1_OFF[a] + b * GR, GR)
                tot = G_BUF[a][l % CORES, rows(c * n + b * GR, GR), :] + GP[l + 1, rr, :G_COLS[a]]
                GP[l + 1, rr, :G_COLS[a]] = tot
                HID[l, rr, :G_COLS[a]] = tot.astype(BF16)
                return carry
            loop(n // GR, add, 0)

            @pl.when(l // CORES != ys_)
            def _():
                g2_copy(l, a).start()

    def grads_last(l):
        @pl.when(l // CORES == ys_)
        def _():
            for a in MLP[::-1] + ATT:
                g2_copy(l, a).wait_recv()

                def add(b, carry):
                    rr = rows(R1_OFF[a] + b * GR, GR)
                    GP[l + 1, rr, :G_COLS[a]] += R2[a][l % CORES, rows(b * GR, GR), :].astype(F32)
                    return carry
                loop(G_HALF[a] // GR, add, 0)

                @pl.when(l == s)
                def _():
                    g3_local(l, a).start()

                @pl.when(l != s)
                def _():
                    g3_remote(l, a).start()

    def grads_sent(l):
        for a in range(NA):
            @pl.when(l // CORES != ys_)
            def _():
                g2_copy(l, a).wait_send()

            @pl.when(l == s)
            def _():
                g3_local(l, a).wait()

            @pl.when((l // CORES == ys_) & (l != s))
            def _():
                g3_remote(l, a).wait_send()

    def v2_copy(l):
        return rcopy(GZ.at[l], PR.at[s], v2s.at[l], v2r.at[s], pp=l)

    def vec_mid(l):
        ZR[l, z] = GV[l]
        for o in range(1, NT):
            q = (z + o) % NT
            rcopy(GV.at[l], ZR.at[l, q], v1s.at[l, o - 1], v1r.at[l, q], tp=q).wait_recv()
        tot = sum(ZR[l, k] for k in range(NT))
        row = lax.broadcasted_iota(jnp.int32, (8, D), 0)
        GZ[l] = jnp.where(row < 4, tot, GV[l])

        @pl.when(l == s)
        def _():
            PR[s] = GZ[l]

        @pl.when(l != s)
        def _():
            v2_copy(l).start()

    GV[...] = jnp.zeros_like(GV)
    @pl.when(ys_ == 1)
    def _():
        for a, hop in ((0, 0), (1, 0), (0, 1), (2, 0), (1, 1)):
            hop_on(a, hop)
        hop_end(0)
    settle(0, FIRST, True)
    xcopy.wait()

    def run(phases, at, handle, after=lambda k: None):
        for k, unused in enumerate(phases):
            after(k)
            for op, lag, u in at.get(k, ()):
                handle(op, lag, u)

    def fwd_layer(l, carry):
        for i in range(NC):
            ar_wait(l - 1, l, i, l)

            def handle(op, lag, u):
                m = i - lag

                def go(p, j):
                    if op == 'mid':
                        ar_mid(p, j, u)
                    else:
                        ar_last(p, p, p + 1, j, u)
                if m >= HOME:
                    @pl.when(l * ys_ < NL - 1)
                    def _():
                        go(l, m)
                elif m >= 0:
                    go(l, m)
                else:
                    @pl.when(l > 0)
                    def _():
                        go(l - 1, m + NC)
            run(forward(l, i), FWD_AT, handle)

            if i < HOME:
                ar_send(l, i)
            else:
                @pl.when(l * ys_ < NL - 1)
                def _():
                    ar_send(l, i)

                @pl.when(l * ys_ == NL - 1)
                def _():
                    guest_send(i)
            if i == 1:
                @pl.when(l == 0)
                def _():
                    gcopy.wait()
                    H[NL + 1] = GP[NL].astype(BF16)

                    @pl.when(s == 1)
                    def _():
                        start_all(y_copies())
            if i == 2:
                @pl.when((l > 0) & (l < NL - 1))
                def _():
                    relay(l + 1, ALL)
            if i == NC - 1:
                @pl.when(l == 0)
                def _():
                    relay(l + 1, ALL)

                @pl.when(l < NL - 1)
                def _():
                    settle(l + 1, FIRST, True)
        return carry
    loop(NL, fwd_layer, 0)

    def y_copies_of(q, n):
        src, dst, got = H.at[NL, :n], y.at[q // CORES, c, :n], yr.at[q]
        return lcopy(src, dst, ys.at[0]), rcopy(src, dst, ys.at[1], got, pp=sib), rcopy(src, dst, ys.at[2], got, pp=oy + c)

    def y_pass(q, n):
        part = y.at[q // CORES, c, :n]
        return rcopy(part, part, ys.at[3], yr.at[q], pp=sib)

    def y_arrived(q, n):
        part = y.at[q // CORES, q % CORES, :n]
        rcopy(part, part, ys.at[1], yr.at[q], pp=sib).wait_recv()

    def each_row(do):
        for row, n, other in ((0, S, HOME * C), (1, HOME * C, S)):
            @pl.when(ys_ == row)
            def _():
                do(row, n, other)

    def ri(l):
        return jnp.where(l == NL - 1, NL + 1, l + 1)

    def pass_of(lb):
        return NL + lb + (1 - ys_) * jnp.minimum(lb, 1)

    def bwd_layer(lb, carry):
        l = NL - 1 - lb
        p = pass_of(lb)
        before = pass_of(lb - 1)
        for n in range(NC):
            i = NC - 1 - n

            ar_wait(before, l + 1, i, lb)

            def handle(op, lag, u):
                m = n - lag

                def go(q, lq, j):
                    if op == 'mid':
                        ar_mid(q, j, u, True)
                    else:
                        ar_last(q, ri(lq), lq, j, u, True)
                if m >= 0:
                    @pl.when(l > 0)
                    def _():
                        go(p, l, NC - 1 - m)
                else:
                    @pl.when(lb > 0)
                    def _():
                        go(before, l + 1, -1 - m)

                    @pl.when(lb == NL * ys_)
                    def _():
                        if op == 'mid':
                            ar_mid(NL - 1, m + NC, u)
                        else:
                            ar_last(NL - 1, NL - 1, NL, m + NC, u)

            def guests(layer, what, j):
                @pl.when(lb == layer + NL * ys_)
                def _():
                    what(j)

            def after(k):
                if k == 0 and i >= HOME:
                    guests(1, guest_in, i)
                if k == 1 and NC > i + 1 >= HOME:
                    guests(1, guest_last, i + 1)
                if k == NC and i >= HOME:
                    guests(1, guest_mid, i)
                if k == 0 and n == 0:
                    @pl.when(lb > 0)
                    def _():
                        grads_mid(l + 1, ATT)
                        for a in ALL:
                            g1_copy(l + 1, a).wait_send()
                if n == NC - 1 and k < 2:
                    g1_copy(l, MLP[1 - k]).start()
                if n == NC - 1 and k in (3, 4):
                    @pl.when(l == 0)
                    def _():
                        grads_mid(l, (MLP[4 - k],))
            run(backward(l, ri(l), i, False), BWD_AT, handle, after)

            if i >= HOME:
                @pl.when(lb == 2 + NL * ys_)
                def _():
                    guest_back(i)

            @pl.when(l > 0)
            def _():
                ar_send(p, i, True)
            if n == NC - 1:
                @pl.when(lb == 2 + NL * ys_)
                def _():
                    guest_out(lambda *copies: start_all(copies))
            if n == 1:
                @pl.when(lb > 0)
                def _():
                    vec_mid(l + 1)
            if n == 2:
                @pl.when(lb == 0)
                def _():
                    def out(row, n, other):
                        for j in range(n // C):
                            ar_wait(NL - 1, NL, j)
                        start_all(y_copies_of(CORES * row + c, n))
                    each_row(out)

                @pl.when(lb > 1)
                def _():
                    grads_last(l + 2)

        for a in ATT:
            g1_copy(l, a).start()
        start_all(v1_copies(l))

        @pl.when(l > 0)
        def _():
            grads_mid(l, MLP)
        return carry
    loop(NL, bwd_layer, 0)

    grads_mid(0, ATT)

    def pass_on(row, n, other):
        y_arrived(CORES * (1 - row) + c, other)
        y_pass(CORES * (1 - row) + c, other).start()
        if row:
            guest_home(c).wait_recv()
            guest_home(c).start()
    each_row(pass_on)
    grads_last(1)
    vec_mid(0)
    grads_last(0)

    for o in range(1, NL):
        q = (s + o) % NL
        rcopy(GZ.at[0], PR.at[q], v2s.at[0], v2r.at[q], pp=q).wait_recv()
    PRE[:8, :D] = sum(PR[k] for k in range(NL))
    vout = lcopy(PRE.at[:8, :D], ovec, osem.at[0])
    vout.start()
    for l in range(NL):
        for cp in v1_copies(l):
            cp.wait_send()
    for l in range(NL):
        @pl.when(l != s)
        def _():
            v2_copy(l).wait_send()
    for a in range(NA):
        rcopy(G_OUT[a].at[g_half(a, 1 - c)], G_OUT[a].at[g_half(a, 1 - c)], g3s.at[a], g3r.at[a], pp=sib).wait_recv()

    def out_done(local, *sent):
        local.wait()
        for cp in sent:
            cp.wait_send()

    def all_out(row, n, other):
        out_done(*y_copies_of(CORES * row + c, n))
        y_pass(CORES * (1 - row) + c, other).wait_send()
        y_arrived(CORES * row + 1 - c, n)
        y_arrived(CORES * (1 - row) + 1 - c, other)
        guest_home(1 - c).wait_recv()
    each_row(all_out)

    @pl.when(ys_ == 0)
    def _():
        guest_out(out_done)

        @pl.when(is_end)
        def _():
            for t in range(HOME * SUB, NC * SUB):
                guest_to_hub(t).wait_send()

        @pl.when(inner)
        def _():
            for t in range(HOME * SUB, NC * SUB):
                guest_to_leaf(t).wait_send()

    @pl.when(ys_ == 1)
    def _():
        guest_home(c).wait_send()
        for i in range(HOME, NC):
            guest_copy(i).wait_send()
    for a in range(NA):
        g1_copy(0, a).wait_send()
    for l in range(NL):
        grads_sent(l)
    for cp in sib_copies():
        cp.wait_send()
    @pl.when(s == 0)
    def _():
        for cp in first_copies():
            cp.wait_send()

    @pl.when(s > 0)
    def _():
        for cp in y_copies():
            cp.wait_send()
    for a in ALL:
        pass_copy(oy + 1, a, c).wait_send()

        @pl.when(ys_ == 0)
        def _():
            pass_copy(oy, a, c).wait_send()

        @pl.when(ys_ == 1)
        def _():
            for hop in range(CORES):
                for cp in hop_copies(a, hop):
                    cp.wait_send()

    @pl.when(is_end)
    def _():
        for t in range(NC * SUB):
            end_copy(0, t).wait_send()

    @pl.when(inner)
    def _():
        for t in range(NC * SUB):
            peer_copy(0, t).wait_send()
            back_copy(0, 1, t).wait_send()
    vout.wait()


def finish(y, gq, go, gu, gd, gv, yo, qo, oo, uo, do, n0, n1, n2, n3, n4, n5, n6, bq,
           yb, qb, ob, ub, db, vb, r0, r1, r2, r3, r4, r5, r6, rq, got, put, small):
    trips = [(gd, db, do), (gu, ub, uo), (go, ob, oo), (gq, qb, qo)]
    trips += [tuple(ref.at[m, r] for ref in (y, yb, yo)) for m in range(y.shape[0]) for r in range(y.shape[1])]
    loads = [pltpu.make_async_copy(a, b, got.at[k]) for k, (a, b, o) in enumerate(trips)]
    stores = [pltpu.make_async_copy(b, o, put.at[k]) for k, (a, b, o) in enumerate(trips)]
    vecs = pltpu.make_async_copy(gv, vb, small.at[len(trips)])
    vecs.start()
    for cp in loads:
        cp.start()
    vecs.wait()
    for row, refs in enumerate(((r0,), (r1,), (r2,), (r3,), (r4, r5), (r6,))):
        for ref in refs:
            ref[...] = vb[row:row + 1, :]
    e = rq.shape[2]
    for k in range(3):
        for h in range(CORES):
            rq[k, h:h + 1, :] = vb[6:7, (CORES * k + h) * e:(CORES * k + h + 1) * e]
    tiny = [pltpu.make_async_copy(a, b, small.at[k]) for k, (a, b) in enumerate(((r0, n0), (r1, n1), (r2, n2), (r3, n3), (r4, n4), (r5, n5), (r6, n6), (rq, bq)))]
    for cp in tiny:
        cp.start()
    for cp, out in zip(loads, stores):
        cp.wait()
        out.start()
    for cp in tiny + stores:
        cp.wait()


def finish_step(y, gq, go, gu, gd, gv, e):
    hbm = pl.BlockSpec(memory_space=pl.ANY)
    row = jax.ShapeDtypeStruct((1, gv.shape[1]), F32)
    outs = [jax.ShapeDtypeStruct(a.shape, a.dtype) for a in (y, gq, go, gu, gd)] + [row] * 7 + [jax.ShapeDtypeStruct((3, CORES, e), F32)]
    bufs = outs[:5] + [gv] + outs[5:]
    return pl.pallas_call(
        finish,
        out_shape=outs,
        in_specs=[hbm] * 6,
        out_specs=[hbm] * len(outs),
        scratch_shapes=[pltpu.VMEM(a.shape, a.dtype) for a in bufs] + [pltpu.SemaphoreType.DMA((9,))] * 3,
        name='neox_out',
    )(y, gq, go, gu, gd, gv)


def group_step(dims, *args):
    x = args[0]
    S, D, E, C, F = dims
    E2 = 2 * E
    hbm = pl.BlockSpec(memory_space=pl.ANY)
    out_shape = [
        jax.ShapeDtypeStruct(x.shape, BF16),
        jax.ShapeDtypeStruct((3 * E2, D), F32),
        jax.ShapeDtypeStruct((E2, D), F32),
        jax.ShapeDtypeStruct((D, F), F32),
        jax.ShapeDtypeStruct((F, D), F32),
        jax.ShapeDtypeStruct((8, D), F32),
    ]

    def vm(*shape, dtype=BF16):
        return pltpu.VMEM(shape, dtype)
    dma = pltpu.SemaphoreType.DMA
    scratch = [
        vm(NL, 3 * E2, D), vm(NL, E2, D), vm(NL, D, F), vm(NL, F, D), vm(NL, 8, D, dtype=F32),
        vm(NL + 2, S, D),
        vm(NL, S, E2), vm(NL, S, E2), vm(NL, S, E2), vm(NL, E2, S), vm(E2, S), vm(NL, S, E2),
        *[vm(NL, 2, (i + 1) * C, C) for i in range(NC)],
        vm(NL, S, F), vm(NL + 1, S, F, dtype=F32),
        vm(CORES, S, D), vm(CORES, S, D), vm(S, D), vm(S + C, D, dtype=F32),
        *[vm(CORES, *k, dtype=F32) for k in ((3 * E2, D), (E2, D), (D, F), (F, D))],
        *[vm(CORES, *k) for k in ((3 * E, D), (E, D), (D // CORES, F), (F // CORES, D))],
        vm(S, E2, dtype=F32), vm(S, E2, dtype=F32),
        vm(CORES, C + 8, E2, dtype=F32),
        *[vm(*k, 8, D, dtype=F32) for k in ((NL,), (NL, NT), (NL,), (NL,))],
        vm(C, D), vm(C, D), vm(C, max(D, F), dtype=F32), vm(C, F), vm(S, C), vm(S, C, dtype=F32),
        *[vm(1, D, dtype=F32)] * 4, vm(1, D), vm(1, D), vm(1, F), vm(3, CORES, E), vm(S, D),
        dma((NA,)), dma((NA + 1,)), dma((CORES, NA + 1)), dma((NL, 2 * NA + 1)), dma((CORES, NA)), dma((3, NA)), dma((NA, 4)), dma((CORES,)), dma((1,)),
        dma((NC * SUB,)), dma((NC * SUB,)), dma((CORES, NC * SUB)), dma((CORES, NC * SUB)), dma((CORES, NC * SUB)),
        dma((NL,)), dma((NL,)), dma((NA,)), dma((CORES, NA)), dma((CORES, NA)), dma((CORES, NA)), dma((CORES, NA)), dma((NA,)),
        dma((NL, NT - 1)), dma((NL, NT)), dma((NL,)), dma((NL,)), dma((1,)), dma((8,)),
        dma((NC,)), dma((NC,)), dma((NC * SUB,)), dma((NC * SUB,)), dma((3,)), dma((CORES,)),
    ]
    return pl.pallas_call(
        functools.partial(body, dims),
        out_shape=out_shape,
        in_specs=[hbm] * len(args),
        out_specs=[hbm] * 6,
        scratch_shapes=scratch,
        compiler_params=pltpu.CompilerParams(collective_id=0, has_side_effects=True, vmem_limit_bytes=67043328),
        name='neox_group',
    )(*args)


def solution(mesh):
    def device_fn(x_in, g_out, ln1_gain, ln1_bias, w_qkv, b_qkv, w_out, b_out, ln2_gain, ln2_bias, w_up, b_up, w_down, b_down):
        n_micro, n_rows, S, D = x_in.shape
        heads, E = w_qkv.shape[2], w_qkv.shape[4]
        F = w_up.shape[2]
        C = S // NC
        wqkv = jnp.transpose(w_qkv[0], (1, 2, 3, 0)).reshape(heads * 3 * E, D)
        bqkv = jnp.transpose(b_qkv[0], (1, 0, 2))
        tab = jnp.asarray(rotary_base(C, NC, E, heads))
        part = group_step((S, D, E, C, F), x_in, g_out, wqkv, w_out[0].reshape(heads * E, D), w_up[0], w_down[0], ln1_gain, ln1_bias, ln2_gain, ln2_bias, b_out, b_down, b_up, bqkv, tab)
        y, gq, go, gup, gdn, n1g, n1b, n2g, n2b, gbo, gbd, gbu, gbq = finish_step(*part, E)
        gq = jnp.transpose(gq.reshape(heads, 3, E, D), (3, 0, 1, 2))[None]
        gbq = jnp.transpose(gbq, (1, 0, 2))[None]
        return (y, n1g, n1b, gq, gbq, go.reshape(1, heads, E, D), gbo, n2g, n2b, gup[None], gbu, gdn[None], gbd)

    return jax.shard_map(device_fn, mesh=mesh, in_specs=(P('dp'), P('dp')) + STAGE_SPECS, out_specs=(P('dp'),) + GRAD_SPECS, check_vma=False)
```

```python
import functools
import math

import jax
import jax.numpy as jnp
import numpy as np
from jax import lax
from jax.experimental import pallas as pl
from jax.experimental.pallas import tpu as pltpu
from jax.sharding import PartitionSpec as P

ROPE_BASE = 10000.0
LN_EPS = 1e-5
STAGE_SPECS = (P('pp'), P('pp'), P('pp', None, 'tp'), P('pp', 'tp'), P('pp', 'tp'), P('pp'), P('pp'), P('pp'), P('pp', None, 'tp'), P('pp', 'tp'), P('pp', 'tp'), P('pp'))
OWN = ('dp', 'pp')
GRAD_SPECS = (P(OWN), P(OWN), P(OWN, None, 'tp'), P(OWN, 'tp'), P(OWN, 'tp'), P(OWN), P(OWN), P(OWN), P(OWN, None, 'tp'), P(OWN, 'tp'), P(OWN, 'tp'), P(OWN))


F32 = jnp.float32
BF16 = jnp.bfloat16
NL = 4
NT = 4
NC = 4
NA = 4
CORES = 2
SUB = 4
FWD_AT = {k: (('mid', 1, k), ('last', 2, k)) for k in range(SUB)}
BWD_AT = {k: (('last', 2, k),) * (k < SUB) + (('mid', 1, k - 1),) * (k > 0) for k in range(SUB + 1)}
LOG2E = 1.4426950408889634
RSQRT2 = 0.7071067811865476
INV_SQRT_2PI = 0.3989422804014327


def nn(a, b):
    return lax.dot_general(a, b, (((1,), (0,)), ((), ())), preferred_element_type=F32)


def nt(a, b):
    return lax.dot_general(a, b, (((1,), (1,)), ((), ())), preferred_element_type=F32)


def tn(a, b):
    return lax.dot_general(a, b, (((0,), (0,)), ((), ())), preferred_element_type=F32)


def loop(n, step, init, unroll=False):
    return lax.fori_loop(0, n, step, init, unroll=unroll)


def col_sum(v):
    return jnp.sum(v, axis=0, keepdims=True)


def row_mean(v):
    return jnp.mean(v, axis=-1, keepdims=True)


def fold(v):
    return jnp.sum(v.reshape(v.shape[0] // 8, 8, v.shape[1]), axis=0)


def rotary_base(chunk, n_chunks, head_dim, n_heads):
    rot_dim = head_dim // 4
    half = rot_dim // CORES
    inv_freq = np.zeros((head_dim,), np.float64)
    inv_freq[:rot_dim] = np.tile(ROPE_BASE ** (-(np.arange(half) * 2.0) / rot_dim), 2)
    inv_freq = np.tile(inv_freq, n_heads)
    pos = np.concatenate([np.arange(chunk), np.arange(8) * (np.arange(8) < n_chunks) * chunk]).astype(np.float64)
    ang = pos[:, None] * inv_freq[None, :]
    return np.stack([np.cos(ang), np.sin(ang)]).astype(np.float32)


def body(dims, x, g, wqkv, wo, wup, wdn, n0, n1, n2, n3, n4, n5, n6, bq, tab,
         y, oqkv, oo, oup, odn, ovec,
         WQ, WO, WU, WD, VEC, H, Q, K, V, KT, VT, CTX, P0, P1, P2, P3, HID, GP, RA, RB, PS, PF,
         GQ, GO, GU, GD, R2Q, R2O, R2U, R2D, DK, DV, TAB, GV, ZR, GZ, PR,
         AS, MS, PRE, DPB, DS, ST, N0, N1, N2, N3, N4, N5, N6, BQ, GX,
         wl, ws, wy, wr, wf, w0s, w0r, xs, gs, sab, sc, ra_s, rb_s, rc_s, ys, yr, g1s, g1r, g2s, g2r, g3s, g3r, v1s, v1r, v2s, v2r, osem, ns, gxs, gxr, gs2, gs3, ygs, ygr):
    S, D, E, C, F = dims
    E2 = 2 * E
    SR = C // SUB
    z = lax.axis_index('tp')
    xg = lax.axis_index('dp')
    s = lax.axis_index('pp')
    ys_ = s // CORES
    c = s % CORES
    sib = s + 1 - 2 * c
    oy = 2 * (1 - ys_)
    is_end = z * (NT - 1 - z) == 0
    inner = z * (NT - 1 - z) > 0
    edge = 1 - jnp.minimum(z * (NT - 1 - z), 1)
    hub = 1 + z // 3
    leaf = jnp.where(z == 1, 0, 3)
    peer = 3 - z
    PX = (P0, P1, P2, P3)
    W_IN = (wqkv, wo, wup, wdn)
    W_BUF = (WQ, WO, WU, WD)
    G_HALF = (3 * E, E, D // CORES, F // CORES)
    ALL = tuple(range(NA))
    FIRST, REST = ALL[:1], ALL[1:]
    ATT, MLP = ALL[:2], ALL[2:]
    G_BUF = (GQ, GO, GU, GD)
    G_OUT = (oqkv, oo, oup, odn)
    G_COLS = (D, D, F, D)
    R1_OFF = tuple(sum(G_HALF[:k]) for k in range(NA))
    R2 = (R2Q, R2O, R2U, R2D)

    def rcopy(src, dst, ss, rs, **dev):
        return pltpu.make_async_remote_copy(src_ref=src, dst_ref=dst, send_sem=ss, recv_sem=rs, device_id=dev, device_id_type=pl.DeviceIdType.MESH)

    def lcopy(src, dst, sem):
        return pltpu.make_async_copy(src, dst, sem)

    def rows(start, n):
        return pl.ds(pl.multiple_of(start, n), n)

    xcopy = lcopy(x.at[ys_, c], H.at[0], xs.at[0])
    xcopy.start()
    gcopy = lcopy(g.at[ys_, c], GP.at[NL], gs.at[0])
    gcopy.start()
    tcopy = lcopy(tab, TAB, xs.at[1])
    tcopy.start()
    for a in range(NA):
        lcopy(W_IN[a], W_BUF[a].at[s], wl.at[a]).start()
    small = [lcopy(a, b, ns.at[k]) for k, (a, b) in enumerate(((n0, N0), (n1, N1), (n2, N2), (n3, N3), (n4, N4), (n5, N5), (n6, N6), (bq, BQ)))]
    for cp in small:
        cp.start()

    bar = pltpu.get_barrier_semaphore()
    for o in range(1, NT):
        pl.semaphore_signal(bar, inc=1, device_id={'tp': (z + o) % NT}, device_id_type=pl.DeviceIdType.MESH)
    for o in range(1, NL):
        pl.semaphore_signal(bar, inc=1, device_id={'pp': (s + o) % NL}, device_id_type=pl.DeviceIdType.MESH)
    pl.semaphore_signal(bar, inc=1, device_id={'dp': 1 - xg}, device_id_type=pl.DeviceIdType.MESH)
    pl.semaphore_wait(bar, NT + NL - 1)

    def half(ref, a, k):
        return ref.at[rows(k * G_HALF[a], G_HALF[a])]

    def sib_copies():
        out = [rcopy(W_IN[a], W_BUF[a].at[s], ws.at[a], wr.at[s, 2 * a], pp=sib) for a in ALL]
        return out + [rcopy(VEC.at[s], VEC.at[s], ws.at[NA], wr.at[s, 2 * NA], pp=sib)]

    def y_copies():
        out = [rcopy(half(W_IN[a], a, k), half(W_BUF[a].at[s], a, k), wy.at[k, a], wr.at[s, 2 * a + k], pp=oy + k) for a in ALL for k in range(CORES)]
        return out[:2] + [rcopy(VEC.at[s], VEC.at[s], wy.at[k, NA], wr.at[s, 2 * NA], pp=oy + k) for k in range(CORES)] + out[2:]

    def quarter(ref, a, q):
        return ref.at[rows(q * (G_HALF[a] // CORES), G_HALF[a] // CORES)]

    def first_copies():
        out = []
        for a in ALL:
            for k in range(CORES):
                q = 2 * xg + k
                out.append(rcopy(quarter(W_IN[a], a, q), quarter(W_BUF[a].at[0], a, q), wy.at[k, a], w0r.at[a, q], pp=oy + k))
        return out + [rcopy(VEC.at[s], VEC.at[s], wy.at[k, NA], wr.at[s, 2 * NA], pp=oy + k) for k in range(CORES)]

    def mine(hop):
        return 2 * (xg if hop == 0 else 1 - xg) + c

    def hop_copies(a, hop):
        part, sem = quarter(W_BUF[a].at[0], a, mine(hop)), w0r.at[a, mine(hop)]
        out = [rcopy(part, part, w0s.at[hop, a], sem, pp=sib)]
        return out if hop else out + [rcopy(part, part, w0s.at[2, a], sem, dp=1 - xg)]

    def hop_on(a, hop):
        copies = hop_copies(a, hop)
        copies[0].wait_recv()
        start_all(copies)

    def hop_end(a):
        for k in range(CORES):
            part = quarter(W_BUF[a].at[0], a, 2 * k + 1 - c)
            rcopy(part, part, w0s.at[0, a], w0r.at[a, 2 * k + 1 - c], pp=sib).wait_recv()

    def start_all(copies):
        for cp in copies:
            cp.start()

    for cp in small:
        cp.wait()
    for k, ref in enumerate((N0, N1, N2, N3, N4, N5, N6)):
        VEC[s, k:k + 1, :] = ref[...].astype(F32)
    VEC[s, 7:8, :3 * E2] = jnp.concatenate([BQ[k, h:h + 1, :].astype(F32) for k in range(3) for h in range(CORES)], axis=1)

    @pl.when(s == 0)
    def _():
        start_all(first_copies())

    @pl.when(s > 1)
    def _():
        start_all(y_copies())
    start_all(sib_copies())

    def pass_copy(l, a, k):
        part = half(W_BUF[a].at[l], a, k)
        return rcopy(part, part, wf.at[l % CORES, a], wr.at[l, 2 * a + k], pp=sib)

    def relay(l, arrays):
        @pl.when(l // CORES != ys_)
        def _():
            for a in arrays:
                pass_copy(l, a, c).wait_recv()
                pass_copy(l, a, c).start()

    def settle(l, arrays, small):
        @pl.when(l == s)
        def _():
            for a in arrays:
                lcopy(W_IN[a], W_BUF[a].at[s], wl.at[a]).wait()

        @pl.when(l == sib)
        def _():
            for a in arrays:
                rcopy(W_IN[a], W_BUF[a].at[l], ws.at[a], wr.at[l, 2 * a], pp=sib).wait_recv()

        @pl.when((l // CORES != ys_) & (l > 0))
        def _():
            for a in arrays:
                pass_copy(l, a, 1 - c).wait_recv()
        if small:
            @pl.when(l != s)
            def _():
                rcopy(VEC.at[l], VEC.at[l], ws.at[NA], wr.at[l, 2 * NA], pp=sib).wait_recv()

    tcopy.wait()

    lane = lax.broadcasted_iota(jnp.int32, (C, E2), 1)
    head_lane = lane // E
    in_head = lane % E
    rot_half = E // 8
    low = in_head < rot_half
    sub_head = lax.broadcasted_iota(jnp.int32, (E2, C), 0) // E
    lower = lax.broadcasted_iota(jnp.int32, (C, C), 0) <= lax.broadcasted_iota(jnp.int32, (C, C), 1)
    c1 = E ** -0.5 * LOG2E

    def tabs(i):
        (cb, sb), (cr, sr) = ([TAB[k, r, :] for k in range(CORES)] for r in (slice(C), slice(C + i, C + i + 1)))
        cs, sn = cb * cr - sb * sr, sb * cr + cb * sr
        return cs, jnp.where(low, -sn, 0.0), jnp.where(low, 0.0, sn)

    def rotate(v, t):
        cs, sa, sb = t
        return v * cs + pltpu.roll(v, E2 - rot_half, 1) * sa + pltpu.roll(v, rot_half, 1) * sb

    def unrotate(v, t):
        cs, sa, sb = t
        return v * cs + pltpu.roll(v * sa, rot_half, 1) + pltpu.roll(v * sb, E2 - rot_half, 1)

    def end_copy(p, t):
        return rcopy(PS.at[t * SR:(t + 1) * SR], RA.at[p % CORES, t * SR:(t + 1) * SR], sab.at[t], ra_s.at[p % CORES, t], tp=hub)

    def peer_copy(p, t):
        return rcopy(PS.at[t * SR:(t + 1) * SR], RB.at[p % CORES, t * SR:(t + 1) * SR], sab.at[t], rb_s.at[p % CORES, t], tp=peer)

    def back_copy(p, di, t):
        return rcopy(H.at[di, t * SR:(t + 1) * SR], H.at[di, t * SR:(t + 1) * SR], sc.at[t], rc_s.at[p % CORES, t], tp=leaf)

    def pf_row(i, back):
        return (NC if back and i == NC - 1 else i) * C

    def ar_send(p, i, back=False):
        @pl.when(is_end)
        def _():
            for t in range(i * SUB, (i + 1) * SUB):
                @pl.when(p > 0)
                def _():
                    end_copy(p, t).wait_send()
                f0 = pf_row(i, back) + (t - i * SUB) * SR
                PS[t * SR:(t + 1) * SR, :] = PF[f0:f0 + SR, :].astype(BF16)
                end_copy(p, t).start()

    def out_bias(l):
        return VEC[l, 4:5, :] + VEC[l, 5:6, :]

    def ar_mid(p, i, u, back=False):
        t = i * SUB + u
        r = slice(t * SR, (t + 1) * SR)
        f0 = pf_row(i, back) + u * SR

        @pl.when(inner)
        def _():
            end_copy(p, t).wait_recv()
            @pl.when(p > 0)
            def _():
                peer_copy(p, t).wait_send()
            PS[r, :] = (PF[f0:f0 + SR, :] + RA[p % CORES, r, :].astype(F32)).astype(BF16)
            peer_copy(p, t).start()

    def ar_last(p, ri, di, i, u, back=False):
        t = i * SUB + u
        r = slice(t * SR, (t + 1) * SR)

        @pl.when(inner)
        def _():
            peer_copy(p, t).wait_recv()
            @pl.when(p > 0)
            def _():
                back_copy(p, di, t).wait_send()
            both = PS[r, :].astype(F32) + RB[p % CORES, r, :].astype(F32)
            own = H[ri, r, :].astype(F32)
            H[di, r, :] = (own + both if back else own + both + out_bias(p)).astype(BF16)
            back_copy(p, di, t).start()

    def ar_wait(p, di, i, on=1):
        @pl.when(on * edge > 0)
        def _():
            for t in range(i * SUB, (i + 1) * SUB):
                back_copy(p, di, t).wait_recv()

    GP1 = NL % 3
    HOME = NC // CORES

    def guest_copy(i):
        part = GX.at[i * C:(i + 1) * C]
        return rcopy(part, part, gxs.at[i], gxr.at[i], pp=c)

    def guest_send(i):
        r = slice(i * C, (i + 1) * C)
        once = jnp.where(z == 1, 1.0, 0.0)
        GX[r, :] = (PF[r, :] + once * (H[NL - 1, r, :].astype(F32) + out_bias(NL - 1))).astype(BF16)
        guest_copy(i).start()

    def guest_hop(t, dst, sem, arrive, to):
        return rcopy(GX.at[t * SR:(t + 1) * SR], dst.at[GP1, t * SR:(t + 1) * SR], sem.at[t], arrive.at[GP1, t], tp=to)

    def guest_to_hub(t):
        return guest_hop(t, RA, gs2, ra_s, hub)

    def guest_to_peer(t):
        return guest_hop(t, RB, gs2, rb_s, peer)

    def guest_to_leaf(t):
        return guest_hop(t, RB, gs3, rc_s, leaf)

    def parts(i):
        return [(t, slice(t * SR, (t + 1) * SR)) for t in range(i * SUB, (i + 1) * SUB)]

    def guest_in(i):
        guest_copy(i).wait_recv()

        @pl.when(is_end)
        def _():
            for t, r in parts(i):
                guest_to_hub(t).start()

    def guest_mid(i):
        @pl.when(inner)
        def _():
            for t, r in parts(i):
                guest_to_hub(t).wait_recv()
                GX[r, :] = (GX[r, :].astype(F32) + RA[GP1, r, :].astype(F32)).astype(BF16)
                guest_to_peer(t).start()

    def guest_last(i):
        @pl.when(inner)
        def _():
            for t, r in parts(i):
                guest_to_peer(t).wait_recv()
                guest_to_peer(t).wait_send()
                GX[r, :] = (GX[r, :].astype(F32) + RB[GP1, r, :].astype(F32)).astype(BF16)
                guest_to_leaf(t).start()

    def guest_back(i):
        @pl.when(is_end)
        def _():
            for t, r in parts(i):
                guest_to_leaf(t).wait_recv()

    def guest_out(act):
        low = slice(HOME * C, S)
        for role, src in ((is_end, RB.at[GP1, low]), (inner, GX.at[low])):
            @pl.when(role)
            def _():
                dst = y.at[1, c, low]
                act(lcopy(src, dst, ygs.at[0]), rcopy(src, dst, ygs.at[1], ygr.at[c], pp=sib), rcopy(src, dst, ygs.at[2], ygr.at[c], pp=s + CORES))

    def guest_home(q):
        return rcopy(y.at[1, q, HOME * C:S], y.at[1, q, HOME * C:S], ygs.at[0], ygr.at[q], pp=sib)

    def stats(hf):
        cen = hf - row_mean(hf)
        rstd = lax.rsqrt(row_mean(cen * cen) + LN_EPS)
        return cen * rstd, rstd

    LB = 32
    GR = 32

    def norms(l, i):
        g1, b1, g2, b2 = (VEC[l, k:k + 1, :] for k in range(NA))

        def step(b, carry):
            hf = H[l, rows(i * C + b * LB, LB), :].astype(F32)
            xhat, unused = stats(hf)
            AS[rows(b * LB, LB), :] = (xhat * g1 + b1).astype(BF16)
            MS[rows(b * LB, LB), :] = (xhat * g2 + b2).astype(BF16)
            return carry
        loop(C // LB, step, 0, unroll=True)

    def by_kind():
        return [(h * 3 + k) * E for k in range(3) for h in range(CORES)]

    def wq(l):
        return jnp.concatenate([WQ[l, r:r + E, :] for r in by_kind()], axis=0)

    def forward(l, i):
        r0, r1 = i * C, (i + 1) * C
        norms(l, i)
        qkv = nt(AS[...], wq(l)) + VEC[l, 7:8, :3 * E2]
        qkv = qkv.astype(BF16).astype(F32)
        t = tabs(i)
        q = rotate(qkv[:, :E2], t).astype(BF16)
        kf = rotate(qkv[:, E2:2 * E2], t)
        vf = qkv[:, 2 * E2:3 * E2]
        Q[l, r0:r1, :] = q
        K[l, r0:r1, :] = kf.astype(BF16)
        V[l, r0:r1, :] = vf.astype(BF16)
        KT[l, :, r0:r1] = jnp.transpose(kf).astype(BF16)
        VT[:, r0:r1] = jnp.transpose(vf).astype(BF16)
        yield

        def far(*hops):
            if i == 0:
                @pl.when((l == 0) & (ys_ == 1))
                def _():
                    for a, hop in hops:
                        hop_on(a, hop)
        far((3, 0))
        RBK = C // CORES
        outs = []
        for h in range(CORES):
            qm = jnp.where(head_lane == h, Q[l, r0:r1, :].astype(F32), 0.0).astype(BF16)
            ST[:r1, :] = nt(K[l, :r1, :], qm)
            ST[r0:r1, :] = jnp.where(lower, ST[r0:r1, :], -1e30)

            def top(b, m):
                return jnp.maximum(m, jnp.max(ST[rows(b * RBK, RBK), :].reshape(RBK // 8, 8, C), axis=0))
            m = jnp.max(loop(r1 // RBK, top, jnp.full((8, C), -3e38, F32), unroll=True), axis=0, keepdims=True)
            mc = m * c1

            def expo(b, tot):
                e = jnp.exp2(ST[rows(b * RBK, RBK), :] * c1 - mc)
                ST[rows(b * RBK, RBK), :] = e
                return tot + fold(e)
            tot = col_sum(loop(r1 // RBK, expo, jnp.zeros((8, C), F32), unroll=True))
            inv = 1.0 / tot

            def put(b, carry):
                PX[i][l, h, rows(b * RBK, RBK), :] = (ST[rows(b * RBK, RBK), :] * inv).astype(BF16)
                return carry
            loop(r1 // RBK, put, 0, unroll=True)
            outs.append(nn(VT[:, :r1], PX[i][l, h]))
            if h == 0:
                yield
        ctx = jnp.transpose(jnp.where(sub_head == 0, outs[0], outs[1])).astype(BF16)
        CTX[l, r0:r1, :] = ctx
        yield
        if i == 0:
            far((2, 1), (3, 1))

            @pl.when((l == 0) & (ys_ == 1))
            def _():
                for a in REST:
                    hop_end(a)
            settle(l, REST, False)
        PF[r0:r1, :] = nn(ctx, WO[l])
        PRE[...] = nn(MS[...], WU[l])
        bup = VEC[l, 6:7, :]
        GB = 32

        def act(b, carry):
            u = PRE[rows(b * GB, GB), :] + bup
            cdf = 0.5 * (1.0 + lax.erf(u * RSQRT2))
            pdf = jnp.exp2(u * u * (-0.5 * LOG2E)) * INV_SQRT_2PI
            HID[l, rows(r0 + b * GB, GB), :] = (u * cdf).astype(BF16)
            GP[l, rows(r0 + b * GB, GB), :] = cdf + u * pdf
            return carry
        loop(C // GB, act, 0, unroll=True)
        PF[r0:r1, :] += nn(HID[l, r0:r1, :], WD[l])
        yield

    def backward(l, dl, i, last):
        r0, r1 = i * C, (i + 1) * C
        par = l % CORES
        first = i == NC - 1

        def acc(ref, val):
            if first:
                ref[par] = val
            else:
                ref[par] += val

        def acc_row(k, val, w=D):
            GV[l, k:k + 1, :w] += val

        norms(l, i)
        dy = H[dl, r0:r1, :]
        acc_row(4, col_sum(dy.astype(F32)))
        PRE[...] = nt(dy, WD[l])
        GB = 32

        def act(b, tot):
            d = PRE[rows(b * GB, GB), :] * GP[l, rows(r0 + b * GB, GB), :]
            DPB[rows(b * GB, GB), :] = d.astype(BF16)
            return tot + fold(d)
        dbu = loop(C // GB, act, jnp.zeros((8, F), F32), unroll=True)
        acc_row(5, col_sum(dbu))
        acc(GD, tn(HID[l, r0:r1, :], dy))
        yield
        acc(GU, tn(MS[...], DPB[...]))
        f0 = pf_row(i, True)
        PF[f0:f0 + C, :] = nt(DPB[...], WU[l])
        yield
        dctx = nt(dy, WO[l]).astype(BF16)
        ctx = CTX[l, r0:r1, :]
        acc(GO, tn(ctx, dy))
        prod = dctx.astype(F32) * ctx.astype(F32)
        q = Q[l, r0:r1, :].astype(F32)
        dcf = dctx.astype(F32)
        RBK = C // CORES
        dqt = []
        for h in range(CORES):
            sel = head_lane == h
            qm = jnp.where(sel, q, 0.0).astype(BF16)
            dcm = jnp.where(sel, dcf, 0.0).astype(BF16)
            dsum = jnp.transpose(jnp.where(sel, prod, 0.0))
            drow = col_sum(dsum)
            ST[:r1, :] = nt(V[l, :r1, :], dcm)

            def sub(b, carry):
                pr = PX[i][l, h, rows(b * RBK, RBK), :].astype(F32)
                DS[rows(b * RBK, RBK), :] = (pr * (ST[rows(b * RBK, RBK), :] - drow)).astype(BF16)
                return carry
            loop(r1 // RBK, sub, 0, unroll=True)
            dk = nn(DS[:r1, :], qm)
            dv = nn(PX[i][l, h], dcm)
            if first and h == 0:
                DK[:r1, :] = dk
                DV[:r1, :] = dv
            else:
                DK[:r1, :] += dk
                DV[:r1, :] += dv
            dqt.append(nn(KT[l, :, :r1], DS[:r1, :]))
            yield
        scale = E ** -0.5
        t = tabs(i)
        dq = unrotate(jnp.transpose(jnp.where(sub_head == 0, dqt[0], dqt[1])) * scale, t)
        dk = unrotate(DK[r0:r1, :] * scale, t)
        dv = DV[r0:r1, :]
        dqkv = jnp.concatenate([dq, dk, dv], axis=1)
        acc_row(6, col_sum(dqkv), 3 * E2)
        dqkv = dqkv.astype(BF16)
        dwq = tn(dqkv, AS[...])
        for k, r in enumerate(by_kind()):
            if first:
                GQ[par, r:r + E, :] = dwq[k * E:(k + 1) * E]
            else:
                GQ[par, r:r + E, :] += dwq[k * E:(k + 1) * E]
        PRE[...] = nn(dqkv, wq(l))
        yield
        g1, g2 = VEC[l, 0:1, :], VEC[l, 2:3, :]

        def lnb(b, tots):
            hf = H[l, rows(r0 + b * LB, LB), :].astype(F32)
            xhat, rstd = stats(hf)
            da = PRE[rows(b * LB, LB), :]
            dm = PF[rows(f0 + b * LB, LB), :]
            dx = da * g1 + dm * g2
            m1 = row_mean(dx)
            m2 = row_mean(dx * xhat)
            if not last:
                PF[rows(f0 + b * LB, LB), :] = rstd * (dx - m1 - xhat * m2)
            terms = (da * xhat, da, dm * xhat, dm)
            return tuple(a + fold(v) for a, v in zip(tots, terms))
        tots = loop(C // LB, lnb, tuple(jnp.zeros((8, D), F32) for _ in range(NA)), unroll=True)
        for k in range(NA):
            acc_row(k, col_sum(tots[k]))
        yield

    def g_half(a, k):
        return rows(k * G_HALF[a], G_HALF[a])

    def r1_view(l, a):
        return GP.at[l + 1, R1_OFF[a]:R1_OFF[a] + G_HALF[a], :G_COLS[a]]

    def g1_copy(l, a):
        return rcopy(G_BUF[a].at[l % CORES, g_half(a, 1 - c)], r1_view(l, a), g1s.at[a], g1r.at[l % CORES, a], pp=sib)

    def g2_copy(l, a):
        return rcopy(HID.at[l, R1_OFF[a]:R1_OFF[a] + G_HALF[a], :G_COLS[a]], R2[a].at[l % CORES], g2s.at[l % CORES, a], g2r.at[l % CORES, a], pp=2 * (l // CORES) + c)

    def g3_local(l, a):
        return lcopy(r1_view(l, a), G_OUT[a].at[g_half(a, c)], g3s.at[l % CORES, a])

    def g3_remote(l, a):
        return rcopy(r1_view(l, a), G_OUT[a].at[g_half(a, c)], g3s.at[l % CORES, a], g3r.at[a], pp=sib)

    def v1_copies(l):
        return [rcopy(GV.at[l], ZR.at[l, z], v1s.at[l, o - 1], v1r.at[l, z], tp=(z + o) % NT) for o in range(1, NT)]

    def grads_mid(l, arrays):
        for a in arrays:
            g1_copy(l, a).wait_recv()
            n = G_HALF[a]

            def add(b, carry):
                rr = rows(R1_OFF[a] + b * GR, GR)
                tot = G_BUF[a][l % CORES, rows(c * n + b * GR, GR), :] + GP[l + 1, rr, :G_COLS[a]]
                GP[l + 1, rr, :G_COLS[a]] = tot
                HID[l, rr, :G_COLS[a]] = tot.astype(BF16)
                return carry
            loop(n // GR, add, 0)

            @pl.when(l // CORES != ys_)
            def _():
                g2_copy(l, a).start()

    def grads_last(l):
        @pl.when(l // CORES == ys_)
        def _():
            for a in MLP[::-1] + ATT:
                g2_copy(l, a).wait_recv()

                def add(b, carry):
                    rr = rows(R1_OFF[a] + b * GR, GR)
                    GP[l + 1, rr, :G_COLS[a]] += R2[a][l % CORES, rows(b * GR, GR), :].astype(F32)
                    return carry
                loop(G_HALF[a] // GR, add, 0)

                @pl.when(l == s)
                def _():
                    g3_local(l, a).start()

                @pl.when(l != s)
                def _():
                    g3_remote(l, a).start()

    def grads_sent(l):
        for a in range(NA):
            @pl.when(l // CORES != ys_)
            def _():
                g2_copy(l, a).wait_send()

            @pl.when(l == s)
            def _():
                g3_local(l, a).wait()

            @pl.when((l // CORES == ys_) & (l != s))
            def _():
                g3_remote(l, a).wait_send()

    def v2_copy(l):
        return rcopy(GZ.at[l], PR.at[s], v2s.at[l], v2r.at[s], pp=l)

    def vec_mid(l):
        ZR[l, z] = GV[l]
        for o in range(1, NT):
            q = (z + o) % NT
            rcopy(GV.at[l], ZR.at[l, q], v1s.at[l, o - 1], v1r.at[l, q], tp=q).wait_recv()
        tot = sum(ZR[l, k] for k in range(NT))
        row = lax.broadcasted_iota(jnp.int32, (8, D), 0)
        GZ[l] = jnp.where(row < 4, tot, GV[l])

        @pl.when(l == s)
        def _():
            PR[s] = GZ[l]

        @pl.when(l != s)
        def _():
            v2_copy(l).start()

    GV[...] = jnp.zeros_like(GV)
    @pl.when(ys_ == 1)
    def _():
        for a, hop in ((0, 0), (1, 0), (0, 1), (2, 0), (1, 1)):
            hop_on(a, hop)
        hop_end(0)
    settle(0, FIRST, True)
    xcopy.wait()

    def run(phases, at, handle, after=lambda k: None):
        for k, unused in enumerate(phases):
            after(k)
            for op, lag, u in at.get(k, ()):
                handle(op, lag, u)

    def fwd_layer(l, carry):
        for i in range(NC):
            ar_wait(l - 1, l, i, l)

            def handle(op, lag, u):
                m = i - lag

                def go(p, j):
                    if op == 'mid':
                        ar_mid(p, j, u)
                    else:
                        ar_last(p, p, p + 1, j, u)
                if m >= HOME:
                    @pl.when(l * ys_ < NL - 1)
                    def _():
                        go(l, m)
                elif m >= 0:
                    go(l, m)
                else:
                    @pl.when(l > 0)
                    def _():
                        go(l - 1, m + NC)
            run(forward(l, i), FWD_AT, handle)

            if i < HOME:
                ar_send(l, i)
            else:
                @pl.when(l * ys_ < NL - 1)
                def _():
                    ar_send(l, i)

                @pl.when(l * ys_ == NL - 1)
                def _():
                    guest_send(i)
            if i == 1:
                @pl.when(l == 0)
                def _():
                    gcopy.wait()
                    H[NL + 1] = GP[NL].astype(BF16)

                    @pl.when(s == 1)
                    def _():
                        start_all(y_copies())
            if i == 2:
                @pl.when((l > 0) & (l < NL - 1))
                def _():
                    relay(l + 1, ALL)
            if i == NC - 1:
                @pl.when(l == 0)
                def _():
                    relay(l + 1, ALL)

                @pl.when(l < NL - 1)
                def _():
                    settle(l + 1, FIRST, True)
        return carry
    loop(NL, fwd_layer, 0)

    def y_copies_of(q, n):
        src, dst, got = H.at[NL, :n], y.at[q // CORES, c, :n], yr.at[q]
        return lcopy(src, dst, ys.at[0]), rcopy(src, dst, ys.at[1], got, pp=sib), rcopy(src, dst, ys.at[2], got, pp=oy + c)

    def y_pass(q, n):
        part = y.at[q // CORES, c, :n]
        return rcopy(part, part, ys.at[3], yr.at[q], pp=sib)

    def y_arrived(q, n):
        part = y.at[q // CORES, q % CORES, :n]
        rcopy(part, part, ys.at[1], yr.at[q], pp=sib).wait_recv()

    def each_row(do):
        for row, n, other in ((0, S, HOME * C), (1, HOME * C, S)):
            @pl.when(ys_ == row)
            def _():
                do(row, n, other)

    def ri(l):
        return jnp.where(l == NL - 1, NL + 1, l + 1)

    def pass_of(lb):
        return NL + lb + (1 - ys_) * jnp.minimum(lb, 1)

    def bwd_layer(lb, carry):
        l = NL - 1 - lb
        p = pass_of(lb)
        before = pass_of(lb - 1)
        for n in range(NC):
            i = NC - 1 - n

            ar_wait(before, l + 1, i, lb)

            def handle(op, lag, u):
                m = n - lag

                def go(q, lq, j):
                    if op == 'mid':
                        ar_mid(q, j, u, True)
                    else:
                        ar_last(q, ri(lq), lq, j, u, True)
                if m >= 0:
                    @pl.when(l > 0)
                    def _():
                        go(p, l, NC - 1 - m)
                else:
                    @pl.when(lb > 0)
                    def _():
                        go(before, l + 1, -1 - m)

                    @pl.when(lb == NL * ys_)
                    def _():
                        if op == 'mid':
                            ar_mid(NL - 1, m + NC, u)
                        else:
                            ar_last(NL - 1, NL - 1, NL, m + NC, u)

            def guests(layer, what, j):
                @pl.when(lb == layer + NL * ys_)
                def _():
                    what(j)

            def after(k):
                if k == 0 and i >= HOME:
                    guests(1, guest_in, i)
                if k == 1 and NC > i + 1 >= HOME:
                    guests(1, guest_last, i + 1)
                if k == NC and i >= HOME:
                    guests(1, guest_mid, i)
                if k == 0 and n == 0:
                    @pl.when(lb > 0)
                    def _():
                        grads_mid(l + 1, ATT)
                        for a in ALL:
                            g1_copy(l + 1, a).wait_send()
                if n == NC - 1 and k < 2:
                    g1_copy(l, MLP[1 - k]).start()
                if n == NC - 1 and k in (3, 4):
                    @pl.when(l < 5 - k)
                    def _():
                        grads_mid(l, (MLP[4 - k],))
            run(backward(l, ri(l), i, False), BWD_AT, handle, after)

            if i >= HOME:
                @pl.when(lb == 2 + NL * ys_)
                def _():
                    guest_back(i)

            @pl.when(l > 0)
            def _():
                ar_send(p, i, True)
            if n == NC - 1:
                @pl.when(lb == 2 + NL * ys_)
                def _():
                    guest_out(lambda *copies: start_all(copies))
            if n == 1:
                @pl.when(lb > 0)
                def _():
                    vec_mid(l + 1)
            if n == 2:
                @pl.when(lb == 0)
                def _():
                    def out(row, n, other):
                        for j in range(n // C):
                            ar_wait(NL - 1, NL, j)
                        start_all(y_copies_of(CORES * row + c, n))
                    each_row(out)

                @pl.when(lb > 1)
                def _():
                    grads_last(l + 2)

        for a in ATT:
            g1_copy(l, a).start()
        start_all(v1_copies(l))

        @pl.when(l > 1)
        def _():
            grads_mid(l, MLP)

        @pl.when(l == 1)
        def _():
            grads_mid(l, MLP[:1])
        return carry
    loop(NL, bwd_layer, 0)

    grads_mid(0, ATT)

    def pass_on(row, n, other):
        y_arrived(CORES * (1 - row) + c, other)
        y_pass(CORES * (1 - row) + c, other).start()
        if row:
            guest_home(c).wait_recv()
            guest_home(c).start()
    each_row(pass_on)
    grads_last(1)
    vec_mid(0)
    grads_last(0)

    for o in range(1, NL):
        q = (s + o) % NL
        rcopy(GZ.at[0], PR.at[q], v2s.at[0], v2r.at[q], pp=q).wait_recv()
    PRE[:8, :D] = sum(PR[k] for k in range(NL))
    vout = lcopy(PRE.at[:8, :D], ovec, osem.at[0])
    vout.start()
    for l in range(NL):
        for cp in v1_copies(l):
            cp.wait_send()
    for l in range(NL):
        @pl.when(l != s)
        def _():
            v2_copy(l).wait_send()
    for a in range(NA):
        rcopy(G_OUT[a].at[g_half(a, 1 - c)], G_OUT[a].at[g_half(a, 1 - c)], g3s.at[a], g3r.at[a], pp=sib).wait_recv()

    def out_done(local, *sent):
        local.wait()
        for cp in sent:
            cp.wait_send()

    def all_out(row, n, other):
        out_done(*y_copies_of(CORES * row + c, n))
        y_pass(CORES * (1 - row) + c, other).wait_send()
        y_arrived(CORES * row + 1 - c, n)
        y_arrived(CORES * (1 - row) + 1 - c, other)
        guest_home(1 - c).wait_recv()
    each_row(all_out)

    @pl.when(ys_ == 0)
    def _():
        guest_out(out_done)

        @pl.when(is_end)
        def _():
            for t in range(HOME * SUB, NC * SUB):
                guest_to_hub(t).wait_send()

        @pl.when(inner)
        def _():
            for t in range(HOME * SUB, NC * SUB):
                guest_to_leaf(t).wait_send()

    @pl.when(ys_ == 1)
    def _():
        guest_home(c).wait_send()
        for i in range(HOME, NC):
            guest_copy(i).wait_send()
    for a in range(NA):
        g1_copy(0, a).wait_send()
    for l in range(NL):
        grads_sent(l)
    for cp in sib_copies():
        cp.wait_send()
    @pl.when(s == 0)
    def _():
        for cp in first_copies():
            cp.wait_send()

    @pl.when(s > 0)
    def _():
        for cp in y_copies():
            cp.wait_send()
    for a in ALL:
        pass_copy(oy + 1, a, c).wait_send()

        @pl.when(ys_ == 0)
        def _():
            pass_copy(oy, a, c).wait_send()

        @pl.when(ys_ == 1)
        def _():
            for hop in range(CORES):
                for cp in hop_copies(a, hop):
                    cp.wait_send()

    @pl.when(is_end)
    def _():
        for t in range(NC * SUB):
            end_copy(0, t).wait_send()

    @pl.when(inner)
    def _():
        for t in range(NC * SUB):
            peer_copy(0, t).wait_send()
            back_copy(0, 1, t).wait_send()
    vout.wait()


def finish(y, gq, go, gu, gd, gv, yo, qo, oo, uo, do, n0, n1, n2, n3, n4, n5, n6, bq,
           yb, qb, ob, ub, db, vb, r0, r1, r2, r3, r4, r5, r6, rq, got, put, small):
    trips = [(gd, db, do), (gu, ub, uo), (go, ob, oo), (gq, qb, qo)]
    trips += [tuple(ref.at[m, r] for ref in (y, yb, yo)) for m in range(y.shape[0]) for r in range(y.shape[1])]
    loads = [pltpu.make_async_copy(a, b, got.at[k]) for k, (a, b, o) in enumerate(trips)]
    stores = [pltpu.make_async_copy(b, o, put.at[k]) for k, (a, b, o) in enumerate(trips)]
    vecs = pltpu.make_async_copy(gv, vb, small.at[len(trips)])
    vecs.start()
    for cp in loads:
        cp.start()
    vecs.wait()
    for row, refs in enumerate(((r0,), (r1,), (r2,), (r3,), (r4, r5), (r6,))):
        for ref in refs:
            ref[...] = vb[row:row + 1, :]
    e = rq.shape[2]
    for k in range(3):
        for h in range(CORES):
            rq[k, h:h + 1, :] = vb[6:7, (CORES * k + h) * e:(CORES * k + h + 1) * e]
    tiny = [pltpu.make_async_copy(a, b, small.at[k]) for k, (a, b) in enumerate(((r0, n0), (r1, n1), (r2, n2), (r3, n3), (r4, n4), (r5, n5), (r6, n6), (rq, bq)))]
    for cp in tiny:
        cp.start()
    for cp, out in zip(loads, stores):
        cp.wait()
        out.start()
    for cp in tiny + stores:
        cp.wait()


def finish_step(y, gq, go, gu, gd, gv, e):
    hbm = pl.BlockSpec(memory_space=pl.ANY)
    row = jax.ShapeDtypeStruct((1, gv.shape[1]), F32)
    outs = [jax.ShapeDtypeStruct(a.shape, a.dtype) for a in (y, gq, go, gu, gd)] + [row] * 7 + [jax.ShapeDtypeStruct((3, CORES, e), F32)]
    bufs = outs[:5] + [gv] + outs[5:]
    return pl.pallas_call(
        finish,
        out_shape=outs,
        in_specs=[hbm] * 6,
        out_specs=[hbm] * len(outs),
        scratch_shapes=[pltpu.VMEM(a.shape, a.dtype) for a in bufs] + [pltpu.SemaphoreType.DMA((9,))] * 3,
        name='neox_out',
    )(y, gq, go, gu, gd, gv)


def group_step(dims, *args):
    x = args[0]
    S, D, E, C, F = dims
    E2 = 2 * E
    hbm = pl.BlockSpec(memory_space=pl.ANY)
    out_shape = [
        jax.ShapeDtypeStruct(x.shape, BF16),
        jax.ShapeDtypeStruct((3 * E2, D), F32),
        jax.ShapeDtypeStruct((E2, D), F32),
        jax.ShapeDtypeStruct((D, F), F32),
        jax.ShapeDtypeStruct((F, D), F32),
        jax.ShapeDtypeStruct((8, D), F32),
    ]

    def vm(*shape, dtype=BF16):
        return pltpu.VMEM(shape, dtype)
    dma = pltpu.SemaphoreType.DMA
    scratch = [
        vm(NL, 3 * E2, D), vm(NL, E2, D), vm(NL, D, F), vm(NL, F, D), vm(NL, 8, D, dtype=F32),
        vm(NL + 2, S, D),
        vm(NL, S, E2), vm(NL, S, E2), vm(NL, S, E2), vm(NL, E2, S), vm(E2, S), vm(NL, S, E2),
        *[vm(NL, 2, (i + 1) * C, C) for i in range(NC)],
        vm(NL, S, F), vm(NL + 1, S, F, dtype=F32),
        vm(CORES, S, D), vm(CORES, S, D), vm(S, D), vm(S + C, D, dtype=F32),
        *[vm(CORES, *k, dtype=F32) for k in ((3 * E2, D), (E2, D), (D, F), (F, D))],
        *[vm(CORES, *k) for k in ((3 * E, D), (E, D), (D // CORES, F), (F // CORES, D))],
        vm(S, E2, dtype=F32), vm(S, E2, dtype=F32),
        vm(CORES, C + 8, E2, dtype=F32),
        *[vm(*k, 8, D, dtype=F32) for k in ((NL,), (NL, NT), (NL,), (NL,))],
        vm(C, D), vm(C, D), vm(C, max(D, F), dtype=F32), vm(C, F), vm(S, C), vm(S, C, dtype=F32),
        *[vm(1, D, dtype=F32)] * 4, vm(1, D), vm(1, D), vm(1, F), vm(3, CORES, E), vm(S, D),
        dma((NA,)), dma((NA + 1,)), dma((CORES, NA + 1)), dma((NL, 2 * NA + 1)), dma((CORES, NA)), dma((3, NA)), dma((NA, 4)), dma((CORES,)), dma((1,)),
        dma((NC * SUB,)), dma((NC * SUB,)), dma((CORES, NC * SUB)), dma((CORES, NC * SUB)), dma((CORES, NC * SUB)),
        dma((NL,)), dma((NL,)), dma((NA,)), dma((CORES, NA)), dma((CORES, NA)), dma((CORES, NA)), dma((CORES, NA)), dma((NA,)),
        dma((NL, NT - 1)), dma((NL, NT)), dma((NL,)), dma((NL,)), dma((1,)), dma((8,)),
        dma((NC,)), dma((NC,)), dma((NC * SUB,)), dma((NC * SUB,)), dma((3,)), dma((CORES,)),
    ]
    return pl.pallas_call(
        functools.partial(body, dims),
        out_shape=out_shape,
        in_specs=[hbm] * len(args),
        out_specs=[hbm] * 6,
        scratch_shapes=scratch,
        compiler_params=pltpu.CompilerParams(collective_id=0, has_side_effects=True, vmem_limit_bytes=67043328),
        name='neox_group',
    )(*args)


def solution(mesh):
    def device_fn(x_in, g_out, ln1_gain, ln1_bias, w_qkv, b_qkv, w_out, b_out, ln2_gain, ln2_bias, w_up, b_up, w_down, b_down):
        n_micro, n_rows, S, D = x_in.shape
        heads, E = w_qkv.shape[2], w_qkv.shape[4]
        F = w_up.shape[2]
        C = S // NC
        wqkv = jnp.transpose(w_qkv[0], (1, 2, 3, 0)).reshape(heads * 3 * E, D)
        bqkv = jnp.transpose(b_qkv[0], (1, 0, 2))
        tab = jnp.asarray(rotary_base(C, NC, E, heads))
        part = group_step((S, D, E, C, F), x_in, g_out, wqkv, w_out[0].reshape(heads * E, D), w_up[0], w_down[0], ln1_gain, ln1_bias, ln2_gain, ln2_bias, b_out, b_down, b_up, bqkv, tab)
        y, gq, go, gup, gdn, n1g, n1b, n2g, n2b, gbo, gbd, gbu, gbq = finish_step(*part, E)
        gq = jnp.transpose(gq.reshape(heads, 3, E, D), (3, 0, 1, 2))[None]
        gbq = jnp.transpose(gbq, (1, 0, 2))[None]
        return (y, n1g, n1b, gq, gbq, go.reshape(1, heads, E, D), gbo, n2g, n2b, gup[None], gbu, gdn[None], gbd)

    return jax.shard_map(device_fn, mesh=mesh, in_specs=(P('dp'), P('dp')) + STAGE_SPECS, out_specs=(P('dp'),) + GRAD_SPECS, check_vma=False)
```

```python
import functools
import math

import jax
import jax.numpy as jnp
import numpy as np
from jax import lax
from jax.experimental import pallas as pl
from jax.experimental.pallas import tpu as pltpu
from jax.sharding import PartitionSpec as P

ROPE_BASE = 10000.0
LN_EPS = 1e-5
STAGE_SPECS = (P('pp'), P('pp'), P('pp', None, 'tp'), P('pp', 'tp'), P('pp', 'tp'), P('pp'), P('pp'), P('pp'), P('pp', None, 'tp'), P('pp', 'tp'), P('pp', 'tp'), P('pp'))
OWN = ('dp', 'pp')
GRAD_SPECS = (P(OWN), P(OWN), P(OWN, None, 'tp'), P(OWN, 'tp'), P(OWN, 'tp'), P(OWN), P(OWN), P(OWN), P(OWN, None, 'tp'), P(OWN, 'tp'), P(OWN, 'tp'), P(OWN))


F32 = jnp.float32
BF16 = jnp.bfloat16
NL = 4
NT = 4
NC = 4
NA = 4
CORES = 2
SUB = 4
FWD_AT = {k: (('mid', 1, k // 2), ('last', 2, k // 2)) for k in (0, 2)}
BWD_AT = {k: (('last', 2, k),) * (k < SUB) + (('mid', 1, k - 1),) * (k > 0) for k in range(SUB + 1)}
LOG2E = 1.4426950408889634
RSQRT2 = 0.7071067811865476
INV_SQRT_2PI = 0.3989422804014327


def nn(a, b):
    return lax.dot_general(a, b, (((1,), (0,)), ((), ())), preferred_element_type=F32)


def nt(a, b):
    return lax.dot_general(a, b, (((1,), (1,)), ((), ())), preferred_element_type=F32)


def tn(a, b):
    return lax.dot_general(a, b, (((0,), (0,)), ((), ())), preferred_element_type=F32)


def loop(n, step, init, unroll=False):
    return lax.fori_loop(0, n, step, init, unroll=unroll)


def col_sum(v):
    return jnp.sum(v, axis=0, keepdims=True)


def row_mean(v):
    return jnp.mean(v, axis=-1, keepdims=True)


def fold(v):
    return jnp.sum(v.reshape(v.shape[0] // 8, 8, v.shape[1]), axis=0)


def rotary_base(chunk, n_chunks, head_dim, n_heads):
    rot_dim = head_dim // 4
    half = rot_dim // CORES
    inv_freq = np.zeros((head_dim,), np.float64)
    inv_freq[:rot_dim] = np.tile(ROPE_BASE ** (-(np.arange(half) * 2.0) / rot_dim), 2)
    inv_freq = np.tile(inv_freq, n_heads)
    pos = np.concatenate([np.arange(chunk), np.arange(8) * (np.arange(8) < n_chunks) * chunk]).astype(np.float64)
    ang = pos[:, None] * inv_freq[None, :]
    return np.stack([np.cos(ang), np.sin(ang)]).astype(np.float32)


def body(dims, x, g, wqkv, wo, wup, wdn, n0, n1, n2, n3, n4, n5, n6, bq, tab,
         y, oqkv, oo, oup, odn, ovec,
         WQ, WO, WU, WD, VEC, H, Q, K, V, KT, VT, CTX, P0, P1, P2, P3, HID, GP, RA, RB, PS, PF,
         GQ, GO, GU, GD, R2Q, R2O, R2U, R2D, DK, DV, TAB, GV, ZR, GZ, PR,
         AS, MS, PRE, DPB, DS, ST, N0, N1, N2, N3, N4, N5, N6, BQ, GX,
         fab, fc, fa_s, fb_s, fc_s, wl, ws, wy, wr, wf, w0s, w0r, xs, gs, sab, sc, ra_s, rb_s, rc_s, ys, yr, g1s, g1r, g2s, g2r, g3s, g3r, v1s, v1r, v2s, v2r, osem, ns, gxs, gxr, gs2, gs3, ygs, ygr):
    S, D, E, C, F = dims
    E2 = 2 * E
    SR = C // SUB
    z = lax.axis_index('tp')
    xg = lax.axis_index('dp')
    s = lax.axis_index('pp')
    ys_ = s // CORES
    c = s % CORES
    sib = s + 1 - 2 * c
    oy = 2 * (1 - ys_)
    is_end = z * (NT - 1 - z) == 0
    inner = z * (NT - 1 - z) > 0
    edge = 1 - jnp.minimum(z * (NT - 1 - z), 1)
    hub = 1 + z // 3
    leaf = jnp.where(z == 1, 0, 3)
    peer = 3 - z
    PX = (P0, P1, P2, P3)
    W_IN = (wqkv, wo, wup, wdn)
    W_BUF = (WQ, WO, WU, WD)
    G_HALF = (3 * E, E, D // CORES, F // CORES)
    ALL = tuple(range(NA))
    FIRST, REST = ALL[:1], ALL[1:]
    ATT, MLP = ALL[:2], ALL[2:]
    G_BUF = (GQ, GO, GU, GD)
    G_OUT = (oqkv, oo, oup, odn)
    G_COLS = (D, D, F, D)
    R1_OFF = tuple(sum(G_HALF[:k]) for k in range(NA))
    R2 = (R2Q, R2O, R2U, R2D)

    def rcopy(src, dst, ss, rs, **dev):
        return pltpu.make_async_remote_copy(src_ref=src, dst_ref=dst, send_sem=ss, recv_sem=rs, device_id=dev, device_id_type=pl.DeviceIdType.MESH)

    def lcopy(src, dst, sem):
        return pltpu.make_async_copy(src, dst, sem)

    def rows(start, n):
        return pl.ds(pl.multiple_of(start, n), n)

    xcopy = lcopy(x.at[ys_, c], H.at[0], xs.at[0])
    xcopy.start()
    gcopy = lcopy(g.at[ys_, c], GP.at[NL], gs.at[0])
    gcopy.start()
    tcopy = lcopy(tab, TAB, xs.at[1])
    tcopy.start()
    for a in range(NA):
        lcopy(W_IN[a], W_BUF[a].at[s], wl.at[a]).start()
    small = [lcopy(a, b, ns.at[k]) for k, (a, b) in enumerate(((n0, N0), (n1, N1), (n2, N2), (n3, N3), (n4, N4), (n5, N5), (n6, N6), (bq, BQ)))]
    for cp in small:
        cp.start()

    bar = pltpu.get_barrier_semaphore()
    for o in range(1, NT):
        pl.semaphore_signal(bar, inc=1, device_id={'tp': (z + o) % NT}, device_id_type=pl.DeviceIdType.MESH)
    for o in range(1, NL):
        pl.semaphore_signal(bar, inc=1, device_id={'pp': (s + o) % NL}, device_id_type=pl.DeviceIdType.MESH)
    pl.semaphore_signal(bar, inc=1, device_id={'dp': 1 - xg}, device_id_type=pl.DeviceIdType.MESH)
    pl.semaphore_wait(bar, NT + NL - 1)

    def half(ref, a, k):
        return ref.at[rows(k * G_HALF[a], G_HALF[a])]

    def sib_copies():
        out = [rcopy(W_IN[a], W_BUF[a].at[s], ws.at[a], wr.at[s, 2 * a], pp=sib) for a in ALL]
        return out + [rcopy(VEC.at[s], VEC.at[s], ws.at[NA], wr.at[s, 2 * NA], pp=sib)]

    def y_copies():
        out = [rcopy(half(W_IN[a], a, k), half(W_BUF[a].at[s], a, k), wy.at[k, a], wr.at[s, 2 * a + k], pp=oy + k) for a in ALL for k in range(CORES)]
        return out[:2] + [rcopy(VEC.at[s], VEC.at[s], wy.at[k, NA], wr.at[s, 2 * NA], pp=oy + k) for k in range(CORES)] + out[2:]

    def quarter(ref, a, q):
        return ref.at[rows(q * (G_HALF[a] // CORES), G_HALF[a] // CORES)]

    def first_copies():
        out = []
        for a in ALL:
            for k in range(CORES):
                q = 2 * xg + k
                out.append(rcopy(quarter(W_IN[a], a, q), quarter(W_BUF[a].at[0], a, q), wy.at[k, a], w0r.at[a, q], pp=oy + k))
        return out + [rcopy(VEC.at[s], VEC.at[s], wy.at[k, NA], wr.at[s, 2 * NA], pp=oy + k) for k in range(CORES)]

    def mine(hop):
        return 2 * (xg if hop == 0 else 1 - xg) + c

    def hop_copies(a, hop):
        part, sem = quarter(W_BUF[a].at[0], a, mine(hop)), w0r.at[a, mine(hop)]
        out = [rcopy(part, part, w0s.at[hop, a], sem, pp=sib)]
        return out if hop else out + [rcopy(part, part, w0s.at[2, a], sem, dp=1 - xg)]

    def hop_on(a, hop):
        copies = hop_copies(a, hop)
        copies[0].wait_recv()
        start_all(copies)

    def hop_end(a):
        for k in range(CORES):
            part = quarter(W_BUF[a].at[0], a, 2 * k + 1 - c)
            rcopy(part, part, w0s.at[0, a], w0r.at[a, 2 * k + 1 - c], pp=sib).wait_recv()

    def start_all(copies):
        for cp in copies:
            cp.start()

    for cp in small:
        cp.wait()
    for k, ref in enumerate((N0, N1, N2, N3, N4, N5, N6)):
        VEC[s, k:k + 1, :] = ref[...].astype(F32)
    VEC[s, 7:8, :3 * E2] = jnp.concatenate([BQ[k, h:h + 1, :].astype(F32) for k in range(3) for h in range(CORES)], axis=1)

    @pl.when(s == 0)
    def _():
        start_all(first_copies())

    @pl.when(s > 1)
    def _():
        start_all(y_copies())
    start_all(sib_copies())

    def pass_copy(l, a, k):
        part = half(W_BUF[a].at[l], a, k)
        return rcopy(part, part, wf.at[l % CORES, a], wr.at[l, 2 * a + k], pp=sib)

    def relay(l, arrays):
        @pl.when(l // CORES != ys_)
        def _():
            for a in arrays:
                pass_copy(l, a, c).wait_recv()
                pass_copy(l, a, c).start()

    def settle(l, arrays, small):
        @pl.when(l == s)
        def _():
            for a in arrays:
                lcopy(W_IN[a], W_BUF[a].at[s], wl.at[a]).wait()

        @pl.when(l == sib)
        def _():
            for a in arrays:
                rcopy(W_IN[a], W_BUF[a].at[l], ws.at[a], wr.at[l, 2 * a], pp=sib).wait_recv()

        @pl.when((l // CORES != ys_) & (l > 0))
        def _():
            for a in arrays:
                pass_copy(l, a, 1 - c).wait_recv()
        if small:
            @pl.when(l != s)
            def _():
                rcopy(VEC.at[l], VEC.at[l], ws.at[NA], wr.at[l, 2 * NA], pp=sib).wait_recv()

    tcopy.wait()

    lane = lax.broadcasted_iota(jnp.int32, (C, E2), 1)
    head_lane = lane // E
    in_head = lane % E
    rot_half = E // 8
    low = in_head < rot_half
    sub_head = lax.broadcasted_iota(jnp.int32, (E2, C), 0) // E
    lower = lax.broadcasted_iota(jnp.int32, (C, C), 0) <= lax.broadcasted_iota(jnp.int32, (C, C), 1)
    c1 = E ** -0.5 * LOG2E

    def tabs(i):
        (cb, sb), (cr, sr) = ([TAB[k, r, :] for k in range(CORES)] for r in (slice(C), slice(C + i, C + i + 1)))
        cs, sn = cb * cr - sb * sr, sb * cr + cb * sr
        return cs, jnp.where(low, -sn, 0.0), jnp.where(low, 0.0, sn)

    def rotate(v, t):
        cs, sa, sb = t
        return v * cs + pltpu.roll(v, E2 - rot_half, 1) * sa + pltpu.roll(v, rot_half, 1) * sb

    def unrotate(v, t):
        cs, sa, sb = t
        return v * cs + pltpu.roll(v * sa, rot_half, 1) + pltpu.roll(v * sb, E2 - rot_half, 1)

    WIDE = SUB // CORES
    SEMS = {1: (sab, sc, ra_s, rb_s, rc_s), WIDE: (fab, fc, fa_s, fb_s, fc_s)}

    def end_copy(p, t, w=1):
        r = slice(t * SR, (t + w) * SR)
        return rcopy(PS.at[r], RA.at[p % CORES, r], SEMS[w][0].at[t], SEMS[w][2].at[p % CORES, t], tp=hub)

    def peer_copy(p, t, w=1):
        r = slice(t * SR, (t + w) * SR)
        return rcopy(PS.at[r], RB.at[p % CORES, r], SEMS[w][0].at[t], SEMS[w][3].at[p % CORES, t], tp=peer)

    def back_copy(p, di, t, w=1):
        r = slice(t * SR, (t + w) * SR)
        return rcopy(H.at[di, r], H.at[di, r], SEMS[w][1].at[t], SEMS[w][4].at[p % CORES, t], tp=leaf)

    def sent_before(copy, p, t, w):
        if w > 1:
            @pl.when(p > 0)
            def _():
                copy(p, t, w).wait_send()
        else:
            @pl.when(p > NL)
            def _():
                copy(p, t).wait_send()
            if t % WIDE == 0:
                @pl.when(p == NL)
                def _():
                    copy(p, t, WIDE).wait_send()

    def pf_row(i, back):
        return (NC if back and i == NC - 1 else i) * C

    def ar_send(p, i, back=False):
        w = 1 if back else WIDE

        @pl.when(is_end)
        def _():
            for t in range(i * SUB, (i + 1) * SUB, w):
                sent_before(end_copy, p, t, w)
                f0 = pf_row(i, back) + (t - i * SUB) * SR
                PS[t * SR:(t + w) * SR, :] = PF[f0:f0 + w * SR, :].astype(BF16)
                end_copy(p, t, w).start()

    def out_bias(l):
        return VEC[l, 4:5, :] + VEC[l, 5:6, :]

    def ar_mid(p, i, u, back=False):
        w = 1 if back else WIDE
        t = i * SUB + u * w
        r = slice(t * SR, (t + w) * SR)
        f0 = pf_row(i, back) + u * w * SR

        @pl.when(inner)
        def _():
            end_copy(p, t, w).wait_recv()
            sent_before(peer_copy, p, t, w)
            PS[r, :] = (PF[f0:f0 + w * SR, :] + RA[p % CORES, r, :].astype(F32)).astype(BF16)
            peer_copy(p, t, w).start()

    def ar_last(p, ri, di, i, u, back=False):
        w = 1 if back else WIDE
        t = i * SUB + u * w
        r = slice(t * SR, (t + w) * SR)

        @pl.when(inner)
        def _():
            peer_copy(p, t, w).wait_recv()

            sent_before(lambda p, t, w=1: back_copy(p, di, t, w), p, t, w)
            both = PS[r, :].astype(F32) + RB[p % CORES, r, :].astype(F32)
            own = H[ri, r, :].astype(F32)
            H[di, r, :] = (own + both if back else own + both + out_bias(p)).astype(BF16)
            back_copy(p, di, t, w).start()

    def ar_wait(p, di, i, w, on=1):
        @pl.when(on * edge > 0)
        def _():
            for t in range(i * SUB, (i + 1) * SUB, w):
                back_copy(p, di, t, w).wait_recv()

    GP1 = NL % 3
    HOME = NC // CORES

    def guest_copy(i):
        part = GX.at[i * C:(i + 1) * C]
        return rcopy(part, part, gxs.at[i], gxr.at[i], pp=c)

    def guest_send(i):
        r = slice(i * C, (i + 1) * C)
        once = jnp.where(z == 1, 1.0, 0.0)
        GX[r, :] = (PF[r, :] + once * (H[NL - 1, r, :].astype(F32) + out_bias(NL - 1))).astype(BF16)
        guest_copy(i).start()

    def guest_hop(t, dst, sem, arrive, to):
        return rcopy(GX.at[t * SR:(t + 1) * SR], dst.at[GP1, t * SR:(t + 1) * SR], sem.at[t], arrive.at[GP1, t], tp=to)

    def guest_to_hub(t):
        return guest_hop(t, RA, gs2, ra_s, hub)

    def guest_to_peer(t):
        return guest_hop(t, RB, gs2, rb_s, peer)

    def guest_to_leaf(t):
        return guest_hop(t, RB, gs3, rc_s, leaf)

    def parts(i):
        return [(t, slice(t * SR, (t + 1) * SR)) for t in range(i * SUB, (i + 1) * SUB)]

    def guest_in(i):
        guest_copy(i).wait_recv()

        @pl.when(is_end)
        def _():
            for t, r in parts(i):
                guest_to_hub(t).start()

    def guest_mid(i):
        @pl.when(inner)
        def _():
            for t, r in parts(i):
                guest_to_hub(t).wait_recv()
                GX[r, :] = (GX[r, :].astype(F32) + RA[GP1, r, :].astype(F32)).astype(BF16)
                guest_to_peer(t).start()

    def guest_last(i):
        @pl.when(inner)
        def _():
            for t, r in parts(i):
                guest_to_peer(t).wait_recv()
                guest_to_peer(t).wait_send()
                GX[r, :] = (GX[r, :].astype(F32) + RB[GP1, r, :].astype(F32)).astype(BF16)
                guest_to_leaf(t).start()

    def guest_back(i):
        @pl.when(is_end)
        def _():
            for t, r in parts(i):
                guest_to_leaf(t).wait_recv()

    def guest_out(act):
        low = slice(HOME * C, S)
        for role, src in ((is_end, RB.at[GP1, low]), (inner, GX.at[low])):
            @pl.when(role)
            def _():
                dst = y.at[1, c, low]
                act(lcopy(src, dst, ygs.at[0]), rcopy(src, dst, ygs.at[1], ygr.at[c], pp=sib), rcopy(src, dst, ygs.at[2], ygr.at[c], pp=s + CORES))

    def guest_home(q):
        return rcopy(y.at[1, q, HOME * C:S], y.at[1, q, HOME * C:S], ygs.at[0], ygr.at[q], pp=sib)

    def stats(hf):
        cen = hf - row_mean(hf)
        rstd = lax.rsqrt(row_mean(cen * cen) + LN_EPS)
        return cen * rstd, rstd

    LB = 32
    GR = 32

    def norms(l, i):
        g1, b1, g2, b2 = (VEC[l, k:k + 1, :] for k in range(NA))

        def step(b, carry):
            hf = H[l, rows(i * C + b * LB, LB), :].astype(F32)
            xhat, unused = stats(hf)
            AS[rows(b * LB, LB), :] = (xhat * g1 + b1).astype(BF16)
            MS[rows(b * LB, LB), :] = (xhat * g2 + b2).astype(BF16)
            return carry
        loop(C // LB, step, 0, unroll=True)

    def by_kind():
        return [(h * 3 + k) * E for k in range(3) for h in range(CORES)]

    def wq(l):
        return jnp.concatenate([WQ[l, r:r + E, :] for r in by_kind()], axis=0)

    def forward(l, i):
        r0, r1 = i * C, (i + 1) * C
        norms(l, i)
        qkv = nt(AS[...], wq(l)) + VEC[l, 7:8, :3 * E2]
        qkv = qkv.astype(BF16).astype(F32)
        t = tabs(i)
        q = rotate(qkv[:, :E2], t).astype(BF16)
        kf = rotate(qkv[:, E2:2 * E2], t)
        vf = qkv[:, 2 * E2:3 * E2]
        Q[l, r0:r1, :] = q
        K[l, r0:r1, :] = kf.astype(BF16)
        V[l, r0:r1, :] = vf.astype(BF16)
        KT[l, :, r0:r1] = jnp.transpose(kf).astype(BF16)
        VT[:, r0:r1] = jnp.transpose(vf).astype(BF16)
        yield

        def far(*hops):
            if i == 0:
                @pl.when((l == 0) & (ys_ == 1))
                def _():
                    for a, hop in hops:
                        hop_on(a, hop)
        far((3, 0))
        RBK = C // CORES
        outs = []
        for h in range(CORES):
            qm = jnp.where(head_lane == h, Q[l, r0:r1, :].astype(F32), 0.0).astype(BF16)
            ST[:r1, :] = nt(K[l, :r1, :], qm)
            ST[r0:r1, :] = jnp.where(lower, ST[r0:r1, :], -1e30)

            def top(b, m):
                return jnp.maximum(m, jnp.max(ST[rows(b * RBK, RBK), :].reshape(RBK // 8, 8, C), axis=0))
            m = jnp.max(loop(r1 // RBK, top, jnp.full((8, C), -3e38, F32), unroll=True), axis=0, keepdims=True)
            mc = m * c1

            def expo(b, tot):
                e = jnp.exp2(ST[rows(b * RBK, RBK), :] * c1 - mc)
                ST[rows(b * RBK, RBK), :] = e
                return tot + fold(e)
            tot = col_sum(loop(r1 // RBK, expo, jnp.zeros((8, C), F32), unroll=True))
            inv = 1.0 / tot

            def put(b, carry):
                PX[i][l, h, rows(b * RBK, RBK), :] = (ST[rows(b * RBK, RBK), :] * inv).astype(BF16)
                return carry
            loop(r1 // RBK, put, 0, unroll=True)
            outs.append(nn(VT[:, :r1], PX[i][l, h]))
            if h == 0:
                yield
        ctx = jnp.transpose(jnp.where(sub_head == 0, outs[0], outs[1])).astype(BF16)
        CTX[l, r0:r1, :] = ctx
        yield
        if i == 0:
            far((2, 1), (3, 1))

            @pl.when((l == 0) & (ys_ == 1))
            def _():
                for a in REST:
                    hop_end(a)
            settle(l, REST, False)
        PF[r0:r1, :] = nn(ctx, WO[l])
        PRE[...] = nn(MS[...], WU[l])
        bup = VEC[l, 6:7, :]
        GB = 32

        def act(b, carry):
            u = PRE[rows(b * GB, GB), :] + bup
            cdf = 0.5 * (1.0 + lax.erf(u * RSQRT2))
            pdf = jnp.exp2(u * u * (-0.5 * LOG2E)) * INV_SQRT_2PI
            HID[l, rows(r0 + b * GB, GB), :] = (u * cdf).astype(BF16)
            GP[l, rows(r0 + b * GB, GB), :] = cdf + u * pdf
            return carry
        loop(C // GB, act, 0, unroll=True)
        PF[r0:r1, :] += nn(HID[l, r0:r1, :], WD[l])
        yield

    def backward(l, dl, i, last):
        r0, r1 = i * C, (i + 1) * C
        par = l % CORES
        first = i == NC - 1

        def acc(ref, val):
            if first:
                ref[par] = val
            else:
                ref[par] += val

        def acc_row(k, val, w=D):
            GV[l, k:k + 1, :w] += val

        norms(l, i)
        dy = H[dl, r0:r1, :]
        acc_row(4, col_sum(dy.astype(F32)))
        PRE[...] = nt(dy, WD[l])
        GB = 32

        def act(b, tot):
            d = PRE[rows(b * GB, GB), :] * GP[l, rows(r0 + b * GB, GB), :]
            DPB[rows(b * GB, GB), :] = d.astype(BF16)
            return tot + fold(d)
        dbu = loop(C // GB, act, jnp.zeros((8, F), F32), unroll=True)
        acc_row(5, col_sum(dbu))
        acc(GD, tn(HID[l, r0:r1, :], dy))
        yield
        acc(GU, tn(MS[...], DPB[...]))
        f0 = pf_row(i, True)
        PF[f0:f0 + C, :] = nt(DPB[...], WU[l])
        yield
        dctx = nt(dy, WO[l]).astype(BF16)
        ctx = CTX[l, r0:r1, :]
        acc(GO, tn(ctx, dy))
        prod = dctx.astype(F32) * ctx.astype(F32)
        q = Q[l, r0:r1, :].astype(F32)
        dcf = dctx.astype(F32)
        RBK = C // CORES
        dqt = []
        for h in range(CORES):
            sel = head_lane == h
            qm = jnp.where(sel, q, 0.0).astype(BF16)
            dcm = jnp.where(sel, dcf, 0.0).astype(BF16)
            dsum = jnp.transpose(jnp.where(sel, prod, 0.0))
            drow = col_sum(dsum)
            ST[:r1, :] = nt(V[l, :r1, :], dcm)

            def sub(b, carry):
                pr = PX[i][l, h, rows(b * RBK, RBK), :].astype(F32)
                DS[rows(b * RBK, RBK), :] = (pr * (ST[rows(b * RBK, RBK), :] - drow)).astype(BF16)
                return carry
            loop(r1 // RBK, sub, 0, unroll=True)
            dk = nn(DS[:r1, :], qm)
            dv = nn(PX[i][l, h], dcm)
            if first and h == 0:
                DK[:r1, :] = dk
                DV[:r1, :] = dv
            else:
                DK[:r1, :] += dk
                DV[:r1, :] += dv
            dqt.append(nn(KT[l, :, :r1], DS[:r1, :]))
            yield
        scale = E ** -0.5
        t = tabs(i)
        dq = unrotate(jnp.transpose(jnp.where(sub_head == 0, dqt[0], dqt[1])) * scale, t)
        dk = unrotate(DK[r0:r1, :] * scale, t)
        dv = DV[r0:r1, :]
        dqkv = jnp.concatenate([dq, dk, dv], axis=1)
        acc_row(6, col_sum(dqkv), 3 * E2)
        dqkv = dqkv.astype(BF16)
        dwq = tn(dqkv, AS[...])
        for k, r in enumerate(by_kind()):
            if first:
                GQ[par, r:r + E, :] = dwq[k * E:(k + 1) * E]
            else:
                GQ[par, r:r + E, :] += dwq[k * E:(k + 1) * E]
        PRE[...] = nn(dqkv, wq(l))
        yield
        g1, g2 = VEC[l, 0:1, :], VEC[l, 2:3, :]

        def lnb(b, tots):
            hf = H[l, rows(r0 + b * LB, LB), :].astype(F32)
            xhat, rstd = stats(hf)
            da = PRE[rows(b * LB, LB), :]
            dm = PF[rows(f0 + b * LB, LB), :]
            dx = da * g1 + dm * g2
            m1 = row_mean(dx)
            m2 = row_mean(dx * xhat)
            if not last:
                PF[rows(f0 + b * LB, LB), :] = rstd * (dx - m1 - xhat * m2)
            terms = (da * xhat, da, dm * xhat, dm)
            return tuple(a + fold(v) for a, v in zip(tots, terms))
        tots = loop(C // LB, lnb, tuple(jnp.zeros((8, D), F32) for _ in range(NA)), unroll=True)
        for k in range(NA):
            acc_row(k, col_sum(tots[k]))
        yield

    def g_half(a, k):
        return rows(k * G_HALF[a], G_HALF[a])

    def r1_view(l, a):
        return GP.at[l + 1, R1_OFF[a]:R1_OFF[a] + G_HALF[a], :G_COLS[a]]

    def g1_copy(l, a):
        return rcopy(G_BUF[a].at[l % CORES, g_half(a, 1 - c)], r1_view(l, a), g1s.at[a], g1r.at[l % CORES, a], pp=sib)

    def g2_copy(l, a):
        return rcopy(HID.at[l, R1_OFF[a]:R1_OFF[a] + G_HALF[a], :G_COLS[a]], R2[a].at[l % CORES], g2s.at[l % CORES, a], g2r.at[l % CORES, a], pp=2 * (l // CORES) + c)

    def g3_local(l, a):
        return lcopy(r1_view(l, a), G_OUT[a].at[g_half(a, c)], g3s.at[l % CORES, a])

    def g3_remote(l, a):
        return rcopy(r1_view(l, a), G_OUT[a].at[g_half(a, c)], g3s.at[l % CORES, a], g3r.at[a], pp=sib)

    def v1_copies(l):
        return [rcopy(GV.at[l], ZR.at[l, z], v1s.at[l, o - 1], v1r.at[l, z], tp=(z + o) % NT) for o in range(1, NT)]

    def grads_mid(l, arrays):
        for a in arrays:
            g1_copy(l, a).wait_recv()
            n = G_HALF[a]

            def add(b, carry):
                rr = rows(R1_OFF[a] + b * GR, GR)
                tot = G_BUF[a][l % CORES, rows(c * n + b * GR, GR), :] + GP[l + 1, rr, :G_COLS[a]]
                GP[l + 1, rr, :G_COLS[a]] = tot
                HID[l, rr, :G_COLS[a]] = tot.astype(BF16)
                return carry
            loop(n // GR, add, 0)

            @pl.when(l // CORES != ys_)
            def _():
                g2_copy(l, a).start()

    def grads_last(l):
        @pl.when(l // CORES == ys_)
        def _():
            for a in MLP[::-1] + ATT:
                g2_copy(l, a).wait_recv()

                def add(b, carry):
                    rr = rows(R1_OFF[a] + b * GR, GR)
                    GP[l + 1, rr, :G_COLS[a]] += R2[a][l % CORES, rows(b * GR, GR), :].astype(F32)
                    return carry
                loop(G_HALF[a] // GR, add, 0)

                @pl.when(l == s)
                def _():
                    g3_local(l, a).start()

                @pl.when(l != s)
                def _():
                    g3_remote(l, a).start()

    def grads_sent(l):
        for a in range(NA):
            @pl.when(l // CORES != ys_)
            def _():
                g2_copy(l, a).wait_send()

            @pl.when(l == s)
            def _():
                g3_local(l, a).wait()

            @pl.when((l // CORES == ys_) & (l != s))
            def _():
                g3_remote(l, a).wait_send()

    def v2_copy(l):
        return rcopy(GZ.at[l], PR.at[s], v2s.at[l], v2r.at[s], pp=l)

    def vec_mid(l):
        ZR[l, z] = GV[l]
        for o in range(1, NT):
            q = (z + o) % NT
            rcopy(GV.at[l], ZR.at[l, q], v1s.at[l, o - 1], v1r.at[l, q], tp=q).wait_recv()
        tot = sum(ZR[l, k] for k in range(NT))
        row = lax.broadcasted_iota(jnp.int32, (8, D), 0)
        GZ[l] = jnp.where(row < 4, tot, GV[l])

        @pl.when(l == s)
        def _():
            PR[s] = GZ[l]

        @pl.when(l != s)
        def _():
            v2_copy(l).start()

    GV[...] = jnp.zeros_like(GV)
    @pl.when(ys_ == 1)
    def _():
        for a, hop in ((0, 0), (1, 0), (0, 1), (2, 0), (1, 1)):
            hop_on(a, hop)
        hop_end(0)
    settle(0, FIRST, True)
    xcopy.wait()

    def run(phases, at, handle, after=lambda k: None):
        for k, unused in enumerate(phases):
            after(k)
            for op, lag, u in at.get(k, ()):
                handle(op, lag, u)

    def fwd_layer(l, carry):
        for i in range(NC):
            ar_wait(l - 1, l, i, WIDE, l)

            def handle(op, lag, u):
                m = i - lag

                def go(p, j):
                    if op == 'mid':
                        ar_mid(p, j, u)
                    else:
                        ar_last(p, p, p + 1, j, u)
                if m >= HOME:
                    @pl.when(l * ys_ < NL - 1)
                    def _():
                        go(l, m)
                elif m >= 0:
                    go(l, m)
                else:
                    @pl.when(l > 0)
                    def _():
                        go(l - 1, m + NC)
            run(forward(l, i), FWD_AT, handle)

            if i < HOME:
                ar_send(l, i)
            else:
                @pl.when(l * ys_ < NL - 1)
                def _():
                    ar_send(l, i)

                @pl.when(l * ys_ == NL - 1)
                def _():
                    guest_send(i)
            if i == 1:
                @pl.when(l == 0)
                def _():
                    gcopy.wait()
                    H[NL + 1] = GP[NL].astype(BF16)

                    @pl.when(s == 1)
                    def _():
                        start_all(y_copies())
            if i == 2:
                @pl.when((l > 0) & (l < NL - 1))
                def _():
                    relay(l + 1, ALL)
            if i == NC - 1:
                @pl.when(l == 0)
                def _():
                    relay(l + 1, ALL)

                @pl.when(l < NL - 1)
                def _():
                    settle(l + 1, FIRST, True)
        return carry
    loop(NL, fwd_layer, 0)

    def y_copies_of(q, n):
        src, dst, got = H.at[NL, :n], y.at[q // CORES, c, :n], yr.at[q]
        return lcopy(src, dst, ys.at[0]), rcopy(src, dst, ys.at[1], got, pp=sib), rcopy(src, dst, ys.at[2], got, pp=oy + c)

    def y_pass(q, n):
        part = y.at[q // CORES, c, :n]
        return rcopy(part, part, ys.at[3], yr.at[q], pp=sib)

    def y_arrived(q, n):
        part = y.at[q // CORES, q % CORES, :n]
        rcopy(part, part, ys.at[1], yr.at[q], pp=sib).wait_recv()

    def each_row(do):
        for row, n, other in ((0, S, HOME * C), (1, HOME * C, S)):
            @pl.when(ys_ == row)
            def _():
                do(row, n, other)

    def ri(l):
        return jnp.where(l == NL - 1, NL + 1, l + 1)

    def pass_of(lb):
        return NL + lb + (1 - ys_) * jnp.minimum(lb, 1)

    def bwd_layer(lb, carry):
        l = NL - 1 - lb
        p = pass_of(lb)
        before = pass_of(lb - 1)
        for n in range(NC):
            i = NC - 1 - n

            ar_wait(before, l + 1, i, 1, lb)

            def handle(op, lag, u):
                m = n - lag

                def go(q, lq, j):
                    if op == 'mid':
                        ar_mid(q, j, u, True)
                    else:
                        ar_last(q, ri(lq), lq, j, u, True)
                if m >= 0:
                    @pl.when(l > 0)
                    def _():
                        go(p, l, NC - 1 - m)
                else:
                    @pl.when(lb > 0)
                    def _():
                        go(before, l + 1, -1 - m)

                    if u % WIDE == 0:
                        @pl.when(lb == NL * ys_)
                        def _():
                            if op == 'mid':
                                ar_mid(NL - 1, m + NC, u // WIDE)
                            else:
                                ar_last(NL - 1, NL - 1, NL, m + NC, u // WIDE)

            def guests(layer, what, j):
                @pl.when(lb == layer + NL * ys_)
                def _():
                    what(j)

            def after(k):
                if k == 0 and i >= HOME:
                    guests(1, guest_in, i)
                if k == 1 and NC > i + 1 >= HOME:
                    guests(1, guest_last, i + 1)
                if k == NC and i >= HOME:
                    guests(1, guest_mid, i)
                if k == 0 and n == 0:
                    @pl.when(lb > 0)
                    def _():
                        grads_mid(l + 1, ATT)
                        for a in ALL:
                            g1_copy(l + 1, a).wait_send()
                if n == NC - 1 and k < 2:
                    g1_copy(l, MLP[1 - k]).start()
                if n == NC - 1 and k in (3, 4):
                    @pl.when(l == 0)
                    def _():
                        grads_mid(l, (MLP[4 - k],))
            run(backward(l, ri(l), i, False), BWD_AT, handle, after)

            if i >= HOME:
                @pl.when(lb == 2 + NL * ys_)
                def _():
                    guest_back(i)

            @pl.when(l > 0)
            def _():
                ar_send(p, i, True)
            if n == NC - 1:
                @pl.when(lb == 2 + NL * ys_)
                def _():
                    guest_out(lambda *copies: start_all(copies))
            if n == 1:
                @pl.when(lb > 0)
                def _():
                    vec_mid(l + 1)
            if n == 2:
                @pl.when(lb == 0)
                def _():
                    def out(row, n, other):
                        for j in range(n // C):
                            ar_wait(NL - 1, NL, j, WIDE)
                        start_all(y_copies_of(CORES * row + c, n))
                    each_row(out)

                @pl.when(lb > 1)
                def _():
                    grads_last(l + 2)

        for a in ATT:
            g1_copy(l, a).start()
        start_all(v1_copies(l))

        @pl.when(l > 0)
        def _():
            grads_mid(l, MLP)
        return carry
    loop(NL, bwd_layer, 0)

    grads_mid(0, ATT)

    def pass_on(row, n, other):
        y_arrived(CORES * (1 - row) + c, other)
        y_pass(CORES * (1 - row) + c, other).start()
        if row:
            guest_home(c).wait_recv()
            guest_home(c).start()
    each_row(pass_on)
    grads_last(1)
    vec_mid(0)
    grads_last(0)

    for o in range(1, NL):
        q = (s + o) % NL
        rcopy(GZ.at[0], PR.at[q], v2s.at[0], v2r.at[q], pp=q).wait_recv()
    PRE[:8, :D] = sum(PR[k] for k in range(NL))
    vout = lcopy(PRE.at[:8, :D], ovec, osem.at[0])
    vout.start()
    for l in range(NL):
        for cp in v1_copies(l):
            cp.wait_send()
    for l in range(NL):
        @pl.when(l != s)
        def _():
            v2_copy(l).wait_send()
    for a in range(NA):
        rcopy(G_OUT[a].at[g_half(a, 1 - c)], G_OUT[a].at[g_half(a, 1 - c)], g3s.at[a], g3r.at[a], pp=sib).wait_recv()

    def out_done(local, *sent):
        local.wait()
        for cp in sent:
            cp.wait_send()

    def all_out(row, n, other):
        out_done(*y_copies_of(CORES * row + c, n))
        y_pass(CORES * (1 - row) + c, other).wait_send()
        y_arrived(CORES * row + 1 - c, n)
        y_arrived(CORES * (1 - row) + 1 - c, other)
        guest_home(1 - c).wait_recv()
    each_row(all_out)

    @pl.when(ys_ == 0)
    def _():
        guest_out(out_done)

        @pl.when(is_end)
        def _():
            for t in range(HOME * SUB, NC * SUB):
                guest_to_hub(t).wait_send()

        @pl.when(inner)
        def _():
            for t in range(HOME * SUB, NC * SUB):
                guest_to_leaf(t).wait_send()

    @pl.when(ys_ == 1)
    def _():
        guest_home(c).wait_send()
        for i in range(HOME, NC):
            guest_copy(i).wait_send()
    for a in range(NA):
        g1_copy(0, a).wait_send()
    for l in range(NL):
        grads_sent(l)
    for cp in sib_copies():
        cp.wait_send()
    @pl.when(s == 0)
    def _():
        for cp in first_copies():
            cp.wait_send()

    @pl.when(s > 0)
    def _():
        for cp in y_copies():
            cp.wait_send()
    for a in ALL:
        pass_copy(oy + 1, a, c).wait_send()

        @pl.when(ys_ == 0)
        def _():
            pass_copy(oy, a, c).wait_send()

        @pl.when(ys_ == 1)
        def _():
            for hop in range(CORES):
                for cp in hop_copies(a, hop):
                    cp.wait_send()

    @pl.when(is_end)
    def _():
        for t in range(NC * SUB):
            end_copy(0, t).wait_send()

    @pl.when(inner)
    def _():
        for t in range(NC * SUB):
            peer_copy(0, t).wait_send()
            back_copy(0, 1, t).wait_send()
    vout.wait()


def finish(y, gq, go, gu, gd, gv, yo, qo, oo, uo, do, n0, n1, n2, n3, n4, n5, n6, bq,
           yb, qb, ob, ub, db, vb, r0, r1, r2, r3, r4, r5, r6, rq, got, put, small):
    trips = [(gd, db, do), (gu, ub, uo), (go, ob, oo), (gq, qb, qo)]
    trips += [tuple(ref.at[m, r] for ref in (y, yb, yo)) for m in range(y.shape[0]) for r in range(y.shape[1])]
    loads = [pltpu.make_async_copy(a, b, got.at[k]) for k, (a, b, o) in enumerate(trips)]
    stores = [pltpu.make_async_copy(b, o, put.at[k]) for k, (a, b, o) in enumerate(trips)]
    vecs = pltpu.make_async_copy(gv, vb, small.at[len(trips)])
    vecs.start()
    for cp in loads:
        cp.start()
    vecs.wait()
    for row, refs in enumerate(((r0,), (r1,), (r2,), (r3,), (r4, r5), (r6,))):
        for ref in refs:
            ref[...] = vb[row:row + 1, :]
    e = rq.shape[2]
    for k in range(3):
        for h in range(CORES):
            rq[k, h:h + 1, :] = vb[6:7, (CORES * k + h) * e:(CORES * k + h + 1) * e]
    tiny = [pltpu.make_async_copy(a, b, small.at[k]) for k, (a, b) in enumerate(((r0, n0), (r1, n1), (r2, n2), (r3, n3), (r4, n4), (r5, n5), (r6, n6), (rq, bq)))]
    for cp in tiny:
        cp.start()
    for cp, out in zip(loads, stores):
        cp.wait()
        out.start()
    for cp in tiny + stores:
        cp.wait()


def finish_step(y, gq, go, gu, gd, gv, e):
    hbm = pl.BlockSpec(memory_space=pl.ANY)
    row = jax.ShapeDtypeStruct((1, gv.shape[1]), F32)
    outs = [jax.ShapeDtypeStruct(a.shape, a.dtype) for a in (y, gq, go, gu, gd)] + [row] * 7 + [jax.ShapeDtypeStruct((3, CORES, e), F32)]
    bufs = outs[:5] + [gv] + outs[5:]
    return pl.pallas_call(
        finish,
        out_shape=outs,
        in_specs=[hbm] * 6,
        out_specs=[hbm] * len(outs),
        scratch_shapes=[pltpu.VMEM(a.shape, a.dtype) for a in bufs] + [pltpu.SemaphoreType.DMA((9,))] * 3,
        name='neox_out',
    )(y, gq, go, gu, gd, gv)


def group_step(dims, *args):
    x = args[0]
    S, D, E, C, F = dims
    E2 = 2 * E
    hbm = pl.BlockSpec(memory_space=pl.ANY)
    out_shape = [
        jax.ShapeDtypeStruct(x.shape, BF16),
        jax.ShapeDtypeStruct((3 * E2, D), F32),
        jax.ShapeDtypeStruct((E2, D), F32),
        jax.ShapeDtypeStruct((D, F), F32),
        jax.ShapeDtypeStruct((F, D), F32),
        jax.ShapeDtypeStruct((8, D), F32),
    ]

    def vm(*shape, dtype=BF16):
        return pltpu.VMEM(shape, dtype)
    dma = pltpu.SemaphoreType.DMA
    scratch = [
        vm(NL, 3 * E2, D), vm(NL, E2, D), vm(NL, D, F), vm(NL, F, D), vm(NL, 8, D, dtype=F32),
        vm(NL + 2, S, D),
        vm(NL, S, E2), vm(NL, S, E2), vm(NL, S, E2), vm(NL, E2, S), vm(E2, S), vm(NL, S, E2),
        *[vm(NL, 2, (i + 1) * C, C) for i in range(NC)],
        vm(NL, S, F), vm(NL + 1, S, F, dtype=F32),
        vm(CORES, S, D), vm(CORES, S, D), vm(S, D), vm(S + C, D, dtype=F32),
        *[vm(CORES, *k, dtype=F32) for k in ((3 * E2, D), (E2, D), (D, F), (F, D))],
        *[vm(CORES, *k) for k in ((3 * E, D), (E, D), (D // CORES, F), (F // CORES, D))],
        vm(S, E2, dtype=F32), vm(S, E2, dtype=F32),
        vm(CORES, C + 8, E2, dtype=F32),
        *[vm(*k, 8, D, dtype=F32) for k in ((NL,), (NL, NT), (NL,), (NL,))],
        vm(C, D), vm(C, D), vm(C, max(D, F), dtype=F32), vm(C, F), vm(S, C), vm(S, C, dtype=F32),
        *[vm(1, D, dtype=F32)] * 4, vm(1, D), vm(1, D), vm(1, F), vm(3, CORES, E), vm(S, D),
        *[dma((NC * SUB,))] * 2, *[dma((CORES, NC * SUB))] * 3,
        dma((NA,)), dma((NA + 1,)), dma((CORES, NA + 1)), dma((NL, 2 * NA + 1)), dma((CORES, NA)), dma((3, NA)), dma((NA, 4)), dma((CORES,)), dma((1,)),
        dma((NC * SUB,)), dma((NC * SUB,)), dma((CORES, NC * SUB)), dma((CORES, NC * SUB)), dma((CORES, NC * SUB)),
        dma((NL,)), dma((NL,)), dma((NA,)), dma((CORES, NA)), dma((CORES, NA)), dma((CORES, NA)), dma((CORES, NA)), dma((NA,)),
        dma((NL, NT - 1)), dma((NL, NT)), dma((NL,)), dma((NL,)), dma((1,)), dma((8,)),
        dma((NC,)), dma((NC,)), dma((NC * SUB,)), dma((NC * SUB,)), dma((3,)), dma((CORES,)),
    ]
    return pl.pallas_call(
        functools.partial(body, dims),
        out_shape=out_shape,
        in_specs=[hbm] * len(args),
        out_specs=[hbm] * 6,
        scratch_shapes=scratch,
        compiler_params=pltpu.CompilerParams(collective_id=0, has_side_effects=True, vmem_limit_bytes=67043328),
        name='neox_group',
    )(*args)


def solution(mesh):
    def device_fn(x_in, g_out, ln1_gain, ln1_bias, w_qkv, b_qkv, w_out, b_out, ln2_gain, ln2_bias, w_up, b_up, w_down, b_down):
        n_micro, n_rows, S, D = x_in.shape
        heads, E = w_qkv.shape[2], w_qkv.shape[4]
        F = w_up.shape[2]
        C = S // NC
        wqkv = jnp.transpose(w_qkv[0], (1, 2, 3, 0)).reshape(heads * 3 * E, D)
        bqkv = jnp.transpose(b_qkv[0], (1, 0, 2))
        tab = jnp.asarray(rotary_base(C, NC, E, heads))
        part = group_step((S, D, E, C, F), x_in, g_out, wqkv, w_out[0].reshape(heads * E, D), w_up[0], w_down[0], ln1_gain, ln1_bias, ln2_gain, ln2_bias, b_out, b_down, b_up, bqkv, tab)
        y, gq, go, gup, gdn, n1g, n1b, n2g, n2b, gbo, gbd, gbu, gbq = finish_step(*part, E)
        gq = jnp.transpose(gq.reshape(heads, 3, E, D), (3, 0, 1, 2))[None]
        gbq = jnp.transpose(gbq, (1, 0, 2))[None]
        return (y, n1g, n1b, gq, gbq, go.reshape(1, heads, E, D), gbo, n2g, n2b, gup[None], gbu, gdn[None], gbd)

    return jax.shard_map(device_fn, mesh=mesh, in_specs=(P('dp'), P('dp')) + STAGE_SPECS, out_specs=(P('dp'),) + GRAD_SPECS, check_vma=False)
```

```python
import functools
import math

import jax
import jax.numpy as jnp
import numpy as np
from jax import lax
from jax.experimental import pallas as pl
from jax.experimental.pallas import tpu as pltpu
from jax.sharding import PartitionSpec as P

ROPE_BASE = 10000.0
LN_EPS = 1e-5
STAGE_SPECS = (P('pp'), P('pp'), P('pp', None, 'tp'), P('pp', 'tp'), P('pp', 'tp'), P('pp'), P('pp'), P('pp'), P('pp', None, 'tp'), P('pp', 'tp'), P('pp', 'tp'), P('pp'))
OWN = ('dp', 'pp')
GRAD_SPECS = (P(OWN), P(OWN), P(OWN, None, 'tp'), P(OWN, 'tp'), P(OWN, 'tp'), P(OWN), P(OWN), P(OWN), P(OWN, None, 'tp'), P(OWN, 'tp'), P(OWN, 'tp'), P(OWN))


F32 = jnp.float32
BF16 = jnp.bfloat16
NL = 4
NT = 4
NC = 4
NA = 4
CORES = 2
SUB = 4
FWD_AT = {0: (('mid', 1, 0), ('last', 2, 0), ('last', 2, 1)), 1: (('mid', 1, 1), ('last', 2, 2)), 2: (('mid', 1, 2),), 3: (('mid', 1, 3), ('last', 2, 3))}
BWD_AT = {k: (('last', 2, k),) * (k < SUB) + (('mid', 1, k - 1),) * (k > 0) for k in range(SUB + 1)}
LOG2E = 1.4426950408889634
RSQRT2 = 0.7071067811865476
INV_SQRT_2PI = 0.3989422804014327


def nn(a, b):
    return lax.dot_general(a, b, (((1,), (0,)), ((), ())), preferred_element_type=F32)


def nt(a, b):
    return lax.dot_general(a, b, (((1,), (1,)), ((), ())), preferred_element_type=F32)


def tn(a, b):
    return lax.dot_general(a, b, (((0,), (0,)), ((), ())), preferred_element_type=F32)


def loop(n, step, init, unroll=False):
    return lax.fori_loop(0, n, step, init, unroll=unroll)


def col_sum(v):
    return jnp.sum(v, axis=0, keepdims=True)


def row_mean(v):
    return jnp.mean(v, axis=-1, keepdims=True)


def fold(v):
    return jnp.sum(v.reshape(v.shape[0] // 8, 8, v.shape[1]), axis=0)


def rotary_base(chunk, n_chunks, head_dim, n_heads):
    rot_dim = head_dim // 4
    half = rot_dim // CORES
    inv_freq = np.zeros((head_dim,), np.float64)
    inv_freq[:rot_dim] = np.tile(ROPE_BASE ** (-(np.arange(half) * 2.0) / rot_dim), 2)
    inv_freq = np.tile(inv_freq, n_heads)
    pos = np.concatenate([np.arange(chunk), np.arange(8) * (np.arange(8) < n_chunks) * chunk]).astype(np.float64)
    ang = pos[:, None] * inv_freq[None, :]
    return np.stack([np.cos(ang), np.sin(ang)]).astype(np.float32)


def body(dims, x, g, wqkv, wo, wup, wdn, n0, n1, n2, n3, n4, n5, n6, bq, tab,
         y, oqkv, oo, oup, odn, ovec,
         WQ, WO, WU, WD, VEC, H, Q, K, V, KT, VT, CTX, P0, P1, P2, P3, HID, GP, RA, RB, PS, PF,
         GQ, GO, GU, GD, R2Q, R2O, R2U, R2D, DK, DV, TAB, GV, ZR, GZ, PR,
         AS, MS, PRE, DPB, DS, ST, N0, N1, N2, N3, N4, N5, N6, BQ, GX,
         wl, ws, wy, wr, wf, w0s, w0r, xs, gs, sab, sc, ra_s, rb_s, rc_s, ys, yr, g1s, g1r, g2s, g2r, g3s, g3r, v1s, v1r, v2s, v2r, osem, ns, gxs, gxr, gs2, gs3, ygs, ygr):
    S, D, E, C, F = dims
    E2 = 2 * E
    SR = C // SUB
    z = lax.axis_index('tp')
    xg = lax.axis_index('dp')
    s = lax.axis_index('pp')
    ys_ = s // CORES
    c = s % CORES
    sib = s + 1 - 2 * c
    oy = 2 * (1 - ys_)
    is_end = z * (NT - 1 - z) == 0
    inner = z * (NT - 1 - z) > 0
    edge = 1 - jnp.minimum(z * (NT - 1 - z), 1)
    hub = 1 + z // 3
    leaf = jnp.where(z == 1, 0, 3)
    peer = 3 - z
    PX = (P0, P1, P2, P3)
    W_IN = (wqkv, wo, wup, wdn)
    W_BUF = (WQ, WO, WU, WD)
    G_HALF = (3 * E, E, D // CORES, F // CORES)
    ALL = tuple(range(NA))
    FIRST, REST = ALL[:1], ALL[1:]
    ATT, MLP = ALL[:2], ALL[2:]
    G_BUF = (GQ, GO, GU, GD)
    G_OUT = (oqkv, oo, oup, odn)
    G_COLS = (D, D, F, D)
    R1_OFF = tuple(sum(G_HALF[:k]) for k in range(NA))
    R2 = (R2Q, R2O, R2U, R2D)

    def rcopy(src, dst, ss, rs, **dev):
        return pltpu.make_async_remote_copy(src_ref=src, dst_ref=dst, send_sem=ss, recv_sem=rs, device_id=dev, device_id_type=pl.DeviceIdType.MESH)

    def lcopy(src, dst, sem):
        return pltpu.make_async_copy(src, dst, sem)

    def rows(start, n):
        return pl.ds(pl.multiple_of(start, n), n)

    xcopy = lcopy(x.at[ys_, c], H.at[0], xs.at[0])
    xcopy.start()
    gcopy = lcopy(g.at[ys_, c], GP.at[NL], gs.at[0])
    gcopy.start()
    tcopy = lcopy(tab, TAB, xs.at[1])
    tcopy.start()
    for a in range(NA):
        lcopy(W_IN[a], W_BUF[a].at[s], wl.at[a]).start()
    small = [lcopy(a, b, ns.at[k]) for k, (a, b) in enumerate(((n0, N0), (n1, N1), (n2, N2), (n3, N3), (n4, N4), (n5, N5), (n6, N6), (bq, BQ)))]
    for cp in small:
        cp.start()

    bar = pltpu.get_barrier_semaphore()
    for o in range(1, NT):
        pl.semaphore_signal(bar, inc=1, device_id={'tp': (z + o) % NT}, device_id_type=pl.DeviceIdType.MESH)
    for o in range(1, NL):
        pl.semaphore_signal(bar, inc=1, device_id={'pp': (s + o) % NL}, device_id_type=pl.DeviceIdType.MESH)
    pl.semaphore_signal(bar, inc=1, device_id={'dp': 1 - xg}, device_id_type=pl.DeviceIdType.MESH)
    pl.semaphore_wait(bar, NT + NL - 1)

    def half(ref, a, k):
        return ref.at[rows(k * G_HALF[a], G_HALF[a])]

    def sib_copies():
        out = [rcopy(W_IN[a], W_BUF[a].at[s], ws.at[a], wr.at[s, 2 * a], pp=sib) for a in ALL]
        return out + [rcopy(VEC.at[s], VEC.at[s], ws.at[NA], wr.at[s, 2 * NA], pp=sib)]

    def y_copies():
        out = [rcopy(half(W_IN[a], a, k), half(W_BUF[a].at[s], a, k), wy.at[k, a], wr.at[s, 2 * a + k], pp=oy + k) for a in ALL for k in range(CORES)]
        return out[:2] + [rcopy(VEC.at[s], VEC.at[s], wy.at[k, NA], wr.at[s, 2 * NA], pp=oy + k) for k in range(CORES)] + out[2:]

    def quarter(ref, a, q):
        return ref.at[rows(q * (G_HALF[a] // CORES), G_HALF[a] // CORES)]

    def first_copies():
        out = []
        for a in ALL:
            for k in range(CORES):
                q = 2 * xg + k
                out.append(rcopy(quarter(W_IN[a], a, q), quarter(W_BUF[a].at[0], a, q), wy.at[k, a], w0r.at[a, q], pp=oy + k))
        return out + [rcopy(VEC.at[s], VEC.at[s], wy.at[k, NA], wr.at[s, 2 * NA], pp=oy + k) for k in range(CORES)]

    def mine(hop):
        return 2 * (xg if hop == 0 else 1 - xg) + c

    def hop_copies(a, hop):
        part, sem = quarter(W_BUF[a].at[0], a, mine(hop)), w0r.at[a, mine(hop)]
        out = [rcopy(part, part, w0s.at[hop, a], sem, pp=sib)]
        return out if hop else out + [rcopy(part, part, w0s.at[2, a], sem, dp=1 - xg)]

    def hop_on(a, hop):
        copies = hop_copies(a, hop)
        copies[0].wait_recv()
        start_all(copies)

    def hop_end(a):
        for k in range(CORES):
            part = quarter(W_BUF[a].at[0], a, 2 * k + 1 - c)
            rcopy(part, part, w0s.at[0, a], w0r.at[a, 2 * k + 1 - c], pp=sib).wait_recv()

    def start_all(copies):
        for cp in copies:
            cp.start()

    for cp in small:
        cp.wait()
    for k, ref in enumerate((N0, N1, N2, N3, N4, N5, N6)):
        VEC[s, k:k + 1, :] = ref[...].astype(F32)
    VEC[s, 7:8, :3 * E2] = jnp.concatenate([BQ[k, h:h + 1, :].astype(F32) for k in range(3) for h in range(CORES)], axis=1)

    @pl.when(s == 0)
    def _():
        start_all(first_copies())

    @pl.when(s > 1)
    def _():
        start_all(y_copies())
    start_all(sib_copies())

    def pass_copy(l, a, k):
        part = half(W_BUF[a].at[l], a, k)
        return rcopy(part, part, wf.at[l % CORES, a], wr.at[l, 2 * a + k], pp=sib)

    def relay(l, arrays):
        @pl.when(l // CORES != ys_)
        def _():
            for a in arrays:
                pass_copy(l, a, c).wait_recv()
                pass_copy(l, a, c).start()

    def settle(l, arrays, small):
        @pl.when(l == s)
        def _():
            for a in arrays:
                lcopy(W_IN[a], W_BUF[a].at[s], wl.at[a]).wait()

        @pl.when(l == sib)
        def _():
            for a in arrays:
                rcopy(W_IN[a], W_BUF[a].at[l], ws.at[a], wr.at[l, 2 * a], pp=sib).wait_recv()

        @pl.when((l // CORES != ys_) & (l > 0))
        def _():
            for a in arrays:
                pass_copy(l, a, 1 - c).wait_recv()
        if small:
            @pl.when(l != s)
            def _():
                rcopy(VEC.at[l], VEC.at[l], ws.at[NA], wr.at[l, 2 * NA], pp=sib).wait_recv()

    tcopy.wait()

    lane = lax.broadcasted_iota(jnp.int32, (C, E2), 1)
    head_lane = lane // E
    in_head = lane % E
    rot_half = E // 8
    low = in_head < rot_half
    sub_head = lax.broadcasted_iota(jnp.int32, (E2, C), 0) // E
    lower = lax.broadcasted_iota(jnp.int32, (C, C), 0) <= lax.broadcasted_iota(jnp.int32, (C, C), 1)
    c1 = E ** -0.5 * LOG2E

    def tabs(i):
        (cb, sb), (cr, sr) = ([TAB[k, r, :] for k in range(CORES)] for r in (slice(C), slice(C + i, C + i + 1)))
        cs, sn = cb * cr - sb * sr, sb * cr + cb * sr
        return cs, jnp.where(low, -sn, 0.0), jnp.where(low, 0.0, sn)

    def rotate(v, t):
        cs, sa, sb = t
        return v * cs + pltpu.roll(v, E2 - rot_half, 1) * sa + pltpu.roll(v, rot_half, 1) * sb

    def unrotate(v, t):
        cs, sa, sb = t
        return v * cs + pltpu.roll(v * sa, rot_half, 1) + pltpu.roll(v * sb, E2 - rot_half, 1)

    def end_copy(p, t):
        return rcopy(PS.at[t * SR:(t + 1) * SR], RA.at[p % CORES, t * SR:(t + 1) * SR], sab.at[t], ra_s.at[p % CORES, t], tp=hub)

    def peer_copy(p, t):
        return rcopy(PS.at[t * SR:(t + 1) * SR], RB.at[p % CORES, t * SR:(t + 1) * SR], sab.at[t], rb_s.at[p % CORES, t], tp=peer)

    def back_copy(p, di, t):
        return rcopy(H.at[di, t * SR:(t + 1) * SR], H.at[di, t * SR:(t + 1) * SR], sc.at[t], rc_s.at[p % CORES, t], tp=leaf)

    def pf_row(i, back):
        return (NC if back and i == NC - 1 else i) * C

    def ar_send(p, i, back=False):
        @pl.when(is_end)
        def _():
            for t in range(i * SUB, (i + 1) * SUB):
                @pl.when(p > 0)
                def _():
                    end_copy(p, t).wait_send()
                f0 = pf_row(i, back) + (t - i * SUB) * SR
                PS[t * SR:(t + 1) * SR, :] = PF[f0:f0 + SR, :].astype(BF16)
                end_copy(p, t).start()

    def out_bias(l):
        return VEC[l, 4:5, :] + VEC[l, 5:6, :]

    def ar_mid(p, i, u, back=False):
        t = i * SUB + u
        r = slice(t * SR, (t + 1) * SR)
        f0 = pf_row(i, back) + u * SR

        @pl.when(inner)
        def _():
            end_copy(p, t).wait_recv()
            @pl.when(p > 0)
            def _():
                peer_copy(p, t).wait_send()
            PS[r, :] = (PF[f0:f0 + SR, :] + RA[p % CORES, r, :].astype(F32)).astype(BF16)
            peer_copy(p, t).start()

    def ar_last(p, ri, di, i, u, back=False):
        t = i * SUB + u
        r = slice(t * SR, (t + 1) * SR)

        @pl.when(inner)
        def _():
            peer_copy(p, t).wait_recv()
            @pl.when(p > 0)
            def _():
                back_copy(p, di, t).wait_send()
            both = PS[r, :].astype(F32) + RB[p % CORES, r, :].astype(F32)
            own = H[ri, r, :].astype(F32)
            H[di, r, :] = (own + both if back else own + both + out_bias(p)).astype(BF16)
            back_copy(p, di, t).start()

    def ar_wait(p, di, i, on=1):
        @pl.when(on * edge > 0)
        def _():
            for t in range(i * SUB, (i + 1) * SUB):
                back_copy(p, di, t).wait_recv()

    GP1 = NL % 3
    HOME = NC // CORES

    def guest_copy(i):
        part = GX.at[i * C:(i + 1) * C]
        return rcopy(part, part, gxs.at[i], gxr.at[i], pp=c)

    def guest_send(i):
        r = slice(i * C, (i + 1) * C)
        once = jnp.where(z == 1, 1.0, 0.0)
        GX[r, :] = (PF[r, :] + once * (H[NL - 1, r, :].astype(F32) + out_bias(NL - 1))).astype(BF16)
        guest_copy(i).start()

    def guest_hop(t, dst, sem, arrive, to):
        return rcopy(GX.at[t * SR:(t + 1) * SR], dst.at[GP1, t * SR:(t + 1) * SR], sem.at[t], arrive.at[GP1, t], tp=to)

    def guest_to_hub(t):
        return guest_hop(t, RA, gs2, ra_s, hub)

    def guest_to_peer(t):
        return guest_hop(t, RB, gs2, rb_s, peer)

    def guest_to_leaf(t):
        return guest_hop(t, RB, gs3, rc_s, leaf)

    def parts(i):
        return [(t, slice(t * SR, (t + 1) * SR)) for t in range(i * SUB, (i + 1) * SUB)]

    def guest_in(i):
        guest_copy(i).wait_recv()

        @pl.when(is_end)
        def _():
            for t, r in parts(i):
                guest_to_hub(t).start()

    def guest_mid(i):
        @pl.when(inner)
        def _():
            for t, r in parts(i):
                guest_to_hub(t).wait_recv()
                GX[r, :] = (GX[r, :].astype(F32) + RA[GP1, r, :].astype(F32)).astype(BF16)
                guest_to_peer(t).start()

    def guest_last(i):
        @pl.when(inner)
        def _():
            for t, r in parts(i):
                guest_to_peer(t).wait_recv()
                guest_to_peer(t).wait_send()
                GX[r, :] = (GX[r, :].astype(F32) + RB[GP1, r, :].astype(F32)).astype(BF16)
                guest_to_leaf(t).start()

    def guest_back(i):
        @pl.when(is_end)
        def _():
            for t, r in parts(i):
                guest_to_leaf(t).wait_recv()

    def guest_out(act):
        low = slice(HOME * C, S)
        for role, src in ((is_end, RB.at[GP1, low]), (inner, GX.at[low])):
            @pl.when(role)
            def _():
                dst = y.at[1, c, low]
                act(lcopy(src, dst, ygs.at[0]), rcopy(src, dst, ygs.at[1], ygr.at[c], pp=sib), rcopy(src, dst, ygs.at[2], ygr.at[c], pp=s + CORES))

    def guest_home(q):
        return rcopy(y.at[1, q, HOME * C:S], y.at[1, q, HOME * C:S], ygs.at[0], ygr.at[q], pp=sib)

    def stats(hf):
        cen = hf - row_mean(hf)
        rstd = lax.rsqrt(row_mean(cen * cen) + LN_EPS)
        return cen * rstd, rstd

    LB = 32
    GR = 32

    def norms(l, i):
        g1, b1, g2, b2 = (VEC[l, k:k + 1, :] for k in range(NA))

        def step(b, carry):
            hf = H[l, rows(i * C + b * LB, LB), :].astype(F32)
            xhat, unused = stats(hf)
            AS[rows(b * LB, LB), :] = (xhat * g1 + b1).astype(BF16)
            MS[rows(b * LB, LB), :] = (xhat * g2 + b2).astype(BF16)
            return carry
        loop(C // LB, step, 0, unroll=True)

    def by_kind():
        return [(h * 3 + k) * E for k in range(3) for h in range(CORES)]

    def wq(l):
        return jnp.concatenate([WQ[l, r:r + E, :] for r in by_kind()], axis=0)

    def forward(l, i):
        r0, r1 = i * C, (i + 1) * C
        norms(l, i)
        qkv = nt(AS[...], wq(l)) + VEC[l, 7:8, :3 * E2]
        qkv = qkv.astype(BF16).astype(F32)
        t = tabs(i)
        q = rotate(qkv[:, :E2], t).astype(BF16)
        kf = rotate(qkv[:, E2:2 * E2], t)
        vf = qkv[:, 2 * E2:3 * E2]
        Q[l, r0:r1, :] = q
        K[l, r0:r1, :] = kf.astype(BF16)
        V[l, r0:r1, :] = vf.astype(BF16)
        KT[l, :, r0:r1] = jnp.transpose(kf).astype(BF16)
        VT[:, r0:r1] = jnp.transpose(vf).astype(BF16)
        yield

        def far(*hops):
            if i == 0:
                @pl.when((l == 0) & (ys_ == 1))
                def _():
                    for a, hop in hops:
                        hop_on(a, hop)
        far((3, 0))
        RBK = C // CORES
        outs = []
        for h in range(CORES):
            qm = jnp.where(head_lane == h, Q[l, r0:r1, :].astype(F32), 0.0).astype(BF16)
            ST[:r1, :] = nt(K[l, :r1, :], qm)
            ST[r0:r1, :] = jnp.where(lower, ST[r0:r1, :], -1e30)

            def top(b, m):
                return jnp.maximum(m, jnp.max(ST[rows(b * RBK, RBK), :].reshape(RBK // 8, 8, C), axis=0))
            m = jnp.max(loop(r1 // RBK, top, jnp.full((8, C), -3e38, F32), unroll=True), axis=0, keepdims=True)
            mc = m * c1

            def expo(b, tot):
                e = jnp.exp2(ST[rows(b * RBK, RBK), :] * c1 - mc)
                ST[rows(b * RBK, RBK), :] = e
                return tot + fold(e)
            tot = col_sum(loop(r1 // RBK, expo, jnp.zeros((8, C), F32), unroll=True))
            inv = 1.0 / tot

            def put(b, carry):
                PX[i][l, h, rows(b * RBK, RBK), :] = (ST[rows(b * RBK, RBK), :] * inv).astype(BF16)
                return carry
            loop(r1 // RBK, put, 0, unroll=True)
            outs.append(nn(VT[:, :r1], PX[i][l, h]))
            if h == 0:
                yield
        ctx = jnp.transpose(jnp.where(sub_head == 0, outs[0], outs[1])).astype(BF16)
        CTX[l, r0:r1, :] = ctx
        yield
        if i == 0:
            far((2, 1), (3, 1))

            @pl.when((l == 0) & (ys_ == 1))
            def _():
                for a in REST:
                    hop_end(a)
            settle(l, REST, False)
        PF[r0:r1, :] = nn(ctx, WO[l])
        PRE[...] = nn(MS[...], WU[l])
        bup = VEC[l, 6:7, :]
        GB = 32

        def act(b, carry):
            u = PRE[rows(b * GB, GB), :] + bup
            cdf = 0.5 * (1.0 + lax.erf(u * RSQRT2))
            pdf = jnp.exp2(u * u * (-0.5 * LOG2E)) * INV_SQRT_2PI
            HID[l, rows(r0 + b * GB, GB), :] = (u * cdf).astype(BF16)
            GP[l, rows(r0 + b * GB, GB), :] = cdf + u * pdf
            return carry
        loop(C // GB, act, 0, unroll=True)
        PF[r0:r1, :] += nn(HID[l, r0:r1, :], WD[l])
        yield

    def backward(l, dl, i, last):
        r0, r1 = i * C, (i + 1) * C
        par = l % CORES
        first = i == NC - 1

        def acc(ref, val):
            if first:
                ref[par] = val
            else:
                ref[par] += val

        def acc_row(k, val, w=D):
            GV[l, k:k + 1, :w] += val

        norms(l, i)
        dy = H[dl, r0:r1, :]
        acc_row(4, col_sum(dy.astype(F32)))
        PRE[...] = nt(dy, WD[l])
        GB = 32

        def act(b, tot):
            d = PRE[rows(b * GB, GB), :] * GP[l, rows(r0 + b * GB, GB), :]
            DPB[rows(b * GB, GB), :] = d.astype(BF16)
            return tot + fold(d)
        dbu = loop(C // GB, act, jnp.zeros((8, F), F32), unroll=True)
        acc_row(5, col_sum(dbu))
        acc(GD, tn(HID[l, r0:r1, :], dy))
        yield
        acc(GU, tn(MS[...], DPB[...]))
        f0 = pf_row(i, True)
        PF[f0:f0 + C, :] = nt(DPB[...], WU[l])
        yield
        dctx = nt(dy, WO[l]).astype(BF16)
        ctx = CTX[l, r0:r1, :]
        acc(GO, tn(ctx, dy))
        prod = dctx.astype(F32) * ctx.astype(F32)
        q = Q[l, r0:r1, :].astype(F32)
        dcf = dctx.astype(F32)
        RBK = C // CORES
        dqt = []
        for h in range(CORES):
            sel = head_lane == h
            qm = jnp.where(sel, q, 0.0).astype(BF16)
            dcm = jnp.where(sel, dcf, 0.0).astype(BF16)
            dsum = jnp.transpose(jnp.where(sel, prod, 0.0))
            drow = col_sum(dsum)
            ST[:r1, :] = nt(V[l, :r1, :], dcm)

            def sub(b, carry):
                pr = PX[i][l, h, rows(b * RBK, RBK), :].astype(F32)
                DS[rows(b * RBK, RBK), :] = (pr * (ST[rows(b * RBK, RBK), :] - drow)).astype(BF16)
                return carry
            loop(r1 // RBK, sub, 0, unroll=True)
            dk = nn(DS[:r1, :], qm)
            dv = nn(PX[i][l, h], dcm)
            if first and h == 0:
                DK[:r1, :] = dk
                DV[:r1, :] = dv
            else:
                DK[:r1, :] += dk
                DV[:r1, :] += dv
            dqt.append(nn(KT[l, :, :r1], DS[:r1, :]))
            yield
        scale = E ** -0.5
        t = tabs(i)
        dq = unrotate(jnp.transpose(jnp.where(sub_head == 0, dqt[0], dqt[1])) * scale, t)
        dk = unrotate(DK[r0:r1, :] * scale, t)
        dv = DV[r0:r1, :]
        dqkv = jnp.concatenate([dq, dk, dv], axis=1)
        acc_row(6, col_sum(dqkv), 3 * E2)
        dqkv = dqkv.astype(BF16)
        dwq = tn(dqkv, AS[...])
        for k, r in enumerate(by_kind()):
            if first:
                GQ[par, r:r + E, :] = dwq[k * E:(k + 1) * E]
            else:
                GQ[par, r:r + E, :] += dwq[k * E:(k + 1) * E]
        PRE[...] = nn(dqkv, wq(l))
        yield
        g1, g2 = VEC[l, 0:1, :], VEC[l, 2:3, :]

        def lnb(b, tots):
            hf = H[l, rows(r0 + b * LB, LB), :].astype(F32)
            xhat, rstd = stats(hf)
            da = PRE[rows(b * LB, LB), :]
            dm = PF[rows(f0 + b * LB, LB), :]
            dx = da * g1 + dm * g2
            m1 = row_mean(dx)
            m2 = row_mean(dx * xhat)
            if not last:
                PF[rows(f0 + b * LB, LB), :] = rstd * (dx - m1 - xhat * m2)
            terms = (da * xhat, da, dm * xhat, dm)
            return tuple(a + fold(v) for a, v in zip(tots, terms))
        tots = loop(C // LB, lnb, tuple(jnp.zeros((8, D), F32) for _ in range(NA)), unroll=True)
        for k in range(NA):
            acc_row(k, col_sum(tots[k]))
        yield

    def g_half(a, k):
        return rows(k * G_HALF[a], G_HALF[a])

    def r1_view(l, a):
        return GP.at[l + 1, R1_OFF[a]:R1_OFF[a] + G_HALF[a], :G_COLS[a]]

    def g1_copy(l, a):
        return rcopy(G_BUF[a].at[l % CORES, g_half(a, 1 - c)], r1_view(l, a), g1s.at[a], g1r.at[l % CORES, a], pp=sib)

    def g2_copy(l, a):
        return rcopy(HID.at[l, R1_OFF[a]:R1_OFF[a] + G_HALF[a], :G_COLS[a]], R2[a].at[l % CORES], g2s.at[l % CORES, a], g2r.at[l % CORES, a], pp=2 * (l // CORES) + c)

    def g3_local(l, a):
        return lcopy(r1_view(l, a), G_OUT[a].at[g_half(a, c)], g3s.at[l % CORES, a])

    def g3_remote(l, a):
        return rcopy(r1_view(l, a), G_OUT[a].at[g_half(a, c)], g3s.at[l % CORES, a], g3r.at[a], pp=sib)

    def v1_copies(l):
        return [rcopy(GV.at[l], ZR.at[l, z], v1s.at[l, o - 1], v1r.at[l, z], tp=(z + o) % NT) for o in range(1, NT)]

    def grads_mid(l, arrays):
        for a in arrays:
            g1_copy(l, a).wait_recv()
            n = G_HALF[a]

            def add(b, carry):
                rr = rows(R1_OFF[a] + b * GR, GR)
                tot = G_BUF[a][l % CORES, rows(c * n + b * GR, GR), :] + GP[l + 1, rr, :G_COLS[a]]
                GP[l + 1, rr, :G_COLS[a]] = tot
                HID[l, rr, :G_COLS[a]] = tot.astype(BF16)
                return carry
            loop(n // GR, add, 0)

            @pl.when(l // CORES != ys_)
            def _():
                g2_copy(l, a).start()

    def grads_last(l):
        @pl.when(l // CORES == ys_)
        def _():
            for a in MLP[::-1] + ATT:
                g2_copy(l, a).wait_recv()

                def add(b, carry):
                    rr = rows(R1_OFF[a] + b * GR, GR)
                    GP[l + 1, rr, :G_COLS[a]] += R2[a][l % CORES, rows(b * GR, GR), :].astype(F32)
                    return carry
                loop(G_HALF[a] // GR, add, 0)

                @pl.when(l == s)
                def _():
                    g3_local(l, a).start()

                @pl.when(l != s)
                def _():
                    g3_remote(l, a).start()

    def grads_sent(l):
        for a in range(NA):
            @pl.when(l // CORES != ys_)
            def _():
                g2_copy(l, a).wait_send()

            @pl.when(l == s)
            def _():
                g3_local(l, a).wait()

            @pl.when((l // CORES == ys_) & (l != s))
            def _():
                g3_remote(l, a).wait_send()

    def v2_copy(l):
        return rcopy(GZ.at[l], PR.at[s], v2s.at[l], v2r.at[s], pp=l)

    def vec_mid(l):
        ZR[l, z] = GV[l]
        for o in range(1, NT):
            q = (z + o) % NT
            rcopy(GV.at[l], ZR.at[l, q], v1s.at[l, o - 1], v1r.at[l, q], tp=q).wait_recv()
        tot = sum(ZR[l, k] for k in range(NT))
        row = lax.broadcasted_iota(jnp.int32, (8, D), 0)
        GZ[l] = jnp.where(row < 4, tot, GV[l])

        @pl.when(l == s)
        def _():
            PR[s] = GZ[l]

        @pl.when(l != s)
        def _():
            v2_copy(l).start()

    GV[...] = jnp.zeros_like(GV)
    @pl.when(ys_ == 1)
    def _():
        for a, hop in ((0, 0), (1, 0), (0, 1), (2, 0), (1, 1)):
            hop_on(a, hop)
        hop_end(0)
    settle(0, FIRST, True)
    xcopy.wait()

    def run(phases, at, handle, after=lambda k: None):
        for k, unused in enumerate(phases):
            after(k)
            for op, lag, u in at.get(k, ()):
                handle(op, lag, u)

    def fwd_layer(l, carry):
        for i in range(NC):
            ar_wait(l - 1, l, i, l)

            def handle(op, lag, u):
                m = i - lag

                def go(p, j):
                    if op == 'mid':
                        ar_mid(p, j, u)
                    else:
                        ar_last(p, p, p + 1, j, u)
                if m >= HOME:
                    @pl.when(l * ys_ < NL - 1)
                    def _():
                        go(l, m)
                elif m >= 0:
                    go(l, m)
                else:
                    @pl.when(l > 0)
                    def _():
                        go(l - 1, m + NC)
            run(forward(l, i), FWD_AT, handle)

            if i < HOME:
                ar_send(l, i)
            else:
                @pl.when(l * ys_ < NL - 1)
                def _():
                    ar_send(l, i)

                @pl.when(l * ys_ == NL - 1)
                def _():
                    guest_send(i)
            if i == 1:
                @pl.when(l == 0)
                def _():
                    gcopy.wait()
                    H[NL + 1] = GP[NL].astype(BF16)

                    @pl.when(s == 1)
                    def _():
                        start_all(y_copies())
            if i == 2:
                @pl.when((l > 0) & (l < NL - 1))
                def _():
                    relay(l + 1, ALL)
            if i == NC - 1:
                @pl.when(l == 0)
                def _():
                    relay(l + 1, ALL)

                @pl.when(l < NL - 1)
                def _():
                    settle(l + 1, FIRST, True)
        return carry
    loop(NL, fwd_layer, 0)

    def y_copies_of(q, n):
        src, dst, got = H.at[NL, :n], y.at[q // CORES, c, :n], yr.at[q]
        return lcopy(src, dst, ys.at[0]), rcopy(src, dst, ys.at[1], got, pp=sib), rcopy(src, dst, ys.at[2], got, pp=oy + c)

    def y_pass(q, n):
        part = y.at[q // CORES, c, :n]
        return rcopy(part, part, ys.at[3], yr.at[q], pp=sib)

    def y_arrived(q, n):
        part = y.at[q // CORES, q % CORES, :n]
        rcopy(part, part, ys.at[1], yr.at[q], pp=sib).wait_recv()

    def each_row(do):
        for row, n, other in ((0, S, HOME * C), (1, HOME * C, S)):
            @pl.when(ys_ == row)
            def _():
                do(row, n, other)

    def ri(l):
        return jnp.where(l == NL - 1, NL + 1, l + 1)

    def pass_of(lb):
        return NL + lb + (1 - ys_) * jnp.minimum(lb, 1)

    def bwd_layer(lb, carry):
        l = NL - 1 - lb
        p = pass_of(lb)
        before = pass_of(lb - 1)
        for n in range(NC):
            i = NC - 1 - n

            ar_wait(before, l + 1, i, lb)

            def handle(op, lag, u):
                m = n - lag

                def go(q, lq, j):
                    if op == 'mid':
                        ar_mid(q, j, u, True)
                    else:
                        ar_last(q, ri(lq), lq, j, u, True)
                if m >= 0:
                    @pl.when(l > 0)
                    def _():
                        go(p, l, NC - 1 - m)
                else:
                    @pl.when(lb > 0)
                    def _():
                        go(before, l + 1, -1 - m)

                    @pl.when(lb == NL * ys_)
                    def _():
                        if op == 'mid':
                            ar_mid(NL - 1, m + NC, u)
                        else:
                            ar_last(NL - 1, NL - 1, NL, m + NC, u)

            def guests(layer, what, j):
                @pl.when(lb == layer + NL * ys_)
                def _():
                    what(j)

            def after(k):
                if k == 0 and i >= HOME:
                    guests(1, guest_in, i)
                if k == 1 and NC > i + 1 >= HOME:
                    guests(1, guest_last, i + 1)
                if k == NC and i >= HOME:
                    guests(1, guest_mid, i)
                if k == 0 and n == 0:
                    @pl.when(lb > 0)
                    def _():
                        grads_mid(l + 1, ATT)
                        for a in ALL:
                            g1_copy(l + 1, a).wait_send()
                if n == NC - 1 and k < 2:
                    g1_copy(l, MLP[1 - k]).start()
                if n == NC - 1 and k in (3, 4):
                    @pl.when(l == 0)
                    def _():
                        grads_mid(l, (MLP[4 - k],))
            run(backward(l, ri(l), i, False), BWD_AT, handle, after)

            if i >= HOME:
                @pl.when(lb == 2 + NL * ys_)
                def _():
                    guest_back(i)

            @pl.when(l > 0)
            def _():
                ar_send(p, i, True)
            if n == NC - 1:
                @pl.when(lb == 2 + NL * ys_)
                def _():
                    guest_out(lambda *copies: start_all(copies))
            if n == 1:
                @pl.when(lb > 0)
                def _():
                    vec_mid(l + 1)
            if n == 2:
                @pl.when(lb == 0)
                def _():
                    def out(row, n, other):
                        for j in range(n // C):
                            ar_wait(NL - 1, NL, j)
                        start_all(y_copies_of(CORES * row + c, n))
                    each_row(out)

                @pl.when(lb > 1)
                def _():
                    grads_last(l + 2)

        for a in ATT:
            g1_copy(l, a).start()
        start_all(v1_copies(l))

        @pl.when(l > 0)
        def _():
            grads_mid(l, MLP)
        return carry
    loop(NL, bwd_layer, 0)

    grads_mid(0, ATT)

    def pass_on(row, n, other):
        y_arrived(CORES * (1 - row) + c, other)
        y_pass(CORES * (1 - row) + c, other).start()
        if row:
            guest_home(c).wait_recv()
            guest_home(c).start()
    each_row(pass_on)
    grads_last(1)
    vec_mid(0)
    grads_last(0)

    for o in range(1, NL):
        q = (s + o) % NL
        rcopy(GZ.at[0], PR.at[q], v2s.at[0], v2r.at[q], pp=q).wait_recv()
    PRE[:8, :D] = sum(PR[k] for k in range(NL))
    vout = lcopy(PRE.at[:8, :D], ovec, osem.at[0])
    vout.start()
    for l in range(NL):
        for cp in v1_copies(l):
            cp.wait_send()
    for l in range(NL):
        @pl.when(l != s)
        def _():
            v2_copy(l).wait_send()
    for a in range(NA):
        rcopy(G_OUT[a].at[g_half(a, 1 - c)], G_OUT[a].at[g_half(a, 1 - c)], g3s.at[a], g3r.at[a], pp=sib).wait_recv()

    def out_done(local, *sent):
        local.wait()
        for cp in sent:
            cp.wait_send()

    def all_out(row, n, other):
        out_done(*y_copies_of(CORES * row + c, n))
        y_pass(CORES * (1 - row) + c, other).wait_send()
        y_arrived(CORES * row + 1 - c, n)
        y_arrived(CORES * (1 - row) + 1 - c, other)
        guest_home(1 - c).wait_recv()
    each_row(all_out)

    @pl.when(ys_ == 0)
    def _():
        guest_out(out_done)

        @pl.when(is_end)
        def _():
            for t in range(HOME * SUB, NC * SUB):
                guest_to_hub(t).wait_send()

        @pl.when(inner)
        def _():
            for t in range(HOME * SUB, NC * SUB):
                guest_to_leaf(t).wait_send()

    @pl.when(ys_ == 1)
    def _():
        guest_home(c).wait_send()
        for i in range(HOME, NC):
            guest_copy(i).wait_send()
    for a in range(NA):
        g1_copy(0, a).wait_send()
    for l in range(NL):
        grads_sent(l)
    for cp in sib_copies():
        cp.wait_send()
    @pl.when(s == 0)
    def _():
        for cp in first_copies():
            cp.wait_send()

    @pl.when(s > 0)
    def _():
        for cp in y_copies():
            cp.wait_send()
    for a in ALL:
        pass_copy(oy + 1, a, c).wait_send()

        @pl.when(ys_ == 0)
        def _():
            pass_copy(oy, a, c).wait_send()

        @pl.when(ys_ == 1)
        def _():
            for hop in range(CORES):
                for cp in hop_copies(a, hop):
                    cp.wait_send()

    @pl.when(is_end)
    def _():
        for t in range(NC * SUB):
            end_copy(0, t).wait_send()

    @pl.when(inner)
    def _():
        for t in range(NC * SUB):
            peer_copy(0, t).wait_send()
            back_copy(0, 1, t).wait_send()
    vout.wait()


def finish(y, gq, go, gu, gd, gv, yo, qo, oo, uo, do, n0, n1, n2, n3, n4, n5, n6, bq,
           yb, qb, ob, ub, db, vb, r0, r1, r2, r3, r4, r5, r6, rq, got, put, small):
    trips = [(gd, db, do), (gu, ub, uo), (go, ob, oo), (gq, qb, qo)]
    trips += [tuple(ref.at[m, r] for ref in (y, yb, yo)) for m in range(y.shape[0]) for r in range(y.shape[1])]
    loads = [pltpu.make_async_copy(a, b, got.at[k]) for k, (a, b, o) in enumerate(trips)]
    stores = [pltpu.make_async_copy(b, o, put.at[k]) for k, (a, b, o) in enumerate(trips)]
    vecs = pltpu.make_async_copy(gv, vb, small.at[len(trips)])
    vecs.start()
    for cp in loads:
        cp.start()
    vecs.wait()
    for row, refs in enumerate(((r0,), (r1,), (r2,), (r3,), (r4, r5), (r6,))):
        for ref in refs:
            ref[...] = vb[row:row + 1, :]
    e = rq.shape[2]
    for k in range(3):
        for h in range(CORES):
            rq[k, h:h + 1, :] = vb[6:7, (CORES * k + h) * e:(CORES * k + h + 1) * e]
    tiny = [pltpu.make_async_copy(a, b, small.at[k]) for k, (a, b) in enumerate(((r0, n0), (r1, n1), (r2, n2), (r3, n3), (r4, n4), (r5, n5), (r6, n6), (rq, bq)))]
    for cp in tiny:
        cp.start()
    for cp, out in zip(loads, stores):
        cp.wait()
        out.start()
    for cp in tiny + stores:
        cp.wait()


def finish_step(y, gq, go, gu, gd, gv, e):
    hbm = pl.BlockSpec(memory_space=pl.ANY)
    row = jax.ShapeDtypeStruct((1, gv.shape[1]), F32)
    outs = [jax.ShapeDtypeStruct(a.shape, a.dtype) for a in (y, gq, go, gu, gd)] + [row] * 7 + [jax.ShapeDtypeStruct((3, CORES, e), F32)]
    bufs = outs[:5] + [gv] + outs[5:]
    return pl.pallas_call(
        finish,
        out_shape=outs,
        in_specs=[hbm] * 6,
        out_specs=[hbm] * len(outs),
        scratch_shapes=[pltpu.VMEM(a.shape, a.dtype) for a in bufs] + [pltpu.SemaphoreType.DMA((9,))] * 3,
        name='neox_out',
    )(y, gq, go, gu, gd, gv)


def group_step(dims, *args):
    x = args[0]
    S, D, E, C, F = dims
    E2 = 2 * E
    hbm = pl.BlockSpec(memory_space=pl.ANY)
    out_shape = [
        jax.ShapeDtypeStruct(x.shape, BF16),
        jax.ShapeDtypeStruct((3 * E2, D), F32),
        jax.ShapeDtypeStruct((E2, D), F32),
        jax.ShapeDtypeStruct((D, F), F32),
        jax.ShapeDtypeStruct((F, D), F32),
        jax.ShapeDtypeStruct((8, D), F32),
    ]

    def vm(*shape, dtype=BF16):
        return pltpu.VMEM(shape, dtype)
    dma = pltpu.SemaphoreType.DMA
    scratch = [
        vm(NL, 3 * E2, D), vm(NL, E2, D), vm(NL, D, F), vm(NL, F, D), vm(NL, 8, D, dtype=F32),
        vm(NL + 2, S, D),
        vm(NL, S, E2), vm(NL, S, E2), vm(NL, S, E2), vm(NL, E2, S), vm(E2, S), vm(NL, S, E2),
        *[vm(NL, 2, (i + 1) * C, C) for i in range(NC)],
        vm(NL, S, F), vm(NL + 1, S, F, dtype=F32),
        vm(CORES, S, D), vm(CORES, S, D), vm(S, D), vm(S + C, D, dtype=F32),
        *[vm(CORES, *k, dtype=F32) for k in ((3 * E2, D), (E2, D), (D, F), (F, D))],
        *[vm(CORES, *k) for k in ((3 * E, D), (E, D), (D // CORES, F), (F // CORES, D))],
        vm(S, E2, dtype=F32), vm(S, E2, dtype=F32),
        vm(CORES, C + 8, E2, dtype=F32),
        *[vm(*k, 8, D, dtype=F32) for k in ((NL,), (NL, NT), (NL,), (NL,))],
        vm(C, D), vm(C, D), vm(C, max(D, F), dtype=F32), vm(C, F), vm(S, C), vm(S, C, dtype=F32),
        *[vm(1, D, dtype=F32)] * 4, vm(1, D), vm(1, D), vm(1, F), vm(3, CORES, E), vm(S, D),
        dma((NA,)), dma((NA + 1,)), dma((CORES, NA + 1)), dma((NL, 2 * NA + 1)), dma((CORES, NA)), dma((3, NA)), dma((NA, 4)), dma((CORES,)), dma((1,)),
        dma((NC * SUB,)), dma((NC * SUB,)), dma((CORES, NC * SUB)), dma((CORES, NC * SUB)), dma((CORES, NC * SUB)),
        dma((NL,)), dma((NL,)), dma((NA,)), dma((CORES, NA)), dma((CORES, NA)), dma((CORES, NA)), dma((CORES, NA)), dma((NA,)),
        dma((NL, NT - 1)), dma((NL, NT)), dma((NL,)), dma((NL,)), dma((1,)), dma((8,)),
        dma((NC,)), dma((NC,)), dma((NC * SUB,)), dma((NC * SUB,)), dma((3,)), dma((CORES,)),
    ]
    return pl.pallas_call(
        functools.partial(body, dims),
        out_shape=out_shape,
        in_specs=[hbm] * len(args),
        out_specs=[hbm] * 6,
        scratch_shapes=scratch,
        compiler_params=pltpu.CompilerParams(collective_id=0, has_side_effects=True, vmem_limit_bytes=67043328),
        name='neox_group',
    )(*args)


def solution(mesh):
    def device_fn(x_in, g_out, ln1_gain, ln1_bias, w_qkv, b_qkv, w_out, b_out, ln2_gain, ln2_bias, w_up, b_up, w_down, b_down):
        n_micro, n_rows, S, D = x_in.shape
        heads, E = w_qkv.shape[2], w_qkv.shape[4]
        F = w_up.shape[2]
        C = S // NC
        wqkv = jnp.transpose(w_qkv[0], (1, 2, 3, 0)).reshape(heads * 3 * E, D)
        bqkv = jnp.transpose(b_qkv[0], (1, 0, 2))
        tab = jnp.asarray(rotary_base(C, NC, E, heads))
        part = group_step((S, D, E, C, F), x_in, g_out, wqkv, w_out[0].reshape(heads * E, D), w_up[0], w_down[0], ln1_gain, ln1_bias, ln2_gain, ln2_bias, b_out, b_down, b_up, bqkv, tab)
        y, gq, go, gup, gdn, n1g, n1b, n2g, n2b, gbo, gbd, gbu, gbq = finish_step(*part, E)
        gq = jnp.transpose(gq.reshape(heads, 3, E, D), (3, 0, 1, 2))[None]
        gbq = jnp.transpose(gbq, (1, 0, 2))[None]
        return (y, n1g, n1b, gq, gbq, go.reshape(1, heads, E, D), gbo, n2g, n2b, gup[None], gbu, gdn[None], gbd)

    return jax.shard_map(device_fn, mesh=mesh, in_specs=(P('dp'), P('dp')) + STAGE_SPECS, out_specs=(P('dp'),) + GRAD_SPECS, check_vma=False)
```
